256 devices in a mesh: fsdp: 32 (over z, y), ep: 8 (over x, core).
Axes of the slice: x: 4, y: 4, z: 8, core: 2. Of those that a mesh axis runs over, the one named last changes fastest.
Arguments:
- layer_in: bfloat16 [65536, 1024], P(('fsdp', 'ep'))
- out_grad: bfloat16 [65536, 1024], P(('fsdp', 'ep'))
- expert_ids: int32 [65536, 8], P(('fsdp', 'ep'))
- gate_vals: float32 [65536, 8], P(('fsdp', 'ep'))
- w_one: bfloat16 [128, 1024, 384], P('ep', 'fsdp')
- w_two: bfloat16 [128, 384, 1024], P('ep', None, 'fsdp')
- w_three: bfloat16 [128, 1024, 384], P('ep', 'fsdp')
Outputs:
- output 1: bfloat16 [65536, 1024], P(('fsdp', 'ep'))
- output 2: float32 [65536, 8], P(('fsdp', 'ep'))
- output 3: float32 [128, 1024, 384], P('ep', 'fsdp')
- output 4: float32 [128, 384, 1024], P('ep', None, 'fsdp')
- output 5: float32 [128, 1024, 384], P('ep', 'fsdp')
All inputs are finite; a program needn't handle non-finite values.
Results may differ from the reference program's by a relative error of at most 0.0103394.
Values are sent between devices in bfloat16 or wider.
A program may use at most 768 MiB of HBM per device.

```python
import jax
import jax.numpy as jnp
from jax import lax

HIDDEN = 1024
EXPERT_FF = 384
EXPERTS = 128
TOP_K = 8
TOKENS_DEV = 256
SHARDS = 256
CAPACITY = 24
TOKENS = SHARDS * TOKENS_DEV


def draw_routing(key):
    key_bias, key_hot, key_noise = jax.random.split(key, 3)
    noise_range = 65536
    spread = noise_range * TOP_K // (2 * EXPERTS)
    bias = jax.random.randint(key_bias, (EXPERTS,), 0, spread + 1)
    hot_expert = jax.random.randint(key_hot, (), 0, EXPERTS)
    expert_pos = jnp.arange(EXPERTS, dtype=jnp.int32)
    bias = bias + jnp.where(expert_pos == hot_expert, noise_range // 4, 0)
    noise = jax.random.randint(key_noise, (TOKENS, EXPERTS), 0, noise_range)
    scores = (noise + bias[None, :]) * EXPERTS + expert_pos[None, :]
    return lax.top_k(scores, TOP_K)[1].astype(jnp.int32)


def setup_inputs(seed: int = 0) -> dict:
    keys = jax.random.split(jax.random.key(seed), 7)
    layer_in = jax.random.normal(keys[0], (TOKENS, HIDDEN), jnp.float32).astype(jnp.bfloat16)
    out_grad = jax.random.normal(keys[1], (TOKENS, HIDDEN), jnp.float32).astype(jnp.bfloat16)
    expert_ids = draw_routing(keys[2])
    gate_vals = jax.random.uniform(keys[3], (TOKENS, TOP_K), jnp.float32, 0.25, 1.0)
    w_one = (jax.random.normal(keys[4], (EXPERTS, HIDDEN, EXPERT_FF), jnp.float32) * HIDDEN ** -0.5).astype(jnp.bfloat16)
    w_two = (jax.random.normal(keys[5], (EXPERTS, EXPERT_FF, HIDDEN), jnp.float32) * EXPERT_FF ** -0.5).astype(jnp.bfloat16)
    w_three = (jax.random.normal(keys[6], (EXPERTS, HIDDEN, EXPERT_FF), jnp.float32) * HIDDEN ** -0.5).astype(jnp.bfloat16)
    return {"layer_in": layer_in, "out_grad": out_grad, "expert_ids": expert_ids, "gate_vals": gate_vals, "w_one": w_one, "w_two": w_two, "w_three": w_three}


def reference(layer_in, out_grad, expert_ids, gate_vals, w_one, w_two, w_three):
    w_one_full = w_one.astype(jnp.float32)
    w_two_full = w_two.astype(jnp.float32)
    w_three_full = w_three.astype(jnp.float32)
    places = EXPERTS * CAPACITY
    expert_pos = jnp.arange(EXPERTS, dtype=jnp.int32)
    token_of = jnp.arange(TOKENS_DEV * TOP_K, dtype=jnp.int32) // TOP_K

    def shard_step(carry, shard):
        x_loc, dy_loc, ids_loc, gates_loc = shard
        flat_ids = ids_loc.reshape(-1)
        onehot = (flat_ids[:, None] == expert_pos[None, :]).astype(jnp.int32)
        before = jnp.cumsum(onehot, axis=0) - onehot
        position = jnp.sum(before * onehot, axis=1)
        slot_of = jnp.where(position < CAPACITY, flat_ids * CAPACITY + position, places)
        source = jnp.full((places,), TOKENS_DEV, jnp.int32).at[slot_of].set(token_of, mode="drop")
        slot_gate = jnp.zeros((places,), jnp.float32).at[slot_of].set(gates_loc.reshape(-1), mode="drop")
        x_buf = jnp.take(x_loc, source, axis=0, mode="fill", fill_value=0).reshape(EXPERTS, CAPACITY, HIDDEN).astype(jnp.float32)
        dy_buf = jnp.take(dy_loc, source, axis=0, mode="fill", fill_value=0).reshape(EXPERTS, CAPACITY, HIDDEN).astype(jnp.float32)
        h_one = jnp.einsum("ecd,edf->ecf", x_buf, w_one_full)
        h_three = jnp.einsum("ecd,edf->ecf", x_buf, w_three_full)
        sig_one = jax.nn.sigmoid(h_one)
        silu_one = h_one * sig_one
        act_bf = (silu_one * h_three).astype(jnp.bfloat16).astype(jnp.float32)
        y_buf = jnp.einsum("ecf,efd->ecd", act_bf, w_two_full)
        gate_buf = jnp.sum(dy_buf * y_buf, axis=-1)
        g_buf = (slot_gate.reshape(EXPERTS, CAPACITY, 1) * dy_buf).astype(jnp.bfloat16).astype(jnp.float32)
        d_act = jnp.einsum("ecd,efd->ecf", g_buf, w_two_full)
        dh_one = (d_act * h_three * sig_one * (1.0 + h_one * (1.0 - sig_one))).astype(jnp.bfloat16).astype(jnp.float32)
        dh_three = (d_act * silu_one).astype(jnp.bfloat16).astype(jnp.float32)
        dx_buf = (jnp.einsum("ecf,edf->ecd", dh_one, w_one_full) + jnp.einsum("ecf,edf->ecd", dh_three, w_three_full)).astype(jnp.bfloat16)
        dx_pick = jnp.take(dx_buf.reshape(places, HIDDEN), slot_of, axis=0, mode="fill", fill_value=0).reshape(TOKENS_DEV, TOP_K, HIDDEN)
        dx_tok = jnp.sum(dx_pick.astype(jnp.float32), axis=1).astype(jnp.bfloat16)
        gate_tok = jnp.take(gate_buf.reshape(places), slot_of, axis=0, mode="fill", fill_value=0).reshape(TOKENS_DEV, TOP_K)
        acc_one, acc_two, acc_three = carry
        acc_one = acc_one + jnp.einsum("ecd,ecf->edf", x_buf, dh_one)
        acc_two = acc_two + jnp.einsum("ecf,ecd->efd", act_bf, g_buf)
        acc_three = acc_three + jnp.einsum("ecd,ecf->edf", x_buf, dh_three)
        return (acc_one, acc_two, acc_three), (dx_tok, gate_tok)

    init = (jnp.zeros((EXPERTS, HIDDEN, EXPERT_FF), jnp.float32), jnp.zeros((EXPERTS, EXPERT_FF, HIDDEN), jnp.float32), jnp.zeros((EXPERTS, HIDDEN, EXPERT_FF), jnp.float32))
    shards = (layer_in.reshape(SHARDS, TOKENS_DEV, HIDDEN), out_grad.reshape(SHARDS, TOKENS_DEV, HIDDEN), expert_ids.reshape(SHARDS, TOKENS_DEV, TOP_K), gate_vals.reshape(SHARDS, TOKENS_DEV, TOP_K))
    (grad_one, grad_two, grad_three), (in_grad, gate_grad) = lax.scan(shard_step, init, shards)
    return in_grad.reshape(TOKENS, HIDDEN), gate_grad.reshape(TOKENS, TOP_K), grad_one, grad_two, grad_three
```

```python
import jax
import jax.numpy as jnp
from jax import lax
from jax.sharding import Mesh, PartitionSpec as P

NZ, NY, NX, NC = 8, 4, 4, 2
PLANE = ("y", "x", "core")


def capacity_of(tok_dev, top_k, experts):
    return max(8, ((tok_dev * top_k * 5) // (4 * experts) + 7) // 8 * 8)


def route_slots(expert_ids, experts, capacity):
    flat_ids = expert_ids.reshape(-1)
    onehot = (flat_ids[:, None] == jnp.arange(experts, dtype=jnp.int32)[None, :]).astype(jnp.int32)
    before = jnp.cumsum(onehot, axis=0) - onehot
    position = jnp.sum(before * onehot, axis=1)
    return jnp.where(position < capacity, flat_ids * capacity + position, experts * capacity)


def slot_sources(slot_of, gate_vals, tok_dev, places):
    top_k = gate_vals.shape[-1]
    token_of = jnp.arange(slot_of.shape[0], dtype=jnp.int32) // top_k
    source = jnp.full((places,), tok_dev, jnp.int32).at[slot_of].set(token_of, mode="drop")
    slot_gate = jnp.zeros((places,), jnp.float32).at[slot_of].set(gate_vals.reshape(-1), mode="drop")
    return source, slot_gate


def take_rows(rows, row_index):
    return jnp.take(rows, row_index, axis=0, mode="fill", fill_value=0)


def dot(spec, a, b):
    return jnp.einsum(spec, a, b, preferred_element_type=jnp.float32)


def expert_grads(x_rows, dy_rows, gate_rows, w_one, w_two_t, w_three):
    h_one = dot("erd,edf->erf", x_rows, w_one)
    h_three = dot("erd,edf->erf", x_rows, w_three)
    sig_one = jax.nn.sigmoid(h_one)
    silu_one = h_one * sig_one
    act_bf = (silu_one * h_three).astype(jnp.bfloat16)
    y_rows = dot("erf,edf->erd", act_bf, w_two_t)
    gate_grad = jnp.sum(dy_rows.astype(jnp.float32) * y_rows, axis=-1)
    g_rows = (gate_rows[..., None] * dy_rows.astype(jnp.float32)).astype(jnp.bfloat16)
    d_act = dot("erd,edf->erf", g_rows, w_two_t)
    dh_one = (d_act * h_three * sig_one * (1.0 + h_one * (1.0 - sig_one))).astype(jnp.bfloat16)
    dh_three = (d_act * silu_one).astype(jnp.bfloat16)
    dx_rows = (dot("erf,edf->erd", dh_one, w_one) + dot("erf,edf->erd", dh_three, w_three)).astype(jnp.bfloat16)
    grad_one = dot("erd,erf->edf", x_rows, dh_one)
    grad_three = dot("erd,erf->edf", x_rows, dh_three)
    grad_two_t = dot("erd,erf->edf", g_rows, act_bf)
    return dx_rows, gate_grad, grad_one, grad_two_t, grad_three


def solution(mesh):
    mesh4 = Mesh(mesh.devices.reshape(NZ, NY, NX, NC), ("z", "y", "x", "core"))
    tok_spec = P(("z", "y", "x", "core"), None)
    up_spec = P(("x", "core"), ("z", "y"), None)
    down_spec = P(("x", "core"), None, ("z", "y"))

    def per_device(layer_in, out_grad, expert_ids, gate_vals, w_one, w_two, w_three):
        tok_dev, hidden = layer_in.shape
        top_k = expert_ids.shape[1]
        local_experts, d_loc, ff = w_one.shape
        ep = NX * NC
        own = local_experts // NY
        experts = local_experts * ep
        capacity = capacity_of(tok_dev, top_k, experts)
        places = experts * capacity
        group = NY * ep
        w_all = jnp.stack([w_one, w_three, w_two.swapaxes(1, 2)]).reshape(3, NY, own, d_loc, ff)
        w_all = lax.all_to_all(w_all.swapaxes(0, 1), "y", 0, 0, tiled=True)
        w_all = lax.all_gather(w_all, "z", axis=0)
        w_full = w_all.transpose(2, 3, 0, 1, 4, 5).reshape(3, own, hidden, ff)

        ids = expert_ids
        ids = (ids % local_experts) // own * (ep * own) + ids // local_experts * own + ids % own
        slot_of = route_slots(ids, experts, capacity)
        source, slot_gate = slot_sources(slot_of, gate_vals, tok_dev, places)
        x_send = take_rows(layer_in, source).reshape(group, own * capacity, hidden)
        dy_send = take_rows(out_grad, source).reshape(group, own * capacity, hidden)
        gate_send = slot_gate.reshape(group, own * capacity)

        def exchange(v):
            return lax.all_to_all(v, PLANE, 0, 0, tiled=True)

        def by_expert(v):
            v = v.reshape((group, own, capacity) + v.shape[2:])
            return v.swapaxes(0, 1).reshape((own, group * capacity) + v.shape[3:])

        def by_source(v):
            v = v.reshape((own, group, capacity) + v.shape[2:])
            return v.swapaxes(0, 1).reshape((group, own * capacity) + v.shape[3:])

        x_rows = by_expert(exchange(x_send))
        dy_rows = by_expert(exchange(dy_send))
        gate_rows = by_expert(exchange(gate_send))
        dx_rows, gate_grad, grad_one, grad_two_t, grad_three = expert_grads(x_rows, dy_rows, gate_rows, w_full[0], w_full[2], w_full[1])

        def home(grad):
            grad = lax.psum_scatter(grad, "z", scatter_dimension=1, tiled=True)
            return grad.reshape(own, NY, d_loc, ff).swapaxes(0, 1)

        grads = jnp.stack([home(grad_one), home(grad_three), home(grad_two_t)], axis=1)
        grads = lax.all_to_all(grads, "y", 0, 0, tiled=True)

        dx_back = exchange(by_source(dx_rows)).reshape(places, hidden)
        gate_back = exchange(by_source(gate_grad)).reshape(places)
        dx_pick = take_rows(dx_back, slot_of).reshape(tok_dev, top_k, hidden)
        in_grad = jnp.sum(dx_pick, axis=1, dtype=jnp.float32).astype(jnp.bfloat16)
        gate_out = take_rows(gate_back, slot_of).reshape(tok_dev, top_k)

        grads = grads.swapaxes(0, 1).reshape(3, local_experts, d_loc, ff)
        return in_grad, gate_out, grads[0], grads[2].swapaxes(1, 2), grads[1]

    return jax.shard_map(per_device, mesh=mesh4, in_specs=(tok_spec, tok_spec, tok_spec, tok_spec, up_spec, down_spec, up_spec), out_specs=(tok_spec, tok_spec, up_spec, down_spec, up_spec), check_vma=False)
```

```python
import functools

import jax
import jax.numpy as jnp
from jax import lax
from jax.experimental import pallas as pl
from jax.experimental.pallas import tpu as pltpu
from jax.sharding import Mesh, PartitionSpec as P

NZ, NY, NX, NC = 8, 4, 4, 2
GROUP = NY * NX * NC
PLANE = ("y", "x", "core")
OWN = 4
F32, BF16 = jnp.float32, jnp.bfloat16
MESH = pl.DeviceIdType.MESH
ANY = pl.BlockSpec(memory_space=pl.ANY)
VMEM = pl.BlockSpec(memory_space=pltpu.VMEM)


def capacity_of(tok_dev, top_k, experts):
    return max(8, ((tok_dev * top_k * 5) // (4 * experts) + 7) // 8 * 8)


def dot(a, b, ca=1, cb=0):
    return lax.dot_general(a, b, (((ca,), (cb,)), ((), ())), preferred_element_type=F32)


def expert_base():
    ep = lax.axis_index("x") * NC + lax.axis_index("core")
    return ep * (NY * OWN) + lax.axis_index("y") * OWN


def strict_upper(n):
    rows = lax.broadcasted_iota(jnp.int32, (n, n), 0)
    cols = lax.broadcasted_iota(jnp.int32, (n, n), 1)
    return (rows < cols).astype(F32).astype(BF16)


RATE, D2D, HOP = 46600.0, 300000.0, 2.0


def gather_order(block_bytes, piece_bytes):
    free, heap, order, have = {}, [], [], {}

    def send(now, name, part, link, arrives, nbytes):
        rate = D2D if link == "core" else RATE
        t = max(now, free.get(link, 0.0)) + nbytes / rate
        free[link] = t
        if arrives is not None:
            heap.append((t + HOP, len(order), len(heap), arrives))
        return (name, part, link)

    def on_block(now, kind, dy, dx):
        out = []
        first, second = ("x", "y") if kind == "X" else ("y", "x")
        d = {"x": dx, "y": dy}

        def go(axis, sign, part):
            nd = dict(d)
            nd[axis] = (d[axis] - sign) % 4
            key = (kind, nd["y"], nd["x"])
            out.append(send(now, (kind, dy, dx), part, axis + ("+" if sign > 0 else "-"), key + (part,), block_bytes / (2 if part is not None else 1)))

        if d[second] == 0:
            if d[first] == 0:
                go(first, 1, None)
                go(first, -1, None)
            elif d[first] == 3:
                go(first, 1, 0)
            elif d[first] == 1:
                go(first, -1, 1)
            go(second, 1, None)
            go(second, -1, None)
        elif d[second] == 3:
            go(second, 1, 0)
        elif d[second] == 1:
            go(second, -1, 1)
        out.append(send(now, (kind, dy, dx), None, "core", None, block_bytes))
        return out

    def on_piece(now, dz, dy):
        out = []
        if dz == 0 or dz in (6, 7) or (dz == 5 and dy in (0, 1)):
            out.append(send(now, ("W", dz, dy), None, "z+", ("W", (dz - 1) % NZ, dy), piece_bytes))
        if dz == 0 or dz in (1, 2) or (dz == 3 and dy in (2, 3)):
            out.append(send(now, ("W", dz, dy), None, "z-", ("W", (dz + 1) % NZ, dy), piece_bytes))
        return out

    first = []
    for dy, link in ((1, "y+"), (3, "y-"), (2, "y+")):
        first.append(send(0.0, ("w", 0, dy), None, link, ("W", 0, (-dy) % 4), piece_bytes))
    first += on_piece(0.0, 0, 0)
    u = on_block(0.0, "U", 0, 0)
    x = on_block(0.0, "X", 0, 0)
    first += u + x
    order.append((None, first))
    while heap:
        now, _, _, name = heap.pop(heap.index(min(heap)))
        if name[0] == "W":
            order.append((name, on_piece(now, name[1], name[2])))
            continue
        kind, dy, dx, part = name
        key = (kind, dy, dx)
        have[key] = have.get(key, 0) + (2 if part is None else 1)
        order.append((name, on_block(now, kind, dy, dx) if have[key] == 2 else []))
    return order


def gather_kernel(order, x_ref, u_ref, meta_ref, w_ref, xa, ua, ma, wa, recv, wrecv, mrecv, drecv, ssem, msem, lsem):
    z, y, x, c = (lax.axis_index(a) for a in ("z", "y", "x", "core"))
    tok = x_ref.shape[0]
    half = tok // 2

    def place(dy, dx, dc=0):
        return lax.rem(y + dy, NY) * (NX * NC) + lax.rem(x + dx, NX) * NC + lax.rem(c + dc, NC)

    def at_offset(k):
        dy, dx, dc = k // (NX * NC), lax.rem(k // NC, NX), lax.rem(k, NC)
        return {"y": lax.rem(y + dy, NY), "x": lax.rem(x + dx, NX), "core": lax.rem(c + dc, NC)}

    me = place(0, 0)
    barrier = pltpu.get_barrier_semaphore()

    @pl.loop(1, GROUP)
    def _(k):
        pl.semaphore_signal(barrier, inc=1, device_id=at_offset(k), device_id_type=MESH)

    for dz in (1, NZ - 1):
        pl.semaphore_signal(barrier, inc=1, device_id={"z": lax.rem(z + dz, NZ)}, device_id_type=MESH)
    pl.semaphore_wait(barrier, GROUP + 1)

    def remote(src, dst, send_sem, recv_sem, target):
        return pltpu.make_async_remote_copy(src_ref=src, dst_ref=dst, send_sem=send_sem, recv_sem=recv_sem, device_id=target, device_id_type=MESH)

    targets = {
        "x+": {"x": lax.rem(x + 1, NX)}, "x-": {"x": lax.rem(x + NX - 1, NX)},
        "y+": {"y": lax.rem(y + 1, NY)}, "y-": {"y": lax.rem(y + NY - 1, NY)},
        "z+": {"z": lax.rem(z + 1, NZ)}, "z-": {"z": lax.rem(z + NZ - 1, NZ)},
        "core": {"core": 1 - c},
    }
    step = {"x+": (0, 3), "x-": (0, 1), "y+": (3, 0), "y-": (1, 0)}

    def block(kind, dy, dx, part=None):
        ref = (xa if kind == "X" else ua).at[place(dy, dx)]
        return ref if part is None else ref.at[pl.ds(part * half, half)]

    def bsem(kind, dy, dx, part):
        return recv.at[0 if kind == "X" else 1, dy * NX + dx, part or 0]

    copies = []

    def issue(name, part, link):
        sem = ssem.at[len(copies)]
        if name[0] == "w":
            dy = name[2]
            to = lax.rem(y + dy, NY)
            copy = remote(w_ref.at[to], wa.at[z, y], sem, wrecv.at[0, (-dy) % NY], {"y": to})
        elif name[0] == "W":
            _, dz, dy = name
            ndz = (dz - 1) % NZ if link == "z+" else (dz + 1) % NZ
            here = wa.at[lax.rem(z + dz, NZ), lax.rem(y + dy, NY)]
            src = w_ref.at[y] if (dz, dy) == (0, 0) else here
            copy = remote(src, here, sem, wrecv.at[ndz, dy], targets[link])
        else:
            kind, dy, dx = name
            if (dy, dx) == (0, 0):
                src = x_ref if kind == "X" else u_ref
                src = src if part is None else src.at[pl.ds(part * half, half)]
            else:
                src = block(kind, dy, dx, part)
            dst = block(kind, dy, dx, part)
            if link == "core":
                rsem = drecv.at[0 if kind == "X" else 1, dy * NX + dx]
            else:
                sy, sx = step[link]
                rsem = bsem(kind, (dy + sy) % NY, (dx + sx) % NX, part)
            copy = remote(src, dst, sem, rsem, targets[link])
        copy.start()
        copies.append(copy)

    local = [
        pltpu.make_async_copy(x_ref, xa.at[me], lsem.at[0]),
        pltpu.make_async_copy(u_ref, ua.at[me], lsem.at[1]),
        pltpu.make_async_copy(meta_ref, ma.at[me], lsem.at[2]),
        pltpu.make_async_copy(w_ref.at[y], wa.at[z, y], lsem.at[3]),
    ]

    def meta_copy(k):
        return remote(meta_ref, ma.at[me], msem.at[k], mrecv.at[k], at_offset(k))

    for name, sends in order:
        if name is None:
            pass
        elif name[0] == "W":
            _, dz, dy = name
            here = wa.at[lax.rem(z + dz, NZ), lax.rem(y + dy, NY)]
            remote(here, here, ssem.at[0], wrecv.at[dz, dy], targets["core"]).wait_recv()
        else:
            here = block(*name)
            remote(here, here, ssem.at[0], bsem(*name), targets["core"]).wait_recv()
        for send in sends:
            issue(*send)
        if name is None:
            for copy in local:
                copy.start()

            @pl.loop(1, GROUP)
            def _(k):
                meta_copy(k).start()

    for kind in (0, 1):
        for k in range(NY * NX):
            here = (ua if kind else xa).at[place(k // NX, k % NX, 1)]
            remote(here, here, ssem.at[0], drecv.at[kind, k], targets["core"]).wait_recv()

    @pl.loop(1, GROUP)
    def _(k):
        meta_copy(k).wait()

    for copy in copies:
        copy.wait_send()
    for copy in local:
        copy.wait()


def gather(x, u, meta, w):
    tok, hidden = x.shape
    order = gather_order(x.size * 2, w.size * 2 // NY)
    sends = sum(len(s) for _, s in order)
    dma = pltpu.SemaphoreType.DMA
    return pl.pallas_call(
        functools.partial(gather_kernel, order),
        name="gather",
        out_shape=(
            jax.ShapeDtypeStruct((GROUP, tok, hidden), BF16),
            jax.ShapeDtypeStruct((GROUP, tok, hidden), BF16),
            jax.ShapeDtypeStruct((GROUP,) + meta.shape, F32),
            jax.ShapeDtypeStruct((NZ,) + w.shape, BF16),
        ),
        in_specs=[VMEM] * 4,
        out_specs=(ANY,) * 4,
        scratch_shapes=[dma((2, NY * NX, 2)), dma((NZ, NY)), dma((GROUP,)), dma((2, NY * NX)), dma((sends,)), dma((GROUP,)), dma((4,))],
        compiler_params=pltpu.CompilerParams(collective_id=0, has_side_effects=True),
    )(x, u, meta, w)


def hits(ids, expert, values):
    return jnp.sum(jnp.where(ids == expert, values, 0.0), axis=0, keepdims=True)


def dispatch_kernel(cap, x_ref, u_ref, meta_ref, xr_ref, ur_ref, gr_ref, s_ref, tri_ref):
    tok, hidden = x_ref.shape[1:]
    rows = OWN * 2 * cap

    @pl.when(pl.program_id(0) == 0)
    def _():
        tri_ref[...] = strict_upper(tok)

    base = expert_base().astype(F32)
    r8 = lax.broadcasted_iota(jnp.int32, (8, tok), 0)
    r = lax.broadcasted_iota(jnp.int32, (rows, tok), 0)
    place = lax.rem(r, cap).astype(F32)
    e_of, p_of = r // (2 * cap), lax.rem(r // cap, 2)
    pick, gates = [], jnp.zeros((rows, tok), F32)
    for p in range(2):
        ids, gate = meta_ref[p, 0:8, :], meta_ref[p, 8:16, :]
        member = jnp.zeros((8, tok), F32)
        for e in range(OWN):
            member = jnp.where(r8 == e, hits(ids, base + e, 1.0), member)
        before = dot(member.astype(BF16), tri_ref[...])
        key = jnp.where(member > 0.0, before, -1.0)
        mine = jnp.full((rows, tok), -1.0, F32)
        for e in range(OWN):
            here = jnp.logical_and(e_of == e, p_of == p)
            mine = jnp.where(here, jnp.broadcast_to(key[e:e + 1, :], (rows, tok)), mine)
            gates = jnp.where(here, jnp.broadcast_to(hits(ids, base + e, gate), (rows, tok)), gates)
        pick.append((place == mine).astype(F32))
    both = pick[0] + pick[1]
    scale = jnp.sum(both * gates, axis=1, keepdims=True)
    s_ref[...] = both.astype(BF16).reshape(s_ref.shape)
    pick = jnp.concatenate(pick, axis=1).astype(BF16)
    xr_ref[...] = dot(pick, x_ref[...].reshape(2 * tok, hidden)).astype(BF16).reshape(xr_ref.shape)
    u_rows = dot(pick, u_ref[...].reshape(2 * tok, hidden))
    ur_ref[...] = u_rows.astype(BF16).reshape(ur_ref.shape)
    gr_ref[...] = (scale * u_rows).astype(BF16).reshape(gr_ref.shape)


def dispatch(cap, xa, ua, ma):
    _, tok, hidden = xa.shape
    rows = GROUP * cap
    out = lambda lanes: jax.ShapeDtypeStruct((OWN, rows, lanes), BF16)
    ospec = lambda lanes: pl.BlockSpec((OWN, 2 * cap, lanes), lambda i: (0, i, 0))
    ispec = lambda a: pl.BlockSpec((2,) + a.shape[1:], lambda i: (i, 0, 0))
    return pl.pallas_call(
        functools.partial(dispatch_kernel, cap),
        name="dispatch",
        out_shape=(out(hidden), out(hidden), out(hidden), out(tok)),
        grid=(GROUP // 2,),
        in_specs=[ispec(xa), ispec(ua), ispec(ma)],
        out_specs=(ospec(hidden), ospec(hidden), ospec(hidden), ospec(tok)),
        scratch_shapes=[pltpu.VMEM((tok, tok), BF16)],
        cost_estimate=pl.CostEstimate(flops=4 * OWN * rows * 2 * tok * hidden, bytes_accessed=4 * xa.size + 6 * OWN * rows * hidden, transcendentals=0),
    )(xa, ua, ma)


def expert_kernel(cap, x_ref, u_ref, g_ref, s_ref, w_ref, dx_ref, val_ref, g1_ref, g3_ref, g2_ref, a_s, d1_s, d3_s, y_s):
    rows, hidden = x_ref.shape[1:]
    ff = w_ref.shape[-1]
    tok = s_ref.shape[-1]
    w1 = w_ref[:, :, 0, 0].reshape(hidden, ff)
    w3 = w_ref[:, :, 1, 0].reshape(hidden, ff)
    w2 = w_ref[:, :, 2, 0].reshape(hidden, ff)
    tile = 256 if rows % 256 == 0 else rows

    @pl.loop(0, rows // tile)
    def _(i):
        at = pl.ds(pl.multiple_of(i * tile, tile), tile)
        x = x_ref[0, at, :]
        h1, h3 = dot(x, w1), dot(x, w3)
        sig = jax.nn.sigmoid(h1)
        silu = h1 * sig
        act = (silu * h3).astype(BF16)
        a_s[at, :] = act
        y = dot(act, w2, 1, 1)
        y_s[at, :] = jnp.sum(u_ref[0, at, :].astype(F32) * y, axis=1, keepdims=True)
        da = dot(g_ref[0, at, :], w2)
        d1 = (da * h3 * sig * (1.0 + h1 * (1.0 - sig))).astype(BF16)
        d3 = (da * silu).astype(BF16)
        d1_s[at, :] = d1
        d3_s[at, :] = d3
        dx_ref[0, at, :] = (dot(d1, w1, 1, 1) + dot(d3, w3, 1, 1)).astype(BF16)

    val = s_ref[0].astype(F32) * y_s[...]
    val_ref[0] = jnp.sum(val.reshape(rows // cap, cap, tok), axis=1)
    dtile = 256 if hidden % 256 == 0 else hidden

    @pl.loop(0, hidden // dtile)
    def _(i):
        at = pl.ds(pl.multiple_of(i * dtile, dtile), dtile)
        x = x_ref[0, :, at]
        g1_ref[0, at, :] = dot(x, d1_s[...], 0, 0)
        g3_ref[0, at, :] = dot(x, d3_s[...], 0, 0)
        g2_ref[0, at, :] = dot(g_ref[0, :, at], a_s[...], 0, 0)


def run_experts(cap, xr, ur, gr, s, wa):
    _, rows, hidden = xr.shape
    tok, ff = s.shape[-1], wa.shape[-1]
    row_spec = lambda lanes: pl.BlockSpec((1, rows, lanes), lambda e: (e, 0, 0))
    grad = jax.ShapeDtypeStruct((OWN, hidden, ff), F32)
    gspec = pl.BlockSpec((1, hidden, ff), lambda e: (e, 0, 0))
    wspec = pl.BlockSpec(wa.shape[:3] + (1,) + wa.shape[4:], lambda e: (0, 0, 0, e, 0, 0))
    return pl.pallas_call(
        functools.partial(expert_kernel, cap),
        name="experts",
        out_shape=(jax.ShapeDtypeStruct(xr.shape, BF16), jax.ShapeDtypeStruct((OWN, GROUP, tok), F32), grad, grad, grad),
        grid=(OWN,),
        in_specs=[row_spec(hidden), row_spec(hidden), row_spec(hidden), row_spec(tok), wspec],
        out_specs=(row_spec(hidden), pl.BlockSpec((1, GROUP, tok), lambda e: (e, 0, 0)), gspec, gspec, gspec),
        scratch_shapes=[pltpu.VMEM((rows, ff), BF16)] * 3 + [pltpu.VMEM((rows, 1), F32)],
        cost_estimate=pl.CostEstimate(flops=18 * OWN * rows * hidden * ff, bytes_accessed=8 * xr.size + 2 * wa.size + 12 * OWN * hidden * ff, transcendentals=0),
        compiler_params=pltpu.CompilerParams(vmem_limit_bytes=60 << 20),
    )(xr, ur, gr, s, wa)


def combine_kernel(cap, dx_ref, val_ref, meta_ref, out_ref, gate_ref, key_s, s_s, acc_s):
    group, places, hidden = dx_ref.shape
    tok = meta_ref.shape[1]
    ids = meta_ref[0:8, :]
    r = lax.broadcasted_iota(jnp.int32, (group * 8, tok), 0)
    d, e = r // 8, lax.rem(r, 8)
    expert = lax.rem(d, NX * NC) * (NY * OWN) + d // (NX * NC) * OWN + e
    expert = jnp.where(e < OWN, expert, -1).astype(F32)
    member = jnp.zeros((group * 8, tok), F32)
    for j in range(8):
        member = member + (jnp.broadcast_to(ids[j:j + 1, :], member.shape) == expert).astype(F32)
    before = dot(member.astype(BF16), strict_upper(tok))
    key_s[...] = jnp.where(member > 0.0, before, -1.0).reshape(key_s.shape)
    rr = lax.broadcasted_iota(jnp.int32, (places, tok), 0)
    place, e_of = lax.rem(rr, cap).astype(F32), rr // cap
    some = 8
    acc_s[...] = jnp.zeros_like(acc_s)

    @pl.loop(0, group // some)
    def _(i):
        @pl.loop(0, some)
        def _(k):
            key = key_s[i * some + k]
            mine = jnp.full((places, tok), -1.0, F32)
            for e in range(OWN):
                mine = jnp.where(e_of == e, jnp.broadcast_to(key[e:e + 1, :], (places, tok)), mine)
            s_s[pl.ds(pl.multiple_of(k * places, places), places), :] = (place == mine).astype(F32).astype(BF16)

        acc_s[...] += dot(s_s[...], dx_ref[pl.ds(i * some, some)].reshape(some * places, hidden), 0, 0)

    out_ref[...] = acc_s[...].astype(BF16)

    def gate_step(k, total):
        for e in range(OWN):
            number = lax.rem(k, NX * NC) * (NY * OWN) + k // (NX * NC) * OWN + e
            row = val_ref[k, e:e + 1, :]
            total = total + jnp.where(ids == number.astype(F32), jnp.broadcast_to(row, ids.shape), 0.0)
        return total

    gate_ref[...] = lax.fori_loop(0, group, gate_step, jnp.zeros((8, tok), F32))


def combine(cap, dx_back, val_back, meta):
    group, places, hidden = dx_back.shape
    tok = meta.shape[1]
    return pl.pallas_call(
        functools.partial(combine_kernel, cap),
        name="combine",
        out_shape=(jax.ShapeDtypeStruct((tok, hidden), BF16), jax.ShapeDtypeStruct((8, tok), F32)),
        in_specs=[VMEM] * 3,
        out_specs=(VMEM, VMEM),
        scratch_shapes=[pltpu.VMEM((group, 8, tok), F32), pltpu.VMEM((8 * places, tok), BF16), pltpu.VMEM((tok, hidden), F32)],
        cost_estimate=pl.CostEstimate(flops=2 * group * places * tok * hidden, bytes_accessed=2 * dx_back.size, transcendentals=0),
    )(dx_back, val_back, meta)


def solution(mesh):
    mesh4 = Mesh(mesh.devices.reshape(NZ, NY, NX, NC), ("z", "y", "x", "core"))
    tok_spec = P(("z", "y", "x", "core"), None)
    up_spec = P(("x", "core"), ("z", "y"), None)
    down_spec = P(("x", "core"), None, ("z", "y"))

    def per_device(layer_in, out_grad, expert_ids, gate_vals, w_one, w_two, w_three):
        tok_dev, hidden = layer_in.shape
        top_k = expert_ids.shape[1]
        local_experts, d_loc, ff = w_one.shape
        cap = capacity_of(tok_dev, top_k, local_experts * NX * NC)
        w = jnp.stack([w_one, w_three, w_two.swapaxes(1, 2)]).reshape(3, NY, OWN, d_loc, ff).swapaxes(0, 1)
        meta = jnp.concatenate([expert_ids.T.astype(F32), gate_vals.T])
        xa, ua, ma, wa = gather(layer_in, out_grad, meta, w)
        xr, ur, gr, s = dispatch(cap, xa, ua, ma)
        dx, val, g1, g3, g2 = run_experts(cap, xr, ur, gr, s, wa)

        def home(grad):
            grad = lax.psum_scatter(grad, "z", scatter_dimension=1, tiled=True)
            return grad.reshape(OWN, NY, d_loc, ff).swapaxes(0, 1)

        grads = jnp.stack([home(g1), home(g3), home(g2)], axis=1)
        grads = lax.all_to_all(grads, "y", 0, 0, tiled=True)

        dx = dx.reshape(OWN, GROUP, cap, hidden).swapaxes(0, 1).reshape(GROUP, OWN * cap, hidden)
        dx_back = lax.all_to_all(dx, PLANE, 0, 0, tiled=True)
        val_back = lax.all_to_all(val.swapaxes(0, 1), PLANE, 0, 0, tiled=True)
        in_grad, gate_out = combine(cap, dx_back, val_back, meta)

        grads = grads.swapaxes(0, 1).reshape(3, local_experts, d_loc, ff)
        return in_grad, gate_out.T, grads[0], grads[2].swapaxes(1, 2), grads[1]

    return jax.shard_map(per_device, mesh=mesh4, in_specs=(tok_spec, tok_spec, tok_spec, tok_spec, up_spec, down_spec, up_spec), out_specs=(tok_spec, tok_spec, up_spec, down_spec, up_spec), check_vma=False)
```

```python
import functools

import jax
import jax.numpy as jnp
from jax import lax
from jax.experimental import pallas as pl
from jax.experimental.pallas import tpu as pltpu
from jax.sharding import Mesh, PartitionSpec as P

NZ, NY, NX, NC = 8, 4, 4, 2
GROUP = NY * NX * NC
PLANE = ("y", "x", "core")
OWN = 4
F32, BF16 = jnp.float32, jnp.bfloat16
MESH = pl.DeviceIdType.MESH
ANY = pl.BlockSpec(memory_space=pl.ANY)
VMEM = pl.BlockSpec(memory_space=pltpu.VMEM)


def capacity_of(tok_dev, top_k, experts):
    return max(8, ((tok_dev * top_k * 5) // (4 * experts) + 7) // 8 * 8)


def dot(a, b, ca=1, cb=0):
    return lax.dot_general(a, b, (((ca,), (cb,)), ((), ())), preferred_element_type=F32)


def expert_base():
    ep = lax.axis_index("x") * NC + lax.axis_index("core")
    return ep * (NY * OWN) + lax.axis_index("y") * OWN


def strict_upper(n):
    rows = lax.broadcasted_iota(jnp.int32, (n, n), 0)
    cols = lax.broadcasted_iota(jnp.int32, (n, n), 1)
    return (rows < cols).astype(F32).astype(BF16)


RATE, D2D, HOP = 46600.0, 300000.0, 2.0


def gather_order(block_bytes, piece_bytes):
    free, heap, order, have = {}, [], [], {}

    def send(now, name, part, link, arrives, nbytes):
        rate = D2D if link == "core" else RATE
        t = max(now, free.get(link, 0.0)) + nbytes / rate
        free[link] = t
        if arrives is not None:
            heap.append((t + HOP, len(order), len(heap), arrives))
        return (name, part, link)

    def on_block(now, kind, dy, dx):
        out = []
        first, second = ("x", "y") if kind == "X" else ("y", "x")
        d = {"x": dx, "y": dy}

        def go(axis, sign, part):
            nd = dict(d)
            nd[axis] = (d[axis] - sign) % 4
            key = (kind, nd["y"], nd["x"])
            out.append(send(now, (kind, dy, dx), part, axis + ("+" if sign > 0 else "-"), key + (part,), block_bytes / (2 if part is not None else 1)))

        if d[second] == 0:
            if d[first] == 0:
                go(first, 1, None)
                go(first, -1, None)
            elif d[first] == 3:
                go(first, 1, 0)
            elif d[first] == 1:
                go(first, -1, 1)
            go(second, 1, None)
            go(second, -1, None)
        elif d[second] == 3:
            go(second, 1, 0)
        elif d[second] == 1:
            go(second, -1, 1)
        out.append(send(now, (kind, dy, dx), None, "core", None, block_bytes))
        return out

    def on_piece(now, dz, dy):
        out = []
        if dz == 0 or dz in (6, 7) or (dz == 5 and dy in (0, 1)):
            out.append(send(now, ("W", dz, dy), None, "z+", ("W", (dz - 1) % NZ, dy), piece_bytes))
        if dz == 0 or dz in (1, 2) or (dz == 3 and dy in (2, 3)):
            out.append(send(now, ("W", dz, dy), None, "z-", ("W", (dz + 1) % NZ, dy), piece_bytes))
        return out

    first = []
    for dy, link in ((1, "y+"), (3, "y-"), (2, "y+")):
        first.append(send(0.0, ("w", 0, dy), None, link, ("W", 0, (-dy) % 4), piece_bytes))
    first += on_piece(0.0, 0, 0)
    u = on_block(0.0, "U", 0, 0)
    x = on_block(0.0, "X", 0, 0)
    first += u + x
    order.append((None, first))
    while heap:
        now, _, _, name = heap.pop(heap.index(min(heap)))
        if name[0] == "W":
            order.append((name, on_piece(now, name[1], name[2])))
            continue
        kind, dy, dx, part = name
        key = (kind, dy, dx)
        have[key] = have.get(key, 0) + (2 if part is None else 1)
        order.append((name, on_block(now, kind, dy, dx) if have[key] == 2 else []))
    return order


def gather_kernel(order, x_ref, u_ref, meta_ref, w_ref, xa, ua, ma, wa, recv, wrecv, mrecv, drecv, ssem, msem, lsem):
    z, y, x, c = (lax.axis_index(a) for a in ("z", "y", "x", "core"))
    tok = x_ref.shape[0]
    half = tok // 2

    def place(dy, dx, dc=0):
        return lax.rem(y + dy, NY) * (NX * NC) + lax.rem(x + dx, NX) * NC + lax.rem(c + dc, NC)

    def at_offset(k):
        dy, dx, dc = k // (NX * NC), lax.rem(k // NC, NX), lax.rem(k, NC)
        return {"y": lax.rem(y + dy, NY), "x": lax.rem(x + dx, NX), "core": lax.rem(c + dc, NC)}

    me = place(0, 0)
    barrier = pltpu.get_barrier_semaphore()

    @pl.loop(1, GROUP)
    def _(k):
        pl.semaphore_signal(barrier, inc=1, device_id=at_offset(k), device_id_type=MESH)

    for dz in (1, NZ - 1):
        pl.semaphore_signal(barrier, inc=1, device_id={"z": lax.rem(z + dz, NZ)}, device_id_type=MESH)
    pl.semaphore_wait(barrier, GROUP + 1)

    def remote(src, dst, send_sem, recv_sem, target):
        return pltpu.make_async_remote_copy(src_ref=src, dst_ref=dst, send_sem=send_sem, recv_sem=recv_sem, device_id=target, device_id_type=MESH)

    targets = {
        "x+": {"x": lax.rem(x + 1, NX)}, "x-": {"x": lax.rem(x + NX - 1, NX)},
        "y+": {"y": lax.rem(y + 1, NY)}, "y-": {"y": lax.rem(y + NY - 1, NY)},
        "z+": {"z": lax.rem(z + 1, NZ)}, "z-": {"z": lax.rem(z + NZ - 1, NZ)},
        "core": {"core": 1 - c},
    }
    step = {"x+": (0, 3), "x-": (0, 1), "y+": (3, 0), "y-": (1, 0)}

    def block(kind, dy, dx, part=None):
        ref = (xa if kind == "X" else ua).at[place(dy, dx)]
        return ref if part is None else ref.at[pl.ds(part * half, half)]

    def bsem(kind, dy, dx, part):
        return recv.at[0 if kind == "X" else 1, dy * NX + dx, part or 0]

    copies = []

    def issue(name, part, link):
        sem = ssem.at[len(copies)]
        if name[0] == "w":
            dy = name[2]
            to = lax.rem(y + dy, NY)
            copy = remote(w_ref.at[to], wa.at[z, y], sem, wrecv.at[0, (-dy) % NY], {"y": to})
        elif name[0] == "W":
            _, dz, dy = name
            ndz = (dz - 1) % NZ if link == "z+" else (dz + 1) % NZ
            here = wa.at[lax.rem(z + dz, NZ), lax.rem(y + dy, NY)]
            src = w_ref.at[y] if (dz, dy) == (0, 0) else here
            copy = remote(src, here, sem, wrecv.at[ndz, dy], targets[link])
        else:
            kind, dy, dx = name
            if (dy, dx) == (0, 0):
                src = x_ref if kind == "X" else u_ref
                src = src if part is None else src.at[pl.ds(part * half, half)]
            else:
                src = block(kind, dy, dx, part)
            dst = block(kind, dy, dx, part)
            if link == "core":
                rsem = drecv.at[0 if kind == "X" else 1, dy * NX + dx]
            else:
                sy, sx = step[link]
                rsem = bsem(kind, (dy + sy) % NY, (dx + sx) % NX, part)
            copy = remote(src, dst, sem, rsem, targets[link])
        copy.start()
        copies.append(copy)

    local = [
        pltpu.make_async_copy(x_ref, xa.at[me], lsem.at[0]),
        pltpu.make_async_copy(u_ref, ua.at[me], lsem.at[1]),
        pltpu.make_async_copy(meta_ref, ma.at[me], lsem.at[2]),
        pltpu.make_async_copy(w_ref.at[y], wa.at[z, y], lsem.at[3]),
    ]

    def meta_copy(k):
        return remote(meta_ref, ma.at[me], msem.at[k], mrecv.at[k], at_offset(k))

    for name, sends in order:
        if name is None:
            pass
        elif name[0] == "W":
            _, dz, dy = name
            here = wa.at[lax.rem(z + dz, NZ), lax.rem(y + dy, NY)]
            remote(here, here, ssem.at[0], wrecv.at[dz, dy], targets["core"]).wait_recv()
        else:
            here = block(*name)
            remote(here, here, ssem.at[0], bsem(*name), targets["core"]).wait_recv()
        for send in sends:
            issue(*send)
        if name is None:
            for copy in local:
                copy.start()

            @pl.loop(1, GROUP)
            def _(k):
                meta_copy(k).start()

    for kind in (0, 1):
        for k in range(NY * NX):
            here = (ua if kind else xa).at[place(k // NX, k % NX, 1)]
            remote(here, here, ssem.at[0], drecv.at[kind, k], targets["core"]).wait_recv()

    @pl.loop(1, GROUP)
    def _(k):
        meta_copy(k).wait()

    for copy in copies:
        copy.wait_send()
    for copy in local:
        copy.wait()


def gather(x, u, meta, w):
    tok, hidden = x.shape
    order = gather_order(x.size * 2, w.size * 2 // NY)
    sends = sum(len(s) for _, s in order)
    dma = pltpu.SemaphoreType.DMA
    return pl.pallas_call(
        functools.partial(gather_kernel, order),
        name="gather",
        out_shape=(
            jax.ShapeDtypeStruct((GROUP, tok, hidden), BF16),
            jax.ShapeDtypeStruct((GROUP, tok, hidden), BF16),
            jax.ShapeDtypeStruct((GROUP,) + meta.shape, F32),
            jax.ShapeDtypeStruct((NZ,) + w.shape, BF16),
        ),
        in_specs=[VMEM] * 4,
        out_specs=(ANY,) * 4,
        scratch_shapes=[dma((2, NY * NX, 2)), dma((NZ, NY)), dma((GROUP,)), dma((2, NY * NX)), dma((sends,)), dma((GROUP,)), dma((4,))],
        compiler_params=pltpu.CompilerParams(collective_id=0, has_side_effects=True),
    )(x, u, meta, w)


def hits(ids, expert, values):
    return jnp.sum(jnp.where(ids == expert, values, 0.0), axis=0, keepdims=True)


def dispatch_kernel(cap, x_ref, u_ref, meta_ref, xr_ref, ur_ref, gr_ref, s_ref, tri_ref):
    tok, hidden = x_ref.shape[1:]
    rows = OWN * 2 * cap

    @pl.when(pl.program_id(0) == 0)
    def _():
        tri_ref[...] = strict_upper(tok)

    base = expert_base().astype(F32)
    r8 = lax.broadcasted_iota(jnp.int32, (8, tok), 0)
    r = lax.broadcasted_iota(jnp.int32, (rows, tok), 0)
    place = lax.rem(r, cap).astype(F32)
    e_of, p_of = r // (2 * cap), lax.rem(r // cap, 2)
    pick, gates = [], jnp.zeros((rows, tok), F32)
    for p in range(2):
        ids, gate = meta_ref[p, 0:8, :], meta_ref[p, 8:16, :]
        member = jnp.zeros((8, tok), F32)
        for e in range(OWN):
            member = jnp.where(r8 == e, hits(ids, base + e, 1.0), member)
        before = dot(member.astype(BF16), tri_ref[...])
        key = jnp.where(member > 0.0, before, -1.0)
        mine = jnp.full((rows, tok), -1.0, F32)
        for e in range(OWN):
            here = jnp.logical_and(e_of == e, p_of == p)
            mine = jnp.where(here, jnp.broadcast_to(key[e:e + 1, :], (rows, tok)), mine)
            gates = jnp.where(here, jnp.broadcast_to(hits(ids, base + e, gate), (rows, tok)), gates)
        pick.append((place == mine).astype(F32))
    both = pick[0] + pick[1]
    scale = jnp.sum(both * gates, axis=1, keepdims=True)
    s_ref[...] = both.astype(BF16).reshape(s_ref.shape)
    pick = jnp.concatenate(pick, axis=1).astype(BF16)
    xr_ref[...] = dot(pick, x_ref[...].reshape(2 * tok, hidden)).astype(BF16).reshape(xr_ref.shape)
    u_rows = dot(pick, u_ref[...].reshape(2 * tok, hidden))
    ur_ref[...] = u_rows.astype(BF16).reshape(ur_ref.shape)
    gr_ref[...] = (scale * u_rows).astype(BF16).reshape(gr_ref.shape)


def dispatch(cap, xa, ua, ma):
    _, tok, hidden = xa.shape
    rows = GROUP * cap
    out = lambda lanes: jax.ShapeDtypeStruct((OWN, rows, lanes), BF16)
    ospec = lambda lanes: pl.BlockSpec((OWN, 2 * cap, lanes), lambda i: (0, i, 0))
    ispec = lambda a: pl.BlockSpec((2,) + a.shape[1:], lambda i: (i, 0, 0))
    return pl.pallas_call(
        functools.partial(dispatch_kernel, cap),
        name="dispatch",
        out_shape=(out(hidden), out(hidden), out(hidden), out(tok)),
        grid=(GROUP // 2,),
        in_specs=[ispec(xa), ispec(ua), ispec(ma)],
        out_specs=(ospec(hidden), ospec(hidden), ospec(hidden), ospec(tok)),
        scratch_shapes=[pltpu.VMEM((tok, tok), BF16)],
        cost_estimate=pl.CostEstimate(flops=4 * OWN * rows * 2 * tok * hidden, bytes_accessed=4 * xa.size + 6 * OWN * rows * hidden, transcendentals=0),
    )(xa, ua, ma)


FAR, SUM3, NEW3, TWO, ONE = range(5)


def expert_kernel(cap, xr, ur, gr, sel, wa, meta_ref, grads, in_grad_ref, gate_ref, dxb, valb, dxs,
                  xb, ub, gb, sb, wb, a_s, d1_s, d3_s, y_s, dx_s, val_s, vb, key_s, acc_s, G, r4, r3, r2, r1,
                  lsem, wsem, rsend, rrecv, ysend, yrecv, dsend, drecv, vsem, osem):
    z, y, x, c = (lax.axis_index(a) for a in ("z", "y", "x", "core"))
    rows, hidden = xb.shape
    ff, tok = a_s.shape[-1], sb.shape[-1]
    d_loc = hidden // (NZ * NY)
    me = y * (NX * NC) + x * NC + c

    def at_offset(k):
        dy, dx, dc = k // (NX * NC), lax.rem(k // NC, NX), lax.rem(k, NC)
        return {"y": lax.rem(y + dy, NY), "x": lax.rem(x + dx, NX), "core": lax.rem(c + dc, NC)}

    def place_of(d):
        return d["y"] * (NX * NC) + d["x"] * NC + d["core"]

    def remote(src, dst, send_sem, recv_sem, target):
        return pltpu.make_async_remote_copy(src_ref=src, dst_ref=dst, send_sem=send_sem, recv_sem=recv_sem, device_id=target, device_id_type=MESH)

    def row_copies(e):
        pairs = ((xr, xb), (gr, gb), (ur, ub), (sel, sb))
        return [pltpu.make_async_copy(src.at[e], dst, lsem.at[i]) for i, (src, dst) in enumerate(pairs)]

    def weight_copies(e, slot):
        return [pltpu.make_async_copy(wa.at[:, :, m, e], wb.at[slot, m], wsem.at[slot, m]) for m in range(3)]

    for copy in weight_copies(0, 0) + row_copies(0):
        copy.start()

    barrier = pltpu.get_barrier_semaphore()

    @pl.loop(1, GROUP)
    def _(k):
        pl.semaphore_signal(barrier, inc=1, device_id=at_offset(k), device_id_type=MESH)

    for dz in (1, NZ - 1):
        pl.semaphore_signal(barrier, inc=1, device_id={"z": lax.rem(z + dz, NZ)}, device_id_type=MESH)
    pl.semaphore_wait(barrier, GROUP + 1)

    def chunk(e, way, dist):
        return G.at[e, lax.rem(z + (dist if way else NZ - dist), NZ)]

    def hop(e, way, kind):
        h = way
        src, dst = {
            FAR: lambda: (chunk(e, way, 4).at[h], r4.at[way, e]),
            SUM3: lambda: (r4.at[way, e], r3.at[way, e, h]),
            NEW3: lambda: (chunk(e, way, 3).at[1 - h], r3.at[way, e, 1 - h]),
            TWO: lambda: (r3.at[way, e], r2.at[way, e]),
            ONE: lambda: (r2.at[way, e], r1.at[way, e]),
        }[kind]()
        to = lax.rem(z + (1 if way else NZ - 1), NZ)
        return remote(src, dst, rsend.at[way, e, kind], rrecv.at[way, e, kind], {"z": to})

    def add_into(dst, *others):
        parts = dst.shape[:-2]

        def flat(ref, i):
            index = []
            for n in reversed(parts):
                index.append(lax.rem(i, n))
                i = i // n
            return ref.at[tuple(reversed(index))]

        n = 1
        for p in parts:
            n *= p

        @pl.loop(0, n)
        def _(i):
            total = flat(dst, i)[...]
            for other in others:
                total = total + flat(other, i)[...]
            flat(dst, i)[...] = total

    def dx_copy(e, k):
        to = at_offset(k)
        src = dxs.at[e, pl.ds(pl.multiple_of(place_of(to) * cap, 8), cap)]
        return remote(src, dxb.at[me, pl.ds(pl.multiple_of(e * cap, 8), cap)], dsend.at[e], drecv.at[e], to)

    def own_dx_copy(e):
        src = dxs.at[e, pl.ds(pl.multiple_of(me * cap, 8), cap)]
        return pltpu.make_async_copy(src, dxb.at[me, pl.ds(pl.multiple_of(e * cap, 8), cap)], drecv.at[e])

    tile = 256 if rows % 256 == 0 else rows
    dtile = 2 * hidden // NZ
    half = hidden // NZ // 2

    @pl.loop(0, OWN)
    def _(e):
        slot = lax.rem(e, 2)
        for copy in weight_copies(e, slot) + row_copies(e):
            copy.wait()

        @pl.when(e < OWN - 1)
        def _():
            for copy in weight_copies(e + 1, 1 - slot):
                copy.start()

        def w(m):
            return wb[slot, m].reshape(hidden, ff)

        @pl.loop(0, rows // tile)
        def _(i):
            at = pl.ds(pl.multiple_of(i * tile, tile), tile)
            x_rows = xb[at, :]
            h1, h3 = dot(x_rows, w(0)), dot(x_rows, w(1))
            sig = jax.nn.sigmoid(h1)
            silu = h1 * sig
            act = (silu * h3).astype(BF16)
            a_s[at, :] = act
            y_rows = dot(act, w(2), 1, 1)
            y_s[at, :] = jnp.sum(ub[at, :].astype(F32) * y_rows, axis=1, keepdims=True)
            da = dot(gb[at, :], w(2))
            d1 = (da * h3 * sig * (1.0 + h1 * (1.0 - sig))).astype(BF16)
            d3 = (da * silu).astype(BF16)
            d1_s[at, :] = d1
            d3_s[at, :] = d3
            dx_s[at, :] = (dot(d1, w(0), 1, 1) + dot(d3, w(1), 1, 1)).astype(BF16)

        out = pltpu.make_async_copy(dx_s, dxs.at[e], osem.at[0])
        out.start()

        @pl.loop(0, NZ // 2)
        def _(i):
            at = pl.ds(pl.multiple_of(i * dtile, dtile), dtile)
            x_cols, g_cols = xb[:, at], gb[:, at]
            for m, part in enumerate((dot(x_cols, d1_s[...], 0, 0), dot(x_cols, d3_s[...], 0, 0), dot(g_cols, a_s[...], 0, 0))):
                for j in range(4):
                    G[e, 2 * i + j // 2, j % 2, m] = part[j * half:(j + 1) * half]

        for way in (0, 1):
            for kind in (FAR, NEW3):
                hop(e, way, kind).start()
        val = sb[...].astype(F32) * y_s[...]
        val_s[e] = jnp.sum(val.reshape(rows // cap, cap, tok), axis=1)
        out.wait()

        @pl.when(e < OWN - 1)
        def _():
            for copy in row_copies(e + 1):
                copy.start()

        own_dx_copy(e).start()

        @pl.loop(1, GROUP)
        def _(k):
            dx_copy(e, k).start()

    def val_copy(k):
        to = at_offset(k)
        return remote(val_s.at[:, place_of(to)], valb.at[:, me], vsem.at[0, k], vsem.at[1, k], to)

    own_val = pltpu.make_async_copy(val_s.at[:, me], valb.at[:, me], vsem.at[0, 0])
    own_val.start()

    @pl.loop(1, GROUP)
    def _(k):
        val_copy(k).start()

    def step(arrived, dist, leaves):
        @pl.loop(0, OWN)
        def _(e):
            for way in (0, 1):
                for kind in arrived:
                    hop(e, way, kind).wait_recv()
                if leaves == SUM3:
                    add_into(r4.at[way, e], chunk(e, way, dist).at[way])
                else:
                    add_into((r3 if leaves == TWO else r2).at[way, e], chunk(e, way, dist))
                hop(e, way, leaves).start()

    step((FAR,), 3, SUM3)
    step((SUM3, NEW3), 2, TWO)

    group, places = dxb.shape[:2]
    ids = meta_ref[0:8, :]
    r = lax.broadcasted_iota(jnp.int32, (group * 8, tok), 0)
    d_of, e_of = r // 8, lax.rem(r, 8)
    expert = lax.rem(d_of, NX * NC) * (NY * OWN) + d_of // (NX * NC) * OWN + e_of
    expert = jnp.where(e_of < OWN, expert, -1).astype(F32)
    member = jnp.zeros((group * 8, tok), F32)
    for j in range(8):
        member = member + (jnp.broadcast_to(ids[j:j + 1, :], member.shape) == expert).astype(F32)
    before = dot(member.astype(BF16), strict_upper(tok))
    key_s[...] = jnp.where(member > 0.0, before, -1.0).reshape(key_s.shape)
    rr = lax.broadcasted_iota(jnp.int32, (places, tok), 0)
    place, e_row = lax.rem(rr, cap).astype(F32), rr // cap
    some = rows // places

    @pl.loop(0, OWN)
    def _(e):
        pltpu.make_async_copy(dxb.at[:, pl.ds(pl.multiple_of(e * cap, 8), cap)], dxb.at[:, pl.ds(pl.multiple_of(e * cap, 8), cap)], drecv.at[e]).wait()

    own_val.wait()

    @pl.loop(1, GROUP)
    def _(k):
        val_copy(k).wait()

    back = [pltpu.make_async_copy(dxb.at[pl.ds(i * some, some)], (xb if i % 2 == 0 else gb).reshape(some, places, hidden), lsem.at[i % 2]) for i in range(group // some)]
    vals = pltpu.make_async_copy(valb, vb, lsem.at[2])
    vals.start()
    back[0].start()
    for i in range(group // some):
        if i + 1 < len(back):
            back[i + 1].start()

        @pl.loop(0, some)
        def _(k):
            key = key_s[i * some + k]
            mine = jnp.full((places, tok), -1.0, F32)
            for e in range(OWN):
                mine = jnp.where(e_row == e, jnp.broadcast_to(key[e:e + 1, :], (places, tok)), mine)
            sb[pl.ds(pl.multiple_of(k * places, places), places), :] = (place == mine).astype(F32).astype(BF16)

        back[i].wait()
        part = dot(sb[...], (xb if i % 2 == 0 else gb)[...], 0, 0)
        acc_s[...] = part if i == 0 else acc_s[...] + part

    in_grad_ref[...] = acc_s[...].astype(BF16)
    vals.wait()

    def gate_step(k, total):
        number = lax.rem(k, NX * NC) * (NY * OWN) + k // (NX * NC) * OWN
        for e in range(OWN):
            row = vb[e, pl.ds(k, 1), :]
            total = total + jnp.where(ids == (number + e).astype(F32), jnp.broadcast_to(row, ids.shape), 0.0)
        return total

    gate_ref[...] = lax.fori_loop(0, group, gate_step, jnp.zeros((8, tok), F32))

    step((TWO,), 1, ONE)

    def keep(e, dy):
        to = lax.rem(y + dy, NY)
        src = r1.at[0, e, to // 2, :, pl.ds(pl.multiple_of(lax.rem(to, 2) * d_loc, 8), d_loc)]
        dst = grads.at[:, y * OWN + e]
        if dy == 0:
            return pltpu.make_async_copy(src, dst, ysend.at[e, 0])
        return remote(src, dst, ysend.at[e, dy], yrecv.at[e, (-dy) % NY], {"y": to})

    @pl.loop(0, OWN)
    def _(e):
        for way in (0, 1):
            hop(e, way, ONE).wait_recv()
        add_into(r1.at[0, e], r1.at[1, e], G.at[e, z])
        for dy in range(NY):
            keep(e, dy).start()

    @pl.loop(0, OWN)
    def _(e):
        keep(e, 0).wait()
        for dy in range(1, NY):
            remote(grads.at[:, lax.rem(y + dy, NY) * OWN + e], grads.at[:, lax.rem(y + dy, NY) * OWN + e], ysend.at[e, dy], yrecv.at[e, dy], {"y": lax.rem(y + dy, NY)}).wait_recv()
            keep(e, dy).wait_send()
        for way in (0, 1):
            for kind in range(5):
                hop(e, way, kind).wait_send()

        sent = dxs.at[e, pl.ds(0, (GROUP - 1) * cap)]
        pltpu.make_async_copy(sent, sent, dsend.at[e]).wait()


def run_experts(cap, xr, ur, gr, sel, wa, meta):
    _, rows, hidden = xr.shape
    tok, ff = sel.shape[-1], wa.shape[-1]
    d_loc = hidden // (NZ * NY)
    half = hidden // NZ // 2
    dma = pltpu.SemaphoreType.DMA
    v = pltpu.VMEM
    shape = jax.ShapeDtypeStruct
    outs = pl.pallas_call(
        functools.partial(expert_kernel, cap),
        name="experts",
        out_shape=(
            shape((3, NY * OWN, d_loc, ff), F32),
            shape((tok, hidden), BF16),
            shape((8, tok), F32),
            shape((GROUP, OWN * cap, hidden), BF16),
            shape((OWN, GROUP, tok), F32),
            shape((OWN, rows, hidden), BF16),
        ),
        in_specs=[ANY] * 5 + [VMEM],
        out_specs=(ANY, VMEM, VMEM, ANY, ANY, ANY),
        scratch_shapes=[
            v((rows, hidden), BF16), v((rows, hidden), BF16), v((rows, hidden), BF16), v((rows, tok), BF16),
            v((2, 3, NZ, NY, d_loc, ff), BF16), v((rows, ff), BF16), v((rows, ff), BF16), v((rows, ff), BF16), v((rows, 1), F32),
            v((rows, hidden), BF16), v((OWN, GROUP, tok), F32), v((OWN, GROUP, tok), F32), v((GROUP, 8, tok), F32), v((tok, hidden), F32),
            v((OWN, NZ, 2, 3, half, ff), F32), v((2, OWN, 3, half, ff), F32),
            v((2, OWN, 2, 3, half, ff), F32), v((2, OWN, 2, 3, half, ff), F32), v((2, OWN, 2, 3, half, ff), F32),
            dma((4,)), dma((2, 3)), dma((2, OWN, 5)), dma((2, OWN, 5)), dma((OWN, NY)), dma((OWN, NY)),
            dma((OWN,)), dma((OWN,)), dma((2, GROUP)), dma((1,)),
        ],
        compiler_params=pltpu.CompilerParams(collective_id=1, has_side_effects=True, vmem_limit_bytes=67043328),
    )(xr, ur, gr, sel, wa, meta)
    return outs[:3]


def solution(mesh):
    mesh4 = Mesh(mesh.devices.reshape(NZ, NY, NX, NC), ("z", "y", "x", "core"))
    tok_spec = P(("z", "y", "x", "core"), None)
    up_spec = P(("x", "core"), ("z", "y"), None)
    down_spec = P(("x", "core"), None, ("z", "y"))

    def per_device(layer_in, out_grad, expert_ids, gate_vals, w_one, w_two, w_three):
        tok_dev, hidden = layer_in.shape
        top_k = expert_ids.shape[1]
        local_experts, d_loc, ff = w_one.shape
        cap = capacity_of(tok_dev, top_k, local_experts * NX * NC)
        w = jnp.stack([w_one, w_three, w_two.swapaxes(1, 2)]).reshape(3, NY, OWN, d_loc, ff).swapaxes(0, 1)
        meta = jnp.concatenate([expert_ids.T.astype(F32), gate_vals.T])
        xa, ua, ma, wa = gather(layer_in, out_grad, meta, w)
        xr, ur, gr, s = dispatch(cap, xa, ua, ma)
        grads, in_grad, gate_out = run_experts(cap, xr, ur, gr, s, wa, meta)
        return in_grad, gate_out.T, grads[0], grads[2].swapaxes(1, 2), grads[1]

    return jax.shard_map(per_device, mesh=mesh4, in_specs=(tok_spec, tok_spec, tok_spec, tok_spec, up_spec, down_spec, up_spec), out_specs=(tok_spec, tok_spec, up_spec, down_spec, up_spec), check_vma=False)
```

```python
import functools

import jax
import jax.numpy as jnp
from jax import lax
from jax.experimental import pallas as pl
from jax.experimental.pallas import tpu as pltpu
from jax.sharding import Mesh, PartitionSpec as P

NZ, NY, NX, NC = 8, 4, 4, 2
GROUP = NY * NX * NC
PLANE = ("y", "x", "core")
OWN = 4
F32, BF16 = jnp.float32, jnp.bfloat16
MESH = pl.DeviceIdType.MESH
ANY = pl.BlockSpec(memory_space=pl.ANY)
VMEM = pl.BlockSpec(memory_space=pltpu.VMEM)


def capacity_of(tok_dev, top_k, experts):
    return max(8, ((tok_dev * top_k * 5) // (4 * experts) + 7) // 8 * 8)


def dot(a, b, ca=1, cb=0):
    return lax.dot_general(a, b, (((ca,), (cb,)), ((), ())), preferred_element_type=F32)


def expert_base():
    ep = lax.axis_index("x") * NC + lax.axis_index("core")
    return ep * (NY * OWN) + lax.axis_index("y") * OWN


def strict_upper(n):
    rows = lax.broadcasted_iota(jnp.int32, (n, n), 0)
    cols = lax.broadcasted_iota(jnp.int32, (n, n), 1)
    return (rows < cols).astype(F32).astype(BF16)


def here():
    return tuple(lax.axis_index(a) for a in ("z", "y", "x", "core"))


def at_offset(k):
    _, y, x, c = here()
    dy, dx, dc = k // (NX * NC), lax.rem(k // NC, NX), lax.rem(k, NC)
    return {"y": lax.rem(y + dy, NY), "x": lax.rem(x + dx, NX), "core": lax.rem(c + dc, NC)}


def place_of(d):
    return d["y"] * (NX * NC) + d["x"] * NC + d["core"]


def z_at(dz):
    return {"z": lax.rem(lax.axis_index("z") + dz, NZ)}


def remote(src, dst, send_sem, recv_sem, target):
    return pltpu.make_async_remote_copy(src_ref=src, dst_ref=dst, send_sem=send_sem, recv_sem=recv_sem, device_id=target, device_id_type=MESH)


def enter():
    barrier = pltpu.get_barrier_semaphore()

    @pl.loop(1, GROUP)
    def _(k):
        pl.semaphore_signal(barrier, device_id=at_offset(k), device_id_type=MESH)

    for dz in (1, NZ - 1):
        pl.semaphore_signal(barrier, device_id=z_at(dz), device_id_type=MESH)
    return lambda: pl.semaphore_wait(barrier, GROUP + 1)


RATE, D2D, HOP, STEP = 46600.0, 300000.0, 2.0, 1.5


def gather_order(rows_bytes, cut, piece_bytes):
    size = {"A": rows_bytes * cut, "B": rows_bytes * (1.0 - cut)}
    free, coming, order, have, ready = {}, [], [], {}, {}

    def send(now, name, part, link, arrives, nbytes):
        rate = D2D if link == "core" else RATE
        t = max(now, free.get(link, 0.0)) + nbytes / rate
        free[link] = t
        coming.append((t + HOP, len(order), len(coming), arrives))
        return (name, part, link)

    def on_rows(now, kind, dy, dx):
        out = []
        first, second = ("x", "y") if kind == "A" else ("y", "x")
        d = {"x": dx, "y": dy}

        def go(axis, sign, part):
            nd = dict(d)
            nd[axis] = (d[axis] - sign) % 4
            arrives = (kind, nd["y"], nd["x"], part)
            out.append(send(now, (kind, dy, dx), part, axis + ("+" if sign > 0 else "-"), arrives, size[kind] / (2 if part is not None else 1)))

        if d[second] == 0:
            if d[first] == 0:
                go(first, 1, None)
                go(first, -1, None)
            elif d[first] == 3:
                go(first, 1, 0)
            elif d[first] == 1:
                go(first, -1, 1)
            go(second, 1, None)
            go(second, -1, None)
        elif d[second] == 3:
            go(second, 1, 0)
        elif d[second] == 1:
            go(second, -1, 1)
        out.append(send(now, (kind, dy, dx), None, "core", ("core", kind, dy, dx), size[kind]))
        return out

    def on_piece(now, dz, dy):
        out = []
        if dz == 0 or dz in (6, 7) or (dz == 5 and dy in (0, 1)):
            out.append(send(now, ("W", dz, dy), None, "z+", ("W", (dz - 1) % NZ, dy, None), piece_bytes))
        if dz == 0 or dz in (1, 2) or (dz == 3 and dy in (2, 3)):
            out.append(send(now, ("W", dz, dy), None, "z-", ("W", (dz + 1) % NZ, dy, None), piece_bytes))
        return out

    def arrived_for(dy, dx, now):
        return all(ready.get((kind, dy, dx), 1e9) <= now and ready.get(("core", kind, dy, dx), 1e9) <= now for kind in "AB")

    first = []
    for dy, link in ((1, "y+"), (3, "y-")):
        first.append(send(0.0, ("w", dy), None, link, ("W", 0, (-dy) % NY, None), piece_bytes))
    for part, link in ((0, "y+"), (1, "y-")):
        first.append(send(0.0, ("w", 2), part, link, ("R", part), piece_bytes / 2))
    first += on_piece(0.0, 0, 0) + on_rows(0.0, "B", 0, 0) + on_rows(0.0, "A", 0, 0)
    ready[("A", 0, 0)] = ready[("B", 0, 0)] = 0.0
    order.append((None, first))
    todo = [(dy, dx) for dy in range(NY) for dx in range(NX)]
    now = 0.0
    while coming or todo:
        coming.sort()
        place = next((p for p in todo if arrived_for(*p, now)), None)
        if place is not None and not (coming and coming[0][0] <= now):
            todo.remove(place)
            order.append((("place",) + place, []))
            now += STEP
            continue
        t, _, _, name = coming.pop(0)
        now = max(now, t)
        if name[0] == "core":
            ready[name] = now
        elif name[0] == "R":
            part = name[1]
            order.append((name, [send(now, ("R",), part, "y+" if part == 0 else "y-", ("W", 0, 2, part), piece_bytes / 2)]))
        else:
            key, part = name[:3], name[3]
            have[key] = have.get(key, 0) + (2 if part is None else 1)
            whole = have[key] == 2
            if name[0] == "W":
                order.append((name, on_piece(now, name[1], name[2]) if whole else []))
            else:
                if whole:
                    ready[key] = now
                order.append((name, on_rows(now, *key) if whole else []))
    return order


def hits(ids, expert, values):
    return jnp.sum(jnp.where(ids == expert, values, 0.0), axis=0, keepdims=True)


def gather_kernel(order, cap, cut, x_hbm, u_hbm, ids_ref, gate_ref, w1_hbm, w3_hbm, w2_hbm, xr, ur, gr, sel, wa,
                  rows, metas, wown, wv, relay, tri, sx, su, sg, ss,
                  recv, core_recv, wrecv, relay_recv, mrecv, send_sem, msend, load_sem, store_sem, wstore):
    z, y, x, c = here()
    tok = x_hbm.shape[0]
    own = wv.shape[3]

    def place(dy, dx, dc=0):
        return place_of(at_offset(dy * (NX * NC) + dx * NC + dc))

    me = place(0, 0)
    loads = [
        pltpu.make_async_copy(x_hbm, rows.at[me, pl.ds(0, tok)], load_sem.at[0]),
        pltpu.make_async_copy(u_hbm, rows.at[me, pl.ds(tok, tok)], load_sem.at[1]),
    ]
    for m, w in enumerate((w1_hbm, w3_hbm, w2_hbm)):
        loads.append(pltpu.make_async_copy(w.reshape(NY, own, *w.shape[1:]), wown.at[:, m], load_sem.at[2 + m]))
    for copy in loads:
        copy.start()
    metas[me, 0:8, :] = ids_ref[...].astype(F32)
    metas[me, 8:16, :] = gate_ref[...]

    all_in = enter()
    tri[...] = strict_upper(tok)
    for copy in loads:
        copy.wait()
    all_in()

    targets = {"core": {"core": 1 - c}}
    for sign, n in (("+", 1), ("-", -1)):
        targets["x" + sign] = {"x": lax.rem(x + n + NX, NX)}
        targets["y" + sign] = {"y": lax.rem(y + n + NY, NY)}
        targets["z" + sign] = z_at(n + NZ)
    step = {"x+": (0, 3), "x-": (0, 1), "y+": (3, 0), "y-": (1, 0)}
    spans = {"A": (0, cut), "B": (cut, 2 * tok - cut)}

    def block(kind, dy, dx, part=None, dc=0):
        start, size = spans[kind]
        if part is not None:
            size //= 2
            start += part * size
        return rows.at[place(dy, dx, dc), pl.ds(start, size)]

    def bsem(kind, dy, dx, part):
        return recv.at[0 if kind == "A" else 1, dy * NX + dx, part or 0]

    def piece(dz, dy, part=None):
        here = wv.at[lax.rem(z + dz, NZ), lax.rem(y + dy, NY)]
        return here if part is None else here.at[:, pl.ds(part * (own // 2), own // 2)]

    copies = []

    def issue(name, part, link):
        sem = send_sem.at[len(copies)]
        if name[0] == "w":
            dy = name[1]
            src = wown.at[lax.rem(y + dy, NY)]
            if part is None:
                copy = remote(src, piece(0, 0), sem, wrecv.at[0, (-dy) % NY, 0], targets[link])
            else:
                src = src.at[:, pl.ds(part * (own // 2), own // 2)]
                copy = remote(src, relay.at[part], sem, relay_recv.at[part], targets[link])
        elif name[0] == "R":
            dst = piece(0, 3 if part == 0 else 1, part)
            copy = remote(relay.at[part], dst, sem, wrecv.at[0, 2, part], targets[link])
        elif name[0] == "W":
            _, dz, dy = name
            ndz = (dz - 1) % NZ if link == "z+" else (dz + 1) % NZ
            src = wown.at[y] if (dz, dy) == (0, 0) else piece(dz, dy)
            copy = remote(src, piece(dz, dy), sem, wrecv.at[ndz, dy, 0], targets[link])
        else:
            kind, dy, dx = name
            here = block(kind, dy, dx, part)
            if link == "core":
                rsem = core_recv.at[0 if kind == "A" else 1, dy * NX + dx]
            else:
                oy, ox = step[link]
                rsem = bsem(kind, (dy + oy) % NY, (dx + ox) % NX, part)
            copy = remote(here, here, sem, rsem, targets[link])
        copy.start()
        copies.append(copy)

    def wait(here, sem):
        remote(here, here, send_sem.at[0], sem, targets["core"]).wait_recv()

    def meta_copy(k):
        return remote(metas.at[me], metas.at[me], msend.at[k], mrecv.at[k], at_offset(k))

    base = expert_base().astype(F32)
    n_rows = OWN * 2 * cap
    stores = []

    def put(dy, dx):
        n = len(stores)
        slot = n % 2
        if n >= 2:
            for copy in stores[n - 2]:
                copy.wait()
        for dc in (0, 1):
            if (dy, dx, dc) != (0, 0, 0):
                k = ((-dy) % NY) * (NX * NC) + ((-dx) % NX) * NC + dc
                wait(metas.at[place(dy, dx, dc)], mrecv.at[k])
        for i, kind in enumerate("AB"):
            wait(block(kind, dy, dx, None, 1), core_recv.at[i, dy * NX + dx])
        chip = lax.rem(y + dy, NY) * NX + lax.rem(x + dx, NX)
        r8 = lax.broadcasted_iota(jnp.int32, (8, tok), 0)
        r = lax.broadcasted_iota(jnp.int32, (n_rows, tok), 0)
        at = lax.rem(r, cap).astype(F32)
        e_of, p_of = r // (2 * cap), lax.rem(r // cap, 2)
        pick, gates = [], jnp.zeros((n_rows, tok), F32)
        for p in range(2):
            ids, gate = metas[2 * chip + p, 0:8, :], metas[2 * chip + p, 8:16, :]
            member = jnp.zeros((8, tok), F32)
            for e in range(OWN):
                member = jnp.where(r8 == e, hits(ids, base + e, 1.0), member)
            before = dot(member.astype(BF16), tri[...])
            key = jnp.where(member > 0.0, before, -1.0)
            mine = jnp.full((n_rows, tok), -1.0, F32)
            for e in range(OWN):
                here = jnp.logical_and(e_of == e, p_of == p)
                mine = jnp.where(here, jnp.broadcast_to(key[e:e + 1, :], (n_rows, tok)), mine)
                gates = jnp.where(here, jnp.broadcast_to(hits(ids, base + e, gate), (n_rows, tok)), gates)
            pick.append((at == mine).astype(F32))
        both = pick[0] + pick[1]
        scale = jnp.sum(both * gates, axis=1, keepdims=True)
        ss[slot] = both.astype(BF16).reshape(ss.shape[1:])
        pick = [p.astype(BF16) for p in pick]
        x_rows = dot(pick[0], rows[2 * chip, 0:tok, :]) + dot(pick[1], rows[2 * chip + 1, 0:tok, :])
        sx[slot] = x_rows.astype(BF16).reshape(sx.shape[1:])
        u_rows = dot(pick[0], rows[2 * chip, tok:2 * tok, :]) + dot(pick[1], rows[2 * chip + 1, tok:2 * tok, :])
        su[slot] = u_rows.astype(BF16).reshape(su.shape[1:])
        sg[slot] = (scale * u_rows).astype(BF16).reshape(sg.shape[1:])
        span = pl.ds(pl.multiple_of(chip * 2 * cap, 2 * cap), 2 * cap)
        out = [pltpu.make_async_copy(s.at[slot], d.at[:, span], store_sem.at[slot, i]) for i, (s, d) in enumerate(((sx, xr), (su, ur), (sg, gr), (ss, sel)))]
        for copy in out:
            copy.start()
        stores.append(out)

    wstores = []

    def keep(src, dz, dy):
        copy = pltpu.make_async_copy(src, wa.at[lax.rem(z + dz, NZ), lax.rem(y + dy, NY)], wstore.at[len(wstores)])
        copy.start()
        wstores.append(copy)

    parts = {}
    for name, sends in order:
        if name is None:
            pass
        elif name[0] == "place":
            put(*name[1:])
        elif name[0] == "R":
            wait(relay.at[name[1]], relay_recv.at[name[1]])
        elif name[0] == "W":
            _, dz, dy, part = name
            wait(piece(dz, dy, part), wrecv.at[dz, dy, part or 0])
        else:
            wait(block(*name), bsem(*name))
        for send in sends:
            issue(*send)
        if name is None:
            keep(wown.at[y], 0, 0)

            @pl.loop(1, GROUP)
            def _(k):
                meta_copy(k).start()
        elif name[0] == "W":
            parts[name[1:3]] = parts.get(name[1:3], 0) + (2 if name[3] is None else 1)
            if parts[name[1:3]] == 2:
                keep(piece(name[1], name[2]), name[1], name[2])

    for out in stores[-2:]:
        for copy in out:
            copy.wait()
    for copy in wstores:
        copy.wait()

    @pl.loop(1, GROUP)
    def _(k):
        meta_copy(k).wait_send()

    for copy in copies:
        copy.wait_send()


def gather(cap, x, u, ids, gates, w1, w3, w2):
    tok, hidden = x.shape
    local_experts, d_loc, ff = w1.shape
    own = local_experts // NY
    cut = tok - tok // 8 if tok % 256 == 0 else tok
    piece = (3, own, d_loc, ff)
    piece_bytes = 2 * 3 * own * d_loc * ff
    order = gather_order(4 * tok * hidden, cut / (2 * tok), piece_bytes)
    sends = sum(len(s) for _, s in order)
    dma, v = pltpu.SemaphoreType.DMA, pltpu.VMEM
    rows = GROUP * cap
    out = lambda lanes: jax.ShapeDtypeStruct((OWN, rows, lanes), BF16)
    stage = lambda lanes: v((2, OWN, 2 * cap, lanes), BF16)
    return pl.pallas_call(
        functools.partial(gather_kernel, order, cap, cut),
        name="gather",
        out_shape=(out(hidden), out(hidden), out(hidden), out(tok), jax.ShapeDtypeStruct((NZ, NY) + piece, BF16)),
        in_specs=[ANY, ANY, VMEM, VMEM, ANY, ANY, ANY],
        out_specs=(ANY,) * 5,
        scratch_shapes=[
            v((GROUP, 2 * tok, hidden), BF16), v((GROUP, 16, tok), F32), v((NY,) + piece, BF16), v((NZ, NY) + piece, BF16),
            v((2, 3, own // 2, d_loc, ff), BF16), v((tok, tok), BF16), stage(hidden), stage(hidden), stage(hidden), stage(tok),
            dma((2, NY * NX, 2)), dma((2, NY * NX)), dma((NZ, NY, 2)), dma((2,)), dma((GROUP,)), dma((sends,)), dma((GROUP,)),
            dma((5,)), dma((2, 4)), dma((NZ * NY,)),
        ],
        compiler_params=pltpu.CompilerParams(collective_id=0, has_side_effects=True, vmem_limit_bytes=67043328),
    )(x, u, ids, gates, w1, w3, w2)


FAR, SUM3, NEW3, TWO, ONE = range(5)


def expert_kernel(cap, xr, ur, gr, sel, wa, ids_ref, grads, in_grad_ref, gate_ref, dxb, valb, dxs,
                  xb, ub, gb, sb, wb, a_s, d1_s, d3_s, y_s, dx_s, val_s, vb, key_s, acc_s, G, r4, r3, r2, r1,
                  lsem, wsem, rsend, rrecv, ysend, yrecv, dsend, drecv, vsem, osem):
    z, y, x, c = here()
    rows, hidden = xb.shape
    ff, tok = a_s.shape[-1], sb.shape[-1]
    d_loc = hidden // (NZ * NY)
    me = place_of(at_offset(0))

    def row_copies(e):
        pairs = ((xr, xb), (gr, gb), (ur, ub), (sel, sb))
        return [pltpu.make_async_copy(src.at[e], dst, lsem.at[i]) for i, (src, dst) in enumerate(pairs)]

    def weight_copies(e, slot):
        return [pltpu.make_async_copy(wa.at[:, :, m, e], wb.at[slot, m], wsem.at[slot, m]) for m in range(3)]

    for copy in weight_copies(0, 0) + row_copies(0):
        copy.start()

    enter()()

    def chunk(e, way, dist):
        return G.at[e, z_at(dist if way else NZ - dist)["z"]]

    def hop(e, way, kind):
        h = way
        src, dst = {
            FAR: lambda: (chunk(e, way, 4).at[h], r4.at[way, e]),
            SUM3: lambda: (r4.at[way, e], r3.at[way, e, h]),
            NEW3: lambda: (chunk(e, way, 3).at[1 - h], r3.at[way, e, 1 - h]),
            TWO: lambda: (r3.at[way, e], r2.at[way, e]),
            ONE: lambda: (r2.at[way, e], r1.at[way, e]),
        }[kind]()
        return remote(src, dst, rsend.at[way, e, kind], rrecv.at[way, e, kind], z_at(1 if way else NZ - 1))

    def add_into(dst, *others):
        parts = dst.shape[:-2]

        def flat(ref, i):
            index = []
            for n in reversed(parts):
                index.append(lax.rem(i, n))
                i = i // n
            return ref.at[tuple(reversed(index))]

        n = 1
        for p in parts:
            n *= p

        @pl.loop(0, n)
        def _(i):
            total = flat(dst, i)[...]
            for other in others:
                total = total + flat(other, i)[...]
            flat(dst, i)[...] = total

    def dx_copy(e, k):
        to = at_offset(k)
        src = dxs.at[e, pl.ds(pl.multiple_of(place_of(to) * cap, 8), cap)]
        return remote(src, dxb.at[me, pl.ds(pl.multiple_of(e * cap, 8), cap)], dsend.at[e], drecv.at[e], to)

    def own_dx_copy(e):
        src = dxs.at[e, pl.ds(pl.multiple_of(me * cap, 8), cap)]
        return pltpu.make_async_copy(src, dxb.at[me, pl.ds(pl.multiple_of(e * cap, 8), cap)], drecv.at[e])

    tile = 256 if rows % 256 == 0 else rows
    dtile = 2 * hidden // NZ
    half = hidden // NZ // 2

    @pl.loop(0, OWN)
    def _(e):
        slot = lax.rem(e, 2)
        for copy in weight_copies(e, slot) + row_copies(e):
            copy.wait()

        @pl.when(e < OWN - 1)
        def _():
            for copy in weight_copies(e + 1, 1 - slot):
                copy.start()

        def w(m):
            return wb[slot, m].reshape(hidden, ff)

        @pl.loop(0, rows // tile)
        def _(i):
            at = pl.ds(pl.multiple_of(i * tile, tile), tile)
            x_rows = xb[at, :]
            h1, h3 = dot(x_rows, w(0)), dot(x_rows, w(1))
            sig = jax.nn.sigmoid(h1)
            silu = h1 * sig
            act = (silu * h3).astype(BF16)
            a_s[at, :] = act
            y_rows = dot(act, w(2), 1, 1)
            y_s[at, :] = jnp.sum(ub[at, :].astype(F32) * y_rows, axis=1, keepdims=True)
            da = dot(gb[at, :], w(2))
            d1 = (da * h3 * sig * (1.0 + h1 * (1.0 - sig))).astype(BF16)
            d3 = (da * silu).astype(BF16)
            d1_s[at, :] = d1
            d3_s[at, :] = d3
            dx_s[at, :] = (dot(d1, w(0), 1, 1) + dot(d3, w(1), 1, 1)).astype(BF16)

        out = pltpu.make_async_copy(dx_s, dxs.at[e], osem.at[0])
        out.start()

        @pl.loop(0, NZ // 2)
        def _(i):
            at = pl.ds(pl.multiple_of(i * dtile, dtile), dtile)
            x_cols, g_cols = xb[:, at], gb[:, at]
            for m, part in enumerate((dot(x_cols, d1_s[...], 0, 0), dot(x_cols, d3_s[...], 0, 0), dot(g_cols, a_s[...], 0, 0))):
                for j in range(4):
                    G[e, 2 * i + j // 2, j % 2, m] = part[j * half:(j + 1) * half]

        for way in (0, 1):
            for kind in (FAR, NEW3):
                hop(e, way, kind).start()
        val = sb[...].astype(F32) * y_s[...]
        val_s[e] = jnp.sum(val.reshape(rows // cap, cap, tok), axis=1)
        out.wait()

        @pl.when(e < OWN - 1)
        def _():
            for copy in row_copies(e + 1):
                copy.start()

        own_dx_copy(e).start()

        @pl.loop(1, GROUP)
        def _(k):
            dx_copy(e, k).start()

    def val_copy(k):
        to = at_offset(k)
        return remote(val_s.at[:, place_of(to)], valb.at[:, me], vsem.at[0, k], vsem.at[1, k], to)

    own_val = pltpu.make_async_copy(val_s.at[:, me], valb.at[:, me], vsem.at[0, 0])
    own_val.start()

    @pl.loop(1, GROUP)
    def _(k):
        val_copy(k).start()

    def step(arrived, dist, leaves):
        @pl.loop(0, OWN)
        def _(e):
            for way in (0, 1):
                for kind in arrived:
                    hop(e, way, kind).wait_recv()
                if leaves == SUM3:
                    add_into(r4.at[way, e], chunk(e, way, dist).at[way])
                else:
                    add_into((r3 if leaves == TWO else r2).at[way, e], chunk(e, way, dist))
                hop(e, way, leaves).start()

    step((FAR,), 3, SUM3)
    step((SUM3, NEW3), 2, TWO)

    group, places = dxb.shape[:2]
    ids = ids_ref[...].astype(F32)
    r = lax.broadcasted_iota(jnp.int32, (group * 8, tok), 0)
    d_of, e_of = r // 8, lax.rem(r, 8)
    expert = lax.rem(d_of, NX * NC) * (NY * OWN) + d_of // (NX * NC) * OWN + e_of
    expert = jnp.where(e_of < OWN, expert, -1).astype(F32)
    member = jnp.zeros((group * 8, tok), F32)
    for j in range(8):
        member = member + (jnp.broadcast_to(ids[j:j + 1, :], member.shape) == expert).astype(F32)
    before = dot(member.astype(BF16), strict_upper(tok))
    key_s[...] = jnp.where(member > 0.0, before, -1.0).reshape(key_s.shape)
    rr = lax.broadcasted_iota(jnp.int32, (places, tok), 0)
    place, e_row = lax.rem(rr, cap).astype(F32), rr // cap
    some = rows // places

    @pl.loop(0, OWN)
    def _(e):
        pltpu.make_async_copy(dxb.at[:, pl.ds(pl.multiple_of(e * cap, 8), cap)], dxb.at[:, pl.ds(pl.multiple_of(e * cap, 8), cap)], drecv.at[e]).wait()

    own_val.wait()

    @pl.loop(1, GROUP)
    def _(k):
        val_copy(k).wait()

    back = [pltpu.make_async_copy(dxb.at[pl.ds(i * some, some)], (xb if i % 2 == 0 else gb).reshape(some, places, hidden), lsem.at[i % 2]) for i in range(group // some)]
    vals = pltpu.make_async_copy(valb, vb, lsem.at[2])
    vals.start()
    back[0].start()
    for i in range(group // some):
        if i + 1 < len(back):
            back[i + 1].start()

        @pl.loop(0, some)
        def _(k):
            key = key_s[i * some + k]
            mine = jnp.full((places, tok), -1.0, F32)
            for e in range(OWN):
                mine = jnp.where(e_row == e, jnp.broadcast_to(key[e:e + 1, :], (places, tok)), mine)
            sb[pl.ds(pl.multiple_of(k * places, places), places), :] = (place == mine).astype(F32).astype(BF16)

        back[i].wait()
        part = dot(sb[...], (xb if i % 2 == 0 else gb)[...], 0, 0)
        acc_s[...] = part if i == 0 else acc_s[...] + part

    in_grad_ref[...] = acc_s[...].astype(BF16)
    vals.wait()

    def gate_step(k, total):
        number = lax.rem(k, NX * NC) * (NY * OWN) + k // (NX * NC) * OWN
        for e in range(OWN):
            row = vb[e, pl.ds(k, 1), :]
            total = total + jnp.where(ids == (number + e).astype(F32), jnp.broadcast_to(row, ids.shape), 0.0)
        return total

    gate_ref[...] = lax.fori_loop(0, group, gate_step, jnp.zeros((8, tok), F32))

    step((TWO,), 1, ONE)

    def keep(e, dy):
        to = lax.rem(y + dy, NY)
        src = r1.at[0, e, to // 2, :, pl.ds(pl.multiple_of(lax.rem(to, 2) * d_loc, 8), d_loc)]
        dst = grads.at[:, y * OWN + e]
        if dy == 0:
            return pltpu.make_async_copy(src, dst, ysend.at[e, 0])
        return remote(src, dst, ysend.at[e, dy], yrecv.at[e, (-dy) % NY], {"y": to})

    @pl.loop(0, OWN)
    def _(e):
        for way in (0, 1):
            hop(e, way, ONE).wait_recv()
        add_into(r1.at[0, e], r1.at[1, e], G.at[e, z])
        for dy in range(NY):
            keep(e, dy).start()

    @pl.loop(0, OWN)
    def _(e):
        keep(e, 0).wait()
        for dy in range(1, NY):
            remote(grads.at[:, lax.rem(y + dy, NY) * OWN + e], grads.at[:, lax.rem(y + dy, NY) * OWN + e], ysend.at[e, dy], yrecv.at[e, dy], {"y": lax.rem(y + dy, NY)}).wait_recv()
            keep(e, dy).wait_send()
        for way in (0, 1):
            for kind in range(5):
                hop(e, way, kind).wait_send()

        sent = dxs.at[e, pl.ds(0, (GROUP - 1) * cap)]
        pltpu.make_async_copy(sent, sent, dsend.at[e]).wait()


def run_experts(cap, xr, ur, gr, sel, wa, ids):
    _, rows, hidden = xr.shape
    tok, ff = sel.shape[-1], wa.shape[-1]
    d_loc = hidden // (NZ * NY)
    half = hidden // NZ // 2
    dma = pltpu.SemaphoreType.DMA
    v = pltpu.VMEM
    shape = jax.ShapeDtypeStruct
    outs = pl.pallas_call(
        functools.partial(expert_kernel, cap),
        name="experts",
        out_shape=(
            shape((3, NY * OWN, d_loc, ff), F32),
            shape((tok, hidden), BF16),
            shape((8, tok), F32),
            shape((GROUP, OWN * cap, hidden), BF16),
            shape((OWN, GROUP, tok), F32),
            shape((OWN, rows, hidden), BF16),
        ),
        in_specs=[ANY] * 5 + [VMEM],
        out_specs=(ANY, VMEM, VMEM, ANY, ANY, ANY),
        scratch_shapes=[
            v((rows, hidden), BF16), v((rows, hidden), BF16), v((rows, hidden), BF16), v((rows, tok), BF16),
            v((2, 3, NZ, NY, d_loc, ff), BF16), v((rows, ff), BF16), v((rows, ff), BF16), v((rows, ff), BF16), v((rows, 1), F32),
            v((rows, hidden), BF16), v((OWN, GROUP, tok), F32), v((OWN, GROUP, tok), F32), v((GROUP, 8, tok), F32), v((tok, hidden), F32),
            v((OWN, NZ, 2, 3, half, ff), F32), v((2, OWN, 3, half, ff), F32),
            v((2, OWN, 2, 3, half, ff), F32), v((2, OWN, 2, 3, half, ff), F32), v((2, OWN, 2, 3, half, ff), F32),
            dma((4,)), dma((2, 3)), dma((2, OWN, 5)), dma((2, OWN, 5)), dma((OWN, NY)), dma((OWN, NY)),
            dma((OWN,)), dma((OWN,)), dma((2, GROUP)), dma((1,)),
        ],
        compiler_params=pltpu.CompilerParams(collective_id=1, has_side_effects=True, vmem_limit_bytes=67043328),
    )(xr, ur, gr, sel, wa, ids)
    return outs[:3]


def solution(mesh):
    mesh4 = Mesh(mesh.devices.reshape(NZ, NY, NX, NC), ("z", "y", "x", "core"))
    tok_spec = P(("z", "y", "x", "core"), None)
    up_spec = P(("x", "core"), ("z", "y"), None)
    down_spec = P(("x", "core"), None, ("z", "y"))

    def per_device(layer_in, out_grad, expert_ids, gate_vals, w_one, w_two, w_three):
        tok_dev, hidden = layer_in.shape
        top_k = expert_ids.shape[1]
        local_experts, d_loc, ff = w_one.shape
        cap = capacity_of(tok_dev, top_k, local_experts * NX * NC)
        ids = expert_ids.T
        xr, ur, gr, sel, wa = gather(cap, layer_in, out_grad, ids, gate_vals.T, w_one, w_three, w_two.swapaxes(1, 2))
        grads, in_grad, gate_out = run_experts(cap, xr, ur, gr, sel, wa, ids)
        return in_grad, gate_out.T, grads[0], grads[2].swapaxes(1, 2), grads[1]

    return jax.shard_map(per_device, mesh=mesh4, in_specs=(tok_spec, tok_spec, tok_spec, tok_spec, up_spec, down_spec, up_spec), out_specs=(tok_spec, tok_spec, up_spec, down_spec, up_spec), check_vma=False)
```

```python
import functools

import jax
import jax.numpy as jnp
from jax import lax
from jax.experimental import pallas as pl
from jax.experimental.pallas import tpu as pltpu
from jax.sharding import Mesh, PartitionSpec as P

NZ, NY, NX, NC = 8, 4, 4, 2
GROUP = NY * NX * NC
PLANE = ("y", "x", "core")
OWN = 4
F32, BF16 = jnp.float32, jnp.bfloat16
ANY = pl.BlockSpec(memory_space=pl.ANY)
VMEM = pl.BlockSpec(memory_space=pltpu.VMEM)


def capacity_of(tok_dev, top_k, experts):
    return max(8, ((tok_dev * top_k * 5) // (4 * experts) + 7) // 8 * 8)


def contract(ca, cb):
    return lambda a, b: lax.dot_general(a, b, (((ca,), (cb,)), ((), ())), preferred_element_type=F32)


dot, dot_nt, dot_tn = contract(1, 0), contract(1, 1), contract(0, 0)


def params(number):
    return pltpu.CompilerParams(collective_id=number, has_side_effects=True, vmem_limit_bytes=67043328)


def each_other(body):
    return pl.loop(1, GROUP)(body)


def strict_upper(n):
    rows = lax.broadcasted_iota(jnp.int32, (n, n), 0)
    cols = lax.broadcasted_iota(jnp.int32, (n, n), 1)
    return (rows < cols).astype(F32).astype(BF16)


def here():
    return tuple(lax.axis_index(a) for a in ("z", "y", "x", "core"))


def at_offset(k):
    _, y, x, c = here()
    dy, dx, dc = k // (NX * NC), lax.rem(k // NC, NX), lax.rem(k, NC)
    return {"y": lax.rem(y + dy, NY), "x": lax.rem(x + dx, NX), "core": lax.rem(c + dc, NC)}


def place_of(d):
    return d["y"] * (NX * NC) + d["x"] * NC + d["core"]


def z_at(dz):
    return {"z": lax.rem(lax.axis_index("z") + dz, NZ)}


def remote(src, dst, send_sem, recv_sem, target):
    return pltpu.make_async_remote_copy(src_ref=src, dst_ref=dst, send_sem=send_sem, recv_sem=recv_sem, device_id=target, device_id_type=pl.DeviceIdType.MESH)


def enter():
    barrier = pltpu.get_barrier_semaphore()

    @each_other
    def _(k):
        pl.semaphore_signal(barrier, device_id=at_offset(k), device_id_type=pl.DeviceIdType.MESH)

    for dz in (1, NZ - 1):
        pl.semaphore_signal(barrier, device_id=z_at(dz), device_id_type=pl.DeviceIdType.MESH)
    return lambda: pl.semaphore_wait(barrier, GROUP + 1)


RATE, D2D, HOP, STEP = 46600.0, 300000.0, 2.0, 1.5


def gather_order(rows_bytes, cut, piece_bytes):
    size = {"A": rows_bytes * cut, "B": rows_bytes * (1.0 - cut)}
    free, coming, order, have, ready = {}, [], [], {}, {}

    def send(now, name, part, link, arrives, nbytes):
        rate = D2D if link == "core" else RATE
        t = max(now, free.get(link, 0.0)) + nbytes / rate
        free[link] = t
        coming.append((t + HOP, len(order), len(coming), arrives))
        return (name, part, link)

    def on_rows(now, kind, dy, dx):
        out = []
        first, second = ("x", "y") if kind == "A" else ("y", "x")
        d = {"x": dx, "y": dy}

        def go(axis, sign, part):
            nd = dict(d)
            nd[axis] = (d[axis] - sign) % 4
            arrives = (kind, nd["y"], nd["x"], part)
            out.append(send(now, (kind, dy, dx), part, axis + ("+" if sign > 0 else "-"), arrives, size[kind] / (2 if part is not None else 1)))

        if d[second] == 0:
            if d[first] == 0:
                go(first, 1, None)
                go(first, -1, None)
            elif d[first] == 3:
                go(first, 1, 0)
            elif d[first] == 1:
                go(first, -1, 1)
            go(second, 1, None)
            go(second, -1, None)
        elif d[second] == 3:
            go(second, 1, 0)
        elif d[second] == 1:
            go(second, -1, 1)
        out.append(send(now, (kind, dy, dx), None, "core", ("core", kind, dy, dx), size[kind]))
        return out

    def on_piece(now, dz, dy):
        out = []
        if dz == 0 or dz in (6, 7) or (dz == 5 and dy in (0, 1)):
            out.append(send(now, ("W", dz, dy), None, "z+", ("W", (dz - 1) % NZ, dy, None), piece_bytes))
        if dz == 0 or dz in (1, 2) or (dz == 3 and dy in (2, 3)):
            out.append(send(now, ("W", dz, dy), None, "z-", ("W", (dz + 1) % NZ, dy, None), piece_bytes))
        return out

    def arrived_for(dy, dx, now):
        return all(ready.get((kind, dy, dx), 1e9) <= now and ready.get(("core", kind, dy, dx), 1e9) <= now for kind in "AB")

    first = []
    for dy, link in ((1, "y+"), (3, "y-")):
        first.append(send(0.0, ("w", dy), None, link, ("W", 0, (-dy) % NY, None), piece_bytes))
    for part, link in ((0, "y+"), (1, "y-")):
        first.append(send(0.0, ("w", 2), part, link, ("R", part), piece_bytes / 2))
    first += on_piece(0.0, 0, 0) + on_rows(0.0, "B", 0, 0) + on_rows(0.0, "A", 0, 0)
    ready[("A", 0, 0)] = ready[("B", 0, 0)] = 0.0
    order.append((None, first))
    todo = [(dy, dx) for dy in range(NY) for dx in range(NX)]
    now = 0.0
    while coming or todo:
        coming.sort()
        place = next((p for p in todo if arrived_for(*p, now)), None)
        if place is not None and not (coming and coming[0][0] <= now):
            todo.remove(place)
            order.append((("place",) + place, []))
            now += STEP
            continue
        t, _, _, name = coming.pop(0)
        now = max(now, t)
        if name[0] == "core":
            ready[name] = now
        elif name[0] == "R":
            part = name[1]
            order.append((name, [send(now, ("R",), part, "y+" if part == 0 else "y-", ("W", 0, 2, part), piece_bytes / 2)]))
        else:
            key, part = name[:3], name[3]
            have[key] = have.get(key, 0) + (2 if part is None else 1)
            whole = have[key] == 2
            if name[0] == "W":
                order.append((name, on_piece(now, name[1], name[2]) if whole else []))
            else:
                if whole:
                    ready[key] = now
                order.append((name, on_rows(now, *key) if whole else []))
    return order


def first_expert(d):
    return lax.rem(d, NX * NC) * (NY * OWN) + d // (NX * NC) * OWN


def gather_kernel(order, cap, cut, x_hbm, u_hbm, ids_ref, gate_ref, w1_hbm, w3_hbm, w2_hbm, xr, ur, gr, sel, wa,
                  rows, metas, gates_out, wown, wv, relay, tri, sx, su, sg, ss,
                  recv, core_recv, wrecv, relay_recv, mrecv, send_sem, msend, load_sem, store_sem, wstore):
    z, y, x, c = here()
    tok = x_hbm.shape[0]
    own = wv.shape[3]

    def place(dy, dx, dc=0):
        return place_of(at_offset(dy * (NX * NC) + dx * NC + dc))

    me = place(0, 0)
    loads = [
        pltpu.make_async_copy(x_hbm, rows.at[me, pl.ds(0, tok)], load_sem.at[0]),
        pltpu.make_async_copy(u_hbm, rows.at[me, pl.ds(tok, tok)], load_sem.at[1]),
    ]
    for m, w in enumerate((w1_hbm, w3_hbm, w2_hbm)):
        loads.append(pltpu.make_async_copy(w.reshape(NY, own, *w.shape[1:]), wown.at[:, m], load_sem.at[2 + m]))
    for copy in loads:
        copy.start()

    @pl.loop(0, GROUP)
    def _(d):
        number = first_expert(d) + lax.broadcasted_iota(jnp.int32, (OWN, tok), 0)
        value = jnp.full((OWN, tok), -1.0, F32)
        for j in range(ids_ref.shape[0]):
            chosen = ids_ref[pl.ds(j, 1), :] == number
            value = jnp.where(chosen, jnp.broadcast_to(gate_ref[pl.ds(j, 1), :], value.shape), value)
        gates_out[d] = value

    metas[me] = gates_out[me]

    all_in = enter()
    tri[...] = strict_upper(tok)
    for copy in loads:
        copy.wait()
    all_in()

    targets = {"core": {"core": 1 - c}}
    for sign, n in (("+", 1), ("-", -1)):
        targets["x" + sign] = {"x": lax.rem(x + n + NX, NX)}
        targets["y" + sign] = {"y": lax.rem(y + n + NY, NY)}
        targets["z" + sign] = z_at(n + NZ)
    step = {"x+": (0, 3), "x-": (0, 1), "y+": (3, 0), "y-": (1, 0)}
    spans = {"A": (0, cut), "B": (cut, 2 * tok - cut)}

    def block(kind, dy, dx, part=None, dc=0):
        start, size = spans[kind]
        if part is not None:
            size //= 2
            start += part * size
        return rows.at[place(dy, dx, dc), pl.ds(start, size)]

    def bsem(kind, dy, dx, part):
        return recv.at[0 if kind == "A" else 1, dy * NX + dx, part or 0]

    def piece(dz, dy, part=None):
        here = wv.at[lax.rem(z + dz, NZ), lax.rem(y + dy, NY)]
        return here if part is None else here.at[:, pl.ds(part * (own // 2), own // 2)]

    copies = []

    def issue(name, part, link):
        sem = send_sem.at[len(copies)]
        if name[0] == "w":
            dy = name[1]
            src = wown.at[lax.rem(y + dy, NY)]
            if part is None:
                copy = remote(src, piece(0, 0), sem, wrecv.at[0, (-dy) % NY, 0], targets[link])
            else:
                src = src.at[:, pl.ds(part * (own // 2), own // 2)]
                copy = remote(src, relay.at[part], sem, relay_recv.at[part], targets[link])
        elif name[0] == "R":
            dst = piece(0, 3 if part == 0 else 1, part)
            copy = remote(relay.at[part], dst, sem, wrecv.at[0, 2, part], targets[link])
        elif name[0] == "W":
            _, dz, dy = name
            ndz = (dz - 1) % NZ if link == "z+" else (dz + 1) % NZ
            src = wown.at[y] if (dz, dy) == (0, 0) else piece(dz, dy)
            copy = remote(src, piece(dz, dy), sem, wrecv.at[ndz, dy, 0], targets[link])
        else:
            kind, dy, dx = name
            here = block(kind, dy, dx, part)
            if link == "core":
                rsem = core_recv.at[0 if kind == "A" else 1, dy * NX + dx]
            else:
                oy, ox = step[link]
                rsem = bsem(kind, (dy + oy) % NY, (dx + ox) % NX, part)
            copy = remote(here, here, sem, rsem, targets[link])
        copy.start()
        copies.append(copy)

    def wait(here, sem):
        remote(here, here, send_sem.at[0], sem, targets["core"]).wait_recv()

    def meta_copy(k):
        to = at_offset(k)
        return remote(gates_out.at[place_of(to)], metas.at[me], msend.at[k], mrecv.at[k], to)

    n_rows = OWN * 2 * cap
    stores = []

    def put(dy, dx):
        slot = len(stores) % 2
        if stores[1:]:
            for copy in stores[-2]:
                copy.wait()
        for dc in (0, 1):
            if (dy, dx, dc) != (0, 0, 0):
                k = ((-dy) % NY) * (NX * NC) + ((-dx) % NX) * NC + dc
                wait(metas.at[place(dy, dx, dc)], mrecv.at[k])
        for i, kind in enumerate("AB"):
            wait(block(kind, dy, dx, None, 1), core_recv.at[i, dy * NX + dx])
        chip = lax.rem(y + dy, NY) * NX + lax.rem(x + dx, NX)
        n = 2 * OWN
        which = lax.broadcasted_iota(jnp.int32, (n, tok), 0)
        gate = jnp.zeros((n, tok), F32)
        for i in range(n):
            gate = jnp.where(which == i, jnp.broadcast_to(metas[2 * chip + i // OWN, pl.ds(i % OWN, 1), :], gate.shape), gate)
        member = gate >= 0.0
        key = jnp.where(member, dot(member.astype(F32).astype(BF16), tri[...]), -1.0)
        r = lax.broadcasted_iota(jnp.int32, (n_rows, tok), 0)
        at = lax.rem(r, cap).astype(F32)
        row_of = lax.rem(r // cap, 2) * OWN + r // (2 * cap)
        mine, gates = jnp.full((n_rows, tok), -1.0, F32), jnp.zeros((n_rows, tok), F32)
        for i in range(n):
            mine = jnp.where(row_of == i, jnp.broadcast_to(key[i:i + 1, :], mine.shape), mine)
            gates = jnp.where(row_of == i, jnp.broadcast_to(gate[i:i + 1, :], mine.shape), gates)
        found = at == mine
        pick = [jnp.logical_and(found, row_of // OWN == p).astype(F32) for p in range(2)]
        both = pick[0] + pick[1]
        scale = jnp.sum(both * gates, axis=1, keepdims=True)
        ss[slot] = both.astype(BF16).reshape(ss.shape[1:])
        pick = [p.astype(BF16) for p in pick]
        x_rows = dot(pick[0], rows[2 * chip, 0:tok, :]) + dot(pick[1], rows[2 * chip + 1, 0:tok, :])
        sx[slot] = x_rows.astype(BF16).reshape(sx.shape[1:])
        u_rows = dot(pick[0], rows[2 * chip, tok:2 * tok, :]) + dot(pick[1], rows[2 * chip + 1, tok:2 * tok, :])
        su[slot] = u_rows.astype(BF16).reshape(su.shape[1:])
        sg[slot] = (scale * u_rows).astype(BF16).reshape(sg.shape[1:])
        span = pl.ds(pl.multiple_of(chip * 2 * cap, 2 * cap), 2 * cap)
        out = [pltpu.make_async_copy(s.at[slot], d.at[:, span], store_sem.at[slot, i]) for i, (s, d) in enumerate(((sx, xr), (su, ur), (sg, gr), (ss, sel)))]
        for copy in out:
            copy.start()
        stores.append(out)

    wstores = []

    def keep(src, dz, dy):
        copy = pltpu.make_async_copy(src, wa.at[lax.rem(z + dz, NZ), lax.rem(y + dy, NY)], wstore.at[len(wstores)])
        copy.start()
        wstores.append(copy)

    parts = {}
    for name, sends in order:
        if name is None:
            pass
        elif name[0] == "place":
            put(*name[1:])
        elif name[0] == "R":
            wait(relay.at[name[1]], relay_recv.at[name[1]])
        elif name[0] == "W":
            _, dz, dy, part = name
            wait(piece(dz, dy, part), wrecv.at[dz, dy, part or 0])
        else:
            wait(block(*name), bsem(*name))
        for send in sends:
            issue(*send)
        if name is None:
            keep(wown.at[y], 0, 0)

            @each_other
            def _(k):
                meta_copy(k).start()
        elif name[0] == "W":
            parts[name[1:3]] = parts.get(name[1:3], 0) + (2 if name[3] is None else 1)
            if parts[name[1:3]] == 2:
                keep(piece(name[1], name[2]), name[1], name[2])

    for out in stores[-2:]:
        for copy in out:
            copy.wait()
    for copy in wstores:
        copy.wait()

    @each_other
    def _(k):
        meta_copy(k).wait_send()

    for copy in copies:
        copy.wait_send()


def gather(cap, x, u, ids, gates, w1, w3, w2):
    tok, hidden = x.shape
    local_experts, d_loc, ff = w1.shape
    own = local_experts // NY
    cut = tok - tok // 8 if tok % 256 == 0 else tok
    piece = (3, own, d_loc, ff)
    piece_bytes = 2 * 3 * own * d_loc * ff
    order = gather_order(4 * tok * hidden, cut / (2 * tok), piece_bytes)
    sends = sum(len(s) for _, s in order)
    dma, v = pltpu.SemaphoreType.DMA, pltpu.VMEM
    rows = GROUP * cap
    out = lambda lanes: jax.ShapeDtypeStruct((OWN, rows, lanes), BF16)
    stage = lambda lanes: v((2, OWN, 2 * cap, lanes), BF16)
    return pl.pallas_call(
        functools.partial(gather_kernel, order, cap, cut),
        name="gather",
        out_shape=(out(hidden), out(hidden), out(hidden), out(tok), jax.ShapeDtypeStruct((NZ, NY) + piece, BF16)),
        in_specs=[ANY, ANY, VMEM, VMEM, ANY, ANY, ANY],
        out_specs=(ANY,) * 5,
        scratch_shapes=[
            v((GROUP, 2 * tok, hidden), BF16), v((GROUP, OWN, tok), F32), v((GROUP, OWN, tok), F32), v((NY,) + piece, BF16), v((NZ, NY) + piece, BF16),
            v((2, 3, own // 2, d_loc, ff), BF16), v((tok, tok), BF16), stage(hidden), stage(hidden), stage(hidden), stage(tok),
            dma((2, NY * NX, 2)), dma((2, NY * NX)), dma((NZ, NY, 2)), dma((2,)), dma((GROUP,)), dma((sends,)), dma((GROUP,)),
            dma((5,)), dma((2, 4)), dma((NZ * NY,)),
        ],
        compiler_params=params(0),
    )(x, u, ids, gates, w1, w3, w2)


FAR, SUM3, NEW3, TWO, ONE, HOPS = 0, 1, 2, 3, 4, 7


def expert_kernel(cap, xr, ur, gr, sel, wa, ids_ref, grads, in_grad_ref, gate_ref, dxb, valb, dxs,
                  xb, ub, gb, sb, wb, a_s, d1_s, d3_s, y_s, dx_s, val_s, vb, key_s, acc_s, G, r4, r3, r2, r1,
                  lsem, wsem, rsend, rrecv, ysend, yrecv, dsend, drecv, vsem, osem):
    z, y, x, c = here()
    rows, hidden = xb.shape
    ff, tok = a_s.shape[-1], sb.shape[-1]
    d_loc = hidden // (NZ * NY)
    me = place_of(at_offset(0))

    def row_copies(e):
        pairs = ((xr, xb), (gr, gb), (ur, ub), (sel, sb))
        return [pltpu.make_async_copy(src.at[e], dst, lsem.at[i]) for i, (src, dst) in enumerate(pairs)]

    def weight_copies(e, slot):
        return [pltpu.make_async_copy(wa.at[:, :, m, e], wb.at[slot, m], wsem.at[slot, m]) for m in range(3)]

    for copy in weight_copies(0, 0) + row_copies(0):
        copy.start()

    all_in = enter()

    def chunk(e, way, dist):
        return G.at[e, z_at(dist if way else NZ - dist)["z"]]

    def hop(e, way, kind):
        h = way
        src, dst = {
            FAR: lambda: (chunk(e, way, 4).at[h], r4.at[way, e]),
            SUM3: lambda: (r4.at[way, e], r3.at[way, e, h]),
            NEW3: lambda: (chunk(e, way, 3).at[1 - h], r3.at[way, e, 1 - h]),
            TWO: lambda: (r3.at[way, e], r2.at[way, e]),
        }.get(kind, lambda: (r2.at[way, e, :, kind - ONE], r1.at[way, e, :, kind - ONE]))()
        return remote(src, dst, rsend.at[way, e, kind], rrecv.at[way, e, kind], z_at(1 if way else NZ - 1))

    def add_into(dst, *others):
        parts = dst.shape[:-2]

        def flat(ref, i):
            index = []
            for n in reversed(parts):
                index.append(lax.rem(i, n))
                i = i // n
            return ref.at[tuple(reversed(index))]

        n = 1
        for p in parts:
            n *= p

        @pl.loop(0, n)
        def _(i):
            total = flat(dst, i)[...]
            for other in others:
                total = total + flat(other, i)[...]
            flat(dst, i)[...] = total

    def dx_copy(e, k):
        to = at_offset(k)
        src = dxs.at[e, pl.ds(pl.multiple_of(place_of(to) * cap, 8), cap)]
        return remote(src, dxb.at[me, pl.ds(pl.multiple_of(e * cap, 8), cap)], dsend.at[e], drecv.at[e], to)

    def own_dx_copy(e):
        src = dxs.at[e, pl.ds(pl.multiple_of(me * cap, 8), cap)]
        return pltpu.make_async_copy(src, dxb.at[me, pl.ds(pl.multiple_of(e * cap, 8), cap)], drecv.at[e])

    tile = 256 if rows % 256 == 0 else rows
    dtile = hidden // NZ
    half = dtile // 2

    @pl.loop(0, OWN)
    def _(e):
        slot = lax.rem(e, 2)
        for copy in weight_copies(e, slot) + row_copies(e):
            copy.wait()

        @pl.when(e < OWN - 1)
        def _():
            for copy in weight_copies(e + 1, 1 - slot):
                copy.start()

        def w(m):
            return wb[slot, m].reshape(hidden, ff)

        @pl.loop(0, rows // tile)
        def _(i):
            at = pl.ds(pl.multiple_of(i * tile, tile), tile)
            x_rows = xb[at, :]
            h1, h3 = dot(x_rows, w(0)), dot(x_rows, w(1))
            sig = jax.nn.sigmoid(h1)
            silu = h1 * sig
            act = (silu * h3).astype(BF16)
            a_s[at, :] = act
            y_rows = dot_nt(act, w(2))
            y_s[at, :] = jnp.sum(ub[at, :].astype(F32) * y_rows, axis=1, keepdims=True)
            da = dot(gb[at, :], w(2))
            d1 = (da * h3 * sig * (1.0 + h1 * (1.0 - sig))).astype(BF16)
            d3 = (da * silu).astype(BF16)
            d1_s[at, :] = d1
            d3_s[at, :] = d3
            dx_s[at, :] = (dot_nt(d1, w(0)) + dot_nt(d3, w(1))).astype(BF16)

        out = pltpu.make_async_copy(dx_s, dxs.at[e], osem.at[0])
        out.start()

        @pl.loop(0, NZ // 2)
        def _(i):
            pair = [z_at(n + 2 * i)["z"] for n in (3, 4)]

            def cols(ref):
                return jnp.concatenate([ref[:, pl.ds(pl.multiple_of(k * dtile, dtile), dtile)] for k in pair], axis=1)

            x_cols, g_cols = cols(xb), cols(gb)
            for m, part in enumerate((dot_tn(x_cols, d1_s[...]), dot_tn(x_cols, d3_s[...]), dot_tn(g_cols, a_s[...]))):
                for j in range(4):
                    G[e, pair[j // 2], j % 2, m] = part[j * half:(j + 1) * half]

            @pl.when(i == 0)
            def _():
                @pl.when(e == 0)
                def _():
                    all_in()

                for way, kind in ((0, FAR), (1, FAR), (1, NEW3)):
                    hop(e, way, kind).start()

            @pl.when(i == 1)
            def _():
                hop(e, 0, NEW3).start()

        val = sb[...].astype(F32) * y_s[...]
        val_s[e] = jnp.sum(val.reshape(rows // cap, cap, tok), axis=1)
        out.wait()

        @pl.when(e < OWN - 1)
        def _():
            for copy in row_copies(e + 1):
                copy.start()

        own_dx_copy(e).start()

        @each_other
        def _(k):
            dx_copy(e, k).start()

    def val_copy(k):
        to = at_offset(k)
        return remote(val_s.at[:, place_of(to)], valb.at[:, me], vsem.at[0, k], vsem.at[1, k], to)

    own_val = pltpu.make_async_copy(val_s.at[:, me], valb.at[:, me], vsem.at[0, 0])
    own_val.start()

    @each_other
    def _(k):
        val_copy(k).start()

    def step(arrived, dist, leaves):
        @pl.loop(0, OWN)
        def _(e):
            for way in (0, 1):
                for kind in arrived:
                    hop(e, way, kind).wait_recv()
                mine = chunk(e, way, dist)
                if leaves == SUM3:
                    add_into(r4.at[way, e], mine.at[way])
                elif leaves == TWO:
                    add_into(r3.at[way, e], mine)
                if leaves < ONE:
                    hop(e, way, leaves).start()
            if leaves == ONE:
                for m in range(3):
                    for way in (0, 1):
                        add_into(r2.at[way, e, :, m], chunk(e, way, dist).at[:, m])
                        hop(e, way, ONE + m).start()

    step((FAR,), 3, SUM3)
    step((SUM3, NEW3), 2, TWO)

    group, places = dxb.shape[:2]
    ids = ids_ref[...].astype(F32)
    r = lax.broadcasted_iota(jnp.int32, (group * 8, tok), 0)
    d_of, e_of = r // 8, lax.rem(r, 8)
    expert = lax.rem(d_of, NX * NC) * (NY * OWN) + d_of // (NX * NC) * OWN + e_of
    expert = jnp.where(e_of < OWN, expert, -1).astype(F32)
    member = jnp.zeros((group * 8, tok), F32)
    for j in range(8):
        member = member + (jnp.broadcast_to(ids[j:j + 1, :], member.shape) == expert).astype(F32)
    before = dot(member.astype(BF16), strict_upper(tok))
    key_s[...] = jnp.where(member > 0.0, before, -1.0).reshape(key_s.shape)
    rr = lax.broadcasted_iota(jnp.int32, (places, tok), 0)
    place, e_row = lax.rem(rr, cap).astype(F32), rr // cap
    some = rows // places

    @pl.loop(0, OWN)
    def _(e):
        pltpu.make_async_copy(dxb.at[:, pl.ds(pl.multiple_of(e * cap, 8), cap)], dxb.at[:, pl.ds(pl.multiple_of(e * cap, 8), cap)], drecv.at[e]).wait()

    own_val.wait()

    @each_other
    def _(k):
        val_copy(k).wait()

    back = [pltpu.make_async_copy(dxb.at[pl.ds(i * some, some)], (xb if i % 2 == 0 else gb).reshape(some, places, hidden), lsem.at[i % 2]) for i in range(group // some)]
    vals = pltpu.make_async_copy(valb, vb, lsem.at[2])
    vals.start()
    back[0].start()
    for i in range(group // some):
        if i + 1 < len(back):
            back[i + 1].start()

        @pl.loop(0, some)
        def _(k):
            key = key_s[i * some + k]
            mine = jnp.full((places, tok), -1.0, F32)
            for e in range(OWN):
                mine = jnp.where(e_row == e, jnp.broadcast_to(key[e:e + 1, :], (places, tok)), mine)
            sb[pl.ds(pl.multiple_of(k * places, places), places), :] = (place == mine).astype(F32).astype(BF16)

        back[i].wait()
        part = dot_tn(sb[...], (xb if i % 2 == 0 else gb)[...])
        acc_s[...] = part if i == 0 else acc_s[...] + part

    in_grad_ref[...] = acc_s[...].astype(BF16)
    vals.wait()

    def gate_step(k, total):
        number = lax.rem(k, NX * NC) * (NY * OWN) + k // (NX * NC) * OWN
        for e in range(OWN):
            row = vb[e, pl.ds(k, 1), :]
            total = total + jnp.where(ids == (number + e).astype(F32), jnp.broadcast_to(row, ids.shape), 0.0)
        return total

    gate_ref[...] = lax.fori_loop(0, group, gate_step, jnp.zeros((8, tok), F32))

    step((TWO,), 1, ONE)

    def keep(e, m, dy):
        to = lax.rem(y + dy, NY)
        src = r1.at[0, e, to // 2, m, pl.ds(pl.multiple_of(lax.rem(to, 2) * d_loc, 8), d_loc)]
        dst = grads.at[m, y * OWN + e]
        if dy == 0:
            return pltpu.make_async_copy(src, dst, ysend.at[e, m, dy])
        return remote(src, dst, ysend.at[e, m, dy], yrecv.at[e, m, (-dy) % NY], {"y": to})

    @pl.loop(0, OWN)
    def _(e):
        for m in range(3):
            for way in (0, 1):
                hop(e, way, ONE + m).wait_recv()
            add_into(r1.at[0, e, :, m], r1.at[1, e, :, m], G.at[e, z, :, m])
            for dy in range(NY):
                keep(e, m, dy).start()

    @pl.loop(0, OWN)
    def _(e):
        for m in range(3):
            keep(e, m, 0).wait()
            for dy in range(1, NY):
                got = grads.at[m, lax.rem(y + dy, NY) * OWN + e]
                remote(got, got, ysend.at[e, m, dy], yrecv.at[e, m, dy], z_at(1)).wait_recv()
                keep(e, m, dy).wait_send()
        for way in (0, 1):
            for kind in range(HOPS):
                hop(e, way, kind).wait_send()

        sent = dxs.at[e, pl.ds(0, (GROUP - 1) * cap)]
        pltpu.make_async_copy(sent, sent, dsend.at[e]).wait()


def run_experts(cap, xr, ur, gr, sel, wa, ids):
    _, rows, hidden = xr.shape
    tok, ff = sel.shape[-1], wa.shape[-1]
    d_loc = hidden // (NZ * NY)
    half = hidden // NZ // 2
    dma = pltpu.SemaphoreType.DMA
    v = pltpu.VMEM
    shape = jax.ShapeDtypeStruct
    outs = pl.pallas_call(
        functools.partial(expert_kernel, cap),
        name="experts",
        out_shape=(
            shape((3, NY * OWN, d_loc, ff), F32),
            shape((tok, hidden), BF16),
            shape((8, tok), F32),
            shape((GROUP, OWN * cap, hidden), BF16),
            shape((OWN, GROUP, tok), F32),
            shape((OWN, rows, hidden), BF16),
        ),
        in_specs=[ANY] * 5 + [VMEM],
        out_specs=(ANY, VMEM, VMEM, ANY, ANY, ANY),
        scratch_shapes=[
            v((rows, hidden), BF16), v((rows, hidden), BF16), v((rows, hidden), BF16), v((rows, tok), BF16),
            v((2, 3, NZ, NY, d_loc, ff), BF16), v((rows, ff), BF16), v((rows, ff), BF16), v((rows, ff), BF16), v((rows, 1), F32),
            v((rows, hidden), BF16), v((OWN, GROUP, tok), F32), v((OWN, GROUP, tok), F32), v((GROUP, 8, tok), F32), v((tok, hidden), F32),
            v((OWN, NZ, 2, 3, half, ff), F32), v((2, OWN, 3, half, ff), F32),
            v((2, OWN, 2, 3, half, ff), F32), v((2, OWN, 2, 3, half, ff), F32), v((2, OWN, 2, 3, half, ff), F32),
            dma((4,)), dma((2, 3)), dma((2, OWN, HOPS)), dma((2, OWN, HOPS)), dma((OWN, 3, NY)), dma((OWN, 3, NY)),
            dma((OWN,)), dma((OWN,)), dma((2, GROUP)), dma((1,)),
        ],
        compiler_params=params(1),
    )(xr, ur, gr, sel, wa, ids)
    return outs[:3]


def finish_kernel(grads, in_grad, gate, *refs):
    n = 5
    outs, bufs, sems = refs[:n], refs[n:2 * n], refs[-1]
    ins = [grads.at[m] for m in range(3)] + [in_grad, gate]
    load = [pltpu.make_async_copy(a, b, sems.at[0, i]) for i, (a, b) in enumerate(zip(ins, bufs))]
    store = [pltpu.make_async_copy(b, o, sems.at[1, i]) for i, (b, o) in enumerate(zip(bufs, outs))]
    for copy in load:
        copy.start()
    for i in range(n):
        load[i].wait()
        store[i].start()
    for copy in store:
        copy.wait()


def finish(grads, in_grad, gate):
    shapes = [grads.shape[1:]] * 3 + [in_grad.shape, gate.shape]
    types = [grads.dtype] * 3 + [in_grad.dtype, gate.dtype]
    return pl.pallas_call(
        finish_kernel,
        name="finish",
        out_shape=[jax.ShapeDtypeStruct(s, t) for s, t in zip(shapes, types)],
        in_specs=[ANY] * 3,
        out_specs=[ANY] * len(shapes),
        scratch_shapes=[pltpu.VMEM(s, t) for s, t in zip(shapes, types)] + [pltpu.SemaphoreType.DMA((2, len(shapes)))],
    )(grads, in_grad, gate)


def solution(mesh):
    mesh4 = Mesh(mesh.devices.reshape(NZ, NY, NX, NC), ("z", "y", "x", "core"))
    tok_spec = P(("z", "y", "x", "core"), None)
    up_spec = P(("x", "core"), ("z", "y"), None)
    down_spec = P(("x", "core"), None, ("z", "y"))

    def per_device(layer_in, out_grad, expert_ids, gate_vals, w_one, w_two, w_three):
        tok_dev, hidden = layer_in.shape
        top_k = expert_ids.shape[1]
        local_experts, d_loc, ff = w_one.shape
        cap = capacity_of(tok_dev, top_k, local_experts * NX * NC)
        ids = expert_ids.T
        xr, ur, gr, sel, wa = gather(cap, layer_in, out_grad, ids, gate_vals.T, w_one, w_three, w_two.swapaxes(1, 2))
        grads, in_grad, gate_out = run_experts(cap, xr, ur, gr, sel, wa, ids)
        g1, g3, g2, in_grad, gate_out = finish(grads, in_grad, gate_out)
        return in_grad, gate_out.T, g1, g2.swapaxes(1, 2), g3

    return jax.shard_map(per_device, mesh=mesh4, in_specs=(tok_spec, tok_spec, tok_spec, tok_spec, up_spec, down_spec, up_spec), out_specs=(tok_spec, tok_spec, up_spec, down_spec, up_spec), check_vma=False)
```

```python
import functools

import jax
import jax.numpy as jnp
from jax import lax
from jax.experimental import pallas as pl
from jax.experimental.pallas import tpu as pltpu
from jax.sharding import Mesh, PartitionSpec as P

NZ, NY, NX, NC = 8, 4, 4, 2
GROUP = NY * NX * NC
PLANE = ("y", "x", "core")
OWN = 4
F32, BF16 = jnp.float32, jnp.bfloat16
ANY = pl.BlockSpec(memory_space=pl.ANY)
VMEM = pl.BlockSpec(memory_space=pltpu.VMEM)


def capacity_of(tok_dev, top_k, experts):
    return max(8, ((tok_dev * top_k * 5) // (4 * experts) + 7) // 8 * 8)


def rem(a, b):
    return a % b if isinstance(a, int) else lax.rem(a, b)


def contract(ca, cb):
    return lambda a, b: lax.dot_general(a, b, (((ca,), (cb,)), ((), ())), preferred_element_type=F32)


dot, dot_nt, dot_tn = contract(1, 0), contract(1, 1), contract(0, 0)


def params(number):
    return pltpu.CompilerParams(collective_id=number, has_side_effects=True, vmem_limit_bytes=67043328)


def each_other(body):
    return pl.loop(1, GROUP)(body)


def strict_upper(n):
    rows = lax.broadcasted_iota(jnp.int32, (n, n), 0)
    cols = lax.broadcasted_iota(jnp.int32, (n, n), 1)
    return (rows < cols).astype(F32).astype(BF16)


def here():
    return tuple(lax.axis_index(a) for a in ("z", "y", "x", "core"))


def at_offset(k):
    _, y, x, c = here()
    dy, dx, dc = k // (NX * NC), rem(k // NC, NX), rem(k, NC)
    return {"y": rem(y + dy, NY), "x": rem(x + dx, NX), "core": rem(c + dc, NC)}


def place_of(d):
    return d["y"] * (NX * NC) + d["x"] * NC + d["core"]


def z_at(dz):
    return {"z": rem(lax.axis_index("z") + dz, NZ)}


def remote(src, dst, send_sem, recv_sem, target):
    return pltpu.make_async_remote_copy(src_ref=src, dst_ref=dst, send_sem=send_sem, recv_sem=recv_sem, device_id=target, device_id_type=pl.DeviceIdType.MESH)


def enter():
    barrier = pltpu.get_barrier_semaphore()

    @each_other
    def _(k):
        pl.semaphore_signal(barrier, device_id=at_offset(k), device_id_type=pl.DeviceIdType.MESH)

    for dz in (1, NZ - 1):
        pl.semaphore_signal(barrier, device_id=z_at(dz), device_id_type=pl.DeviceIdType.MESH)
    return lambda: pl.semaphore_wait(barrier, GROUP + 1)


RATE, D2D, HOP, PUT, TILE = 46600.0, 300000.0, 2.0, 1.0, 2.5
CHIPS = 4

PIECE = {(0, None): (0, 1), (1, None): (1, 3), (1, 0): (1, 1), (1, 1): (2, 2)}
RELAYS = ((0, None, "y+"), (1, 0, "y+"), (1, 1, "y-"))


def gather_order(rows_bytes, cut, expert_bytes):
    size = {"A": rows_bytes * cut, "B": rows_bytes * (1.0 - cut)}
    free, coming, order, have, ready = {}, [], [], {}, {}

    def send(now, name, part, link, arrives, nbytes):
        t = max(now, free.get(link, 0.0)) + nbytes / (D2D if link == "core" else RATE)
        free[link] = t
        coming.append((t + HOP, len(order), len(coming), arrives))
        return (name, part, link)

    def on_rows(now, kind, dy, dx):
        out = []
        first, second = "xy" if kind == "A" else "yx"
        d = {"x": dx, "y": dy}

        def go(axis, sign, part):
            nd = dict(d)
            nd[axis] = (d[axis] - sign) % 4
            arrives = (kind, nd["y"], nd["x"], part)
            out.append(send(now, (kind, dy, dx), part, axis + "-+"[sign > 0], arrives, size[kind] / (1 if part is None else 2)))

        for axis in [first, second] if d[second] == 0 else [second]:
            if d[axis] == 0:
                go(axis, 1, None)
                go(axis, -1, None)
            elif d[axis] == 3:
                go(axis, 1, 0)
            elif d[axis] == 1:
                go(axis, -1, 1)
            if axis == first and d[first] != 0:
                go(second, 1, None)
                go(second, -1, None)
                break
        out.append(send(now, (kind, dy, dx), None, "core", ("core", kind, dy, dx), size[kind]))
        return out

    def weights(now, name, group, part, link, arrives):
        return send(now, name, part, link, arrives + (group, part), PIECE[group, part][1] * expert_bytes)

    def on_piece(now, dz, dy, group):
        out = []
        for link, step, far in (("z+", -1, dy < 2), ("z-", 1, dy >= 2)):
            if (step * dz) % NZ < 3 + far:
                out.append(weights(now, ("W", dz, dy, group), group, None, link, ("W", (dz + step) % NZ, dy)))
        return out

    def is_ready(dy, dx, now):
        return all(ready.get(key, 1e9) <= now for kind in "AB" for key in ((kind, dy, dx), ("core", kind, dy, dx)))

    first = []
    for group in range(2):
        for dy, link in ((1, "y+"), (3, "y-")):
            first.append(weights(0.0, ("w", dy, group), group, None, link, ("W", 0, (-dy) % NY)))
        for i, (g, part, link) in enumerate(RELAYS):
            if g == group:
                first.append((("r", i), part, link))
                weights(0.0, "r", g, part, link, ("R", i))
        first += on_piece(0.0, 0, 0, group)
    first += on_rows(0.0, "B", 0, 0) + on_rows(0.0, "A", 0, 0)
    ready["A", 0, 0] = ready["B", 0, 0] = 0.0
    order.append((None, first))
    todo, puts, tiles, now = [(dy, dx) for dy in range(NY) for dx in range(NX)], 0, 0, 0.0
    while coming or todo or tiles * CHIPS < puts:
        coming.sort()
        if not (coming and coming[0][0] <= now):
            place = next((p for p in todo if is_ready(*p, now)), None)
            if place is not None:
                todo.remove(place)
                order.append((("put",) + place, []))
                puts += 1
                now += PUT
                continue
            if puts >= (tiles + 1) * CHIPS and sum(key[0] == "W" and key[-1] == 0 for key in ready) == NZ * NY - 1:
                order.append((("tile", tiles), []))
                tiles += 1
                now += TILE
                continue
        t, _, _, name = coming.pop(0)
        now = max(now, t)
        if name[0] == "core":
            ready[name] = now
        elif name[0] == "R":
            i, group, part = name[1:]
            order.append((name[:2], [weights(now, name[:2], group, part, RELAYS[i][2], ("W", 0, 2))]))
        else:
            key, part = name[:-1], name[-1]
            have[key] = have.get(key, 0) + (2 if part is None else 1)
            sends = []
            if have[key] == 2:
                ready[key] = now
                sends = (on_piece if name[0] == "W" else on_rows)(now, *(key[1:] if name[0] == "W" else key))
            order.append((name, sends))
    return order


def first_expert(d):
    return rem(d, NX * NC) * (NY * OWN) + d // (NX * NC) * OWN


FAR, SUM3, NEW3, TWO, ONE, HOPS = 0, 1, 2, 3, 4, 7


def layer_kernel(order, cap, cut, scope_one, scope_two, x_hbm, u_hbm, ids_ref, gates_ref, w1_hbm, w3_hbm, w2_hbm,
                 grads, in_grad_ref, gate_ref, dxb, valb, dxs, xr, ur, gr, sel,
                 metas, gates_out, wown, wv, relay, xb, ub, gb, sb, a_s, d1_s, d3_s, y_s, dx_s, val_s, vb, key_s, acc_s,
                 recv, core_recv, wrecv, relay_recv, mrecv, send_sem, msend, load_sem, store_sem,
                 lsem, rsend, rrecv, ysend, yrecv, dsend, drecv, vsem, osem, in_scope):
    z, y, x, c = here()
    tok, hidden = x_hbm.shape
    rows, ff = xb.shape[0], a_s.shape[-1]
    d_loc = hidden // (NZ * NY)
    me = place_of(at_offset(0))

    def place(dy, dx, dc=0):
        return place_of(at_offset(dy * (NX * NC) + dx * NC + dc))

    targets = {"core": {"core": 1 - c}}
    for sign, n in (("+", 1), ("-", -1)):
        targets["x" + sign] = {"x": rem(x + n + NX, NX)}
        targets["y" + sign] = {"y": rem(y + n + NY, NY)}
        targets["z" + sign] = z_at(n + NZ)

    def wait(ref, sem):
        remote(ref, ref, send_sem.at[0], sem, targets["core"]).wait_recv()

    def w(e, m):
        return wv[:, :, e, m].reshape(hidden, ff)

    def expert_rows(e, spans):
        def cut_of(ref):
            return jnp.concatenate([ref[s, :] for s in spans]) if spans[1:] else ref[spans[0], :]

        def save(ref, value):
            n = value.shape[0] // len(spans)
            for i, s in enumerate(spans):
                ref[s, :] = value[i * n:(i + 1) * n]

        x_rows = cut_of(xb)
        h1, h3 = dot(x_rows, w(e, 0)), dot(x_rows, w(e, 1))
        sig = jax.nn.sigmoid(h1)
        silu = h1 * sig
        act = (silu * h3).astype(BF16)
        save(a_s, act)
        y_rows = dot_nt(act, w(e, 2))
        save(y_s, jnp.sum(cut_of(ub).astype(F32) * y_rows, axis=1, keepdims=True))
        da = dot(cut_of(gb), w(e, 2))
        d1 = (da * h3 * sig * (1.0 + h1 * (1.0 - sig))).astype(BF16)
        d3 = (da * silu).astype(BF16)
        save(d1_s, d1)
        save(d3_s, d3)
        save(dx_s, (dot_nt(d1, w(e, 0)) + dot_nt(d3, w(e, 1))).astype(BF16))

    def gather(all_rows, tri, sx, su, sg, ss):
        loads = [
            pltpu.make_async_copy(x_hbm, all_rows.at[me, pl.ds(0, tok)], load_sem.at[0]),
            pltpu.make_async_copy(u_hbm, all_rows.at[me, pl.ds(tok, tok)], load_sem.at[1]),
        ]
        for m, ref in enumerate((w1_hbm, w3_hbm, w2_hbm)):
            loads.append(pltpu.make_async_copy(ref.reshape(NY, OWN, d_loc, ff), wown.at[:, :, m], load_sem.at[2 + m]))
        for copy in loads:
            copy.start()
        all_in = enter()

        @pl.loop(0, GROUP)
        def _(d):
            number = first_expert(d) + lax.broadcasted_iota(jnp.int32, (OWN, tok), 0)
            value = jnp.full((OWN, tok), -1.0, F32)
            for j in range(ids_ref.shape[0]):
                chosen = ids_ref[pl.ds(j, 1), :] == number
                value = jnp.where(chosen, jnp.broadcast_to(gates_ref[pl.ds(j, 1), :], value.shape), value)
            gates_out[d] = value

        metas[me] = gates_out[me]
        tri[...] = strict_upper(tok)
        for copy in loads:
            copy.wait()
        all_in()

        back = {"x+": (0, 3), "x-": (0, 1), "y+": (3, 0), "y-": (1, 0)}
        spans = {"A": (0, cut), "B": (cut, 2 * tok - cut)}

        def block(kind, dy, dx, part=None, dc=0):
            start, size = spans[kind]
            if part is not None:
                size //= 2
                start += part * size
            return all_rows.at[place(dy, dx, dc), pl.ds(start, size)]

        def bsem(kind, dy, dx, part):
            return recv.at[0 if kind == "A" else 1, dy * NX + dx, part or 0]

        def piece(dz, dy, group, part=None):
            return wv.at[z_at(dz)["z"], rem(y + dy, NY), pl.ds(*PIECE[group, part])]

        row_copies = []

        def issue(name, part, link):
            number = len(row_copies) + len(weight_copies)
            sem = send_sem.at[number]
            group, part_of = None, None
            if name[0] == "w":
                _, dy, group = name
                src = wown.at[rem(y + dy, NY), pl.ds(*PIECE[group, None])]
                copy = remote(src, piece(0, 0, group), sem, wrecv.at[0, (-dy) % NY, group, 0], targets[link])
            elif name[0] in "rR":
                group, part_of, _ = RELAYS[name[1]]
                span = pl.ds(*PIECE[group, part_of])
                if name[0] == "r":
                    copy = remote(wown.at[rem(y + 2, NY), span], relay.at[span], sem, relay_recv.at[name[1]], targets[link])
                else:
                    dst = piece(0, back[link][0], group, part_of)
                    copy = remote(relay.at[span], dst, sem, wrecv.at[0, 2, group, part_of or 0], targets[link])
            elif name[0] == "W":
                _, dz, dy, group = name
                ndz = (dz - 1) % NZ if link == "z+" else (dz + 1) % NZ
                own = wown.at[y, pl.ds(*PIECE[group, None])]
                copy = remote(own if dz == dy == 0 else piece(dz, dy, group), piece(dz, dy, group), sem, wrecv.at[ndz, dy, group, 0], targets[link])
            else:
                kind, dy, dx = name
                ref = block(kind, dy, dx, part)
                if link == "core":
                    rsem = core_recv.at[0 if kind == "A" else 1, dy * NX + dx]
                else:
                    oy, ox = back[link]
                    rsem = bsem(kind, (dy + oy) % NY, (dx + ox) % NX, part)
                copy = remote(ref, ref, sem, rsem, targets[link])
            copy.start()
            if group is None:
                row_copies.append(copy)
            else:
                weight_copies.append((number, group, part_of))

        def meta_copy(k):
            to = at_offset(k)
            return remote(gates_out.at[place_of(to)], metas.at[me], msend.at[k], mrecv.at[k], to)

        n_rows = OWN * 2 * cap
        stores, chips = [], []

        def put(dy, dx):
            slot = len(stores) % 2
            if stores[1:]:
                for copy in stores[-2]:
                    copy.wait()
            for dc in (0, 1):
                if dy or dx or dc:
                    k = ((-dy) % NY) * (NX * NC) + ((-dx) % NX) * NC + dc
                    wait(metas.at[place(dy, dx, dc)], mrecv.at[k])
            for i, kind in enumerate("AB"):
                wait(block(kind, dy, dx, None, 1), core_recv.at[i, dy * NX + dx])
            chip = rem(y + dy, NY) * NX + rem(x + dx, NX)
            n = 2 * OWN
            which = lax.broadcasted_iota(jnp.int32, (n, tok), 0)
            gate = jnp.zeros((n, tok), F32)
            for i in range(n):
                gate = jnp.where(which == i, jnp.broadcast_to(metas[2 * chip + i // OWN, pl.ds(i % OWN, 1), :], gate.shape), gate)
            member = gate >= 0.0
            key = jnp.where(member, dot(member.astype(F32).astype(BF16), tri[...]), -1.0)
            r = lax.broadcasted_iota(jnp.int32, (n_rows, tok), 0)
            at = rem(r, cap).astype(F32)
            row_of = rem(r // cap, 2) * OWN + r // (2 * cap)
            mine, gates = jnp.full((n_rows, tok), -1.0, F32), jnp.zeros((n_rows, tok), F32)
            for i in range(n):
                mine = jnp.where(row_of == i, jnp.broadcast_to(key[i:i + 1, :], mine.shape), mine)
                gates = jnp.where(row_of == i, jnp.broadcast_to(gate[i:i + 1, :], mine.shape), gates)
            found = at == mine
            pick = [jnp.logical_and(found, row_of // OWN == p).astype(F32) for p in range(2)]
            both = pick[0] + pick[1]
            scale = jnp.sum(both * gates, axis=1, keepdims=True)
            pick = [p.astype(BF16) for p in pick]
            x_rows = dot(pick[0], all_rows[2 * chip, 0:tok, :]) + dot(pick[1], all_rows[2 * chip + 1, 0:tok, :])
            u_rows = dot(pick[0], all_rows[2 * chip, tok:2 * tok, :]) + dot(pick[1], all_rows[2 * chip + 1, tok:2 * tok, :])
            span = pl.ds(pl.multiple_of(chip * 2 * cap, 2 * cap), 2 * cap)
            out = []
            for i, (value, first, stage, far) in enumerate(((x_rows, xb, sx, xr), (u_rows, ub, su, ur), (scale * u_rows, gb, sg, gr), (both, sb, ss, sel))):
                value = value.astype(BF16)
                first[span, :] = value[:2 * cap]
                stage[slot] = value[2 * cap:].reshape(stage.shape[1:])
                out.append(pltpu.make_async_copy(stage.at[slot], far.at[:, span], store_sem.at[slot, i]))
                out[-1].start()
            stores.append(out)
            chips.append(span)

        for name, sends in order:
            if name is None:
                pass
            elif name[0] == "put":
                put(*name[1:])
            elif name[0] == "tile":
                expert_rows(0, chips[name[1] * CHIPS:(name[1] + 1) * CHIPS])
            elif name[0] == "R":
                group, part, _ = RELAYS[name[1]]
                wait(relay.at[pl.ds(*PIECE[group, part])], relay_recv.at[name[1]])
            elif name[0] == "W":
                _, dz, dy, group, part = name
                wait(piece(dz, dy, group, part), wrecv.at[dz, dy, group, part or 0])
            else:
                wait(block(*name), bsem(*name))
            for send in sends:
                issue(*send)
            if name is None:
                wv[z, y] = wown[y]

                @each_other
                def _(k):
                    meta_copy(k).start()

        for out in stores[-2:]:
            for copy in out:
                copy.wait()

        @each_other
        def _(k):
            meta_copy(k).wait_send()

        for copy in row_copies:
            copy.wait_send()

    def reduce(G, r4, r3, r2, r1):
        for dz in (1, NZ - 1):
            pl.semaphore_signal(in_scope, device_id=z_at(dz), device_id_type=pl.DeviceIdType.MESH)

        def row_loads(e):
            pairs = ((xr, xb), (gr, gb), (ur, ub), (sel, sb))
            return [pltpu.make_async_copy(src.at[e - 1], dst, lsem.at[i]) for i, (src, dst) in enumerate(pairs)]

        def chunk(e, way, dist):
            return G.at[e, z_at(dist if way else NZ - dist)["z"]]

        def hop(e, way, kind):
            h = way
            src, dst = {
                FAR: lambda: (chunk(e, way, 4).at[h], r4.at[way, e]),
                SUM3: lambda: (r4.at[way, e], r3.at[way, e, h]),
                NEW3: lambda: (chunk(e, way, 3).at[1 - h], r3.at[way, e, 1 - h]),
                TWO: lambda: (r3.at[way, e], r2.at[way, e]),
            }.get(kind, lambda: (r2.at[way, e, :, kind - ONE], r1.at[way, e, :, kind - ONE]))()
            return remote(src, dst, rsend.at[way, e, kind], rrecv.at[way, e, kind], z_at(1 if way else NZ - 1))

        def add_into(dst, *others):
            parts = dst.shape[:-2]

            def flat(ref, i):
                index = []
                for n in reversed(parts):
                    index.append(rem(i, n))
                    i = i // n
                return ref.at[tuple(reversed(index))]

            n = 1
            for p in parts:
                n *= p

            @pl.loop(0, n)
            def _(i):
                total = flat(dst, i)[...]
                for other in others:
                    total = total + flat(other, i)[...]
                flat(dst, i)[...] = total

        def own_rows(s):
            return pl.ds(pl.multiple_of(s * cap, 8), cap)

        def dx_copy(e, k):
            to = at_offset(k)
            return remote(dxs.at[e, own_rows(place_of(to))], dxb.at[me, own_rows(e)], dsend.at[e], drecv.at[e], to)

        tile = 256 if rows % 256 == 0 else rows
        dtile = hidden // NZ
        half = dtile // 2

        def weight_gradients(e):
            out = pltpu.make_async_copy(dx_s, dxs.at[e], osem.at[0])
            out.start()

            @pl.loop(0, NZ // 2)
            def _(i):
                pair = [z_at(n + 2 * i)["z"] for n in (3, 4)]

                def cols(ref):
                    return jnp.concatenate([ref[:, pl.ds(pl.multiple_of(k * dtile, dtile), dtile)] for k in pair], axis=1)

                x_cols, g_cols = cols(xb), cols(gb)
                for m, part in enumerate((dot_tn(x_cols, d1_s[...]), dot_tn(x_cols, d3_s[...]), dot_tn(g_cols, a_s[...]))):
                    for j in range(4):
                        G[e, pair[j // 2], j % 2, m] = part[j * half:(j + 1) * half]

                @pl.when(i == 0)
                def _():
                    if isinstance(e, int):
                        pl.semaphore_wait(in_scope, 2)
                    for way, kind in ((0, FAR), (1, FAR), (1, NEW3)):
                        hop(e, way, kind).start()

                @pl.when(i == 1)
                def _():
                    hop(e, 0, NEW3).start()

            val = sb[...].astype(F32) * y_s[...]
            val_s[e] = jnp.sum(val.reshape(rows // cap, cap, tok), axis=1)
            out.wait()

        def send_back(e):
            pltpu.make_async_copy(dxs.at[e, own_rows(me)], dxb.at[me, own_rows(e)], drecv.at[e]).start()

            @each_other
            def _(k):
                dx_copy(e, k).start()

        weight_gradients(0)
        for copy in row_loads(1):
            copy.start()
        send_back(0)

        @pl.loop(1, OWN)
        def _(e):
            for copy in row_loads(e):
                copy.wait()

            @pl.loop(0, rows // tile)
            def _(i):
                expert_rows(e, [pl.ds(pl.multiple_of(i * tile, tile), tile)])

            weight_gradients(e)

            @pl.when(e < OWN - 1)
            def _():
                for copy in row_loads(e + 1):
                    copy.start()

            send_back(e)

        def val_copy(k):
            to = at_offset(k)
            return remote(val_s.at[:, place_of(to)], valb.at[:, me], vsem.at[0, k], vsem.at[1, k], to)

        own_val = pltpu.make_async_copy(val_s.at[:, me], valb.at[:, me], vsem.at[0, 0])
        own_val.start()

        @each_other
        def _(k):
            val_copy(k).start()

        def step(arrived, dist, leaves):
            @pl.loop(0, OWN)
            def _(e):
                for way in (0, 1):
                    for kind in arrived:
                        hop(e, way, kind).wait_recv()
                    mine = chunk(e, way, dist)
                    if leaves == SUM3:
                        add_into(r4.at[way, e], mine.at[way])
                    elif leaves == TWO:
                        add_into(r3.at[way, e], mine)
                    if leaves < ONE:
                        hop(e, way, leaves).start()
                if leaves == ONE:
                    for m in range(3):
                        for way in (0, 1):
                            add_into(r2.at[way, e, :, m], chunk(e, way, dist).at[:, m])
                            hop(e, way, ONE + m).start()

        step((FAR,), 3, SUM3)
        step((SUM3, NEW3), 2, TWO)

        group, places = dxb.shape[:2]
        ids = ids_ref[...].astype(F32)
        r = lax.broadcasted_iota(jnp.int32, (group * 8, tok), 0)
        e_of = rem(r, 8)
        expert = jnp.where(e_of < OWN, first_expert(r // 8) + e_of, -1).astype(F32)
        member = jnp.zeros((group * 8, tok), F32)
        for j in range(ids.shape[0]):
            member = member + (jnp.broadcast_to(ids[j:j + 1, :], member.shape) == expert).astype(F32)
        before = dot(member.astype(BF16), strict_upper(tok))
        key_s[...] = jnp.where(member > 0.0, before, -1.0).reshape(key_s.shape)
        rr = lax.broadcasted_iota(jnp.int32, (places, tok), 0)
        at, e_row = rem(rr, cap).astype(F32), rr // cap
        some = rows // places

        @pl.loop(0, OWN)
        def _(e):
            got = dxb.at[:, own_rows(e)]
            pltpu.make_async_copy(got, got, drecv.at[e]).wait()

        own_val.wait()

        @each_other
        def _(k):
            val_copy(k).wait()

        bufs = (xb, gb)
        loads = [pltpu.make_async_copy(dxb.at[pl.ds(i * some, some)], bufs[i % 2].reshape(some, places, hidden), lsem.at[i % 2]) for i in range(group // some)]
        vals = pltpu.make_async_copy(valb, vb, lsem.at[2])
        vals.start()
        loads[0].start()
        for i, load in enumerate(loads):
            for later in loads[i + 1:i + 2]:
                later.start()

            @pl.loop(0, some)
            def _(k):
                key = key_s[i * some + k]
                mine = jnp.full((places, tok), -1.0, F32)
                for e in range(OWN):
                    mine = jnp.where(e_row == e, jnp.broadcast_to(key[e:e + 1, :], (places, tok)), mine)
                sb[pl.ds(pl.multiple_of(k * places, places), places), :] = (at == mine).astype(F32).astype(BF16)

            load.wait()
            part = dot_tn(sb[...], bufs[i % 2][...])
            acc_s[...] = acc_s[...] + part if i else part

        in_grad_ref[...] = acc_s[...].astype(BF16)
        vals.wait()

        def gate_step(k, total):
            for e in range(OWN):
                row = vb[e, pl.ds(k, 1), :]
                total = total + jnp.where(ids == (first_expert(k) + e).astype(F32), jnp.broadcast_to(row, ids.shape), 0.0)
            return total

        gate_ref[...] = lax.fori_loop(0, group, gate_step, jnp.zeros(ids.shape, F32))

        step((TWO,), 1, ONE)

        def keep(e, m, dy):
            to = rem(y + dy, NY)
            src = r1.at[0, e, to // 2, m, pl.ds(pl.multiple_of(rem(to, 2) * d_loc, 8), d_loc)]
            dst = grads.at[m, y * OWN + e]
            if dy == 0:
                return pltpu.make_async_copy(src, dst, ysend.at[e, m, dy])
            return remote(src, dst, ysend.at[e, m, dy], yrecv.at[e, m, (-dy) % NY], {"y": to})

        @pl.loop(0, OWN)
        def _(e):
            for m in range(3):
                for way in (0, 1):
                    hop(e, way, ONE + m).wait_recv()
                add_into(r1.at[0, e, :, m], r1.at[1, e, :, m], G.at[e, z, :, m])
                for dy in range(NY):
                    keep(e, m, dy).start()

        @pl.loop(0, OWN)
        def _(e):
            for m in range(3):
                keep(e, m, 0).wait()
                for dy in range(1, NY):
                    wait(grads.at[m, rem(y + dy, NY) * OWN + e], yrecv.at[e, m, dy])
                    keep(e, m, dy).wait_send()
            for way in (0, 1):
                for kind in range(HOPS):
                    hop(e, way, kind).wait_send()

            sent = dxs.at[e, pl.ds(0, (GROUP - 1) * cap)]
            pltpu.make_async_copy(sent, sent, dsend.at[e]).wait()

    weight_copies = []
    pl.run_scoped(gather, *scope_one)
    pl.run_scoped(reduce, *scope_two)
    for number, group, part in weight_copies:
        ref = wown.at[0, pl.ds(*PIECE[group, part])]
        remote(ref, ref, send_sem.at[number], relay_recv.at[0], targets["core"]).wait_send()


def layer(cap, x, u, ids, gates, w1, w3, w2):
    tok, hidden = x.shape
    local_experts, d_loc, ff = w1.shape
    rows = GROUP * cap
    half = hidden // NZ // 2
    cut = tok - tok // 8 if tok % 256 == 0 else tok
    order = gather_order(4 * tok * hidden, cut / (2 * tok), 2 * w1.size * 3 // local_experts)
    sends = sum(len(s) for _, s in order)
    dma, v, shape = pltpu.SemaphoreType.DMA, pltpu.VMEM, jax.ShapeDtypeStruct
    far = lambda lanes: shape((OWN - 1, rows, lanes), BF16)
    near = lambda lanes: v((rows, lanes), BF16)
    stage = lambda lanes: v((2, OWN - 1, 2 * cap, lanes), BF16)
    sums = [v((2, OWN, 2, 3, half, ff), F32)] * 3
    scope_one = [v((GROUP, 2 * tok, hidden), BF16), v((tok, tok), BF16), stage(hidden), stage(hidden), stage(hidden), stage(tok)]
    scope_two = [v((OWN, NZ, 2, 3, half, ff), F32), v((2, OWN, 3, half, ff), F32)] + sums
    per_expert = v((OWN, GROUP, tok), F32)
    gate_rows = v((GROUP, OWN, tok), F32)
    outs = pl.pallas_call(
        functools.partial(layer_kernel, order, cap, cut, scope_one, scope_two),
        name="layer",
        out_shape=(
            shape((3, local_experts, d_loc, ff), F32), shape((tok, hidden), BF16), shape(ids.shape, F32),
            shape((GROUP, OWN * cap, hidden), BF16), shape((OWN, GROUP, tok), F32), shape((OWN, rows, hidden), BF16),
            far(hidden), far(hidden), far(hidden), far(tok),
        ),
        in_specs=[ANY, ANY, VMEM, VMEM, ANY, ANY, ANY],
        out_specs=(ANY, VMEM, VMEM) + (ANY,) * 7,
        scratch_shapes=[
            gate_rows, gate_rows, v((NY, OWN, 3, d_loc, ff), BF16), v((NZ, NY, OWN, 3, d_loc, ff), BF16), v((OWN, 3, d_loc, ff), BF16),
            near(hidden), near(hidden), near(hidden), near(tok), near(ff), near(ff), near(ff), v((rows, 1), F32),
            near(hidden), per_expert, per_expert, v((GROUP, 8, tok), F32), v((tok, hidden), F32),
            dma((2, NY * NX, 2)), dma((2, NY * NX)), dma((NZ, NY, 2, 2)), dma((len(RELAYS),)), dma((GROUP,)), dma((sends,)), dma((GROUP,)),
            dma((5,)), dma((2, 4)),
            dma((4,)), dma((2, OWN, HOPS)), dma((2, OWN, HOPS)), dma((OWN, 3, NY)), dma((OWN, 3, NY)),
            dma((OWN,)), dma((OWN,)), dma((2, GROUP)), dma((1,)), pltpu.SemaphoreType.REGULAR,
        ],
        compiler_params=params(0),
    )(x, u, ids, gates, w1, w3, w2)
    return outs[:3]


def finish_kernel(grads, in_grad, gate, *refs):
    n = 5
    outs, bufs, sems = refs[:n], refs[n:2 * n], refs[-1]
    ins = [grads.at[m] for m in range(3)] + [in_grad, gate]
    load = [pltpu.make_async_copy(a, b, sems.at[0, i]) for i, (a, b) in enumerate(zip(ins, bufs))]
    store = [pltpu.make_async_copy(b, o, sems.at[1, i]) for i, (b, o) in enumerate(zip(bufs, outs))]
    for copy in load:
        copy.start()
    for i in range(n):
        load[i].wait()
        store[i].start()
    for copy in store:
        copy.wait()


def finish(grads, in_grad, gate):
    shapes = [grads.shape[1:]] * 3 + [in_grad.shape, gate.shape]
    types = [grads.dtype] * 3 + [in_grad.dtype, gate.dtype]
    return pl.pallas_call(
        finish_kernel,
        name="finish",
        out_shape=[jax.ShapeDtypeStruct(s, t) for s, t in zip(shapes, types)],
        in_specs=[ANY] * 3,
        out_specs=[ANY] * len(shapes),
        scratch_shapes=[pltpu.VMEM(s, t) for s, t in zip(shapes, types)] + [pltpu.SemaphoreType.DMA((2, len(shapes)))],
    )(grads, in_grad, gate)


def solution(mesh):
    mesh4 = Mesh(mesh.devices.reshape(NZ, NY, NX, NC), ("z", "y", "x", "core"))
    tok_spec = P(("z", "y", "x", "core"), None)
    up_spec = P(("x", "core"), ("z", "y"), None)
    down_spec = P(("x", "core"), None, ("z", "y"))

    def per_device(layer_in, out_grad, expert_ids, gate_vals, w_one, w_two, w_three):
        tok_dev, hidden = layer_in.shape
        top_k = expert_ids.shape[1]
        local_experts, d_loc, ff = w_one.shape
        cap = capacity_of(tok_dev, top_k, local_experts * NX * NC)
        ids = expert_ids.T
        grads, in_grad, gate_out = layer(cap, layer_in, out_grad, ids, gate_vals.T, w_one, w_three, w_two.swapaxes(1, 2))
        g1, g3, g2, in_grad, gate_out = finish(grads, in_grad, gate_out)
        return in_grad, gate_out.T, g1, g2.swapaxes(1, 2), g3

    return jax.shard_map(per_device, mesh=mesh4, in_specs=(tok_spec, tok_spec, tok_spec, tok_spec, up_spec, down_spec, up_spec), out_specs=(tok_spec, tok_spec, up_spec, down_spec, up_spec), check_vma=False)
```

```python
import functools

import jax
import jax.numpy as jnp
from jax import lax
from jax.experimental import pallas as pl
from jax.experimental.pallas import tpu as pltpu
from jax.sharding import Mesh, PartitionSpec as P

NZ, NY, NX, NC = 8, 4, 4, 2
GROUP = NY * NX * NC
PLANE = ("y", "x", "core")
OWN = 4
F32, BF16 = jnp.float32, jnp.bfloat16
ANY = pl.BlockSpec(memory_space=pl.ANY)
VMEM = pl.BlockSpec(memory_space=pltpu.VMEM)


def capacity_of(tok_dev, top_k, experts):
    return max(8, ((tok_dev * top_k * 5) // (4 * experts) + 7) // 8 * 8)


def rem(a, b):
    return a % b if isinstance(a, int) else lax.rem(a, b)


def contract(ca, cb):
    return lambda a, b: lax.dot_general(a, b, (((ca,), (cb,)), ((), ())), preferred_element_type=F32)


dot, dot_nt, dot_tn = contract(1, 0), contract(1, 1), contract(0, 0)


def params(number):
    return pltpu.CompilerParams(collective_id=number, has_side_effects=True, vmem_limit_bytes=67043328)


def each_other(body):
    return pl.loop(1, GROUP)(body)


def strict_upper(n):
    rows = lax.broadcasted_iota(jnp.int32, (n, n), 0)
    cols = lax.broadcasted_iota(jnp.int32, (n, n), 1)
    return (rows < cols).astype(F32).astype(BF16)


def here():
    return tuple(lax.axis_index(a) for a in ("z", "y", "x", "core"))


def at_offset(k):
    _, y, x, c = here()
    dy, dx, dc = k // (NX * NC), rem(k // NC, NX), rem(k, NC)
    return {"y": rem(y + dy, NY), "x": rem(x + dx, NX), "core": rem(c + dc, NC)}


def place_of(d):
    return d["y"] * (NX * NC) + d["x"] * NC + d["core"]


def z_at(dz):
    return {"z": rem(lax.axis_index("z") + dz, NZ)}


def remote(src, dst, send_sem, recv_sem, target):
    return pltpu.make_async_remote_copy(src_ref=src, dst_ref=dst, send_sem=send_sem, recv_sem=recv_sem, device_id=target, device_id_type=pl.DeviceIdType.MESH)


def start(copy):
    copy.start()


def enter():
    barrier = pltpu.get_barrier_semaphore()

    @each_other
    def _(k):
        pl.semaphore_signal(barrier, device_id=at_offset(k), device_id_type=pl.DeviceIdType.MESH)

    for dz in (1, NZ - 1):
        pl.semaphore_signal(barrier, device_id=z_at(dz), device_id_type=pl.DeviceIdType.MESH)
    return lambda: pl.semaphore_wait(barrier, GROUP + 1)


RATE, D2D, HOP = 46600.0, 400000.0, 2.3
PUT, TILE, ROWS = 1.0, 1.0, 0.4
STEP = 5
AHEAD = 5.0

PIECE = {(0, None): (0, 1), (1, None): (1, 3), (1, 0): (1, 1), (1, 1): (2, 2)}
RELAYS = ((0, None, "y+"), (1, 0, "y+"), (1, 1, "y-"))


def gather_order(rows_bytes, cut, expert_bytes):
    size = {"A": rows_bytes * cut, "B": rows_bytes * (1.0 - cut)}
    free, pending, coming, order, have, ready = {}, {}, [], [], {}, {}

    def send(now, name, part, link, arrives, nbytes):
        t = max(now, free.get(link, 0.0)) + nbytes / (D2D if link == "core" else RATE)
        free[link] = t
        coming.append((t + HOP, len(order), len(coming), arrives))
        return (name, part, link)

    def later(rank, name, part, link, arrives, nbytes):
        queue = pending.setdefault(link, [])
        queue.append((rank, len(order), len(queue), (name, part, link, arrives, nbytes)))

    def turn(now):
        out = []
        for link, queue in pending.items():
            queue.sort()
            while queue and free.get(link, 0.0) - now < AHEAD:
                out.append(send(now, *queue.pop(0)[-1]))
        return out

    def on_rows(kind, dy, dx):
        first, second = "xy" if kind == "A" else "yx"
        d = {"x": dx, "y": dy}

        def go(axis, sign, part):
            nd = dict(d)
            nd[axis] = (d[axis] - sign) % 4
            rank = 4 + (axis == second) + (part is not None)
            later(rank, (kind, dy, dx), part, axis + "-+"[sign > 0], (kind, nd["y"], nd["x"], part), size[kind] / (1 if part is None else 2))

        for axis in [first, second] if d[second] == 0 else [second]:
            if d[axis] == 3:
                go(axis, 1, 0)
            elif d[axis] == 1:
                go(axis, -1, 1)
            elif d[axis] == 0:
                go(axis, 1, None)
                go(axis, -1, None)

    def core(now, key, part):
        return send(now, key, part, "core", ("core",) + key + (part,), size[key[0]] / (1 if part is None else 2))

    def weights(rank, name, group, part, link, arrives):
        later(rank, name, part, link, arrives + (group, part), PIECE[group, part][1] * expert_bytes)

    def on_piece(dz, dy, group):
        for link, step, far in (("z+", -1, dy < 2), ("z-", 1, dy >= 2)):
            gone = (step * dz) % NZ
            if gone < 3 + far:
                weights(4 * group + gone, ("W", dz, dy, group), group, None, link, ("W", (dz + step) % NZ, dy))

    def arrived(key, part):
        have[key] = have.get(key, 0) + (2 if part is None else 1)
        if have[key] == 2:
            ready[key] = True
        return have[key] == 2

    for i, (group, part, link) in enumerate(RELAYS):
        weights(0, ("r", i), group, part, link, ("R", i))
    for group in range(2):
        for dy, link in ((1, "y+"), (3, "y-")):
            weights(2, ("w", dy, group), group, None, link, ("W", 0, (-dy) % NY))
        on_piece(0, 0, group)
    sends = []
    for kind in "BA":
        arrived((kind, 0, 0), None)
        on_rows(kind, 0, 0)
        sends.append(core(0.0, (kind, 0, 0), None))
    order.append((None, turn(0.0) + sends))
    todo, puts, done, now = [(dy, dx) for dy in range(NY) for dx in range(NX)], 0, 0, 0.0
    while coming or todo or done < puts:
        coming.sort()
        soon = coming[0][0] if coming else 1e9
        if soon > now:
            place = next((p for p in todo if all(pre + (kind,) + p in ready for kind in "AB" for pre in ((), ("core",)))), None)
            if place is not None:
                todo.remove(place)
                order.append((("put",) + place, turn(now)))
                puts += 1
                now += PUT
                continue
            step = min(STEP, puts - done)
            weights_in = sum(key[0] == "W" and key[-1] == 0 for key in ready) == NZ * NY - 1
            if weights_in and (step >= 3 and soon - now > TILE or not todo):
                order.append((("tile", done, done + step), turn(now)))
                done += step
                now += TILE + ROWS * step
                continue
        t, _, _, name = coming.pop(0)
        now = max(now, t)
        key, part = name[:-1], name[-1]
        if name[0] == "core":
            arrived(key, part)
            continue
        sends = []
        if name[0] == "R":
            i, group, part = name[1:]
            weights(1, name[:2], group, part, RELAYS[i][2], ("W", 0, 2))
            name = name[:2]
        elif name[0] == "W":
            if arrived(key, part):
                on_piece(*key[1:])
        else:
            sends = [core(now, key, part)]
            if arrived(key, part):
                on_rows(*key)
        order.append((name, sends + turn(now)))
    return order


def first_expert(d):
    return rem(d, NX * NC) * (NY * OWN) + d // (NX * NC) * OWN


FAR, SUM3, NEW3, TWO, ONE, HOPS = 0, 1, 2, 3, 4, 10


def layer_kernel(order, cap, cut, scope_one, scope_two, x_hbm, u_hbm, ids_ref, gates_ref, w1_hbm, w3_hbm, w2_hbm,
                 grads, in_grad_ref, gate_ref, dxb, valb, dxs, xr, ur, gr, sel,
                 metas, gates_out, wown, wv, relay, xb, ub, gb, sb, a_s, d1_s, d3_s, y_s, dx_s, val_s, vb, key_s, acc_s,
                 recv, core_recv, wrecv, relay_recv, mrecv, send_sem, msend, load_sem, store_sem,
                 lsem, rsend, rrecv, ysend, yrecv, dsend, drecv, vsem, osem, in_scope):
    z, y, x, c = here()
    tok, hidden = x_hbm.shape
    rows, ff = xb.shape[0], a_s.shape[-1]
    d_loc = hidden // (NZ * NY)
    me = place_of(at_offset(0))

    def place(dy, dx, dc=0):
        return place_of(at_offset(dy * (NX * NC) + dx * NC + dc))

    targets = {"core": {"core": 1 - c}}
    for sign, n in (("+", 1), ("-", -1)):
        targets["x" + sign] = {"x": rem(x + n + NX, NX)}
        targets["y" + sign] = {"y": rem(y + n + NY, NY)}
        targets["z" + sign] = z_at(n + NZ)

    def wait(ref, sem):
        remote(ref, ref, send_sem.at[0], sem, targets["core"]).wait_recv()

    def w(e, m):
        return wv[:, :, e, m].reshape(hidden, ff)

    def expert_rows(e, spans):
        def cut_of(ref):
            return jnp.concatenate([ref[s, :] for s in spans]) if spans[1:] else ref[spans[0], :]

        def save(ref, value):
            n = value.shape[0] // len(spans)
            for i, s in enumerate(spans):
                ref[s, :] = value[i * n:(i + 1) * n]

        x_rows = cut_of(xb)
        h1, h3 = dot(x_rows, w(e, 0)), dot(x_rows, w(e, 1))
        sig = jax.nn.sigmoid(h1)
        silu = h1 * sig
        act = (silu * h3).astype(BF16)
        save(a_s, act)
        y_rows = dot_nt(act, w(e, 2))
        save(y_s, jnp.sum(cut_of(ub).astype(F32) * y_rows, axis=1, keepdims=True))
        da = dot(cut_of(gb), w(e, 2))
        d1 = (da * h3 * sig * (1.0 + h1 * (1.0 - sig))).astype(BF16)
        d3 = (da * silu).astype(BF16)
        save(d1_s, d1)
        save(d3_s, d3)
        save(dx_s, (dot_nt(d1, w(e, 0)) + dot_nt(d3, w(e, 1))).astype(BF16))

    def gather(all_rows, tri, sx, su, sg, ss):
        loads = [
            pltpu.make_async_copy(x_hbm, all_rows.at[me, pl.ds(0, tok)], load_sem.at[0]),
            pltpu.make_async_copy(u_hbm, all_rows.at[me, pl.ds(tok, tok)], load_sem.at[1]),
        ]
        for m, ref in enumerate((w1_hbm, w3_hbm, w2_hbm)):
            loads.append(pltpu.make_async_copy(ref.reshape(NY, OWN, d_loc, ff), wown.at[:, :, m], load_sem.at[2 + m]))
        for copy in loads:
            copy.start()
        all_in = enter()

        @pl.loop(0, GROUP)
        def _(d):
            number = first_expert(d) + lax.broadcasted_iota(jnp.int32, (OWN, tok), 0)
            value = jnp.full((OWN, tok), -1.0, F32)
            for j in range(ids_ref.shape[0]):
                chosen = ids_ref[pl.ds(j, 1), :] == number
                value = jnp.where(chosen, jnp.broadcast_to(gates_ref[pl.ds(j, 1), :], value.shape), value)
            gates_out[d] = value

        metas[me] = gates_out[me]
        tri[...] = strict_upper(tok)
        for copy in loads:
            copy.wait()
        all_in()

        back = {"x+": (0, 3), "x-": (0, 1), "y+": (3, 0), "y-": (1, 0)}
        spans = {"A": (0, cut), "B": (cut, 2 * tok - cut)}

        def block(kind, dy, dx, part=None, dc=0):
            start, size = spans[kind]
            if part is not None:
                size //= 2
                start += part * size
            return all_rows.at[place(dy, dx, dc), pl.ds(start, size)]

        def bsem(kind, dy, dx, part):
            return recv.at[0 if kind == "A" else 1, dy * NX + dx, part or 0]

        def piece(dz, dy, group, part=None):
            return wv.at[z_at(dz)["z"], rem(y + dy, NY), pl.ds(*PIECE[group, part])]

        row_copies = []

        def issue(name, part, link):
            number = len(row_copies) + len(weight_copies)
            sem = send_sem.at[number]
            group, part_of = None, None
            if name[0] == "w":
                _, dy, group = name
                src = wown.at[rem(y + dy, NY), pl.ds(*PIECE[group, None])]
                copy = remote(src, piece(0, 0, group), sem, wrecv.at[0, (-dy) % NY, group, 0], targets[link])
            elif name[0] in "rR":
                group, part_of, _ = RELAYS[name[1]]
                span = pl.ds(*PIECE[group, part_of])
                if name[0] == "r":
                    copy = remote(wown.at[rem(y + 2, NY), span], relay.at[span], sem, relay_recv.at[name[1]], targets[link])
                else:
                    dst = piece(0, back[link][0], group, part_of)
                    copy = remote(relay.at[span], dst, sem, wrecv.at[0, 2, group, part_of or 0], targets[link])
            elif name[0] == "W":
                _, dz, dy, group = name
                ndz = (dz - 1) % NZ if link == "z+" else (dz + 1) % NZ
                own = wown.at[y, pl.ds(*PIECE[group, None])]
                copy = remote(own if dz == dy == 0 else piece(dz, dy, group), piece(dz, dy, group), sem, wrecv.at[ndz, dy, group, 0], targets[link])
            else:
                kind, dy, dx = name
                ref = block(kind, dy, dx, part)
                if link == "core":
                    rsem = core_recv.at[0 if kind == "A" else 1, dy * NX + dx, part or 0]
                else:
                    oy, ox = back[link]
                    rsem = bsem(kind, (dy + oy) % NY, (dx + ox) % NX, part)
                copy = remote(ref, ref, sem, rsem, targets[link])
            copy.start()
            if group is None:
                row_copies.append(copy)
            else:
                weight_copies.append((number, group, part_of))

        def meta_copy(k):
            to = at_offset(k)
            return remote(gates_out.at[place_of(to)], metas.at[me], msend.at[k], mrecv.at[k], to)

        n_rows = OWN * 2 * cap
        stores, chips = [], []

        def put(dy, dx):
            slot = len(stores) % 2
            if stores[1:]:
                for copy in stores[-2]:
                    copy.wait()
            for dc in (0, 1):
                if dy or dx or dc:
                    k = ((-dy) % NY) * (NX * NC) + ((-dx) % NX) * NC + dc
                    wait(metas.at[place(dy, dx, dc)], mrecv.at[k])
            for i, (kind, last) in enumerate((("A", dx if dy == 0 else dy), ("B", dy if dx == 0 else dx))):
                for part in (0, 1) if last == 2 else (None,):
                    wait(block(kind, dy, dx, part, 1), core_recv.at[i, dy * NX + dx, part or 0])
            chip = rem(y + dy, NY) * NX + rem(x + dx, NX)
            n = 2 * OWN
            which = lax.broadcasted_iota(jnp.int32, (n, tok), 0)
            gate = jnp.zeros((n, tok), F32)
            for i in range(n):
                gate = jnp.where(which == i, jnp.broadcast_to(metas[2 * chip + i // OWN, pl.ds(i % OWN, 1), :], gate.shape), gate)
            member = gate >= 0.0
            key = jnp.where(member, dot(member.astype(F32).astype(BF16), tri[...]), -1.0)
            r = lax.broadcasted_iota(jnp.int32, (n_rows, tok), 0)
            at = rem(r, cap).astype(F32)
            row_of = rem(r // cap, 2) * OWN + r // (2 * cap)
            mine, gates = jnp.full((n_rows, tok), -1.0, F32), jnp.zeros((n_rows, tok), F32)
            for i in range(n):
                mine = jnp.where(row_of == i, jnp.broadcast_to(key[i:i + 1, :], mine.shape), mine)
                gates = jnp.where(row_of == i, jnp.broadcast_to(gate[i:i + 1, :], mine.shape), gates)
            found = at == mine
            pick = [jnp.logical_and(found, row_of // OWN == p).astype(F32) for p in range(2)]
            both = pick[0] + pick[1]
            scale = jnp.sum(both * gates, axis=1, keepdims=True)
            pick = [p.astype(BF16) for p in pick]
            x_rows = dot(pick[0], all_rows[2 * chip, 0:tok, :]) + dot(pick[1], all_rows[2 * chip + 1, 0:tok, :])
            u_rows = dot(pick[0], all_rows[2 * chip, tok:2 * tok, :]) + dot(pick[1], all_rows[2 * chip + 1, tok:2 * tok, :])
            span = pl.ds(pl.multiple_of(chip * 2 * cap, 2 * cap), 2 * cap)
            out = []
            for i, (value, first, stage, far) in enumerate(((x_rows, xb, sx, xr), (u_rows, ub, su, ur), (scale * u_rows, gb, sg, gr), (both, sb, ss, sel))):
                value = value.astype(BF16)
                first[span, :] = value[:2 * cap]
                stage[slot] = value[2 * cap:].reshape(stage.shape[1:])
                out.append(pltpu.make_async_copy(stage.at[slot], far.at[:, span], store_sem.at[slot, i]))
                out[-1].start()
            stores.append(out)
            chips.append(span)

        for name, sends in order:
            if name is None:
                pass
            elif name[0] == "put":
                put(*name[1:])
            elif name[0] == "tile":
                expert_rows(0, chips[name[1]:name[2]])
            elif name[0] == "R":
                group, part, _ = RELAYS[name[1]]
                wait(relay.at[pl.ds(*PIECE[group, part])], relay_recv.at[name[1]])
            elif name[0] == "W":
                _, dz, dy, group, part = name
                wait(piece(dz, dy, group, part), wrecv.at[dz, dy, group, part or 0])
            else:
                wait(block(*name), bsem(*name))
            for send in sends:
                issue(*send)
            if name is None:
                wv[z, y] = wown[y]

                @each_other
                def _(k):
                    meta_copy(k).start()

        for out in stores[-2:]:
            for copy in out:
                copy.wait()

        @each_other
        def _(k):
            meta_copy(k).wait_send()

        for copy in row_copies:
            copy.wait_send()

    def reduce(G, r4, r3, r2, r1):
        for dz in (1, NZ - 1):
            pl.semaphore_signal(in_scope, device_id=z_at(dz), device_id_type=pl.DeviceIdType.MESH)

        def row_loads(e):
            pairs = ((xr, xb), (gr, gb), (ur, ub), (sel, sb))
            return [pltpu.make_async_copy(src.at[e - 1], dst, lsem.at[i]) for i, (src, dst) in enumerate(pairs)]

        def chunk(e, way, dist):
            return G.at[e, z_at(dist if way else NZ - dist)["z"]]

        def half_of(ref, way, e, kind):
            return ref.at[way, e, (kind - ONE) % 2, (kind - ONE) // 2]

        def hop(e, way, kind):
            h = way
            src, dst = {
                FAR: lambda: (chunk(e, way, 4).at[h], r4.at[way, e]),
                SUM3: lambda: (r4.at[way, e], r3.at[way, e, h]),
                NEW3: lambda: (chunk(e, way, 3).at[1 - h], r3.at[way, e, 1 - h]),
                TWO: lambda: (r3.at[way, e], r2.at[way, e]),
            }.get(kind, lambda: (half_of(r2, way, e, kind), half_of(r1, way, e, kind)))()
            return remote(src, dst, rsend.at[way, e, kind], rrecv.at[way, e, kind], z_at(1 if way else NZ - 1))

        def add_into(dst, *others):
            parts = dst.shape[:-2]
            if not parts:
                total = dst[...]
                for other in others:
                    total = total + other[...]
                dst[...] = total
                return

            def flat(ref, i):
                index = []
                for n in reversed(parts):
                    index.append(rem(i, n))
                    i = i // n
                return ref.at[tuple(reversed(index))]

            n = 1
            for p in parts:
                n *= p

            @pl.loop(0, n)
            def _(i):
                total = flat(dst, i)[...]
                for other in others:
                    total = total + flat(other, i)[...]
                flat(dst, i)[...] = total

        def own_rows(s):
            return pl.ds(pl.multiple_of(s * cap, 8), cap)

        def dx_copy(e, k):
            to = at_offset(k)
            return remote(dxs.at[e, own_rows(place_of(to))], dxb.at[me, own_rows(e)], dsend.at[e], drecv.at[e], to)

        tile = 256 if rows % 256 == 0 else rows
        dtile = hidden // NZ
        half = dtile // 2

        def weight_gradients(e):
            out = pltpu.make_async_copy(dx_s, dxs.at[e], osem.at[0])
            out.start()

            @pl.loop(0, NZ // 2)
            def _(i):
                pair = [z_at(n + 2 * i)["z"] for n in (3, 4)]

                def cols(ref):
                    return jnp.concatenate([ref[:, pl.ds(pl.multiple_of(k * dtile, dtile), dtile)] for k in pair], axis=1)

                x_cols, g_cols = cols(xb), cols(gb)
                for m, part in enumerate((dot_tn(x_cols, d1_s[...]), dot_tn(x_cols, d3_s[...]), dot_tn(g_cols, a_s[...]))):
                    for j in range(4):
                        G[e, pair[j // 2], j % 2, m] = part[j * half:(j + 1) * half]

                @pl.when(i == 0)
                def _():
                    if isinstance(e, int):
                        pl.semaphore_wait(in_scope, 2)
                    for way, kind in ((0, FAR), (1, FAR), (1, NEW3)):
                        hop(e, way, kind).start()

                @pl.when(i == 1)
                def _():
                    hop(e, 0, NEW3).start()

            val = sb[...].astype(F32) * y_s[...]
            val_s[e] = jnp.sum(val.reshape(rows // cap, cap, tok), axis=1)
            out.wait()

        def send_back(e):
            pltpu.make_async_copy(dxs.at[e, own_rows(me)], dxb.at[me, own_rows(e)], drecv.at[e]).start()

            @each_other
            def _(k):
                dx_copy(e, k).start()

        weight_gradients(0)
        for copy in row_loads(1):
            copy.start()
        send_back(0)

        @pl.loop(1, OWN)
        def _(e):
            for copy in row_loads(e):
                copy.wait()

            @pl.loop(0, rows // tile)
            def _(i):
                expert_rows(e, [pl.ds(pl.multiple_of(i * tile, tile), tile)])

            weight_gradients(e)

            @pl.when(e < OWN - 1)
            def _():
                for copy in row_loads(e + 1):
                    copy.start()

            send_back(e)

        def val_copy(k):
            to = at_offset(k)
            return remote(val_s.at[:, place_of(to)], valb.at[:, me], vsem.at[0, k], vsem.at[1, k], to)

        own_val = pltpu.make_async_copy(val_s.at[:, me], valb.at[:, me], vsem.at[0, 0])
        own_val.start()

        @each_other
        def _(k):
            val_copy(k).start()

        def step(arrived, dist, leaves):
            @pl.loop(0, OWN)
            def _(e):
                for way in (0, 1):
                    for kind in arrived:
                        hop(e, way, kind).wait_recv()
                    mine = chunk(e, way, dist)
                    if leaves == SUM3:
                        add_into(r4.at[way, e], mine.at[way])
                    elif leaves == TWO:
                        add_into(r3.at[way, e], mine)
                    if leaves < ONE:
                        hop(e, way, leaves).start()
                if leaves == ONE:
                    for kind in range(ONE, HOPS):
                        for way in (0, 1):
                            add_into(half_of(r2, way, e, kind), half_of(G, e, z_at(dist if way else NZ - dist)["z"], kind))
                            hop(e, way, kind).start()

        step((FAR,), 3, SUM3)
        step((SUM3, NEW3), 2, TWO)

        group, places = dxb.shape[:2]
        ids = ids_ref[...].astype(F32)
        r = lax.broadcasted_iota(jnp.int32, (group * 8, tok), 0)
        e_of = rem(r, 8)
        expert = jnp.where(e_of < OWN, first_expert(r // 8) + e_of, -1).astype(F32)
        member = jnp.zeros((group * 8, tok), F32)
        for j in range(ids.shape[0]):
            member = member + (jnp.broadcast_to(ids[j:j + 1, :], member.shape) == expert).astype(F32)
        before = dot(member.astype(BF16), strict_upper(tok))
        key_s[...] = jnp.where(member > 0.0, before, -1.0).reshape(key_s.shape)
        rr = lax.broadcasted_iota(jnp.int32, (places, tok), 0)
        at, e_row = rem(rr, cap).astype(F32), rr // cap
        some = rows // places

        @pl.loop(0, OWN)
        def _(e):
            got = dxb.at[:, own_rows(e)]
            pltpu.make_async_copy(got, got, drecv.at[e]).wait()

        own_val.wait()

        @each_other
        def _(k):
            val_copy(k).wait()

        bufs = (xb, gb)
        loads = [pltpu.make_async_copy(dxb.at[pl.ds(i * some, some)], bufs[i % 2].reshape(some, places, hidden), lsem.at[i % 2]) for i in range(group // some)]
        vals = pltpu.make_async_copy(valb, vb, lsem.at[2])
        vals.start()
        loads[0].start()
        for i, load in enumerate(loads):
            for later in loads[i + 1:i + 2]:
                later.start()

            @pl.loop(0, some)
            def _(k):
                key = key_s[i * some + k]
                mine = jnp.full((places, tok), -1.0, F32)
                for e in range(OWN):
                    mine = jnp.where(e_row == e, jnp.broadcast_to(key[e:e + 1, :], (places, tok)), mine)
                sb[pl.ds(pl.multiple_of(k * places, places), places), :] = (at == mine).astype(F32).astype(BF16)

            load.wait()
            part = dot_tn(sb[...], bufs[i % 2][...])
            acc_s[...] = acc_s[...] + part if i else part

        in_grad_ref[...] = acc_s[...].astype(BF16)
        vals.wait()

        def gate_step(k, total):
            for e in range(OWN):
                row = vb[e, pl.ds(k, 1), :]
                total = total + jnp.where(ids == (first_expert(k) + e).astype(F32), jnp.broadcast_to(row, ids.shape), 0.0)
            return total

        gate_ref[...] = lax.fori_loop(0, group, gate_step, jnp.zeros(ids.shape, F32))

        step((TWO,), 1, ONE)

        def keep(e, m, to, then_remote, then_local):
            src = r1.at[0, e, to // 2, m, pl.ds(to % 2 * d_loc, d_loc)]
            dst = grads.at[m, y * OWN + e]

            @pl.when(y != to)
            def _():
                then_remote(remote(src, dst, ysend.at[e, m, to], yrecv.at[e, m, y], {"y": to}))

            @pl.when(y == to)
            def _():
                then_local(pltpu.make_async_copy(src, dst, ysend.at[e, m, to]))

        @pl.loop(0, OWN)
        def _(e):
            for kind in range(ONE, HOPS):
                for way in (0, 1):
                    hop(e, way, kind).wait_recv()
                add_into(half_of(r1, 0, e, kind), half_of(r1, 1, e, kind), half_of(G, e, z, kind))
                m, h = (kind - ONE) // 2, (kind - ONE) % 2
                for to in (2 * h, 2 * h + 1):
                    keep(e, m, to, start, start)

        @pl.loop(0, OWN)
        def _(e):
            for m in range(3):
                for at in range(NY):
                    def both(copy):
                        wait(grads.at[m, at * OWN + e], yrecv.at[e, m, at])
                        copy.wait_send()

                    keep(e, m, at, both, lambda copy: copy.wait())
            for way in (0, 1):
                for kind in range(HOPS):
                    hop(e, way, kind).wait_send()

            sent = dxs.at[e, pl.ds(0, (GROUP - 1) * cap)]
            pltpu.make_async_copy(sent, sent, dsend.at[e]).wait()

    weight_copies = []
    pl.run_scoped(gather, *scope_one)
    pl.run_scoped(reduce, *scope_two)
    for number, group, part in weight_copies:
        ref = wown.at[0, pl.ds(*PIECE[group, part])]
        remote(ref, ref, send_sem.at[number], relay_recv.at[0], targets["core"]).wait_send()


def layer(cap, x, u, ids, gates, w1, w3, w2):
    tok, hidden = x.shape
    local_experts, d_loc, ff = w1.shape
    rows = GROUP * cap
    half = hidden // NZ // 2
    cut = tok - tok // 8 if tok % 256 == 0 else tok
    order = gather_order(4 * tok * hidden, cut / (2 * tok), 2 * w1.size * 3 // local_experts)
    sends = sum(len(s) for _, s in order)
    dma, v, shape = pltpu.SemaphoreType.DMA, pltpu.VMEM, jax.ShapeDtypeStruct
    far = lambda lanes: shape((OWN - 1, rows, lanes), BF16)
    near = lambda lanes: v((rows, lanes), BF16)
    stage = lambda lanes: v((2, OWN - 1, 2 * cap, lanes), BF16)
    sums = [v((2, OWN, 2, 3, half, ff), F32)] * 3
    scope_one = [v((GROUP, 2 * tok, hidden), BF16), v((tok, tok), BF16), stage(hidden), stage(hidden), stage(hidden), stage(tok)]
    scope_two = [v((OWN, NZ, 2, 3, half, ff), F32), v((2, OWN, 3, half, ff), F32)] + sums
    per_expert = v((OWN, GROUP, tok), F32)
    gate_rows = v((GROUP, OWN, tok), F32)
    outs = pl.pallas_call(
        functools.partial(layer_kernel, order, cap, cut, scope_one, scope_two),
        name="layer",
        out_shape=(
            shape((3, local_experts, d_loc, ff), F32), shape((tok, hidden), BF16), shape(ids.shape, F32),
            shape((GROUP, OWN * cap, hidden), BF16), shape((OWN, GROUP, tok), F32), shape((OWN, rows, hidden), BF16),
            far(hidden), far(hidden), far(hidden), far(tok),
        ),
        in_specs=[ANY, ANY, VMEM, VMEM, ANY, ANY, ANY],
        out_specs=(ANY, VMEM, VMEM) + (ANY,) * 7,
        scratch_shapes=[
            gate_rows, gate_rows, v((NY, OWN, 3, d_loc, ff), BF16), v((NZ, NY, OWN, 3, d_loc, ff), BF16), v((OWN, 3, d_loc, ff), BF16),
            near(hidden), near(hidden), near(hidden), near(tok), near(ff), near(ff), near(ff), v((rows, 1), F32),
            near(hidden), per_expert, per_expert, v((GROUP, 8, tok), F32), v((tok, hidden), F32),
            dma((2, NY * NX, 2)), dma((2, NY * NX, 2)), dma((NZ, NY, 2, 2)), dma((len(RELAYS),)), dma((GROUP,)), dma((sends,)), dma((GROUP,)),
            dma((5,)), dma((2, 4)),
            dma((4,)), dma((2, OWN, HOPS)), dma((2, OWN, HOPS)), dma((OWN, 3, NY)), dma((OWN, 3, NY)),
            dma((OWN,)), dma((OWN,)), dma((2, GROUP)), dma((1,)), pltpu.SemaphoreType.REGULAR,
        ],
        compiler_params=params(0),
    )(x, u, ids, gates, w1, w3, w2)
    return outs[:3]


def finish_kernel(grads, in_grad, gate, *refs):
    n = 5
    outs, bufs, sems = refs[:n], refs[n:2 * n], refs[-1]
    ins = [grads.at[m] for m in range(3)] + [in_grad, gate]
    load = [pltpu.make_async_copy(a, b, sems.at[0, i]) for i, (a, b) in enumerate(zip(ins, bufs))]
    store = [pltpu.make_async_copy(b, o, sems.at[1, i]) for i, (b, o) in enumerate(zip(bufs, outs))]
    for copy in load:
        copy.start()
    for i in range(n):
        load[i].wait()
        store[i].start()
    for copy in store:
        copy.wait()


def finish(grads, in_grad, gate):
    shapes = [grads.shape[1:]] * 3 + [in_grad.shape, gate.shape]
    types = [grads.dtype] * 3 + [in_grad.dtype, gate.dtype]
    return pl.pallas_call(
        finish_kernel,
        name="finish",
        out_shape=[jax.ShapeDtypeStruct(s, t) for s, t in zip(shapes, types)],
        in_specs=[ANY] * 3,
        out_specs=[ANY] * len(shapes),
        scratch_shapes=[pltpu.VMEM(s, t) for s, t in zip(shapes, types)] + [pltpu.SemaphoreType.DMA((2, len(shapes)))],
    )(grads, in_grad, gate)


def solution(mesh):
    mesh4 = Mesh(mesh.devices.reshape(NZ, NY, NX, NC), ("z", "y", "x", "core"))
    tok_spec = P(("z", "y", "x", "core"), None)
    up_spec = P(("x", "core"), ("z", "y"), None)
    down_spec = P(("x", "core"), None, ("z", "y"))

    def per_device(layer_in, out_grad, expert_ids, gate_vals, w_one, w_two, w_three):
        tok_dev, hidden = layer_in.shape
        top_k = expert_ids.shape[1]
        local_experts, d_loc, ff = w_one.shape
        cap = capacity_of(tok_dev, top_k, local_experts * NX * NC)
        ids = expert_ids.T
        grads, in_grad, gate_out = layer(cap, layer_in, out_grad, ids, gate_vals.T, w_one, w_three, w_two.swapaxes(1, 2))
        g1, g3, g2, in_grad, gate_out = finish(grads, in_grad, gate_out)
        return in_grad, gate_out.T, g1, g2.swapaxes(1, 2), g3

    return jax.shard_map(per_device, mesh=mesh4, in_specs=(tok_spec, tok_spec, tok_spec, tok_spec, up_spec, down_spec, up_spec), out_specs=(tok_spec, tok_spec, up_spec, down_spec, up_spec), check_vma=False)
```

```python
import functools

import jax
import jax.numpy as jnp
from jax import lax
from jax.experimental import pallas as pl
from jax.experimental.pallas import tpu as pltpu
from jax.sharding import Mesh, PartitionSpec as P

NZ, NY, NX, NC = 8, 4, 4, 2
GROUP = NY * NX * NC
PLANE = ("y", "x", "core")
OWN = 4
F32, BF16 = jnp.float32, jnp.bfloat16
ANY = pl.BlockSpec(memory_space=pl.ANY)


def capacity_of(tok_dev, top_k, experts):
    return max(8, ((tok_dev * top_k * 5) // (4 * experts) + 7) // 8 * 8)


def rem(a, b):
    return a % b if isinstance(a, int) else lax.rem(a, b)


def contract(ca, cb):
    return lambda a, b: lax.dot_general(a, b, (((ca,), (cb,)), ((), ())), preferred_element_type=F32)


dot, dot_nt, dot_tn = contract(1, 0), contract(1, 1), contract(0, 0)


def params(number):
    return pltpu.CompilerParams(collective_id=number, has_side_effects=True, vmem_limit_bytes=67043328)


def each_other(body):
    return pl.loop(1, GROUP)(body)


def strict_upper(n):
    rows = lax.broadcasted_iota(jnp.int32, (n, n), 0)
    cols = lax.broadcasted_iota(jnp.int32, (n, n), 1)
    return (rows < cols).astype(F32).astype(BF16)


def here():
    return tuple(lax.axis_index(a) for a in ("z", "y", "x", "core"))


def at_offset(k):
    _, y, x, c = here()
    dy, dx, dc = k // (NX * NC), rem(k // NC, NX), rem(k, NC)
    return {"y": rem(y + dy, NY), "x": rem(x + dx, NX), "core": rem(c + dc, NC)}


def place_of(d):
    return d["y"] * (NX * NC) + d["x"] * NC + d["core"]


def z_at(dz):
    return {"z": rem(lax.axis_index("z") + dz, NZ)}


def remote(src, dst, send_sem, recv_sem, target):
    return pltpu.make_async_remote_copy(src_ref=src, dst_ref=dst, send_sem=send_sem, recv_sem=recv_sem, device_id=target, device_id_type=pl.DeviceIdType.MESH)


def start(copy):
    copy.start()


def enter():
    barrier = pltpu.get_barrier_semaphore()

    @each_other
    def _(k):
        pl.semaphore_signal(barrier, device_id=at_offset(k), device_id_type=pl.DeviceIdType.MESH)

    for dz in (1, NZ - 1):
        pl.semaphore_signal(barrier, device_id=z_at(dz), device_id_type=pl.DeviceIdType.MESH)
    return lambda: pl.semaphore_wait(barrier, GROUP + 1)


RATE, D2D, HOP = 46600.0, 400000.0, 2.3
PUT, TILE, ROWS = 1.0, 1.0, 0.4
STEP = 5
AHEAD, MORE = 5.0, 0.2

PIECE = {(0, None): (0, 1), (1, None): (1, 3), (1, 0): (1, 1), (1, 1): (2, 2)}
RELAYS = ((0, None, "y+"), (1, 0, "y+"), (1, 1, "y-"))


def gather_order(rows_bytes, cut, expert_bytes):
    size = {"A": rows_bytes * cut, "B": rows_bytes * (1.0 - cut)}
    free, pending, coming, order, have, ready = {}, {}, [], [], {}, {}

    def send(now, name, part, link, arrives, nbytes):
        t = max(now, free.get(link, 0.0)) + nbytes / (D2D if link == "core" else RATE)
        free[link] = t
        coming.append((t + HOP, len(order), len(coming), arrives))
        return (name, part, link)

    def later(rank, name, part, link, arrives, nbytes):
        queue = pending.setdefault(link, [])
        queue.append((rank, len(order), len(queue), (name, part, link, arrives, nbytes)))

    def turn(now):
        out = []
        for link, queue in pending.items():
            queue.sort()
            while queue and free.get(link, 0.0) - now < AHEAD + MORE * now:
                out.append(send(now, *queue.pop(0)[-1]))
        return out

    def on_rows(kind, dy, dx):
        first, second = "xy" if kind == "A" else "yx"
        d = {"x": dx, "y": dy}

        def go(axis, sign, part):
            nd = dict(d)
            nd[axis] = (d[axis] - sign) % 4
            rank = 4 + (axis == second) + (part is not None)
            later(rank, (kind, dy, dx), part, axis + "-+"[sign > 0], (kind, nd["y"], nd["x"], part), size[kind] / (1 if part is None else 2))

        for axis in [first, second] if d[second] == 0 else [second]:
            if d[axis] == 3:
                go(axis, 1, 0)
            elif d[axis] == 1:
                go(axis, -1, 1)
            elif d[axis] == 0:
                go(axis, 1, None)
                go(axis, -1, None)

    def core(now, key, part):
        return send(now, key, part, "core", ("core",) + key + (part,), size[key[0]] / (1 if part is None else 2))

    def weights(rank, name, group, part, link, arrives):
        later(rank, name, part, link, arrives + (group, part), PIECE[group, part][1] * expert_bytes)

    def on_piece(dz, dy, group):
        for link, step, far in (("z+", -1, dy < 2), ("z-", 1, dy >= 2)):
            gone = (step * dz) % NZ
            if gone < 3 + far:
                weights(4 * group + gone, ("W", dz, dy, group), group, None, link, ("W", (dz + step) % NZ, dy))

    def arrived(key, part):
        have[key] = have.get(key, 0) + (2 if part is None else 1)
        if have[key] == 2:
            ready[key] = True
        return have[key] == 2

    for i, (group, part, link) in enumerate(RELAYS):
        weights(0, ("r", i), group, part, link, ("R", i))
    for group in range(2):
        for dy, link in ((1, "y+"), (3, "y-")):
            weights(2, ("w", dy, group), group, None, link, ("W", 0, (-dy) % NY))
        on_piece(0, 0, group)
    sends = []
    for kind in "BA":
        arrived((kind, 0, 0), None)
        on_rows(kind, 0, 0)
        sends.append(core(0.0, (kind, 0, 0), None))
    order.append((None, turn(0.0) + sends))
    todo, puts, done, now = [(dy, dx) for dy in range(NY) for dx in range(NX)], 0, 0, 0.0
    while coming or todo or done < puts:
        coming.sort()
        soon = coming[0][0] if coming else 1e9
        if soon > now:
            place = next((p for p in todo if all(pre + (kind,) + p in ready for kind in "AB" for pre in ((), ("core",)))), None)
            if place is not None:
                todo.remove(place)
                order.append((("put",) + place, turn(now)))
                puts += 1
                now += PUT
                continue
            step = min(STEP, puts - done)
            weights_in = sum(key[0] == "W" and key[-1] == 0 for key in ready) == NZ * NY - 1
            if weights_in and (step >= 3 and soon - now > TILE or not todo):
                order.append((("tile", done, done + step), turn(now)))
                done += step
                now += TILE + ROWS * step
                continue
        t, _, _, name = coming.pop(0)
        now = max(now, t)
        key, part = name[:-1], name[-1]
        if name[0] == "core":
            arrived(key, part)
            continue
        sends = []
        if name[0] == "R":
            i, group, part = name[1:]
            weights(1, name[:2], group, part, RELAYS[i][2], ("W", 0, 2))
            name = name[:2]
        elif name[0] == "W":
            if arrived(key, part):
                on_piece(*key[1:])
        else:
            sends = [core(now, key, part)]
            if arrived(key, part):
                on_rows(*key)
        order.append((name, sends + turn(now)))
    return order


def passed_on(dz, dy):
    return dz != NZ // 2 and dz not in ((3,) if dy < 2 else (5,))


def first_expert(d):
    return rem(d, NX * NC) * (NY * OWN) + d // (NX * NC) * OWN


FAR, SUM3, NEW3, TWO, ONE, HOPS = 0, 1, 2, 3, 4, 10


def layer_kernel(order, cap, cut, scope_one, scope_two, x_hbm, u_hbm, ids_hbm, gates_hbm, w1_hbm, w3_hbm, w2_hbm,
                 grads, in_grad_hbm, gate_hbm, dxb, valb, dxs, xr, ur, gr, sel,
                 ids_ref, gates_ref, in_grad_ref, gate_ref, metas, gates_out, wown, wv, relay, xb, ub, gb, sb, a_s, d1_s, d3_s, y_s, dx_s, val_s, vb, key_s, acc_s,
                 recv, core_recv, wrecv, relay_recv, mrecv, send_sem, msend, load_sem, store_sem,
                 lsem, rsend, rrecv, ysend, yrecv, dsend, drecv, vsem, osem, in_scope):
    z, y, x, c = here()
    tok, hidden = x_hbm.shape
    rows, ff = xb.shape[0], a_s.shape[-1]
    d_loc = hidden // (NZ * NY)
    me = place_of(at_offset(0))

    def place(dy, dx, dc=0):
        return place_of(at_offset(dy * (NX * NC) + dx * NC + dc))

    targets = {"core": {"core": 1 - c}}
    for sign, n in (("+", 1), ("-", -1)):
        targets["x" + sign] = {"x": rem(x + n + NX, NX)}
        targets["y" + sign] = {"y": rem(y + n + NY, NY)}
        targets["z" + sign] = z_at(n + NZ)

    def wait(ref, sem):
        remote(ref, ref, send_sem.at[0], sem, targets["core"]).wait_recv()

    def piece(dz, dy, group, part=None):
        return wv.at[z_at(dz)["z"], rem(y + dy, NY), pl.ds(*PIECE[group, part])]

    def wait_weights(dz, dy, group, part):
        wait(piece(dz, dy, group, part), wrecv.at[dz, dy, group, part or 0])

    def w(e, m):
        return wv[:, :, e, m].reshape(hidden, ff)

    def expert_rows(e, spans):
        def cut_of(ref):
            return jnp.concatenate([ref[s, :] for s in spans]) if spans[1:] else ref[spans[0], :]

        def save(ref, value):
            n = value.shape[0] // len(spans)
            for i, s in enumerate(spans):
                ref[s, :] = value[i * n:(i + 1) * n]

        x_rows = cut_of(xb)
        h1, h3 = dot(x_rows, w(e, 0)), dot(x_rows, w(e, 1))
        sig = jax.nn.sigmoid(h1)
        silu = h1 * sig
        act = (silu * h3).astype(BF16)
        save(a_s, act)
        y_rows = dot_nt(act, w(e, 2))
        save(y_s, jnp.sum(cut_of(ub).astype(F32) * y_rows, axis=1, keepdims=True))
        da = dot(cut_of(gb), w(e, 2))
        d1 = (da * h3 * sig * (1.0 + h1 * (1.0 - sig))).astype(BF16)
        d3 = (da * silu).astype(BF16)
        save(d1_s, d1)
        save(d3_s, d3)
        save(dx_s, (dot_nt(d1, w(e, 0)) + dot_nt(d3, w(e, 1))).astype(BF16))

    def gather(all_rows, tri, sx, su, sg, ss):
        loads = [
            pltpu.make_async_copy(x_hbm, all_rows.at[me, pl.ds(0, tok)], load_sem.at[0]),
            pltpu.make_async_copy(u_hbm, all_rows.at[me, pl.ds(tok, tok)], load_sem.at[1]),
        ]
        for m, ref in enumerate((w1_hbm, w3_hbm, w2_hbm)):
            loads.append(pltpu.make_async_copy(ref.reshape(NY, OWN, d_loc, ff), wown.at[:, :, m], load_sem.at[2 + m]))
        tables = [pltpu.make_async_copy(a, b, load_sem.at[i]) for i, a, b in ((5, ids_hbm, ids_ref), (6, gates_hbm, gates_ref))]
        for copy in tables + loads:
            copy.start()
        all_in = enter()
        for copy in tables:
            copy.wait()

        @pl.loop(0, GROUP)
        def _(d):
            number = first_expert(d) + lax.broadcasted_iota(jnp.int32, (OWN, tok), 0)
            value = jnp.full((OWN, tok), -1.0, F32)
            for j in range(ids_ref.shape[0]):
                chosen = ids_ref[pl.ds(j, 1), :] == number
                value = jnp.where(chosen, jnp.broadcast_to(gates_ref[pl.ds(j, 1), :], value.shape), value)
            gates_out[d] = value

        metas[me] = gates_out[me]
        tri[...] = strict_upper(tok)
        for copy in loads:
            copy.wait()
        all_in()

        back = {"x+": (0, 3), "x-": (0, 1), "y+": (3, 0), "y-": (1, 0)}
        spans = {"A": (0, cut), "B": (cut, 2 * tok - cut)}

        def block(kind, dy, dx, part=None, dc=0):
            start, size = spans[kind]
            if part is not None:
                size //= 2
                start += part * size
            return all_rows.at[place(dy, dx, dc), pl.ds(start, size)]

        def bsem(kind, dy, dx, part):
            return recv.at[0 if kind == "A" else 1, dy * NX + dx, part or 0]

        row_copies = []

        def issue(name, part, link):
            number = len(row_copies) + len(weight_copies)
            sem = send_sem.at[number]
            group, part_of = None, None
            if name[0] == "w":
                _, dy, group = name
                src = wown.at[rem(y + dy, NY), pl.ds(*PIECE[group, None])]
                copy = remote(src, piece(0, 0, group), sem, wrecv.at[0, (-dy) % NY, group, 0], targets[link])
            elif name[0] in "rR":
                group, part_of, _ = RELAYS[name[1]]
                span = pl.ds(*PIECE[group, part_of])
                if name[0] == "r":
                    copy = remote(wown.at[rem(y + 2, NY), span], relay.at[span], sem, relay_recv.at[name[1]], targets[link])
                else:
                    dst = piece(0, back[link][0], group, part_of)
                    copy = remote(relay.at[span], dst, sem, wrecv.at[0, 2, group, part_of or 0], targets[link])
            elif name[0] == "W":
                _, dz, dy, group = name
                ndz = (dz - 1) % NZ if link == "z+" else (dz + 1) % NZ
                own = wown.at[y, pl.ds(*PIECE[group, None])]
                copy = remote(own if dz == dy == 0 else piece(dz, dy, group), piece(dz, dy, group), sem, wrecv.at[ndz, dy, group, 0], targets[link])
            else:
                kind, dy, dx = name
                ref = block(kind, dy, dx, part)
                if link == "core":
                    rsem = core_recv.at[0 if kind == "A" else 1, dy * NX + dx, part or 0]
                else:
                    oy, ox = back[link]
                    rsem = bsem(kind, (dy + oy) % NY, (dx + ox) % NX, part)
                copy = remote(ref, ref, sem, rsem, targets[link])
            copy.start()
            if group is None:
                row_copies.append(copy)
            else:
                weight_copies.append((number, group, part_of))

        def meta_copy(k):
            to = at_offset(k)
            return remote(gates_out.at[place_of(to)], metas.at[me], msend.at[k], mrecv.at[k], to)

        n_rows = OWN * 2 * cap
        stores, chips = [], []

        def put(dy, dx):
            slot = len(stores) % 2
            if stores[1:]:
                for copy in stores[-2]:
                    copy.wait()
            for dc in (0, 1):
                if dy or dx or dc:
                    k = ((-dy) % NY) * (NX * NC) + ((-dx) % NX) * NC + dc
                    wait(metas.at[place(dy, dx, dc)], mrecv.at[k])
            for i, (kind, last) in enumerate((("A", dx if dy == 0 else dy), ("B", dy if dx == 0 else dx))):
                for part in (0, 1) if last == 2 else (None,):
                    wait(block(kind, dy, dx, part, 1), core_recv.at[i, dy * NX + dx, part or 0])
            chip = rem(y + dy, NY) * NX + rem(x + dx, NX)
            n = 2 * OWN
            which = lax.broadcasted_iota(jnp.int32, (n, tok), 0)
            gate = jnp.zeros((n, tok), F32)
            for i in range(n):
                gate = jnp.where(which == i, jnp.broadcast_to(metas[2 * chip + i // OWN, pl.ds(i % OWN, 1), :], gate.shape), gate)
            member = gate >= 0.0
            key = jnp.where(member, dot(member.astype(F32).astype(BF16), tri[...]), -1.0)
            r = lax.broadcasted_iota(jnp.int32, (n_rows, tok), 0)
            at = rem(r, cap).astype(F32)
            row_of = rem(r // cap, 2) * OWN + r // (2 * cap)
            mine, gates = jnp.full((n_rows, tok), -1.0, F32), jnp.zeros((n_rows, tok), F32)
            for i in range(n):
                mine = jnp.where(row_of == i, jnp.broadcast_to(key[i:i + 1, :], mine.shape), mine)
                gates = jnp.where(row_of == i, jnp.broadcast_to(gate[i:i + 1, :], mine.shape), gates)
            found = at == mine
            pick = [jnp.logical_and(found, row_of // OWN == p).astype(F32) for p in range(2)]
            both = pick[0] + pick[1]
            scale = jnp.sum(both * gates, axis=1, keepdims=True)
            pick = [p.astype(BF16) for p in pick]
            x_rows = dot(pick[0], all_rows[2 * chip, 0:tok, :]) + dot(pick[1], all_rows[2 * chip + 1, 0:tok, :])
            u_rows = dot(pick[0], all_rows[2 * chip, tok:2 * tok, :]) + dot(pick[1], all_rows[2 * chip + 1, tok:2 * tok, :])
            span = pl.ds(pl.multiple_of(chip * 2 * cap, 2 * cap), 2 * cap)
            out = []
            for i, (value, first, stage, far) in enumerate(((x_rows, xb, sx, xr), (u_rows, ub, su, ur), (scale * u_rows, gb, sg, gr), (both, sb, ss, sel))):
                value = value.astype(BF16)
                first[span, :] = value[:2 * cap]
                stage[slot] = value[2 * cap:].reshape(stage.shape[1:])
                out.append(pltpu.make_async_copy(stage.at[slot], far.at[:, span], store_sem.at[slot, i]))
                out[-1].start()
            stores.append(out)
            chips.append(span)

        for name, sends in order:
            if name is None:
                pass
            elif name[0] == "put":
                put(*name[1:])
            elif name[0] == "tile":
                expert_rows(0, chips[name[1]:name[2]])
            elif name[0] == "R":
                group, part, _ = RELAYS[name[1]]
                wait(relay.at[pl.ds(*PIECE[group, part])], relay_recv.at[name[1]])
            elif name[0] == "W":
                if passed_on(*name[1:3]) or not name[3]:
                    wait_weights(*name[1:])
                else:
                    last_weights.append(name[1:])
            else:
                wait(block(*name), bsem(*name))
            for send in sends:
                issue(*send)
            if name is None:
                wv[z, y] = wown[y]

                @each_other
                def _(k):
                    meta_copy(k).start()

        for out in stores[-2:]:
            for copy in out:
                copy.wait()

        @each_other
        def _(k):
            meta_copy(k).wait_send()

        for copy in row_copies:
            copy.wait_send()

    def reduce(G, r4, r3, r2, r1):
        for dz in (1, NZ - 1):
            pl.semaphore_signal(in_scope, device_id=z_at(dz), device_id_type=pl.DeviceIdType.MESH)

        def row_loads(e):
            pairs = ((xr, xb), (gr, gb), (ur, ub), (sel, sb))
            return [pltpu.make_async_copy(src.at[e - 1], dst, lsem.at[i]) for i, (src, dst) in enumerate(pairs)]

        def chunk(e, way, dist):
            return G.at[e, z_at(dist if way else NZ - dist)["z"]]

        def half_of(ref, way, e, kind):
            return ref.at[way, e, (kind - ONE) % 2, (kind - ONE) // 2]

        def hop(e, way, kind):
            h = way
            src, dst = {
                FAR: lambda: (chunk(e, way, 4).at[h], r4.at[way, e]),
                SUM3: lambda: (r4.at[way, e], r3.at[way, e, h]),
                NEW3: lambda: (chunk(e, way, 3).at[1 - h], r3.at[way, e, 1 - h]),
                TWO: lambda: (r3.at[way, e], r2.at[way, e]),
            }.get(kind, lambda: (half_of(r2, way, e, kind), half_of(r1, way, e, kind)))()
            return remote(src, dst, rsend.at[way, e, kind], rrecv.at[way, e, kind], z_at(1 if way else NZ - 1))

        def add_into(dst, *others):
            parts = dst.shape[:-2]
            if not parts:
                total = dst[...]
                for other in others:
                    total = total + other[...]
                dst[...] = total
                return

            def flat(ref, i):
                index = []
                for n in reversed(parts):
                    index.append(rem(i, n))
                    i = i // n
                return ref.at[tuple(reversed(index))]

            n = 1
            for p in parts:
                n *= p

            @pl.loop(0, n)
            def _(i):
                total = flat(dst, i)[...]
                for other in others:
                    total = total + flat(other, i)[...]
                flat(dst, i)[...] = total

        def own_rows(s):
            return pl.ds(pl.multiple_of(s * cap, 8), cap)

        def dx_copy(e, k):
            to = at_offset(k)
            return remote(dxs.at[e, own_rows(place_of(to))], dxb.at[me, own_rows(e)], dsend.at[e], drecv.at[e], to)

        tile = 256 if rows % 256 == 0 else rows
        dtile = hidden // NZ
        half = dtile // 2

        def weight_gradients(e):
            out = pltpu.make_async_copy(dx_s, dxs.at[e], osem.at[0])
            out.start()

            @pl.loop(0, NZ // 2)
            def _(i):
                pair = [z_at(n + 2 * i)["z"] for n in (3, 4)]

                def cols(ref):
                    return jnp.concatenate([ref[:, pl.ds(pl.multiple_of(k * dtile, dtile), dtile)] for k in pair], axis=1)

                x_cols, g_cols = cols(xb), cols(gb)
                for m, part in enumerate((dot_tn(x_cols, d1_s[...]), dot_tn(x_cols, d3_s[...]), dot_tn(g_cols, a_s[...]))):
                    for j in range(4):
                        G[e, pair[j // 2], j % 2, m] = part[j * half:(j + 1) * half]

                @pl.when(i == 0)
                def _():
                    if isinstance(e, int):
                        pl.semaphore_wait(in_scope, 2)
                    for way, kind in ((0, FAR), (1, FAR), (1, NEW3)):
                        hop(e, way, kind).start()

                @pl.when(i == 1)
                def _():
                    hop(e, 0, NEW3).start()

            val = sb[...].astype(F32) * y_s[...]
            val_s[e] = jnp.sum(val.reshape(rows // cap, cap, tok), axis=1)
            out.wait()

        def send_back(e):
            pltpu.make_async_copy(dxs.at[e, own_rows(me)], dxb.at[me, own_rows(e)], drecv.at[e]).start()

            @each_other
            def _(k):
                dx_copy(e, k).start()

        def far_sums(e):
            for way in (0, 1):
                hop(e, way, FAR).wait_recv()
                add_into(r4.at[way, e], chunk(e, way, 3).at[way])
                hop(e, way, SUM3).start()

        weight_gradients(0)
        for copy in row_loads(1):
            copy.start()
        send_back(0)
        for name in last_weights:
            wait_weights(*name)

        @pl.loop(1, OWN)
        def _(e):
            for copy in row_loads(e):
                copy.wait()

            @pl.loop(0, rows // tile)
            def _(i):
                expert_rows(e, [pl.ds(pl.multiple_of(i * tile, tile), tile)])

            weight_gradients(e)

            @pl.when(e < OWN - 1)
            def _():
                for copy in row_loads(e + 1):
                    copy.start()

            send_back(e)
            far_sums(e - 1)

        far_sums(OWN - 1)

        def val_copy(k):
            to = at_offset(k)
            return remote(val_s.at[:, place_of(to)], valb.at[:, me], vsem.at[0, k], vsem.at[1, k], to)

        own_val = pltpu.make_async_copy(val_s.at[:, me], valb.at[:, me], vsem.at[0, 0])
        own_val.start()

        @each_other
        def _(k):
            val_copy(k).start()

        def step(arrived, dist, leaves):
            @pl.loop(0, OWN)
            def _(e):
                for way in (0, 1):
                    for kind in arrived:
                        hop(e, way, kind).wait_recv()
                    if leaves == TWO:
                        add_into(r3.at[way, e], chunk(e, way, dist))
                        hop(e, way, TWO).start()
                if leaves == ONE:
                    for kind in range(ONE, HOPS):
                        for way in (0, 1):
                            add_into(half_of(r2, way, e, kind), half_of(G, e, z_at(dist if way else NZ - dist)["z"], kind))
                            hop(e, way, kind).start()

        step((SUM3, NEW3), 2, TWO)

        group, places = dxb.shape[:2]
        ids = ids_ref[...].astype(F32)
        r = lax.broadcasted_iota(jnp.int32, (group * 8, tok), 0)
        e_of = rem(r, 8)
        expert = jnp.where(e_of < OWN, first_expert(r // 8) + e_of, -1).astype(F32)
        member = jnp.zeros((group * 8, tok), F32)
        for j in range(ids.shape[0]):
            member = member + (jnp.broadcast_to(ids[j:j + 1, :], member.shape) == expert).astype(F32)
        before = dot(member.astype(BF16), strict_upper(tok))
        key_s[...] = jnp.where(member > 0.0, before, -1.0).reshape(key_s.shape)
        rr = lax.broadcasted_iota(jnp.int32, (places, tok), 0)
        at, e_row = rem(rr, cap).astype(F32), rr // cap
        some = rows // places

        @pl.loop(0, OWN)
        def _(e):
            got = dxb.at[:, own_rows(e)]
            pltpu.make_async_copy(got, got, drecv.at[e]).wait()

        own_val.wait()

        @each_other
        def _(k):
            val_copy(k).wait()

        bufs = (xb, gb)
        loads = [pltpu.make_async_copy(dxb.at[pl.ds(i * some, some)], bufs[i % 2].reshape(some, places, hidden), lsem.at[i % 2]) for i in range(group // some)]
        vals = pltpu.make_async_copy(valb, vb, lsem.at[2])
        vals.start()
        loads[0].start()
        for i, load in enumerate(loads):
            for later in loads[i + 1:i + 2]:
                later.start()

            @pl.loop(0, some)
            def _(k):
                key = key_s[i * some + k]
                mine = jnp.full((places, tok), -1.0, F32)
                for e in range(OWN):
                    mine = jnp.where(e_row == e, jnp.broadcast_to(key[e:e + 1, :], (places, tok)), mine)
                sb[pl.ds(pl.multiple_of(k * places, places), places), :] = (at == mine).astype(F32).astype(BF16)

            load.wait()
            part = dot_tn(sb[...], bufs[i % 2][...])
            acc_s[...] = acc_s[...] + part if i else part

        in_grad_ref[...] = acc_s[...].astype(BF16)
        vals.wait()

        def gate_step(k, total):
            for e in range(OWN):
                row = vb[e, pl.ds(k, 1), :]
                total = total + jnp.where(ids == (first_expert(k) + e).astype(F32), jnp.broadcast_to(row, ids.shape), 0.0)
            return total

        gate_ref[...] = lax.fori_loop(0, group, gate_step, jnp.zeros(ids.shape, F32))
        results = [pltpu.make_async_copy(a, b, load_sem.at[i]) for i, a, b in ((0, in_grad_ref, in_grad_hbm), (1, gate_ref, gate_hbm))]
        for copy in results:
            copy.start()

        step((TWO,), 1, ONE)

        def keep(e, m, to, then_remote, then_local):
            src = r1.at[0, e, to // 2, m, pl.ds(to % 2 * d_loc, d_loc)]
            dst = grads.at[m, y * OWN + e]

            @pl.when(y != to)
            def _():
                then_remote(remote(src, dst, ysend.at[e, m, to], yrecv.at[e, m, y], {"y": to}))

            @pl.when(y == to)
            def _():
                then_local(pltpu.make_async_copy(src, dst, ysend.at[e, m, to]))

        @pl.loop(0, OWN)
        def _(e):
            for kind in range(ONE, HOPS):
                for way in (0, 1):
                    hop(e, way, kind).wait_recv()
                add_into(half_of(r1, 0, e, kind), half_of(r1, 1, e, kind), half_of(G, e, z, kind))
                m, h = (kind - ONE) // 2, (kind - ONE) % 2
                for to in (2 * h, 2 * h + 1):
                    keep(e, m, to, start, start)

        @pl.loop(0, OWN)
        def _(e):
            for m in range(3):
                for at in range(NY):
                    def both(copy):
                        wait(grads.at[m, at * OWN + e], yrecv.at[e, m, at])
                        copy.wait_send()

                    keep(e, m, at, both, lambda copy: copy.wait())
            for way in (0, 1):
                for kind in range(HOPS):
                    hop(e, way, kind).wait_send()

            sent = dxs.at[e, pl.ds(0, (GROUP - 1) * cap)]
            pltpu.make_async_copy(sent, sent, dsend.at[e]).wait()

        for copy in results:
            copy.wait()

    weight_copies, last_weights = [], []
    pl.run_scoped(gather, *scope_one)
    pl.run_scoped(reduce, *scope_two)
    for number, group, part in weight_copies:
        ref = wown.at[0, pl.ds(*PIECE[group, part])]
        remote(ref, ref, send_sem.at[number], relay_recv.at[0], targets["core"]).wait_send()


def layer(cap, x, u, ids, gates, w1, w3, w2):
    tok, hidden = x.shape
    local_experts, d_loc, ff = w1.shape
    rows = GROUP * cap
    half = hidden // NZ // 2
    cut = tok - tok // 8 if tok % 256 == 0 else tok
    order = gather_order(4 * tok * hidden, cut / (2 * tok), 2 * w1.size * 3 // local_experts)
    sends = sum(len(s) for _, s in order)
    dma, v, shape = pltpu.SemaphoreType.DMA, pltpu.VMEM, jax.ShapeDtypeStruct
    far = lambda lanes: shape((OWN - 1, rows, lanes), BF16)
    near = lambda lanes: v((rows, lanes), BF16)
    stage = lambda lanes: v((2, OWN - 1, 2 * cap, lanes), BF16)
    sums = [v((2, OWN, 2, 3, half, ff), F32)] * 3
    scope_one = [v((GROUP, 2 * tok, hidden), BF16), v((tok, tok), BF16), stage(hidden), stage(hidden), stage(hidden), stage(tok)]
    scope_two = [v((OWN, NZ, 2, 3, half, ff), F32), v((2, OWN, 3, half, ff), F32)] + sums
    per_expert = v((OWN, GROUP, tok), F32)
    gate_rows = v((GROUP, OWN, tok), F32)
    outs = pl.pallas_call(
        functools.partial(layer_kernel, order, cap, cut, scope_one, scope_two),
        name="layer",
        out_shape=(
            shape((3, local_experts, d_loc, ff), F32), shape((tok, hidden), BF16), shape(ids.shape, F32),
            shape((GROUP, OWN * cap, hidden), BF16), shape((OWN, GROUP, tok), F32), shape((OWN, rows, hidden), BF16),
            far(hidden), far(hidden), far(hidden), far(tok),
        ),
        in_specs=[ANY] * 7,
        out_specs=(ANY,) * 10,
        scratch_shapes=[
            v(ids.shape, ids.dtype), v(ids.shape, F32), v((tok, hidden), BF16), v(ids.shape, F32), gate_rows, gate_rows, v((NY, OWN, 3, d_loc, ff), BF16), v((NZ, NY, OWN, 3, d_loc, ff), BF16), v((OWN, 3, d_loc, ff), BF16),
            near(hidden), near(hidden), near(hidden), near(tok), near(ff), near(ff), near(ff), v((rows, 1), F32),
            near(hidden), per_expert, per_expert, v((GROUP, 8, tok), F32), v((tok, hidden), F32),
            dma((2, NY * NX, 2)), dma((2, NY * NX, 2)), dma((NZ, NY, 2, 2)), dma((len(RELAYS),)), dma((GROUP,)), dma((sends,)), dma((GROUP,)),
            dma((7,)), dma((2, 4)),
            dma((4,)), dma((2, OWN, HOPS)), dma((2, OWN, HOPS)), dma((OWN, 3, NY)), dma((OWN, 3, NY)),
            dma((OWN,)), dma((OWN,)), dma((2, GROUP)), dma((1,)), pltpu.SemaphoreType.REGULAR,
        ],
        compiler_params=params(0),
    )(x, u, ids, gates, w1, w3, w2)
    return outs[:3]


def finish_kernel(grads, in_grad, gate, *refs):
    n = 5
    outs, bufs, sems = refs[:n], refs[n:2 * n], refs[-1]
    ins = [grads.at[m] for m in range(3)] + [in_grad, gate]
    load = [pltpu.make_async_copy(a, b, sems.at[0, i]) for i, (a, b) in enumerate(zip(ins, bufs))]
    store = [pltpu.make_async_copy(b, o, sems.at[1, i]) for i, (b, o) in enumerate(zip(bufs, outs))]
    for copy in load:
        copy.start()
    for i in range(n):
        load[i].wait()
        store[i].start()
    for copy in store:
        copy.wait()


def finish(grads, in_grad, gate):
    shapes = [grads.shape[1:]] * 3 + [in_grad.shape, gate.shape]
    types = [grads.dtype] * 3 + [in_grad.dtype, gate.dtype]
    return pl.pallas_call(
        finish_kernel,
        name="finish",
        out_shape=[jax.ShapeDtypeStruct(s, t) for s, t in zip(shapes, types)],
        in_specs=[ANY] * 3,
        out_specs=[ANY] * len(shapes),
        scratch_shapes=[pltpu.VMEM(s, t) for s, t in zip(shapes, types)] + [pltpu.SemaphoreType.DMA((2, len(shapes)))],
    )(grads, in_grad, gate)


def solution(mesh):
    mesh4 = Mesh(mesh.devices.reshape(NZ, NY, NX, NC), ("z", "y", "x", "core"))
    tok_spec = P(("z", "y", "x", "core"), None)
    up_spec = P(("x", "core"), ("z", "y"), None)
    down_spec = P(("x", "core"), None, ("z", "y"))

    def per_device(layer_in, out_grad, expert_ids, gate_vals, w_one, w_two, w_three):
        tok_dev, hidden = layer_in.shape
        top_k = expert_ids.shape[1]
        local_experts, d_loc, ff = w_one.shape
        cap = capacity_of(tok_dev, top_k, local_experts * NX * NC)
        ids = expert_ids.T
        grads, in_grad, gate_out = layer(cap, layer_in, out_grad, ids, gate_vals.T, w_one, w_three, w_two.swapaxes(1, 2))
        g1, g3, g2, in_grad, gate_out = finish(grads, in_grad, gate_out)
        return in_grad, gate_out.T, g1, g2.swapaxes(1, 2), g3

    return jax.shard_map(per_device, mesh=mesh4, in_specs=(tok_spec, tok_spec, tok_spec, tok_spec, up_spec, down_spec, up_spec), out_specs=(tok_spec, tok_spec, up_spec, down_spec, up_spec), check_vma=False)
```

```python
import functools

import jax
import jax.numpy as jnp
from jax import lax
from jax.experimental import pallas as pl
from jax.experimental.pallas import tpu as pltpu
from jax.sharding import Mesh, PartitionSpec as P

NZ, NY, NX, NC = 8, 4, 4, 2
GROUP = NY * NX * NC
PLANE = ("y", "x", "core")
OWN = 4
F32, BF16 = jnp.float32, jnp.bfloat16
ANY = pl.BlockSpec(memory_space=pl.ANY)


def capacity_of(tok_dev, top_k, experts):
    return max(8, ((tok_dev * top_k * 5) // (4 * experts) + 7) // 8 * 8)


def rem(a, b):
    return a % b if isinstance(a, int) else lax.rem(a, b)


def contract(ca, cb):
    return lambda a, b: lax.dot_general(a, b, (((ca,), (cb,)), ((), ())), preferred_element_type=F32)


dot, dot_nt, dot_tn = contract(1, 0), contract(1, 1), contract(0, 0)


def params(number):
    return pltpu.CompilerParams(collective_id=number, has_side_effects=True, vmem_limit_bytes=67043328)


def each_other(body):
    return pl.loop(1, GROUP)(body)


def strict_upper(n):
    rows = lax.broadcasted_iota(jnp.int32, (n, n), 0)
    cols = lax.broadcasted_iota(jnp.int32, (n, n), 1)
    return (rows < cols).astype(F32).astype(BF16)


def here():
    return tuple(lax.axis_index(a) for a in ("z", "y", "x", "core"))


def at_offset(k):
    _, y, x, c = here()
    dy, dx, dc = k // (NX * NC), rem(k // NC, NX), rem(k, NC)
    return {"y": rem(y + dy, NY), "x": rem(x + dx, NX), "core": rem(c + dc, NC)}


def place_of(d):
    return d["y"] * (NX * NC) + d["x"] * NC + d["core"]


def z_at(dz):
    return {"z": rem(lax.axis_index("z") + dz, NZ)}


def remote(src, dst, send_sem, recv_sem, target):
    return pltpu.make_async_remote_copy(src_ref=src, dst_ref=dst, send_sem=send_sem, recv_sem=recv_sem, device_id=target, device_id_type=pl.DeviceIdType.MESH)


def start(copy):
    copy.start()


def enter():
    barrier = pltpu.get_barrier_semaphore()

    @each_other
    def _(k):
        pl.semaphore_signal(barrier, device_id=at_offset(k), device_id_type=pl.DeviceIdType.MESH)

    for dz in (1, NZ - 1):
        pl.semaphore_signal(barrier, device_id=z_at(dz), device_id_type=pl.DeviceIdType.MESH)
    return lambda: pl.semaphore_wait(barrier, GROUP + 1)


RATE, D2D, HOP = 44700.0, 400000.0, 2.3
PUT, TILE, ROWS = 1.0, 1.0, 0.4
STEP = 5
AHEAD, MORE = 5.0, 0.05

PIECE = {(0, None): (0, 1), (1, None): (1, 3), (1, 0): (1, 1), (1, 1): (2, 2)}
RELAYS = ((0, None, "y+"), (1, 0, "y+"), (1, 1, "y-"))


KINDS = ("A0", "A1", "B0", "B1")


def gather_order(sizes, expert_bytes):
    free, pending, coming, order, have, ready = {}, {}, [], [], {}, {}

    def send(now, name, link, arrives, nbytes):
        t = max(now, free.get(link, 0.0)) + nbytes / (D2D if link == "core" else RATE)
        free[link] = t
        coming.append((t + HOP, len(order), len(coming), arrives))
        return (name, link)

    def later(rank, name, link, arrives, nbytes):
        queue = pending.setdefault(link, [])
        queue.append((rank, len(order), len(queue), (name, link, arrives, nbytes)))

    def turn(now):
        out = []
        for link, queue in pending.items():
            queue.sort()
            while queue and free.get(link, 0.0) - now < AHEAD + MORE * now:
                out.append(send(now, *queue.pop(0)[-1]))
        return out

    def on_rows(kind, dy, dx):
        first, second = "xy" if kind[0] == "A" else "yx"
        d = {"x": dx, "y": dy}
        for axis in [first, second] if d[second] == 0 else [second]:
            for sign in (1, -1):
                if d[axis] == 0 or d[axis] == -sign % 4 and kind[1] == "10"[sign > 0]:
                    nd = dict(d)
                    nd[axis] = (d[axis] - sign) % 4
                    rank = 4 + (axis == second) + (d[axis] != 0)
                    later(rank, (kind, dy, dx), axis + "-+"[sign > 0], (kind, nd["y"], nd["x"]), sizes[kind])

    def core(now, key):
        return send(now, key, "core", ("core",) + key, sizes[key[0]])

    def weights(rank, name, group, part, link, arrives):
        later(rank, name, link, arrives + (group, part), PIECE[group, part][1] * expert_bytes)

    def on_piece(dz, dy, group):
        for link, step, far in (("z+", -1, dy < 2), ("z-", 1, dy >= 2)):
            gone = (step * dz) % NZ
            if gone < 3 + far:
                weights(4 * group + gone, ("W", dz, dy, group), group, None, link, ("W", (dz + step) % NZ, dy))

    def arrived(key, part=None):
        have[key] = have.get(key, 0) + (2 if part is None else 1)
        if have[key] == 2:
            ready[key] = True
        return have[key] == 2

    for i, (group, part, link) in enumerate(RELAYS):
        weights(0, ("r", i), group, part, link, ("R", i))
    for group in range(2):
        for dy, link in ((1, "y+"), (3, "y-")):
            weights(2, ("w", dy, group), group, None, link, ("W", 0, (-dy) % NY))
        on_piece(0, 0, group)
    sends = []
    for kind in KINDS[::-1]:
        arrived((kind, 0, 0))
        on_rows(kind, 0, 0)
        sends.append(core(0.0, (kind, 0, 0)))
    order.append((None, turn(0.0) + sends))
    todo, puts, done, now = [(dy, dx) for dy in range(NY) for dx in range(NX)], 0, 0, 0.0
    while coming or todo or done < puts:
        coming.sort()
        soon = coming[0][0] if coming else 1e9
        if soon > now:
            place = next((p for p in todo if all(pre + (kind,) + p in ready for kind in KINDS for pre in ((), ("core",)))), None)
            if place is not None:
                todo.remove(place)
                order.append((("put",) + place, turn(now)))
                puts += 1
                now += PUT
                continue
            step = min(STEP, puts - done)
            weights_in = sum(key[0] == "W" and key[-1] == 0 for key in ready) == NZ * NY - 1
            if weights_in and (step >= 3 and soon - now > TILE or not todo):
                order.append((("tile", done, done + step), turn(now)))
                done += step
                now += TILE + ROWS * step
                continue
        t, _, _, name = coming.pop(0)
        now = max(now, t)
        if name[0] == "core":
            arrived(name)
            continue
        sends = []
        if name[0] == "R":
            i, group, part = name[1:]
            weights(1, name[:2], group, part, RELAYS[i][2], ("W", 0, 2))
            name = name[:2]
        elif name[0] == "W":
            if arrived(name[:-1], name[-1]):
                on_piece(*name[1:-1])
        else:
            sends = [core(now, name)]
            arrived(name)
            on_rows(*name)
        order.append((name, sends + turn(now)))
    return order


def passed_on(dz, dy):
    return dz != NZ // 2 and dz not in ((3,) if dy < 2 else (5,))


def first_expert(d):
    return rem(d, NX * NC) * (NY * OWN) + d // (NX * NC) * OWN


FAR, SUM3, NEW3, TWO, ONE, HOPS = 0, 1, 2, 3, 4, 10


def layer_kernel(order, cap, spans, scope_one, scope_two, x_hbm, u_hbm, ids_hbm, gates_hbm, w1_hbm, w3_hbm, w2_hbm,
                 grads, in_grad_hbm, gate_hbm, dxb, valb, dxs, xr, ur, gr, sel,
                 ids_ref, gates_ref, in_grad_ref, gate_ref, metas, gates_out, wown, wv, relay, xb, ub, gb, sb, a_s, d1_s, d3_s, y_s, dx_s, val_s, vb, key_s, acc_s,
                 recv, core_recv, wrecv, relay_recv, mrecv, send_sem, msend, load_sem, store_sem,
                 lsem, rsend, rrecv, ysend, yrecv, dsend, drecv, vsem, osem, in_scope):
    z, y, x, c = here()
    tok, hidden = x_hbm.shape
    rows, ff = xb.shape[0], a_s.shape[-1]
    d_loc = hidden // (NZ * NY)
    me = place_of(at_offset(0))

    def place(dy, dx, dc=0):
        return place_of(at_offset(dy * (NX * NC) + dx * NC + dc))

    targets = {"core": {"core": 1 - c}}
    for sign, n in (("+", 1), ("-", -1)):
        targets["x" + sign] = {"x": rem(x + n + NX, NX)}
        targets["y" + sign] = {"y": rem(y + n + NY, NY)}
        targets["z" + sign] = z_at(n + NZ)

    def wait(ref, sem):
        remote(ref, ref, send_sem.at[0], sem, targets["core"]).wait_recv()

    def piece(dz, dy, group, part=None):
        return wv.at[z_at(dz)["z"], rem(y + dy, NY), pl.ds(*PIECE[group, part])]

    def wait_weights(dz, dy, group, part):
        wait(piece(dz, dy, group, part), wrecv.at[dz, dy, group, part or 0])

    def w(e, m):
        return wv[:, :, e, m].reshape(hidden, ff)

    def expert_rows(e, spans):
        def cut_of(ref):
            return jnp.concatenate([ref[s, :] for s in spans]) if spans[1:] else ref[spans[0], :]

        def save(ref, value):
            n = value.shape[0] // len(spans)
            for i, s in enumerate(spans):
                ref[s, :] = value[i * n:(i + 1) * n]

        x_rows = cut_of(xb)
        h1, h3 = dot(x_rows, w(e, 0)), dot(x_rows, w(e, 1))
        sig = jax.nn.sigmoid(h1)
        silu = h1 * sig
        act = (silu * h3).astype(BF16)
        save(a_s, act)
        y_rows = dot_nt(act, w(e, 2))
        save(y_s, jnp.sum(cut_of(ub).astype(F32) * y_rows, axis=1, keepdims=True))
        da = dot(cut_of(gb), w(e, 2))
        d1 = (da * h3 * sig * (1.0 + h1 * (1.0 - sig))).astype(BF16)
        d3 = (da * silu).astype(BF16)
        save(d1_s, d1)
        save(d3_s, d3)
        save(dx_s, (dot_nt(d1, w(e, 0)) + dot_nt(d3, w(e, 1))).astype(BF16))

    def gather(all_rows, tri, sx, su, sg, ss):
        loads = [
            pltpu.make_async_copy(x_hbm, all_rows.at[me, pl.ds(0, tok)], load_sem.at[0]),
            pltpu.make_async_copy(u_hbm, all_rows.at[me, pl.ds(tok, tok)], load_sem.at[1]),
        ]
        for m, ref in enumerate((w1_hbm, w3_hbm, w2_hbm)):
            loads.append(pltpu.make_async_copy(ref.reshape(NY, OWN, d_loc, ff), wown.at[:, :, m], load_sem.at[2 + m]))
        tables = [pltpu.make_async_copy(a, b, load_sem.at[i]) for i, a, b in ((5, ids_hbm, ids_ref), (6, gates_hbm, gates_ref))]
        for copy in tables + loads:
            copy.start()
        all_in = enter()
        for copy in tables:
            copy.wait()

        @pl.loop(0, GROUP)
        def _(d):
            number = first_expert(d) + lax.broadcasted_iota(jnp.int32, (OWN, tok), 0)
            value = jnp.full((OWN, tok), -1.0, F32)
            for j in range(ids_ref.shape[0]):
                chosen = ids_ref[pl.ds(j, 1), :] == number
                value = jnp.where(chosen, jnp.broadcast_to(gates_ref[pl.ds(j, 1), :], value.shape), value)
            gates_out[d] = value

        metas[me] = gates_out[me]
        tri[...] = strict_upper(tok)
        for copy in loads:
            copy.wait()
        all_in()

        back = {"x+": (0, 3), "x-": (0, 1), "y+": (3, 0), "y-": (1, 0)}
        def block(kind, dy, dx, dc=0):
            return all_rows.at[place(dy, dx, dc), pl.ds(*spans[kind])]

        row_copies = []

        def issue(name, link):
            number = len(row_copies) + len(weight_copies)
            sem = send_sem.at[number]
            group, part_of = None, None
            if name[0] == "w":
                _, dy, group = name
                src = wown.at[rem(y + dy, NY), pl.ds(*PIECE[group, None])]
                copy = remote(src, piece(0, 0, group), sem, wrecv.at[0, (-dy) % NY, group, 0], targets[link])
            elif name[0] in "rR":
                group, part_of, _ = RELAYS[name[1]]
                span = pl.ds(*PIECE[group, part_of])
                if name[0] == "r":
                    copy = remote(wown.at[rem(y + 2, NY), span], relay.at[span], sem, relay_recv.at[name[1]], targets[link])
                else:
                    dst = piece(0, back[link][0], group, part_of)
                    copy = remote(relay.at[span], dst, sem, wrecv.at[0, 2, group, part_of or 0], targets[link])
            elif name[0] == "W":
                _, dz, dy, group = name
                ndz = (dz - 1) % NZ if link == "z+" else (dz + 1) % NZ
                own = wown.at[y, pl.ds(*PIECE[group, None])]
                copy = remote(own if dz == dy == 0 else piece(dz, dy, group), piece(dz, dy, group), sem, wrecv.at[ndz, dy, group, 0], targets[link])
            else:
                kind, dy, dx = name
                ref = block(*name)
                oy, ox = back.get(link, (0, 0))
                arrivals = core_recv if link == "core" else recv
                rsem = arrivals.at[KINDS.index(kind), (dy + oy) % NY * NX + (dx + ox) % NX]
                copy = remote(ref, ref, sem, rsem, targets[link])
            copy.start()
            if group is None:
                row_copies.append(copy)
            else:
                weight_copies.append((number, group, part_of))

        def meta_copy(k):
            to = at_offset(k)
            return remote(gates_out.at[place_of(to)], metas.at[me], msend.at[k], mrecv.at[k], to)

        n_rows = OWN * 2 * cap
        stores, chips = [], []

        def put(dy, dx):
            slot = len(stores) % 2
            if stores[1:]:
                for copy in stores[-2]:
                    copy.wait()
            for dc in (0, 1):
                if dy or dx or dc:
                    k = ((-dy) % NY) * (NX * NC) + ((-dx) % NX) * NC + dc
                    wait(metas.at[place(dy, dx, dc)], mrecv.at[k])
            for i, kind in enumerate(KINDS):
                wait(block(kind, dy, dx, 1), core_recv.at[i, dy * NX + dx])
            chip = rem(y + dy, NY) * NX + rem(x + dx, NX)
            n = 2 * OWN
            which = lax.broadcasted_iota(jnp.int32, (n, tok), 0)
            gate = jnp.zeros((n, tok), F32)
            for i in range(n):
                gate = jnp.where(which == i, jnp.broadcast_to(metas[2 * chip + i // OWN, pl.ds(i % OWN, 1), :], gate.shape), gate)
            member = gate >= 0.0
            key = jnp.where(member, dot(member.astype(F32).astype(BF16), tri[...]), -1.0)
            r = lax.broadcasted_iota(jnp.int32, (n_rows, tok), 0)
            at = rem(r, cap).astype(F32)
            row_of = rem(r // cap, 2) * OWN + r // (2 * cap)
            mine, gates = jnp.full((n_rows, tok), -1.0, F32), jnp.zeros((n_rows, tok), F32)
            for i in range(n):
                mine = jnp.where(row_of == i, jnp.broadcast_to(key[i:i + 1, :], mine.shape), mine)
                gates = jnp.where(row_of == i, jnp.broadcast_to(gate[i:i + 1, :], mine.shape), gates)
            found = at == mine
            pick = [jnp.logical_and(found, row_of // OWN == p).astype(F32) for p in range(2)]
            both = pick[0] + pick[1]
            scale = jnp.sum(both * gates, axis=1, keepdims=True)
            pick = [p.astype(BF16) for p in pick]
            x_rows = dot(pick[0], all_rows[2 * chip, 0:tok, :]) + dot(pick[1], all_rows[2 * chip + 1, 0:tok, :])
            u_rows = dot(pick[0], all_rows[2 * chip, tok:2 * tok, :]) + dot(pick[1], all_rows[2 * chip + 1, tok:2 * tok, :])
            span = pl.ds(pl.multiple_of(chip * 2 * cap, 2 * cap), 2 * cap)
            out = []
            for i, (value, first, stage, far) in enumerate(((x_rows, xb, sx, xr), (u_rows, ub, su, ur), (scale * u_rows, gb, sg, gr), (both, sb, ss, sel))):
                value = value.astype(BF16)
                first[span, :] = value[:2 * cap]
                stage[slot] = value[2 * cap:].reshape(stage.shape[1:])
                out.append(pltpu.make_async_copy(stage.at[slot], far.at[:, span], store_sem.at[slot, i]))
                out[-1].start()
            stores.append(out)
            chips.append(span)

        for name, sends in order:
            if name is None:
                pass
            elif name[0] == "put":
                put(*name[1:])
            elif name[0] == "tile":
                expert_rows(0, chips[name[1]:name[2]])
            elif name[0] == "R":
                group, part, _ = RELAYS[name[1]]
                wait(relay.at[pl.ds(*PIECE[group, part])], relay_recv.at[name[1]])
            elif name[0] == "W":
                if passed_on(*name[1:3]) or not name[3]:
                    wait_weights(*name[1:])
                else:
                    last_weights.append(name[1:])
            else:
                kind, dy, dx = name
                wait(block(*name), recv.at[KINDS.index(kind), dy * NX + dx])
            for send in sends:
                issue(*send)
            if name is None:
                wv[z, y] = wown[y]

                @each_other
                def _(k):
                    meta_copy(k).start()

        for out in stores[-2:]:
            for copy in out:
                copy.wait()

        @each_other
        def _(k):
            meta_copy(k).wait_send()

        for copy in row_copies:
            copy.wait_send()

    def reduce(G, r4, r3, r2, r1):
        for dz in (1, NZ - 1):
            pl.semaphore_signal(in_scope, device_id=z_at(dz), device_id_type=pl.DeviceIdType.MESH)

        def row_loads(e):
            pairs = ((xr, xb), (gr, gb), (ur, ub), (sel, sb))
            return [pltpu.make_async_copy(src.at[e - 1], dst, lsem.at[i]) for i, (src, dst) in enumerate(pairs)]

        def chunk(e, way, dist):
            return G.at[e, z_at(dist if way else NZ - dist)["z"]]

        def half_of(ref, way, e, kind):
            return ref.at[way, e, (kind - ONE) % 2, (kind - ONE) // 2]

        def hop(e, way, kind):
            h = way
            src, dst = {
                FAR: lambda: (chunk(e, way, 4).at[h], r4.at[way, e]),
                SUM3: lambda: (r4.at[way, e], r3.at[way, e, h]),
                NEW3: lambda: (chunk(e, way, 3).at[1 - h], r3.at[way, e, 1 - h]),
                TWO: lambda: (r3.at[way, e], r2.at[way, e]),
            }.get(kind, lambda: (half_of(r2, way, e, kind), half_of(r1, way, e, kind)))()
            return remote(src, dst, rsend.at[way, e, kind], rrecv.at[way, e, kind], z_at(1 if way else NZ - 1))

        def add_into(dst, *others):
            parts = dst.shape[:-2]
            if not parts:
                total = dst[...]
                for other in others:
                    total = total + other[...]
                dst[...] = total
                return

            def flat(ref, i):
                index = []
                for n in reversed(parts):
                    index.append(rem(i, n))
                    i = i // n
                return ref.at[tuple(reversed(index))]

            n = 1
            for p in parts:
                n *= p

            @pl.loop(0, n)
            def _(i):
                total = flat(dst, i)[...]
                for other in others:
                    total = total + flat(other, i)[...]
                flat(dst, i)[...] = total

        def own_rows(s):
            return pl.ds(pl.multiple_of(s * cap, 8), cap)

        def dx_copy(e, k):
            to = at_offset(k)
            return remote(dxs.at[e, own_rows(place_of(to))], dxb.at[me, own_rows(e)], dsend.at[e], drecv.at[e], to)

        tile = 256 if rows % 256 == 0 else rows
        dtile = hidden // NZ
        half = dtile // 2

        def weight_gradients(e):
            out = pltpu.make_async_copy(dx_s, dxs.at[e], osem.at[0])
            out.start()

            @pl.loop(0, NZ // 2)
            def _(i):
                pair = [z_at(n + 2 * i)["z"] for n in (3, 4)]

                def cols(ref):
                    return jnp.concatenate([ref[:, pl.ds(pl.multiple_of(k * dtile, dtile), dtile)] for k in pair], axis=1)

                x_cols, g_cols = cols(xb), cols(gb)
                for m, part in enumerate((dot_tn(x_cols, d1_s[...]), dot_tn(x_cols, d3_s[...]), dot_tn(g_cols, a_s[...]))):
                    for j in range(4):
                        G[e, pair[j // 2], j % 2, m] = part[j * half:(j + 1) * half]

                @pl.when(i == 0)
                def _():
                    if isinstance(e, int):
                        pl.semaphore_wait(in_scope, 2)
                    for way, kind in ((0, FAR), (1, FAR), (1, NEW3)):
                        hop(e, way, kind).start()

                @pl.when(i == 1)
                def _():
                    hop(e, 0, NEW3).start()

            val = sb[...].astype(F32) * y_s[...]
            val_s[e] = jnp.sum(val.reshape(rows // cap, cap, tok), axis=1)
            out.wait()

        def send_back(e):
            pltpu.make_async_copy(dxs.at[e, own_rows(me)], dxb.at[me, own_rows(e)], drecv.at[e]).start()

            @each_other
            def _(k):
                dx_copy(e, k).start()

        def far_sums(e):
            for way in (0, 1):
                hop(e, way, FAR).wait_recv()
                add_into(r4.at[way, e], chunk(e, way, 3).at[way])
                hop(e, way, SUM3).start()

        weight_gradients(0)
        for copy in row_loads(1):
            copy.start()
        send_back(0)
        for name in last_weights:
            wait_weights(*name)

        @pl.loop(1, OWN)
        def _(e):
            for copy in row_loads(e):
                copy.wait()

            @pl.loop(0, rows // tile)
            def _(i):
                expert_rows(e, [pl.ds(pl.multiple_of(i * tile, tile), tile)])

            weight_gradients(e)

            @pl.when(e < OWN - 1)
            def _():
                for copy in row_loads(e + 1):
                    copy.start()

            send_back(e)
            far_sums(e - 1)

        far_sums(OWN - 1)

        def val_copy(k):
            to = at_offset(k)
            return remote(val_s.at[:, place_of(to)], valb.at[:, me], vsem.at[0, k], vsem.at[1, k], to)

        own_val = pltpu.make_async_copy(val_s.at[:, me], valb.at[:, me], vsem.at[0, 0])
        own_val.start()

        @each_other
        def _(k):
            val_copy(k).start()

        def step(arrived, dist, leaves):
            @pl.loop(0, OWN)
            def _(e):
                for way in (0, 1):
                    for kind in arrived:
                        hop(e, way, kind).wait_recv()
                    if leaves == TWO:
                        add_into(r3.at[way, e], chunk(e, way, dist))
                        hop(e, way, TWO).start()
                if leaves == ONE:
                    for kind in range(ONE, HOPS):
                        for way in (0, 1):
                            add_into(half_of(r2, way, e, kind), half_of(G, e, z_at(dist if way else NZ - dist)["z"], kind))
                            hop(e, way, kind).start()

        step((SUM3, NEW3), 2, TWO)

        group, places = dxb.shape[:2]
        ids = ids_ref[...].astype(F32)
        r = lax.broadcasted_iota(jnp.int32, (group * 8, tok), 0)
        e_of = rem(r, 8)
        expert = jnp.where(e_of < OWN, first_expert(r // 8) + e_of, -1).astype(F32)
        member = jnp.zeros((group * 8, tok), F32)
        for j in range(ids.shape[0]):
            member = member + (jnp.broadcast_to(ids[j:j + 1, :], member.shape) == expert).astype(F32)
        before = dot(member.astype(BF16), strict_upper(tok))
        key_s[...] = jnp.where(member > 0.0, before, -1.0).reshape(key_s.shape)
        rr = lax.broadcasted_iota(jnp.int32, (places, tok), 0)
        at, e_row = rem(rr, cap).astype(F32), rr // cap
        some = rows // places

        @pl.loop(0, OWN)
        def _(e):
            got = dxb.at[:, own_rows(e)]
            pltpu.make_async_copy(got, got, drecv.at[e]).wait()

        own_val.wait()

        @each_other
        def _(k):
            val_copy(k).wait()

        bufs = (xb, gb)
        loads = [pltpu.make_async_copy(dxb.at[pl.ds(i * some, some)], bufs[i % 2].reshape(some, places, hidden), lsem.at[i % 2]) for i in range(group // some)]
        vals = pltpu.make_async_copy(valb, vb, lsem.at[2])
        vals.start()
        loads[0].start()
        for i, load in enumerate(loads):
            for later in loads[i + 1:i + 2]:
                later.start()

            @pl.loop(0, some)
            def _(k):
                key = key_s[i * some + k]
                mine = jnp.full((places, tok), -1.0, F32)
                for e in range(OWN):
                    mine = jnp.where(e_row == e, jnp.broadcast_to(key[e:e + 1, :], (places, tok)), mine)
                sb[pl.ds(pl.multiple_of(k * places, places), places), :] = (at == mine).astype(F32).astype(BF16)

            load.wait()
            part = dot_tn(sb[...], bufs[i % 2][...])
            acc_s[...] = acc_s[...] + part if i else part

        in_grad_ref[...] = acc_s[...].astype(BF16)
        vals.wait()

        def gate_step(k, total):
            for e in range(OWN):
                row = vb[e, pl.ds(k, 1), :]
                total = total + jnp.where(ids == (first_expert(k) + e).astype(F32), jnp.broadcast_to(row, ids.shape), 0.0)
            return total

        gate_ref[...] = lax.fori_loop(0, group, gate_step, jnp.zeros(ids.shape, F32))
        results = [pltpu.make_async_copy(a, b, load_sem.at[i]) for i, a, b in ((0, in_grad_ref, in_grad_hbm), (1, gate_ref, gate_hbm))]
        for copy in results:
            copy.start()

        step((TWO,), 1, ONE)

        def keep(e, m, to, then_remote, then_local):
            src = r1.at[0, e, to // 2, m, pl.ds(to % 2 * d_loc, d_loc)]
            dst = grads.at[m, y * OWN + e]

            @pl.when(y != to)
            def _():
                then_remote(remote(src, dst, ysend.at[e, m, to], yrecv.at[e, m, y], {"y": to}))

            @pl.when(y == to)
            def _():
                then_local(pltpu.make_async_copy(src, dst, ysend.at[e, m, to]))

        @pl.loop(0, OWN)
        def _(e):
            for kind in range(ONE, HOPS):
                for way in (0, 1):
                    hop(e, way, kind).wait_recv()
                add_into(half_of(r1, 0, e, kind), half_of(r1, 1, e, kind), half_of(G, e, z, kind))
                m, h = (kind - ONE) // 2, (kind - ONE) % 2
                for to in (2 * h, 2 * h + 1):
                    keep(e, m, to, start, start)

        @pl.loop(0, OWN)
        def _(e):
            for m in range(3):
                for at in range(NY):
                    def both(copy):
                        wait(grads.at[m, at * OWN + e], yrecv.at[e, m, at])
                        copy.wait_send()

                    keep(e, m, at, both, lambda copy: copy.wait())
            for way in (0, 1):
                for kind in range(HOPS):
                    hop(e, way, kind).wait_send()

            sent = dxs.at[e, pl.ds(0, (GROUP - 1) * cap)]
            pltpu.make_async_copy(sent, sent, dsend.at[e]).wait()

        for copy in results:
            copy.wait()

    weight_copies, last_weights = [], []
    pl.run_scoped(gather, *scope_one)
    pl.run_scoped(reduce, *scope_two)
    for number, group, part in weight_copies:
        ref = wown.at[0, pl.ds(*PIECE[group, part])]
        remote(ref, ref, send_sem.at[number], relay_recv.at[0], targets["core"]).wait_send()


def layer(cap, x, u, ids, gates, w1, w3, w2):
    tok, hidden = x.shape
    local_experts, d_loc, ff = w1.shape
    rows = GROUP * cap
    half = hidden // NZ // 2
    cut = tok - tok // 8 if tok % 256 == 0 else tok
    halves = [cut // 2] * 2 + [tok - cut // 2] * 2
    spans = {kind: (sum(halves[:i]), halves[i]) for i, kind in enumerate(KINDS)}
    order = gather_order({kind: 2 * hidden * n for kind, (_, n) in spans.items()}, 2 * w1.size * 3 // local_experts)
    sends = sum(len(s) for _, s in order)
    dma, v, shape = pltpu.SemaphoreType.DMA, pltpu.VMEM, jax.ShapeDtypeStruct
    far = lambda lanes: shape((OWN - 1, rows, lanes), BF16)
    near = lambda lanes: v((rows, lanes), BF16)
    stage = lambda lanes: v((2, OWN - 1, 2 * cap, lanes), BF16)
    sums = [v((2, OWN, 2, 3, half, ff), F32)] * 3
    scope_one = [v((GROUP, 2 * tok, hidden), BF16), v((tok, tok), BF16), stage(hidden), stage(hidden), stage(hidden), stage(tok)]
    scope_two = [v((OWN, NZ, 2, 3, half, ff), F32), v((2, OWN, 3, half, ff), F32)] + sums
    per_expert = v((OWN, GROUP, tok), F32)
    gate_rows = v((GROUP, OWN, tok), F32)
    outs = pl.pallas_call(
        functools.partial(layer_kernel, order, cap, spans, scope_one, scope_two),
        name="layer",
        out_shape=(
            shape((3, local_experts, d_loc, ff), F32), shape((tok, hidden), BF16), shape(ids.shape, F32),
            shape((GROUP, OWN * cap, hidden), BF16), shape((OWN, GROUP, tok), F32), shape((OWN, rows, hidden), BF16),
            far(hidden), far(hidden), far(hidden), far(tok),
        ),
        in_specs=[ANY] * 7,
        out_specs=(ANY,) * 10,
        scratch_shapes=[
            v(ids.shape, ids.dtype), v(ids.shape, F32), v((tok, hidden), BF16), v(ids.shape, F32), gate_rows, gate_rows, v((NY, OWN, 3, d_loc, ff), BF16), v((NZ, NY, OWN, 3, d_loc, ff), BF16), v((OWN, 3, d_loc, ff), BF16),
            near(hidden), near(hidden), near(hidden), near(tok), near(ff), near(ff), near(ff), v((rows, 1), F32),
            near(hidden), per_expert, per_expert, v((GROUP, 8, tok), F32), v((tok, hidden), F32),
            dma((len(KINDS), NY * NX)), dma((len(KINDS), NY * NX)), dma((NZ, NY, 2, 2)), dma((len(RELAYS),)), dma((GROUP,)), dma((sends,)), dma((GROUP,)),
            dma((7,)), dma((2, 4)),
            dma((4,)), dma((2, OWN, HOPS)), dma((2, OWN, HOPS)), dma((OWN, 3, NY)), dma((OWN, 3, NY)),
            dma((OWN,)), dma((OWN,)), dma((2, GROUP)), dma((1,)), pltpu.SemaphoreType.REGULAR,
        ],
        compiler_params=params(0),
    )(x, u, ids, gates, w1, w3, w2)
    return outs[:3]


def finish_kernel(grads, in_grad, gate, *refs):
    n = 5
    outs, bufs, sems = refs[:n], refs[n:2 * n], refs[-1]
    ins = [grads.at[m] for m in range(3)] + [in_grad, gate]
    load = [pltpu.make_async_copy(a, b, sems.at[0, i]) for i, (a, b) in enumerate(zip(ins, bufs))]
    store = [pltpu.make_async_copy(b, o, sems.at[1, i]) for i, (b, o) in enumerate(zip(bufs, outs))]
    for copy in load:
        copy.start()
    for i in range(n):
        load[i].wait()
        store[i].start()
    for copy in store:
        copy.wait()


def finish(grads, in_grad, gate):
    shapes = [grads.shape[1:]] * 3 + [in_grad.shape, gate.shape]
    types = [grads.dtype] * 3 + [in_grad.dtype, gate.dtype]
    return pl.pallas_call(
        finish_kernel,
        name="finish",
        out_shape=[jax.ShapeDtypeStruct(s, t) for s, t in zip(shapes, types)],
        in_specs=[ANY] * 3,
        out_specs=[ANY] * len(shapes),
        scratch_shapes=[pltpu.VMEM(s, t) for s, t in zip(shapes, types)] + [pltpu.SemaphoreType.DMA((2, len(shapes)))],
    )(grads, in_grad, gate)


def solution(mesh):
    mesh4 = Mesh(mesh.devices.reshape(NZ, NY, NX, NC), ("z", "y", "x", "core"))
    tok_spec = P(("z", "y", "x", "core"), None)
    up_spec = P(("x", "core"), ("z", "y"), None)
    down_spec = P(("x", "core"), None, ("z", "y"))

    def per_device(layer_in, out_grad, expert_ids, gate_vals, w_one, w_two, w_three):
        tok_dev, hidden = layer_in.shape
        top_k = expert_ids.shape[1]
        local_experts, d_loc, ff = w_one.shape
        cap = capacity_of(tok_dev, top_k, local_experts * NX * NC)
        ids = expert_ids.T
        grads, in_grad, gate_out = layer(cap, layer_in, out_grad, ids, gate_vals.T, w_one, w_three, w_two.swapaxes(1, 2))
        g1, g3, g2, in_grad, gate_out = finish(grads, in_grad, gate_out)
        return in_grad, gate_out.T, g1, g2.swapaxes(1, 2), g3

    return jax.shard_map(per_device, mesh=mesh4, in_specs=(tok_spec, tok_spec, tok_spec, tok_spec, up_spec, down_spec, up_spec), out_specs=(tok_spec, tok_spec, up_spec, down_spec, up_spec), check_vma=False)
```

```python
import functools

import jax
import jax.numpy as jnp
from jax import lax
from jax.experimental import pallas as pl
from jax.experimental.pallas import tpu as pltpu
from jax.sharding import Mesh, PartitionSpec as P

NZ, NY, NX, NC = 8, 4, 4, 2
GROUP = NY * NX * NC
PLANE = ("y", "x", "core")
OWN = 4
F32, BF16 = jnp.float32, jnp.bfloat16
ANY = pl.BlockSpec(memory_space=pl.ANY)


def capacity_of(tok_dev, top_k, experts):
    return max(8, ((tok_dev * top_k * 5) // (4 * experts) + 7) // 8 * 8)


def rem(a, b):
    return a % b if isinstance(a, int) else lax.rem(a, b)


def contract(ca, cb):
    return lambda a, b: lax.dot_general(a, b, (((ca,), (cb,)), ((), ())), preferred_element_type=F32)


dot, dot_nt, dot_tn = contract(1, 0), contract(1, 1), contract(0, 0)


def params(number):
    return pltpu.CompilerParams(collective_id=number, has_side_effects=True, vmem_limit_bytes=67043328)


def each_other(body):
    return pl.loop(1, GROUP)(body)


def strict_upper(n):
    rows = lax.broadcasted_iota(jnp.int32, (n, n), 0)
    cols = lax.broadcasted_iota(jnp.int32, (n, n), 1)
    return (rows < cols).astype(F32).astype(BF16)


def here():
    return tuple(lax.axis_index(a) for a in ("z", "y", "x", "core"))


def at_offset(k):
    _, y, x, c = here()
    dy, dx, dc = k // (NX * NC), rem(k // NC, NX), rem(k, NC)
    return {"y": rem(y + dy, NY), "x": rem(x + dx, NX), "core": rem(c + dc, NC)}


def place_of(d):
    return d["y"] * (NX * NC) + d["x"] * NC + d["core"]


def z_at(dz):
    return {"z": rem(lax.axis_index("z") + dz, NZ)}


def remote(src, dst, send_sem, recv_sem, target):
    return pltpu.make_async_remote_copy(src_ref=src, dst_ref=dst, send_sem=send_sem, recv_sem=recv_sem, device_id=target, device_id_type=pl.DeviceIdType.MESH)


def start(copy):
    copy.start()


def tell(semaphore, targets):
    for target in targets:
        pl.semaphore_signal(semaphore, device_id=target, device_id_type=pl.DeviceIdType.MESH)


RATE, D2D, HOP = 44700.0, 400000.0, 2.3
PUT, TILE, ROWS = 1.0, 1.0, 0.4
STEP = 5
AHEAD, MORE = 5.0, 0.05

PIECE = {(0, None): (0, 1), (1, None): (1, 3), (1, 0): (1, 1), (1, 1): (2, 2)}
RELAYS = ((0, None, "y+"), (1, 0, "y+"), (1, 1, "y-"))


KINDS = ("A0", "A1", "B0", "B1")


def gather_order(sizes, expert_bytes):
    free, pending, coming, order, have, ready = {}, {}, [], [], {}, {}

    def send(now, name, link, arrives, nbytes):
        t = max(now, free.get(link, 0.0)) + nbytes / (D2D if link == "core" else RATE)
        free[link] = t
        coming.append((t + (HOP / 2 if link == "core" else HOP), len(order), len(coming), arrives))
        return (name, link)

    def later(rank, name, link, arrives, nbytes):
        queue = pending.setdefault(link, [])
        queue.append((rank, len(order), len(queue), (name, link, arrives, nbytes)))

    def turn(now):
        out = []
        for link, queue in pending.items():
            queue.sort()
            while queue and free.get(link, 0.0) - now < AHEAD + MORE * now:
                out.append(send(now, *queue.pop(0)[-1]))
        return out

    def on_rows(kind, dy, dx):
        first, second = "xy" if kind[0] == "A" else "yx"
        d = {"x": dx, "y": dy}
        for axis in [first, second] if d[second] == 0 else [second]:
            for sign in (1, -1):
                if d[axis] == 0 or d[axis] == -sign % 4 and kind[1] == "10"[sign > 0]:
                    nd = dict(d)
                    nd[axis] = (d[axis] - sign) % 4
                    rank = 4 + (axis == second) + (d[axis] != 0)
                    later(rank, (kind, dy, dx), axis + "-+"[sign > 0], (kind, nd["y"], nd["x"]), sizes[kind])

    def core(now, key):
        return send(now, key, "core", ("core",) + key, sizes[key[0]])

    def weights(rank, name, group, part, link, arrives):
        later(rank, name, link, arrives + (group, part), PIECE[group, part][1] * expert_bytes)

    def on_piece(dz, dy, group):
        for link, step, far in (("z+", -1, dy < 2), ("z-", 1, dy >= 2)):
            gone = (step * dz) % NZ
            if gone < 3 + far:
                weights(4 * group + gone, ("W", dz, dy, group), group, None, link, ("W", (dz + step) % NZ, dy))

    def arrived(key, part=None):
        have[key] = have.get(key, 0) + (2 if part is None else 1)
        if have[key] == 2:
            ready[key] = True
        return have[key] == 2

    for i, (group, part, link) in enumerate(RELAYS):
        weights(0, ("r", i), group, part, link, ("R", i))
    for group in range(2):
        for dy, link in ((1, "y+"), (3, "y-")):
            weights(2, ("w", dy, group), group, None, link, ("W", 0, (-dy) % NY))
        on_piece(0, 0, group)
    sends = []
    for kind in KINDS[::-1]:
        arrived((kind, 0, 0))
        on_rows(kind, 0, 0)
        sends.append(core(0.0, (kind, 0, 0)))
    order.append((None, turn(0.0) + sends))
    todo, puts, done, now = [(dy, dx) for dy in range(NY) for dx in range(NX)], 0, 0, 0.0
    while coming or todo or done < puts:
        coming.sort()
        soon = coming[0][0] if coming else 1e9
        if soon > now:
            place = next((p for p in todo if all(pre + (kind,) + p in ready for kind in KINDS for pre in ((), ("core",)))), None)
            if place is not None:
                todo.remove(place)
                order.append((("put",) + place, turn(now)))
                puts += 1
                now += PUT
                continue
            step = min(STEP, puts - done)
            weights_in = sum(key[0] == "W" and key[-1] == 0 for key in ready) == NZ * NY - 1
            calm = all(c[-1][0] == "core" for c in coming)
            if weights_in and step and (step >= 3 and soon - now > TILE or calm):
                order.append((("tile", done, done + step), turn(now)))
                done += step
                now += TILE + ROWS * step
                continue
        t, _, _, name = coming.pop(0)
        now = max(now, t)
        if name[0] == "core":
            arrived(name)
            continue
        sends = []
        if name[0] == "R":
            i, group, part = name[1:]
            weights(1, name[:2], group, part, RELAYS[i][2], ("W", 0, 2))
            name = name[:2]
        elif name[0] == "W":
            if arrived(name[:-1], name[-1]):
                on_piece(*name[1:-1])
        else:
            sends = [core(now, name)]
            arrived(name)
            on_rows(*name)
        order.append((name, sends + turn(now)))
    return order


def passed_on(dz, dy):
    return dz != NZ // 2 and dz not in ((3,) if dy < 2 else (5,))


def first_expert(d):
    return rem(d, NX * NC) * (NY * OWN) + d // (NX * NC) * OWN


FAR, SUM3, NEW3, TWO, ONE, HOPS = 0, 1, 2, 3, 4, 16


def layer_kernel(order, cap, spans, scope_one, scope_two, x_hbm, u_hbm, ids_hbm, gates_hbm, w1_hbm, w3_hbm, w2_hbm,
                 grads, in_grad_hbm, gate_hbm, dxb, valb, dxs, xr, ur, gr, sel,
                 ids_ref, gates_ref, in_grad_ref, gate_ref, metas, gates_out, wown, wv, relay, xb, ub, gb, sb, a_s, d1_s, d3_s, y_s, dx_s, val_s, vb, key_s, acc_s,
                 recv, core_recv, wrecv, relay_recv, mrecv, send_sem, msend, load_sem, store_sem,
                 lsem, rsend, rrecv, ysend, yrecv, dsend, drecv, vsem, osem, in_scope, in_plane):
    z, y, x, c = here()
    tok, hidden = x_hbm.shape
    rows, ff = xb.shape[0], a_s.shape[-1]
    d_loc = hidden // (NZ * NY)
    me = place_of(at_offset(0))

    def place(dy, dx, dc=0):
        return place_of(at_offset(dy * (NX * NC) + dx * NC + dc))

    targets = {"core": {"core": 1 - c}}
    for sign, n in (("+", 1), ("-", -1)):
        targets["x" + sign] = {"x": rem(x + n + NX, NX)}
        targets["y" + sign] = {"y": rem(y + n + NY, NY)}
        targets["z" + sign] = z_at(n + NZ)

    def wait(ref, sem):
        remote(ref, ref, send_sem.at[0], sem, targets["core"]).wait_recv()

    def piece(dz, dy, group, part=None):
        return wv.at[z_at(dz)["z"], rem(y + dy, NY), pl.ds(*PIECE[group, part])]

    def wait_weights(dz, dy, group, part):
        wait(piece(dz, dy, group, part), wrecv.at[dz, dy, group, part or 0])

    def w(e, m):
        return wv[:, :, e, m].reshape(hidden, ff)

    def expert_rows(e, spans):
        def cut_of(ref):
            return jnp.concatenate([ref[s, :] for s in spans]) if spans[1:] else ref[spans[0], :]

        def save(ref, value):
            n = value.shape[0] // len(spans)
            for i, s in enumerate(spans):
                ref[s, :] = value[i * n:(i + 1) * n]

        x_rows = cut_of(xb)
        h1, h3 = dot(x_rows, w(e, 0)), dot(x_rows, w(e, 1))
        sig = jax.nn.sigmoid(h1)
        silu = h1 * sig
        act = (silu * h3).astype(BF16)
        save(a_s, act)
        y_rows = dot_nt(act, w(e, 2))
        save(y_s, jnp.sum(cut_of(ub).astype(F32) * y_rows, axis=1, keepdims=True))
        da = dot(cut_of(gb), w(e, 2))
        d1 = (da * h3 * sig * (1.0 + h1 * (1.0 - sig))).astype(BF16)
        d3 = (da * silu).astype(BF16)
        save(d1_s, d1)
        save(d3_s, d3)
        save(dx_s, (dot_nt(d1, w(e, 0)) + dot_nt(d3, w(e, 1))).astype(BF16))

    def gather(all_rows, tri, sx, su, sg, ss):
        loads = [
            pltpu.make_async_copy(x_hbm, all_rows.at[me, pl.ds(0, tok)], load_sem.at[0]),
            pltpu.make_async_copy(u_hbm, all_rows.at[me, pl.ds(tok, tok)], load_sem.at[1]),
        ]
        for m, ref in enumerate((w1_hbm, w3_hbm, w2_hbm)):
            loads.append(pltpu.make_async_copy(ref.reshape(NY, OWN, d_loc, ff), wown.at[:, :, m], load_sem.at[2 + m]))
        tables = [pltpu.make_async_copy(a, b, load_sem.at[i]) for i, a, b in ((5, ids_hbm, ids_ref), (6, gates_hbm, gates_ref))]
        for copy in tables + loads:
            copy.start()
        barrier = pltpu.get_barrier_semaphore()
        tell(barrier, targets.values())
        for copy in tables:
            copy.wait()

        @pl.loop(0, GROUP)
        def _(d):
            number = first_expert(d) + lax.broadcasted_iota(jnp.int32, (OWN, tok), 0)
            value = jnp.full((OWN, tok), -1.0, F32)
            for j in range(ids_ref.shape[0]):
                chosen = ids_ref[pl.ds(j, 1), :] == number
                value = jnp.where(chosen, jnp.broadcast_to(gates_ref[pl.ds(j, 1), :], value.shape), value)
            gates_out[d] = value

        metas[me] = gates_out[me]
        tri[...] = strict_upper(tok)
        for copy in loads:
            copy.wait()
        pl.semaphore_wait(barrier, len(targets))

        back = {"x+": (0, 3), "x-": (0, 1), "y+": (3, 0), "y-": (1, 0)}
        def block(kind, dy, dx, dc=0):
            return all_rows.at[place(dy, dx, dc), pl.ds(*spans[kind])]

        row_copies = []

        def issue(name, link):
            number = len(row_copies) + len(weight_copies)
            sem = send_sem.at[number]
            group, part_of = None, None
            if name[0] == "w":
                _, dy, group = name
                src = wown.at[rem(y + dy, NY), pl.ds(*PIECE[group, None])]
                copy = remote(src, piece(0, 0, group), sem, wrecv.at[0, (-dy) % NY, group, 0], targets[link])
            elif name[0] in "rR":
                group, part_of, _ = RELAYS[name[1]]
                span = pl.ds(*PIECE[group, part_of])
                if name[0] == "r":
                    copy = remote(wown.at[rem(y + 2, NY), span], relay.at[span], sem, relay_recv.at[name[1]], targets[link])
                else:
                    dst = piece(0, back[link][0], group, part_of)
                    copy = remote(relay.at[span], dst, sem, wrecv.at[0, 2, group, part_of or 0], targets[link])
            elif name[0] == "W":
                _, dz, dy, group = name
                ndz = (dz - 1) % NZ if link == "z+" else (dz + 1) % NZ
                own = wown.at[y, pl.ds(*PIECE[group, None])]
                copy = remote(own if dz == dy == 0 else piece(dz, dy, group), piece(dz, dy, group), sem, wrecv.at[ndz, dy, group, 0], targets[link])
            else:
                kind, dy, dx = name
                ref = block(*name)
                oy, ox = back.get(link, (0, 0))
                arrivals = core_recv if link == "core" else recv
                rsem = arrivals.at[KINDS.index(kind), (dy + oy) % NY * NX + (dx + ox) % NX]
                copy = remote(ref, ref, sem, rsem, targets[link])
            copy.start()
            if group is None:
                row_copies.append(copy)
            else:
                weight_copies.append((number, group, part_of))

        def meta_copy(k):
            to = at_offset(k)
            return remote(gates_out.at[place_of(to)], metas.at[me], msend.at[k], mrecv.at[k], to)

        n_rows = OWN * 2 * cap
        stores, chips = [], []

        def put(dy, dx):
            slot = len(stores) % 2
            if stores[1:]:
                for copy in stores[-2]:
                    copy.wait()
            for dc in (0, 1):
                if dy or dx or dc:
                    k = ((-dy) % NY) * (NX * NC) + ((-dx) % NX) * NC + dc
                    wait(metas.at[place(dy, dx, dc)], mrecv.at[k])
            for i, kind in enumerate(KINDS):
                wait(block(kind, dy, dx, 1), core_recv.at[i, dy * NX + dx])
            chip = rem(y + dy, NY) * NX + rem(x + dx, NX)
            n = 2 * OWN
            which = lax.broadcasted_iota(jnp.int32, (n, tok), 0)
            gate = jnp.zeros((n, tok), F32)
            for i in range(n):
                gate = jnp.where(which == i, jnp.broadcast_to(metas[2 * chip + i // OWN, pl.ds(i % OWN, 1), :], gate.shape), gate)
            member = gate >= 0.0
            key = jnp.where(member, dot(member.astype(F32).astype(BF16), tri[...]), -1.0)
            r = lax.broadcasted_iota(jnp.int32, (n_rows, tok), 0)
            at = rem(r, cap).astype(F32)
            row_of = rem(r // cap, 2) * OWN + r // (2 * cap)
            mine, gates = jnp.full((n_rows, tok), -1.0, F32), jnp.zeros((n_rows, tok), F32)
            for i in range(n):
                mine = jnp.where(row_of == i, jnp.broadcast_to(key[i:i + 1, :], mine.shape), mine)
                gates = jnp.where(row_of == i, jnp.broadcast_to(gate[i:i + 1, :], mine.shape), gates)
            found = at == mine
            pick = [jnp.logical_and(found, row_of // OWN == p).astype(F32) for p in range(2)]
            both = pick[0] + pick[1]
            scale = jnp.sum(both * gates, axis=1, keepdims=True)
            pick = [p.astype(BF16) for p in pick]
            x_rows = dot(pick[0], all_rows[2 * chip, 0:tok, :]) + dot(pick[1], all_rows[2 * chip + 1, 0:tok, :])
            u_rows = dot(pick[0], all_rows[2 * chip, tok:2 * tok, :]) + dot(pick[1], all_rows[2 * chip + 1, tok:2 * tok, :])
            span = pl.ds(pl.multiple_of(chip * 2 * cap, 2 * cap), 2 * cap)
            out = []
            for i, (value, first, stage, far) in enumerate(((x_rows, xb, sx, xr), (u_rows, ub, su, ur), (scale * u_rows, gb, sg, gr), (both, sb, ss, sel))):
                value = value.astype(BF16)
                first[span, :] = value[:2 * cap]
                stage[slot] = value[2 * cap:].reshape(stage.shape[1:])
                out.append(pltpu.make_async_copy(stage.at[slot], far.at[:, span], store_sem.at[slot, i]))
                out[-1].start()
            stores.append(out)
            chips.append(span)

        for name, sends in order:
            if name is None:
                pass
            elif name[0] == "put":
                put(*name[1:])
            elif name[0] == "tile":
                expert_rows(0, chips[name[1]:name[2]])
            elif name[0] == "R":
                group, part, _ = RELAYS[name[1]]
                wait(relay.at[pl.ds(*PIECE[group, part])], relay_recv.at[name[1]])
            elif name[0] == "W":
                if passed_on(*name[1:3]) or not name[3]:
                    wait_weights(*name[1:])
                else:
                    last_weights.append(name[1:])
            else:
                kind, dy, dx = name
                wait(block(*name), recv.at[KINDS.index(kind), dy * NX + dx])
            for send in sends:
                issue(*send)
            if name is None:
                wv[z, y] = wown[y]
                near = [t for link, t in targets.items() if link[0] != "z"]
                for far in range(NY // 2 + NX // 2):
                    tell(in_plane.at[far], near)
                    pl.semaphore_wait(in_plane.at[far], len(near))

                @each_other
                def _(k):
                    meta_copy(k).start()

        for out in stores[-2:]:
            for copy in out:
                copy.wait()

        @each_other
        def _(k):
            meta_copy(k).wait_send()

        for copy in row_copies:
            copy.wait_send()

    def reduce(G, r4, r3, r2, r1):
        tell(in_scope, [targets["z+"], targets["z-"]])

        def row_loads(e):
            pairs = ((xr, xb), (gr, gb), (ur, ub), (sel, sb))
            return [pltpu.make_async_copy(src.at[e - 1], dst, lsem.at[i]) for i, (src, dst) in enumerate(pairs)]

        def chunk(e, way, dist):
            return G.at[e, z_at(dist if way else NZ - dist)["z"]]

        def part_of(ref, way, e, kind):
            m, q = (kind - ONE) // NY, (kind - ONE) % NY
            return ref.at[way, e, q // 2, m, pl.ds(q % 2 * d_loc, d_loc)]

        def hop(e, way, kind):
            h = way
            src, dst = {
                FAR: lambda: (chunk(e, way, 4).at[h], r4.at[way, e]),
                SUM3: lambda: (r4.at[way, e], r3.at[way, e, h]),
                NEW3: lambda: (chunk(e, way, 3).at[1 - h], r3.at[way, e, 1 - h]),
                TWO: lambda: (r3.at[way, e], r2.at[way, e]),
            }.get(kind, lambda: (part_of(r2, way, e, kind), part_of(r1, way, e, kind)))()
            return remote(src, dst, rsend.at[way, e, kind], rrecv.at[way, e, kind], z_at(1 if way else NZ - 1))

        def add_into(dst, *others):
            parts = dst.shape[:-2]
            if not parts:
                total = dst[...]
                for other in others:
                    total = total + other[...]
                dst[...] = total
                return

            def flat(ref, i):
                index = []
                for n in reversed(parts):
                    index.append(rem(i, n))
                    i = i // n
                return ref.at[tuple(reversed(index))]

            n = 1
            for p in parts:
                n *= p

            @pl.loop(0, n)
            def _(i):
                total = flat(dst, i)[...]
                for other in others:
                    total = total + flat(other, i)[...]
                flat(dst, i)[...] = total

        def own_rows(s):
            return pl.ds(pl.multiple_of(s * cap, 8), cap)

        def dx_copy(e, k):
            to = at_offset(k)
            return remote(dxs.at[e, own_rows(place_of(to))], dxb.at[me, own_rows(e)], dsend.at[e], drecv.at[e], to)

        tile = 256 if rows % 256 == 0 else rows
        dtile = hidden // NZ
        half = dtile // 2

        def weight_gradients(e):
            out = pltpu.make_async_copy(dx_s, dxs.at[e], osem.at[0])
            out.start()

            @pl.loop(0, NZ // 2)
            def _(i):
                pair = [z_at(n + 2 * i)["z"] for n in (3, 4)]

                def cols(ref):
                    return jnp.concatenate([ref[:, pl.ds(pl.multiple_of(k * dtile, dtile), dtile)] for k in pair], axis=1)

                x_cols, g_cols = cols(xb), cols(gb)
                for m, part in enumerate((dot_tn(x_cols, d1_s[...]), dot_tn(x_cols, d3_s[...]), dot_tn(g_cols, a_s[...]))):
                    for j in range(4):
                        G[e, pair[j // 2], j % 2, m] = part[j * half:(j + 1) * half]

                @pl.when(i == 0)
                def _():
                    if isinstance(e, int):
                        pl.semaphore_wait(in_scope, 2)
                    for way, kind in ((0, FAR), (1, FAR), (1, NEW3)):
                        hop(e, way, kind).start()

                @pl.when(i == 1)
                def _():
                    hop(e, 0, NEW3).start()

            val = sb[...].astype(F32) * y_s[...]
            val_s[e] = jnp.sum(val.reshape(rows // cap, cap, tok), axis=1)
            out.wait()

        def send_back(e):
            pltpu.make_async_copy(dxs.at[e, own_rows(me)], dxb.at[me, own_rows(e)], drecv.at[e]).start()

            @each_other
            def _(k):
                dx_copy(e, k).start()

        def far_sums(e):
            for way in (0, 1):
                hop(e, way, FAR).wait_recv()
                add_into(r4.at[way, e], chunk(e, way, 3).at[way])
                hop(e, way, SUM3).start()

        weight_gradients(0)
        for copy in row_loads(1):
            copy.start()
        send_back(0)
        for name in last_weights:
            wait_weights(*name)

        @pl.loop(1, OWN)
        def _(e):
            for copy in row_loads(e):
                copy.wait()

            @pl.loop(0, rows // tile)
            def _(i):
                expert_rows(e, [pl.ds(pl.multiple_of(i * tile, tile), tile)])

            weight_gradients(e)

            @pl.when(e < OWN - 1)
            def _():
                for copy in row_loads(e + 1):
                    copy.start()

            send_back(e)
            far_sums(e - 1)

        far_sums(OWN - 1)

        def val_copy(k):
            to = at_offset(k)
            return remote(val_s.at[:, place_of(to)], valb.at[:, me], vsem.at[0, k], vsem.at[1, k], to)

        own_val = pltpu.make_async_copy(val_s.at[:, me], valb.at[:, me], vsem.at[0, 0])
        own_val.start()

        @each_other
        def _(k):
            val_copy(k).start()

        def step(arrived, dist, leaves):
            @pl.loop(0, OWN)
            def _(e):
                for way in (0, 1):
                    for kind in arrived:
                        hop(e, way, kind).wait_recv()
                    if leaves == TWO:
                        add_into(r3.at[way, e], chunk(e, way, dist))
                        hop(e, way, TWO).start()
                if leaves == ONE:
                    for kind in range(ONE, HOPS):
                        for way in (0, 1):
                            add_into(part_of(r2, way, e, kind), part_of(G, e, z_at(dist if way else NZ - dist)["z"], kind))
                            hop(e, way, kind).start()

        step((SUM3, NEW3), 2, TWO)

        group, places = dxb.shape[:2]
        ids = ids_ref[...].astype(F32)
        r = lax.broadcasted_iota(jnp.int32, (group * 8, tok), 0)
        e_of = rem(r, 8)
        expert = jnp.where(e_of < OWN, first_expert(r // 8) + e_of, -1).astype(F32)
        member = jnp.zeros((group * 8, tok), F32)
        for j in range(ids.shape[0]):
            member = member + (jnp.broadcast_to(ids[j:j + 1, :], member.shape) == expert).astype(F32)
        before = dot(member.astype(BF16), strict_upper(tok))
        key_s[...] = jnp.where(member > 0.0, before, -1.0).reshape(key_s.shape)
        rr = lax.broadcasted_iota(jnp.int32, (places, tok), 0)
        at, e_row = rem(rr, cap).astype(F32), rr // cap
        some = rows // places

        @pl.loop(0, OWN)
        def _(e):
            got = dxb.at[:, own_rows(e)]
            pltpu.make_async_copy(got, got, drecv.at[e]).wait()

        own_val.wait()

        @each_other
        def _(k):
            val_copy(k).wait()

        bufs = (xb, gb)
        loads = [pltpu.make_async_copy(dxb.at[pl.ds(i * some, some)], bufs[i % 2].reshape(some, places, hidden), lsem.at[i % 2]) for i in range(group // some)]
        vals = pltpu.make_async_copy(valb, vb, lsem.at[2])
        vals.start()
        loads[0].start()
        for i, load in enumerate(loads):
            for later in loads[i + 1:i + 2]:
                later.start()

            @pl.loop(0, some)
            def _(k):
                key = key_s[i * some + k]
                mine = jnp.full((places, tok), -1.0, F32)
                for e in range(OWN):
                    mine = jnp.where(e_row == e, jnp.broadcast_to(key[e:e + 1, :], (places, tok)), mine)
                sb[pl.ds(pl.multiple_of(k * places, places), places), :] = (at == mine).astype(F32).astype(BF16)

            load.wait()
            part = dot_tn(sb[...], bufs[i % 2][...])
            acc_s[...] = acc_s[...] + part if i else part

        in_grad_ref[...] = acc_s[...].astype(BF16)
        vals.wait()

        def gate_step(k, total):
            for e in range(OWN):
                row = vb[e, pl.ds(k, 1), :]
                total = total + jnp.where(ids == (first_expert(k) + e).astype(F32), jnp.broadcast_to(row, ids.shape), 0.0)
            return total

        gate_ref[...] = lax.fori_loop(0, group, gate_step, jnp.zeros(ids.shape, F32))
        results = [pltpu.make_async_copy(a, b, load_sem.at[i]) for i, a, b in ((0, in_grad_ref, in_grad_hbm), (1, gate_ref, gate_hbm))]
        for copy in results:
            copy.start()

        step((TWO,), 1, ONE)

        def keep(e, m, to, then_remote, then_local):
            src = part_of(r1, 0, e, ONE + NY * m + to)
            dst = grads.at[m, y * OWN + e]

            @pl.when(y != to)
            def _():
                then_remote(remote(src, dst, ysend.at[e, m, to], yrecv.at[e, m, y], {"y": to}))

            @pl.when(y == to)
            def _():
                then_local(pltpu.make_async_copy(src, dst, ysend.at[e, m, to]))

        @pl.loop(0, OWN)
        def _(e):
            for kind in range(ONE, HOPS):
                for way in (0, 1):
                    hop(e, way, kind).wait_recv()
                add_into(part_of(r1, 0, e, kind), part_of(r1, 1, e, kind), part_of(G, e, z, kind))
                keep(e, (kind - ONE) // NY, (kind - ONE) % NY, start, start)

        @pl.loop(0, OWN)
        def _(e):
            for m in range(3):
                for at in range(NY):
                    def both(copy):
                        wait(grads.at[m, at * OWN + e], yrecv.at[e, m, at])
                        copy.wait_send()

                    keep(e, m, at, both, lambda copy: copy.wait())
            for way in (0, 1):
                for kind in range(HOPS):
                    hop(e, way, kind).wait_send()

            sent = dxs.at[e, pl.ds(0, (GROUP - 1) * cap)]
            pltpu.make_async_copy(sent, sent, dsend.at[e]).wait()

        for copy in results:
            copy.wait()

    weight_copies, last_weights = [], []
    pl.run_scoped(gather, *scope_one)
    pl.run_scoped(reduce, *scope_two)
    for number, group, part in weight_copies:
        ref = wown.at[0, pl.ds(*PIECE[group, part])]
        remote(ref, ref, send_sem.at[number], relay_recv.at[0], targets["core"]).wait_send()


def layer(cap, x, u, ids, gates, w1, w3, w2):
    tok, hidden = x.shape
    local_experts, d_loc, ff = w1.shape
    rows = GROUP * cap
    half = hidden // NZ // 2
    cut = tok - tok // 8 if tok % 256 == 0 else tok
    halves = [cut // 2] * 2 + [tok - cut // 2] * 2
    spans = {kind: (sum(halves[:i]), halves[i]) for i, kind in enumerate(KINDS)}
    order = gather_order({kind: 2 * hidden * n for kind, (_, n) in spans.items()}, 2 * w1.size * 3 // local_experts)
    sends = sum(len(s) for _, s in order)
    dma, v, shape = pltpu.SemaphoreType.DMA, pltpu.VMEM, jax.ShapeDtypeStruct
    far = lambda lanes: shape((OWN - 1, rows, lanes), BF16)
    near = lambda lanes: v((rows, lanes), BF16)
    stage = lambda lanes: v((2, OWN - 1, 2 * cap, lanes), BF16)
    sums = [v((2, OWN, 2, 3, half, ff), F32)] * 3
    scope_one = [v((GROUP, 2 * tok, hidden), BF16), v((tok, tok), BF16), stage(hidden), stage(hidden), stage(hidden), stage(tok)]
    scope_two = [v((OWN, NZ, 2, 3, half, ff), F32), v((2, OWN, 3, half, ff), F32)] + sums
    per_expert = v((OWN, GROUP, tok), F32)
    gate_rows = v((GROUP, OWN, tok), F32)
    outs = pl.pallas_call(
        functools.partial(layer_kernel, order, cap, spans, scope_one, scope_two),
        name="layer",
        out_shape=(
            shape((3, local_experts, d_loc, ff), F32), shape((tok, hidden), BF16), shape(ids.shape, F32),
            shape((GROUP, OWN * cap, hidden), BF16), shape((OWN, GROUP, tok), F32), shape((OWN, rows, hidden), BF16),
            far(hidden), far(hidden), far(hidden), far(tok),
        ),
        in_specs=[ANY] * 7,
        out_specs=(ANY,) * 10,
        scratch_shapes=[
            v(ids.shape, ids.dtype), v(ids.shape, F32), v((tok, hidden), BF16), v(ids.shape, F32), gate_rows, gate_rows, v((NY, OWN, 3, d_loc, ff), BF16), v((NZ, NY, OWN, 3, d_loc, ff), BF16), v((OWN, 3, d_loc, ff), BF16),
            near(hidden), near(hidden), near(hidden), near(tok), near(ff), near(ff), near(ff), v((rows, 1), F32),
            near(hidden), per_expert, per_expert, v((GROUP, 8, tok), F32), v((tok, hidden), F32),
            dma((len(KINDS), NY * NX)), dma((len(KINDS), NY * NX)), dma((NZ, NY, 2, 2)), dma((len(RELAYS),)), dma((GROUP,)), dma((sends,)), dma((GROUP,)),
            dma((7,)), dma((2, 4)),
            dma((4,)), dma((2, OWN, HOPS)), dma((2, OWN, HOPS)), dma((OWN, 3, NY)), dma((OWN, 3, NY)),
            dma((OWN,)), dma((OWN,)), dma((2, GROUP)), dma((1,)), pltpu.SemaphoreType.REGULAR, pltpu.SemaphoreType.REGULAR((NY // 2 + NX // 2,)),
        ],
        compiler_params=params(0),
    )(x, u, ids, gates, w1, w3, w2)
    return outs[:3]


def finish_kernel(grads, in_grad, gate, *refs):
    n = 5
    outs, bufs, sems = refs[:n], refs[n:2 * n], refs[-1]
    ins = [grads.at[m] for m in range(3)] + [in_grad, gate]
    load, store = [], []
    for i, (a, b, o) in enumerate(zip(ins, bufs, outs)):
        half = a.shape[0] // 2
        for h in range(2):
            at = pl.ds(h * half, half)
            load.append(pltpu.make_async_copy(a.at[at], b.at[at], sems.at[0, i, h]))
            store.append(pltpu.make_async_copy(b.at[at], o.at[at], sems.at[1, i, h]))
    for copy in load:
        copy.start()
    for before, after in zip(load, store):
        before.wait()
        after.start()
    for copy in store:
        copy.wait()


def finish(grads, in_grad, gate):
    shapes = [grads.shape[1:]] * 3 + [in_grad.shape, gate.shape]
    types = [grads.dtype] * 3 + [in_grad.dtype, gate.dtype]
    return pl.pallas_call(
        finish_kernel,
        name="finish",
        out_shape=[jax.ShapeDtypeStruct(s, t) for s, t in zip(shapes, types)],
        in_specs=[ANY] * 3,
        out_specs=[ANY] * len(shapes),
        scratch_shapes=[pltpu.VMEM(s, t) for s, t in zip(shapes, types)] + [pltpu.SemaphoreType.DMA((2, len(shapes), 2))],
    )(grads, in_grad, gate)


def solution(mesh):
    mesh4 = Mesh(mesh.devices.reshape(NZ, NY, NX, NC), ("z", "y", "x", "core"))
    tok_spec = P(("z", "y", "x", "core"), None)
    up_spec = P(("x", "core"), ("z", "y"), None)
    down_spec = P(("x", "core"), None, ("z", "y"))

    def per_device(layer_in, out_grad, expert_ids, gate_vals, w_one, w_two, w_three):
        tok_dev, hidden = layer_in.shape
        top_k = expert_ids.shape[1]
        local_experts, d_loc, ff = w_one.shape
        cap = capacity_of(tok_dev, top_k, local_experts * NX * NC)
        ids = expert_ids.T
        grads, in_grad, gate_out = layer(cap, layer_in, out_grad, ids, gate_vals.T, w_one, w_three, w_two.swapaxes(1, 2))
        g1, g3, g2, in_grad, gate_out = finish(grads, in_grad, gate_out)
        return in_grad, gate_out.T, g1, g2.swapaxes(1, 2), g3

    return jax.shard_map(per_device, mesh=mesh4, in_specs=(tok_spec, tok_spec, tok_spec, tok_spec, up_spec, down_spec, up_spec), out_specs=(tok_spec, tok_spec, up_spec, down_spec, up_spec), check_vma=False)
```

```python
import functools

import jax
import jax.numpy as jnp
from jax import lax
from jax.experimental import pallas as pl
from jax.experimental.pallas import tpu as pltpu
from jax.sharding import Mesh, PartitionSpec as P

NZ, NY, NX, NC = 8, 4, 4, 2
GROUP = NY * NX * NC
PLANE = ("y", "x", "core")
OWN = 4
F32, BF16 = jnp.float32, jnp.bfloat16
ANY = pl.BlockSpec(memory_space=pl.ANY)


def capacity_of(tok_dev, top_k, experts):
    return max(8, ((tok_dev * top_k * 5) // (4 * experts) + 7) // 8 * 8)


def rem(a, b):
    return a % b if isinstance(a, int) else lax.rem(a, b)


def contract(ca, cb):
    return lambda a, b: lax.dot_general(a, b, (((ca,), (cb,)), ((), ())), preferred_element_type=F32)


dot, dot_nt, dot_tn = contract(1, 0), contract(1, 1), contract(0, 0)


def params(number):
    return pltpu.CompilerParams(collective_id=number, has_side_effects=True, vmem_limit_bytes=67043328)


def each_other(body):
    return pl.loop(1, GROUP)(body)


def strict_upper(n):
    rows = lax.broadcasted_iota(jnp.int32, (n, n), 0)
    cols = lax.broadcasted_iota(jnp.int32, (n, n), 1)
    return (rows < cols).astype(F32).astype(BF16)


def here():
    return tuple(lax.axis_index(a) for a in ("z", "y", "x", "core"))


def at_offset(k):
    _, y, x, c = here()
    dy, dx, dc = k // (NX * NC), rem(k // NC, NX), rem(k, NC)
    return {"y": rem(y + dy, NY), "x": rem(x + dx, NX), "core": rem(c + dc, NC)}


def place_of(d):
    return d["y"] * (NX * NC) + d["x"] * NC + d["core"]


def z_at(dz):
    return {"z": rem(lax.axis_index("z") + dz, NZ)}


def remote(src, dst, send_sem, recv_sem, target):
    return pltpu.make_async_remote_copy(src_ref=src, dst_ref=dst, send_sem=send_sem, recv_sem=recv_sem, device_id=target, device_id_type=pl.DeviceIdType.MESH)


def start(copy):
    copy.start()


def tell(semaphore, targets):
    for target in targets:
        pl.semaphore_signal(semaphore, device_id=target, device_id_type=pl.DeviceIdType.MESH)


RATE, D2D, HOP = 44700.0, 400000.0, 2.3
PUT, TILE, ROWS = 1.0, 1.0, 0.4
STEP = 5
AHEAD, MORE = 5.0, 0.05

PIECE = {(0, None): (0, 1), (1, None): (1, 3), (1, 0): (1, 1), (1, 1): (2, 2)}
RELAYS = ((0, None, "y+"), (1, 0, "y+"), (1, 1, "y-"))


KINDS = ("A0", "A1", "B0", "B1")


def gather_order(sizes, expert_bytes):
    free, pending, coming, order, have, ready = {}, {}, [], [], {}, {}

    def send(now, name, link, arrives, nbytes):
        t = max(now, free.get(link, 0.0)) + nbytes / (D2D if link == "core" else RATE)
        free[link] = t
        coming.append((t + (HOP / 2 if link == "core" else HOP), len(order), len(coming), arrives))
        return (name, link)

    def later(rank, name, link, arrives, nbytes):
        queue = pending.setdefault(link, [])
        queue.append((rank, len(order), len(queue), (name, link, arrives, nbytes)))

    def turn(now):
        out = []
        for link, queue in pending.items():
            queue.sort()
            while queue and free.get(link, 0.0) - now < AHEAD + MORE * now:
                out.append(send(now, *queue.pop(0)[-1]))
        return out

    def on_rows(kind, dy, dx):
        first, second = "xy" if kind[0] == "A" else "yx"
        d = {"x": dx, "y": dy}
        for axis in [first, second] if d[second] == 0 else [second]:
            for sign in (1, -1):
                if d[axis] == 0 or d[axis] == -sign % 4 and kind[1] == "10"[sign > 0]:
                    nd = dict(d)
                    nd[axis] = (d[axis] - sign) % 4
                    rank = 4 + (axis == second) + (d[axis] != 0)
                    later(rank, (kind, dy, dx), axis + "-+"[sign > 0], (kind, nd["y"], nd["x"]), sizes[kind])

    def core(now, key):
        return send(now, key, "core", ("core",) + key, sizes[key[0]])

    def weights(rank, name, group, part, link, arrives):
        later(rank, name, link, arrives + (group, part), PIECE[group, part][1] * expert_bytes)

    def on_piece(dz, dy, group):
        for link, step, far in (("z+", -1, dy < 2), ("z-", 1, dy >= 2)):
            gone = (step * dz) % NZ
            if gone < 3 + far:
                weights(4 * group + gone, ("W", dz, dy, group), group, None, link, ("W", (dz + step) % NZ, dy))

    def arrived(key, part=None):
        have[key] = have.get(key, 0) + (2 if part is None else 1)
        if have[key] == 2:
            ready[key] = True
        return have[key] == 2

    for i, (group, part, link) in enumerate(RELAYS):
        weights(0, ("r", i), group, part, link, ("R", i))
    for group in range(2):
        for dy, link in ((1, "y+"), (3, "y-")):
            weights(2, ("w", dy, group), group, None, link, ("W", 0, (-dy) % NY))
        on_piece(0, 0, group)
    sends = []
    for kind in KINDS[::-1]:
        arrived((kind, 0, 0))
        on_rows(kind, 0, 0)
        sends.append(core(0.0, (kind, 0, 0)))
    order.append((None, turn(0.0) + sends))
    todo, puts, done, now = [(dy, dx) for dy in range(NY) for dx in range(NX)], 0, 0, 0.0
    while coming or todo or done < puts:
        coming.sort()
        soon = coming[0][0] if coming else 1e9
        if soon > now:
            place = next((p for p in todo if all(pre + (kind,) + p in ready for kind in KINDS for pre in ((), ("core",)))), None)
            if place is not None:
                todo.remove(place)
                order.append((("put",) + place, turn(now)))
                puts += 1
                now += PUT
                continue
            step = min(STEP, puts - done)
            weights_in = sum(key[0] == "W" and key[-1] == 0 for key in ready) == NZ * NY - 1
            calm = all(c[-1][0] == "core" for c in coming)
            if weights_in and step and (step >= 3 and soon - now > TILE or calm):
                order.append((("tile", done, done + step), turn(now)))
                done += step
                now += TILE + ROWS * step
                continue
        t, _, _, name = coming.pop(0)
        now = max(now, t)
        if name[0] == "core":
            arrived(name)
            continue
        sends = []
        if name[0] == "R":
            i, group, part = name[1:]
            weights(1, name[:2], group, part, RELAYS[i][2], ("W", 0, 2))
            name = name[:2]
        elif name[0] == "W":
            if arrived(name[:-1], name[-1]):
                on_piece(*name[1:-1])
        else:
            sends = [core(now, name)]
            arrived(name)
            on_rows(*name)
        order.append((name, sends + turn(now)))
    return order


def passed_on(dz, dy):
    return dz != NZ // 2 and dz not in ((3,) if dy < 2 else (5,))


def first_expert(d):
    return rem(d, NX * NC) * (NY * OWN) + d // (NX * NC) * OWN


FAR, SUM3, NEW3, TWO, ONE, PART, HOPS = 0, 1, 2, 3, 4, 5, 11


def layer_kernel(order, cap, spans, scope_one, scope_two, x_hbm, u_hbm, ids_hbm, gates_hbm, w1_hbm, w3_hbm, w2_hbm,
                 grads, in_grad_hbm, gate_hbm, dxb, valb, dxs, xr, ur, gr, sel,
                 ids_ref, gates_ref, in_grad_ref, gate_ref, metas, gates_out, wown, wv, relay, xb, ub, gb, sb, a_s, d1_s, d3_s, y_s, dx_s, val_s, vb, key_s, acc_s,
                 recv, core_recv, wrecv, relay_recv, mrecv, send_sem, msend, load_sem, store_sem,
                 lsem, rsend, rrecv, ysend, yrecv, dsend, drecv, vsem, osem, in_scope, in_plane):
    z, y, x, c = here()
    tok, hidden = x_hbm.shape
    rows, ff = xb.shape[0], a_s.shape[-1]
    d_loc = hidden // (NZ * NY)
    me = place_of(at_offset(0))

    def place(dy, dx, dc=0):
        return place_of(at_offset(dy * (NX * NC) + dx * NC + dc))

    targets = {"core": {"core": 1 - c}}
    for sign, n in (("+", 1), ("-", -1)):
        targets["x" + sign] = {"x": rem(x + n + NX, NX)}
        targets["y" + sign] = {"y": rem(y + n + NY, NY)}
        targets["z" + sign] = z_at(n + NZ)

    def wait(ref, sem):
        remote(ref, ref, send_sem.at[0], sem, targets["core"]).wait_recv()

    def piece(dz, dy, group, part=None):
        return wv.at[z_at(dz)["z"], rem(y + dy, NY), pl.ds(*PIECE[group, part])]

    def wait_weights(dz, dy, group, part):
        wait(piece(dz, dy, group, part), wrecv.at[dz, dy, group, part or 0])

    def w(e, m):
        return wv[:, :, e, m].reshape(hidden, ff)

    def expert_rows(e, spans):
        def cut_of(ref):
            return jnp.concatenate([ref[s, :] for s in spans]) if spans[1:] else ref[spans[0], :]

        def save(ref, value):
            n = value.shape[0] // len(spans)
            for i, s in enumerate(spans):
                ref[s, :] = value[i * n:(i + 1) * n]

        x_rows = cut_of(xb)
        h1, h3 = dot(x_rows, w(e, 0)), dot(x_rows, w(e, 1))
        sig = jax.nn.sigmoid(h1)
        silu = h1 * sig
        act = (silu * h3).astype(BF16)
        save(a_s, act)
        y_rows = dot_nt(act, w(e, 2))
        save(y_s, jnp.sum(cut_of(ub).astype(F32) * y_rows, axis=1, keepdims=True))
        da = dot(cut_of(gb), w(e, 2))
        d1 = (da * h3 * sig * (1.0 + h1 * (1.0 - sig))).astype(BF16)
        d3 = (da * silu).astype(BF16)
        save(d1_s, d1)
        save(d3_s, d3)
        save(dx_s, (dot_nt(d1, w(e, 0)) + dot_nt(d3, w(e, 1))).astype(BF16))

    def gather(all_rows, tri, sx, su, sg, ss):
        loads = [
            pltpu.make_async_copy(x_hbm, all_rows.at[me, pl.ds(0, tok)], load_sem.at[0]),
            pltpu.make_async_copy(u_hbm, all_rows.at[me, pl.ds(tok, tok)], load_sem.at[1]),
        ]
        for m, ref in enumerate((w1_hbm, w3_hbm, w2_hbm)):
            loads.append(pltpu.make_async_copy(ref.reshape(NY, OWN, d_loc, ff), wown.at[:, :, m], load_sem.at[2 + m]))
        tables = [pltpu.make_async_copy(a, b, load_sem.at[i]) for i, a, b in ((5, ids_hbm, ids_ref), (6, gates_hbm, gates_ref))]
        for copy in tables + loads:
            copy.start()
        barrier = pltpu.get_barrier_semaphore()
        tell(barrier, targets.values())
        for copy in tables:
            copy.wait()

        @pl.loop(0, GROUP)
        def _(d):
            number = first_expert(d) + lax.broadcasted_iota(jnp.int32, (OWN, tok), 0)
            value = jnp.full((OWN, tok), -1.0, F32)
            for j in range(ids_ref.shape[0]):
                chosen = ids_ref[pl.ds(j, 1), :] == number
                value = jnp.where(chosen, jnp.broadcast_to(gates_ref[pl.ds(j, 1), :], value.shape), value)
            gates_out[d] = value

        metas[me] = gates_out[me]
        tri[...] = strict_upper(tok)
        for copy in loads:
            copy.wait()
        pl.semaphore_wait(barrier, len(targets))

        back = {"x+": (0, 3), "x-": (0, 1), "y+": (3, 0), "y-": (1, 0)}
        def block(kind, dy, dx, dc=0):
            return all_rows.at[place(dy, dx, dc), pl.ds(*spans[kind])]

        row_copies = []

        def issue(name, link):
            number = len(row_copies) + len(weight_copies)
            sem = send_sem.at[number]
            group, part_of = None, None
            if name[0] == "w":
                _, dy, group = name
                src = wown.at[rem(y + dy, NY), pl.ds(*PIECE[group, None])]
                copy = remote(src, piece(0, 0, group), sem, wrecv.at[0, (-dy) % NY, group, 0], targets[link])
            elif name[0] in "rR":
                group, part_of, _ = RELAYS[name[1]]
                span = pl.ds(*PIECE[group, part_of])
                if name[0] == "r":
                    copy = remote(wown.at[rem(y + 2, NY), span], relay.at[span], sem, relay_recv.at[name[1]], targets[link])
                else:
                    dst = piece(0, back[link][0], group, part_of)
                    copy = remote(relay.at[span], dst, sem, wrecv.at[0, 2, group, part_of or 0], targets[link])
            elif name[0] == "W":
                _, dz, dy, group = name
                ndz = (dz - 1) % NZ if link == "z+" else (dz + 1) % NZ
                own = wown.at[y, pl.ds(*PIECE[group, None])]
                copy = remote(own if dz == dy == 0 else piece(dz, dy, group), piece(dz, dy, group), sem, wrecv.at[ndz, dy, group, 0], targets[link])
            else:
                kind, dy, dx = name
                ref = block(*name)
                oy, ox = back.get(link, (0, 0))
                arrivals = core_recv if link == "core" else recv
                rsem = arrivals.at[KINDS.index(kind), (dy + oy) % NY * NX + (dx + ox) % NX]
                copy = remote(ref, ref, sem, rsem, targets[link])
            copy.start()
            if group is None:
                row_copies.append(copy)
            else:
                weight_copies.append((number, group, part_of))

        def meta_copy(k):
            to = at_offset(k)
            return remote(gates_out.at[place_of(to)], metas.at[me], msend.at[k], mrecv.at[k], to)

        n_rows = OWN * 2 * cap
        stores, chips = [], []

        def put(dy, dx):
            slot = len(stores) % 2
            if stores[1:]:
                for copy in stores[-2]:
                    copy.wait()
            for dc in (0, 1):
                if dy or dx or dc:
                    k = ((-dy) % NY) * (NX * NC) + ((-dx) % NX) * NC + dc
                    wait(metas.at[place(dy, dx, dc)], mrecv.at[k])
            for i, kind in enumerate(KINDS):
                wait(block(kind, dy, dx, 1), core_recv.at[i, dy * NX + dx])
            chip = rem(y + dy, NY) * NX + rem(x + dx, NX)
            n = 2 * OWN
            which = lax.broadcasted_iota(jnp.int32, (n, tok), 0)
            gate = jnp.zeros((n, tok), F32)
            for i in range(n):
                gate = jnp.where(which == i, jnp.broadcast_to(metas[2 * chip + i // OWN, pl.ds(i % OWN, 1), :], gate.shape), gate)
            member = gate >= 0.0
            key = jnp.where(member, dot(member.astype(F32).astype(BF16), tri[...]), -1.0)
            r = lax.broadcasted_iota(jnp.int32, (n_rows, tok), 0)
            at = rem(r, cap).astype(F32)
            row_of = rem(r // cap, 2) * OWN + r // (2 * cap)
            mine, gates = jnp.full((n_rows, tok), -1.0, F32), jnp.zeros((n_rows, tok), F32)
            for i in range(n):
                mine = jnp.where(row_of == i, jnp.broadcast_to(key[i:i + 1, :], mine.shape), mine)
                gates = jnp.where(row_of == i, jnp.broadcast_to(gate[i:i + 1, :], mine.shape), gates)
            found = at == mine
            pick = [jnp.logical_and(found, row_of // OWN == p).astype(F32) for p in range(2)]
            both = pick[0] + pick[1]
            scale = jnp.sum(both * gates, axis=1, keepdims=True)
            pick = [p.astype(BF16) for p in pick]
            x_rows = dot(pick[0], all_rows[2 * chip, 0:tok, :]) + dot(pick[1], all_rows[2 * chip + 1, 0:tok, :])
            u_rows = dot(pick[0], all_rows[2 * chip, tok:2 * tok, :]) + dot(pick[1], all_rows[2 * chip + 1, tok:2 * tok, :])
            span = pl.ds(pl.multiple_of(chip * 2 * cap, 2 * cap), 2 * cap)
            out = []
            for i, (value, first, stage, far) in enumerate(((x_rows, xb, sx, xr), (u_rows, ub, su, ur), (scale * u_rows, gb, sg, gr), (both, sb, ss, sel))):
                value = value.astype(BF16)
                first[span, :] = value[:2 * cap]
                stage[slot] = value[2 * cap:].reshape(stage.shape[1:])
                out.append(pltpu.make_async_copy(stage.at[slot], far.at[:, span], store_sem.at[slot, i]))
                out[-1].start()
            stores.append(out)
            chips.append(span)

        for name, sends in order:
            if name is None:
                pass
            elif name[0] == "put":
                put(*name[1:])
            elif name[0] == "tile":
                expert_rows(0, chips[name[1]:name[2]])
            elif name[0] == "R":
                group, part, _ = RELAYS[name[1]]
                wait(relay.at[pl.ds(*PIECE[group, part])], relay_recv.at[name[1]])
            elif name[0] == "W":
                if passed_on(*name[1:3]) or not name[3]:
                    wait_weights(*name[1:])
                else:
                    last_weights.append(name[1:])
            else:
                kind, dy, dx = name
                wait(block(*name), recv.at[KINDS.index(kind), dy * NX + dx])
            for send in sends:
                issue(*send)
            if name is None:
                wv[z, y] = wown[y]
                near = [t for link, t in targets.items() if link[0] != "z"]
                for far in range(NY // 2 + NX // 2):
                    tell(in_plane.at[far], near)
                    pl.semaphore_wait(in_plane.at[far], len(near))

                @each_other
                def _(k):
                    meta_copy(k).start()

        for out in stores[-2:]:
            for copy in out:
                copy.wait()

        @each_other
        def _(k):
            meta_copy(k).wait_send()

        for copy in row_copies:
            copy.wait_send()

    def reduce(G, r4, r3, r2, r1):
        tell(in_scope, [targets["z+"], targets["z-"]])

        def row_loads(e):
            pairs = ((xr, xb), (gr, gb), (ur, ub), (sel, sb))
            return [pltpu.make_async_copy(src.at[e - 1], dst, lsem.at[i]) for i, (src, dst) in enumerate(pairs)]

        def chunk(e, way, dist):
            return G.at[e, z_at(dist if way else NZ - dist)["z"]]

        def part_of(ref, way, e, kind):
            return ref.at[way, e, (kind - PART) % 2, (kind - PART) // 2]

        def hop(e, way, kind):
            h = way
            src, dst = {
                FAR: lambda: (chunk(e, way, 4).at[h], r4.at[way, e]),
                SUM3: lambda: (r4.at[way, e], r3.at[way, e, h]),
                NEW3: lambda: (chunk(e, way, 3).at[1 - h], r3.at[way, e, 1 - h]),
                TWO: lambda: (r3.at[way, e], r2.at[way, e]),
                ONE: lambda: (r2.at[way, e], r1.at[way, e]),
            }.get(kind, lambda: (part_of(r2, way, e, kind), part_of(r1, way, e, kind)))()
            return remote(src, dst, rsend.at[way, e, kind], rrecv.at[way, e, kind], z_at(1 if way else NZ - 1))

        def add_into(dst, *others):
            parts = dst.shape[:-2]
            if not parts:
                total = dst[...]
                for other in others:
                    total = total + other[...]
                dst[...] = total
                return

            def flat(ref, i):
                index = []
                for n in reversed(parts):
                    index.append(rem(i, n))
                    i = i // n
                return ref.at[tuple(reversed(index))]

            n = 1
            for p in parts:
                n *= p

            @pl.loop(0, n)
            def _(i):
                total = flat(dst, i)[...]
                for other in others:
                    total = total + flat(other, i)[...]
                flat(dst, i)[...] = total

        def own_rows(s):
            return pl.ds(pl.multiple_of(s * cap, 8), cap)

        def dx_copy(e, k):
            to = at_offset(k)
            return remote(dxs.at[e, own_rows(place_of(to))], dxb.at[me, own_rows(e)], dsend.at[e], drecv.at[e], to)

        tile = 256 if rows % 256 == 0 else rows
        dtile = hidden // NZ
        half = dtile // 2

        def weight_gradients(e):
            out = pltpu.make_async_copy(dx_s, dxs.at[e], osem.at[0])
            out.start()

            @pl.loop(0, NZ // 2)
            def _(i):
                pair = [z_at(n + 2 * i)["z"] for n in (3, 4)]

                def cols(ref):
                    return jnp.concatenate([ref[:, pl.ds(pl.multiple_of(k * dtile, dtile), dtile)] for k in pair], axis=1)

                x_cols, g_cols = cols(xb), cols(gb)
                for m, part in enumerate((dot_tn(x_cols, d1_s[...]), dot_tn(x_cols, d3_s[...]), dot_tn(g_cols, a_s[...]))):
                    for j in range(4):
                        G[e, pair[j // 2], j % 2, m] = part[j * half:(j + 1) * half]

                @pl.when(i == 0)
                def _():
                    if isinstance(e, int):
                        pl.semaphore_wait(in_scope, 2)
                    for way, kind in ((0, FAR), (1, FAR), (1, NEW3)):
                        hop(e, way, kind).start()

                @pl.when(i == 1)
                def _():
                    hop(e, 0, NEW3).start()

            val = sb[...].astype(F32) * y_s[...]
            val_s[e] = jnp.sum(val.reshape(rows // cap, cap, tok), axis=1)
            out.wait()

        def send_back(e):
            pltpu.make_async_copy(dxs.at[e, own_rows(me)], dxb.at[me, own_rows(e)], drecv.at[e]).start()

            @each_other
            def _(k):
                dx_copy(e, k).start()

        def far_sums(e):
            for way in (0, 1):
                hop(e, way, FAR).wait_recv()
                add_into(r4.at[way, e], chunk(e, way, 3).at[way])
                hop(e, way, SUM3).start()

        weight_gradients(0)
        for copy in row_loads(1):
            copy.start()
        send_back(0)
        for name in last_weights:
            wait_weights(*name)

        @pl.loop(1, OWN)
        def _(e):
            for copy in row_loads(e):
                copy.wait()

            @pl.loop(0, rows // tile)
            def _(i):
                expert_rows(e, [pl.ds(pl.multiple_of(i * tile, tile), tile)])

            weight_gradients(e)

            @pl.when(e < OWN - 1)
            def _():
                for copy in row_loads(e + 1):
                    copy.start()

            send_back(e)
            far_sums(e - 1)

        far_sums(OWN - 1)

        def val_copy(k):
            to = at_offset(k)
            return remote(val_s.at[:, place_of(to)], valb.at[:, me], vsem.at[0, k], vsem.at[1, k], to)

        own_val = pltpu.make_async_copy(val_s.at[:, me], valb.at[:, me], vsem.at[0, 0])
        own_val.start()

        @each_other
        def _(k):
            val_copy(k).start()

        @pl.loop(0, OWN)
        def _(e):
            for way in (0, 1):
                for kind in (SUM3, NEW3):
                    hop(e, way, kind).wait_recv()
                add_into(r3.at[way, e], chunk(e, way, 2))
                hop(e, way, TWO).start()

        group, places = dxb.shape[:2]
        ids = ids_ref[...].astype(F32)
        r = lax.broadcasted_iota(jnp.int32, (group * 8, tok), 0)
        e_of = rem(r, 8)
        expert = jnp.where(e_of < OWN, first_expert(r // 8) + e_of, -1).astype(F32)
        member = jnp.zeros((group * 8, tok), F32)
        for j in range(ids.shape[0]):
            member = member + (jnp.broadcast_to(ids[j:j + 1, :], member.shape) == expert).astype(F32)
        before = dot(member.astype(BF16), strict_upper(tok))
        key_s[...] = jnp.where(member > 0.0, before, -1.0).reshape(key_s.shape)
        rr = lax.broadcasted_iota(jnp.int32, (places, tok), 0)
        at, e_row = rem(rr, cap).astype(F32), rr // cap
        some = rows // places

        @pl.loop(0, OWN)
        def _(e):
            got = dxb.at[:, own_rows(e)]
            pltpu.make_async_copy(got, got, drecv.at[e]).wait()

        own_val.wait()

        @each_other
        def _(k):
            val_copy(k).wait()

        bufs = (xb, gb)
        loads = [pltpu.make_async_copy(dxb.at[pl.ds(i * some, some)], bufs[i % 2].reshape(some, places, hidden), lsem.at[i % 2]) for i in range(group // some)]
        vals = pltpu.make_async_copy(valb, vb, lsem.at[2])
        vals.start()
        loads[0].start()
        for i, load in enumerate(loads):
            for later in loads[i + 1:i + 2]:
                later.start()

            @pl.loop(0, some)
            def _(k):
                key = key_s[i * some + k]
                mine = jnp.full((places, tok), -1.0, F32)
                for e in range(OWN):
                    mine = jnp.where(e_row == e, jnp.broadcast_to(key[e:e + 1, :], (places, tok)), mine)
                sb[pl.ds(pl.multiple_of(k * places, places), places), :] = (at == mine).astype(F32).astype(BF16)

            load.wait()
            part = dot_tn(sb[...], bufs[i % 2][...])
            acc_s[...] = acc_s[...] + part if i else part

        in_grad_ref[...] = acc_s[...].astype(BF16)
        vals.wait()

        def gate_step(k, total):
            for e in range(OWN):
                row = vb[e, pl.ds(k, 1), :]
                total = total + jnp.where(ids == (first_expert(k) + e).astype(F32), jnp.broadcast_to(row, ids.shape), 0.0)
            return total

        gate_ref[...] = lax.fori_loop(0, group, gate_step, jnp.zeros(ids.shape, F32))
        results = [pltpu.make_async_copy(a, b, load_sem.at[i]) for i, a, b in ((0, in_grad_ref, in_grad_hbm), (1, gate_ref, gate_hbm))]
        for copy in results:
            copy.start()

        last = OWN - 1

        @pl.loop(0, last)
        def _(e):
            for way in (0, 1):
                hop(e, way, TWO).wait_recv()
                add_into(r2.at[way, e], chunk(e, way, 1))
                hop(e, way, ONE).start()

        for way in (0, 1):
            hop(last, way, TWO).wait_recv()
        for kind in range(PART, HOPS):
            for way in (0, 1):
                add_into(part_of(r2, way, last, kind), part_of(G, last, z_at(1 if way else NZ - 1)["z"], kind))
                hop(last, way, kind).start()

        def keep(e, m, to, then_remote, then_local):
            src = r1.at[0, e, to // 2, m, pl.ds(to % 2 * d_loc, d_loc)]
            dst = grads.at[m, y * OWN + e]
            n = 0 if isinstance(m, slice) else m

            @pl.when(y != to)
            def _():
                then_remote(remote(src, dst, ysend.at[e, n, to], yrecv.at[e, n, y], {"y": to}))

            @pl.when(y == to)
            def _():
                then_local(pltpu.make_async_copy(src, dst, ysend.at[e, n, to]))

        every = slice(None)

        @pl.loop(0, last)
        def _(e):
            for way in (0, 1):
                hop(e, way, ONE).wait_recv()
            add_into(r1.at[0, e], r1.at[1, e], G.at[e, z])
            for to in range(NY):
                keep(e, every, to, start, start)

        for kind in range(PART, HOPS):
            for way in (0, 1):
                hop(last, way, kind).wait_recv()
            add_into(part_of(r1, 0, last, kind), part_of(r1, 1, last, kind), part_of(G, last, z, kind))
            m, h = (kind - PART) // 2, (kind - PART) % 2
            for to in (2 * h, 2 * h + 1):
                keep(last, m, to, start, start)

        def finish_up(e, kinds, matrices):
            for m in matrices:
                for at in range(NY):
                    def both(copy):
                        wait(grads.at[m, at * OWN + e], yrecv.at[e, 0 if m is every else m, at])
                        copy.wait_send()

                    keep(e, m, at, both, lambda copy: copy.wait())
            for way in (0, 1):
                for kind in kinds:
                    hop(e, way, kind).wait_send()
            sent = dxs.at[e, pl.ds(0, (GROUP - 1) * cap)]
            pltpu.make_async_copy(sent, sent, dsend.at[e]).wait()

        @pl.loop(0, last)
        def _(e):
            finish_up(e, range(PART), [every])

        finish_up(last, [FAR, SUM3, NEW3, TWO, *range(PART, HOPS)], range(3))
        for copy in results:
            copy.wait()

    weight_copies, last_weights = [], []
    pl.run_scoped(gather, *scope_one)
    pl.run_scoped(reduce, *scope_two)
    for number, group, part in weight_copies:
        ref = wown.at[0, pl.ds(*PIECE[group, part])]
        remote(ref, ref, send_sem.at[number], relay_recv.at[0], targets["core"]).wait_send()


def layer(cap, x, u, ids, gates, w1, w3, w2):
    tok, hidden = x.shape
    local_experts, d_loc, ff = w1.shape
    rows = GROUP * cap
    half = hidden // NZ // 2
    cut = tok - tok // 8 if tok % 256 == 0 else tok
    halves = [cut // 2] * 2 + [tok - cut // 2] * 2
    spans = {kind: (sum(halves[:i]), halves[i]) for i, kind in enumerate(KINDS)}
    order = gather_order({kind: 2 * hidden * n for kind, (_, n) in spans.items()}, 2 * w1.size * 3 // local_experts)
    sends = sum(len(s) for _, s in order)
    dma, v, shape = pltpu.SemaphoreType.DMA, pltpu.VMEM, jax.ShapeDtypeStruct
    far = lambda lanes: shape((OWN - 1, rows, lanes), BF16)
    near = lambda lanes: v((rows, lanes), BF16)
    stage = lambda lanes: v((2, OWN - 1, 2 * cap, lanes), BF16)
    sums = [v((2, OWN, 2, 3, half, ff), F32)] * 3
    scope_one = [v((GROUP, 2 * tok, hidden), BF16), v((tok, tok), BF16), stage(hidden), stage(hidden), stage(hidden), stage(tok)]
    scope_two = [v((OWN, NZ, 2, 3, half, ff), F32), v((2, OWN, 3, half, ff), F32)] + sums
    per_expert = v((OWN, GROUP, tok), F32)
    gate_rows = v((GROUP, OWN, tok), F32)
    outs = pl.pallas_call(
        functools.partial(layer_kernel, order, cap, spans, scope_one, scope_two),
        name="layer",
        out_shape=(
            shape((3, local_experts, d_loc, ff), F32), shape((tok, hidden), BF16), shape(ids.shape, F32),
            shape((GROUP, OWN * cap, hidden), BF16), shape((OWN, GROUP, tok), F32), shape((OWN, rows, hidden), BF16),
            far(hidden), far(hidden), far(hidden), far(tok),
        ),
        in_specs=[ANY] * 7,
        out_specs=(ANY,) * 10,
        scratch_shapes=[
            v(ids.shape, ids.dtype), v(ids.shape, F32), v((tok, hidden), BF16), v(ids.shape, F32), gate_rows, gate_rows, v((NY, OWN, 3, d_loc, ff), BF16), v((NZ, NY, OWN, 3, d_loc, ff), BF16), v((OWN, 3, d_loc, ff), BF16),
            near(hidden), near(hidden), near(hidden), near(tok), near(ff), near(ff), near(ff), v((rows, 1), F32),
            near(hidden), per_expert, per_expert, v((GROUP, 8, tok), F32), v((tok, hidden), F32),
            dma((len(KINDS), NY * NX)), dma((len(KINDS), NY * NX)), dma((NZ, NY, 2, 2)), dma((len(RELAYS),)), dma((GROUP,)), dma((sends,)), dma((GROUP,)),
            dma((7,)), dma((2, 4)),
            dma((4,)), dma((2, OWN, HOPS)), dma((2, OWN, HOPS)), dma((OWN, 3, NY)), dma((OWN, 3, NY)),
            dma((OWN,)), dma((OWN,)), dma((2, GROUP)), dma((1,)), pltpu.SemaphoreType.REGULAR, pltpu.SemaphoreType.REGULAR((NY // 2 + NX // 2,)),
        ],
        compiler_params=params(0),
    )(x, u, ids, gates, w1, w3, w2)
    return outs[:3]


def finish_kernel(grads, in_grad, gate, *refs):
    n = 5
    outs, bufs, sems = refs[:n], refs[n:2 * n], refs[-1]
    ins = [grads.at[m] for m in range(3)] + [in_grad, gate]
    load, store = [], []
    for i, (a, b, o) in enumerate(zip(ins, bufs, outs)):
        half = a.shape[0] // 2
        for h in range(2):
            at = pl.ds(h * half, half)
            load.append(pltpu.make_async_copy(a.at[at], b.at[at], sems.at[0, i, h]))
            store.append(pltpu.make_async_copy(b.at[at], o.at[at], sems.at[1, i, h]))
    for copy in load:
        copy.start()
    for before, after in zip(load, store):
        before.wait()
        after.start()
    for copy in store:
        copy.wait()


def finish(grads, in_grad, gate):
    shapes = [grads.shape[1:]] * 3 + [in_grad.shape, gate.shape]
    types = [grads.dtype] * 3 + [in_grad.dtype, gate.dtype]
    return pl.pallas_call(
        finish_kernel,
        name="finish",
        out_shape=[jax.ShapeDtypeStruct(s, t) for s, t in zip(shapes, types)],
        in_specs=[ANY] * 3,
        out_specs=[ANY] * len(shapes),
        scratch_shapes=[pltpu.VMEM(s, t) for s, t in zip(shapes, types)] + [pltpu.SemaphoreType.DMA((2, len(shapes), 2))],
    )(grads, in_grad, gate)


def solution(mesh):
    mesh4 = Mesh(mesh.devices.reshape(NZ, NY, NX, NC), ("z", "y", "x", "core"))
    tok_spec = P(("z", "y", "x", "core"), None)
    up_spec = P(("x", "core"), ("z", "y"), None)
    down_spec = P(("x", "core"), None, ("z", "y"))

    def per_device(layer_in, out_grad, expert_ids, gate_vals, w_one, w_two, w_three):
        tok_dev, hidden = layer_in.shape
        top_k = expert_ids.shape[1]
        local_experts, d_loc, ff = w_one.shape
        cap = capacity_of(tok_dev, top_k, local_experts * NX * NC)
        ids = expert_ids.T
        grads, in_grad, gate_out = layer(cap, layer_in, out_grad, ids, gate_vals.T, w_one, w_three, w_two.swapaxes(1, 2))
        g1, g3, g2, in_grad, gate_out = finish(grads, in_grad, gate_out)
        return in_grad, gate_out.T, g1, g2.swapaxes(1, 2), g3

    return jax.shard_map(per_device, mesh=mesh4, in_specs=(tok_spec, tok_spec, tok_spec, tok_spec, up_spec, down_spec, up_spec), out_specs=(tok_spec, tok_spec, up_spec, down_spec, up_spec), check_vma=False)
```

```python
import functools

import jax
import jax.numpy as jnp
from jax import lax
from jax.experimental import pallas as pl
from jax.experimental.pallas import tpu as pltpu
from jax.sharding import Mesh, PartitionSpec as P

NZ, NY, NX, NC = 8, 4, 4, 2
GROUP = NY * NX * NC
PLANE = ("y", "x", "core")
OWN = 4
F32, BF16 = jnp.float32, jnp.bfloat16
ANY = pl.BlockSpec(memory_space=pl.ANY)


def capacity_of(tok_dev, top_k, experts):
    return max(8, ((tok_dev * top_k * 5) // (4 * experts) + 7) // 8 * 8)


def rem(a, b):
    return a % b if isinstance(a, int) else lax.rem(a, b)


def contract(ca, cb):
    return lambda a, b: lax.dot_general(a, b, (((ca,), (cb,)), ((), ())), preferred_element_type=F32)


dot, dot_nt, dot_tn = contract(1, 0), contract(1, 1), contract(0, 0)


def params(number):
    return pltpu.CompilerParams(collective_id=number, has_side_effects=True, vmem_limit_bytes=67043328)


def each_other(body):
    return pl.loop(1, GROUP)(body)


def strict_upper(n):
    rows = lax.broadcasted_iota(jnp.int32, (n, n), 0)
    cols = lax.broadcasted_iota(jnp.int32, (n, n), 1)
    return (rows < cols).astype(F32).astype(BF16)


def here():
    return tuple(lax.axis_index(a) for a in ("z", "y", "x", "core"))


def at_offset(k):
    _, y, x, c = here()
    dy, dx, dc = k // (NX * NC), rem(k // NC, NX), rem(k, NC)
    return {"y": rem(y + dy, NY), "x": rem(x + dx, NX), "core": rem(c + dc, NC)}


def place_of(d):
    return d["y"] * (NX * NC) + d["x"] * NC + d["core"]


def z_at(dz):
    return {"z": rem(lax.axis_index("z") + dz, NZ)}


def remote(src, dst, send_sem, recv_sem, target):
    return pltpu.make_async_remote_copy(src_ref=src, dst_ref=dst, send_sem=send_sem, recv_sem=recv_sem, device_id=target, device_id_type=pl.DeviceIdType.MESH)


def start(copy):
    copy.start()


def tell(semaphore, targets):
    for target in targets:
        pl.semaphore_signal(semaphore, device_id=target, device_id_type=pl.DeviceIdType.MESH)


RATE, D2D, HOP = 44700.0, 400000.0, 2.3
PUT, TILE, ROWS = 1.0, 1.0, 0.4
STEP = 5
AHEAD, MORE = 5.0, 0.05

PIECE = {(0, None): (0, 1), (1, None): (1, 3), (1, 0): (1, 1), (1, 1): (2, 2)}
RELAYS = ((0, None, "y+"), (1, 0, "y+"), (1, 1, "y-"))


KINDS = ("A0", "A1", "B0", "B1")


def gather_order(sizes, expert_bytes):
    free, pending, coming, order, have, ready = {}, {}, [], [], {}, {}

    def send(now, name, link, arrives, nbytes):
        t = max(now, free.get(link, 0.0)) + nbytes / (D2D if link == "core" else RATE)
        free[link] = t
        coming.append((t + (HOP / 2 if link == "core" else HOP), len(order), len(coming), arrives))
        return (name, link)

    def later(rank, name, link, arrives, nbytes):
        queue = pending.setdefault(link, [])
        queue.append((rank, len(order), len(queue), (name, link, arrives, nbytes)))

    def turn(now):
        out = []
        for link, queue in pending.items():
            queue.sort()
            while queue and free.get(link, 0.0) - now < AHEAD + MORE * now:
                out.append(send(now, *queue.pop(0)[-1]))
        return out

    def on_rows(kind, dy, dx):
        first, second = "xy" if kind[0] == "A" else "yx"
        d = {"x": dx, "y": dy}
        for axis in [first, second] if d[second] == 0 else [second]:
            for sign in (1, -1):
                if d[axis] == 0 or d[axis] == -sign % 4 and kind[1] == "10"[sign > 0]:
                    nd = dict(d)
                    nd[axis] = (d[axis] - sign) % 4
                    rank = 4 + (axis == second) + (d[axis] != 0)
                    later(rank, (kind, dy, dx), axis + "-+"[sign > 0], (kind, nd["y"], nd["x"]), sizes[kind])

    def core(now, key):
        return send(now, key, "core", ("core",) + key, sizes[key[0]])

    def weights(rank, name, group, part, link, arrives):
        later(rank, name, link, arrives + (group, part), PIECE[group, part][1] * expert_bytes)

    def on_piece(dz, dy, group):
        for link, step, far in (("z+", -1, dy < 2), ("z-", 1, dy >= 2)):
            gone = (step * dz) % NZ
            if gone < 3 + far:
                weights(4 * group + gone, ("W", dz, dy, group), group, None, link, ("W", (dz + step) % NZ, dy))

    def arrived(key, part=None):
        have[key] = have.get(key, 0) + (2 if part is None else 1)
        if have[key] == 2:
            ready[key] = True
        return have[key] == 2

    for i, (group, part, link) in enumerate(RELAYS):
        weights(0, ("r", i), group, part, link, ("R", i))
    for group in range(2):
        for dy, link in ((1, "y+"), (3, "y-")):
            weights(2, ("w", dy, group), group, None, link, ("W", 0, (-dy) % NY))
        on_piece(0, 0, group)
    sends = []
    for kind in KINDS[::-1]:
        arrived((kind, 0, 0))
        on_rows(kind, 0, 0)
        sends.append(core(0.0, (kind, 0, 0)))
    order.append((None, turn(0.0) + sends))
    todo, puts, done, now = [(dy, dx) for dy in range(NY) for dx in range(NX)], 0, 0, 0.0
    while coming or todo or done < puts:
        coming.sort()
        soon = coming[0][0] if coming else 1e9
        if soon > now:
            place = next((p for p in todo if all(pre + (kind,) + p in ready for kind in KINDS for pre in ((), ("core",)))), None)
            if place is not None:
                todo.remove(place)
                order.append((("put",) + place, turn(now)))
                puts += 1
                now += PUT
                continue
            step = min(STEP, puts - done)
            weights_in = sum(key[0] == "W" and key[-1] == 0 for key in ready) == NZ * NY - 1
            calm = all(c[-1][0] == "core" for c in coming)
            if weights_in and step and (step >= 3 and soon - now > TILE or calm):
                order.append((("tile", done, done + step), turn(now)))
                done += step
                now += TILE + ROWS * step
                continue
        t, _, _, name = coming.pop(0)
        now = max(now, t)
        if name[0] == "core":
            arrived(name)
            continue
        sends = []
        if name[0] == "R":
            i, group, part = name[1:]
            weights(1, name[:2], group, part, RELAYS[i][2], ("W", 0, 2))
            name = name[:2]
        elif name[0] == "W":
            if arrived(name[:-1], name[-1]):
                on_piece(*name[1:-1])
        else:
            sends = [core(now, name)]
            arrived(name)
            on_rows(*name)
        order.append((name, sends + turn(now)))
    return order


def passed_on(dz, dy):
    return dz != NZ // 2 and dz not in ((3,) if dy < 2 else (5,))


def first_expert(d):
    return rem(d, NX * NC) * (NY * OWN) + d // (NX * NC) * OWN


FAR, SUM3, NEW3, TWO, ONE, PART, HOPS = 0, 1, 2, 3, 4, 5, 11


def layer_kernel(order, cap, spans, scope_one, scope_two, x_hbm, u_hbm, ids_hbm, gates_hbm, w1_hbm, w3_hbm, w2_hbm,
                 grads, in_grad_hbm, gate_hbm, dxb, valb, dxs, xr, ur, gr, sel,
                 ids_ref, gates_ref, in_grad_ref, gate_ref, metas, gates_out, wown, wv, relay, xb, ub, gb, sb, a_s, d1_s, d3_s, y_s, dx_s, val_s, vb, key_s, acc_s,
                 recv, core_recv, wrecv, relay_recv, mrecv, send_sem, msend, load_sem, store_sem,
                 lsem, rsend, rrecv, ysend, yrecv, dsend, drecv, vsem, osem, in_scope, in_plane):
    z, y, x, c = here()
    tok, hidden = x_hbm.shape
    rows, ff = xb.shape[0], a_s.shape[-1]
    d_loc = hidden // (NZ * NY)
    me = place_of(at_offset(0))

    def place(dy, dx, dc=0):
        return place_of(at_offset(dy * (NX * NC) + dx * NC + dc))

    targets = {"core": {"core": 1 - c}}
    for sign, n in (("+", 1), ("-", -1)):
        targets["x" + sign] = {"x": rem(x + n + NX, NX)}
        targets["y" + sign] = {"y": rem(y + n + NY, NY)}
        targets["z" + sign] = z_at(n + NZ)

    def wait(ref, sem):
        remote(ref, ref, send_sem.at[0], sem, targets["core"]).wait_recv()

    def piece(dz, dy, group, part=None):
        return wv.at[z_at(dz)["z"], rem(y + dy, NY), pl.ds(*PIECE[group, part])]

    def wait_weights(dz, dy, group, part):
        wait(piece(dz, dy, group, part), wrecv.at[dz, dy, group, part or 0])

    def w(e, m):
        return wv[:, :, e, m].reshape(hidden, ff)

    def expert_rows(e, spans):
        def cut_of(ref):
            return jnp.concatenate([ref[s, :] for s in spans]) if spans[1:] else ref[spans[0], :]

        def save(ref, value):
            n = value.shape[0] // len(spans)
            for i, s in enumerate(spans):
                ref[s, :] = value[i * n:(i + 1) * n]

        x_rows = cut_of(xb)
        h1, h3 = dot(x_rows, w(e, 0)), dot(x_rows, w(e, 1))
        sig = jax.nn.sigmoid(h1)
        silu = h1 * sig
        act = (silu * h3).astype(BF16)
        save(a_s, act)
        y_rows = dot_nt(act, w(e, 2))
        save(y_s, jnp.sum(cut_of(ub).astype(F32) * y_rows, axis=1, keepdims=True))
        da = dot(cut_of(gb), w(e, 2))
        d1 = (da * h3 * sig * (1.0 + h1 * (1.0 - sig))).astype(BF16)
        d3 = (da * silu).astype(BF16)
        save(d1_s, d1)
        save(d3_s, d3)
        save(dx_s, (dot_nt(d1, w(e, 0)) + dot_nt(d3, w(e, 1))).astype(BF16))

    def gather(all_rows, tri, sx, su, sg, ss):
        loads = [
            pltpu.make_async_copy(x_hbm, all_rows.at[me, pl.ds(0, tok)], load_sem.at[0]),
            pltpu.make_async_copy(u_hbm, all_rows.at[me, pl.ds(tok, tok)], load_sem.at[1]),
        ]
        for m, ref in enumerate((w1_hbm, w3_hbm, w2_hbm)):
            loads.append(pltpu.make_async_copy(ref.reshape(NY, OWN, d_loc, ff), wown.at[:, :, m], load_sem.at[2 + m]))
        tables = [pltpu.make_async_copy(a, b, load_sem.at[i]) for i, a, b in ((5, ids_hbm, ids_ref), (6, gates_hbm, gates_ref))]
        for copy in tables + loads:
            copy.start()
        barrier = pltpu.get_barrier_semaphore()
        tell(barrier, targets.values())
        def make_tables():
            for copy in tables:
                copy.wait()

            @pl.loop(0, GROUP)
            def _(d):
                number = first_expert(d) + lax.broadcasted_iota(jnp.int32, (OWN, tok), 0)
                value = jnp.full((OWN, tok), -1.0, F32)
                for j in range(ids_ref.shape[0]):
                    chosen = ids_ref[pl.ds(j, 1), :] == number
                    value = jnp.where(chosen, jnp.broadcast_to(gates_ref[pl.ds(j, 1), :], value.shape), value)
                gates_out[d] = value

            metas[me] = gates_out[me]
            tri[...] = strict_upper(tok)

        for copy in loads:
            copy.wait()
        pl.semaphore_wait(barrier, len(targets))

        back = {"x+": (0, 3), "x-": (0, 1), "y+": (3, 0), "y-": (1, 0)}
        def block(kind, dy, dx, dc=0):
            return all_rows.at[place(dy, dx, dc), pl.ds(*spans[kind])]

        row_copies = []

        def issue(name, link):
            number = len(row_copies) + len(weight_copies)
            sem = send_sem.at[number]
            group, part_of = None, None
            if name[0] == "w":
                _, dy, group = name
                src = wown.at[rem(y + dy, NY), pl.ds(*PIECE[group, None])]
                copy = remote(src, piece(0, 0, group), sem, wrecv.at[0, (-dy) % NY, group, 0], targets[link])
            elif name[0] in "rR":
                group, part_of, _ = RELAYS[name[1]]
                span = pl.ds(*PIECE[group, part_of])
                if name[0] == "r":
                    copy = remote(wown.at[rem(y + 2, NY), span], relay.at[span], sem, relay_recv.at[name[1]], targets[link])
                else:
                    dst = piece(0, back[link][0], group, part_of)
                    copy = remote(relay.at[span], dst, sem, wrecv.at[0, 2, group, part_of or 0], targets[link])
            elif name[0] == "W":
                _, dz, dy, group = name
                ndz = (dz - 1) % NZ if link == "z+" else (dz + 1) % NZ
                own = wown.at[y, pl.ds(*PIECE[group, None])]
                copy = remote(own if dz == dy == 0 else piece(dz, dy, group), piece(dz, dy, group), sem, wrecv.at[ndz, dy, group, 0], targets[link])
            else:
                kind, dy, dx = name
                ref = block(*name)
                oy, ox = back.get(link, (0, 0))
                arrivals = core_recv if link == "core" else recv
                rsem = arrivals.at[KINDS.index(kind), (dy + oy) % NY * NX + (dx + ox) % NX]
                copy = remote(ref, ref, sem, rsem, targets[link])
            copy.start()
            if group is None:
                row_copies.append(copy)
            else:
                weight_copies.append((number, group, part_of))

        def meta_copy(k):
            to = at_offset(k)
            return remote(gates_out.at[place_of(to)], metas.at[me], msend.at[k], mrecv.at[k], to)

        n_rows = OWN * 2 * cap
        stores, chips = [], []

        def put(dy, dx):
            slot = len(stores) % 2
            if stores[1:]:
                for copy in stores[-2]:
                    copy.wait()
            for dc in (0, 1):
                if dy or dx or dc:
                    k = ((-dy) % NY) * (NX * NC) + ((-dx) % NX) * NC + dc
                    wait(metas.at[place(dy, dx, dc)], mrecv.at[k])
            for i, kind in enumerate(KINDS):
                wait(block(kind, dy, dx, 1), core_recv.at[i, dy * NX + dx])
            chip = rem(y + dy, NY) * NX + rem(x + dx, NX)
            n = 2 * OWN
            which = lax.broadcasted_iota(jnp.int32, (n, tok), 0)
            gate = jnp.zeros((n, tok), F32)
            for i in range(n):
                gate = jnp.where(which == i, jnp.broadcast_to(metas[2 * chip + i // OWN, pl.ds(i % OWN, 1), :], gate.shape), gate)
            member = gate >= 0.0
            key = jnp.where(member, dot(member.astype(F32).astype(BF16), tri[...]), -1.0)
            r = lax.broadcasted_iota(jnp.int32, (n_rows, tok), 0)
            at = rem(r, cap).astype(F32)
            row_of = rem(r // cap, 2) * OWN + r // (2 * cap)
            mine, gates = jnp.full((n_rows, tok), -1.0, F32), jnp.zeros((n_rows, tok), F32)
            for i in range(n):
                mine = jnp.where(row_of == i, jnp.broadcast_to(key[i:i + 1, :], mine.shape), mine)
                gates = jnp.where(row_of == i, jnp.broadcast_to(gate[i:i + 1, :], mine.shape), gates)
            found = at == mine
            pick = [jnp.logical_and(found, row_of // OWN == p).astype(F32) for p in range(2)]
            both = pick[0] + pick[1]
            scale = jnp.sum(both * gates, axis=1, keepdims=True)
            pick = [p.astype(BF16) for p in pick]
            x_rows = dot(pick[0], all_rows[2 * chip, 0:tok, :]) + dot(pick[1], all_rows[2 * chip + 1, 0:tok, :])
            u_rows = dot(pick[0], all_rows[2 * chip, tok:2 * tok, :]) + dot(pick[1], all_rows[2 * chip + 1, tok:2 * tok, :])
            span = pl.ds(pl.multiple_of(chip * 2 * cap, 2 * cap), 2 * cap)
            out = []
            for i, (value, first, stage, far) in enumerate(((x_rows, xb, sx, xr), (u_rows, ub, su, ur), (scale * u_rows, gb, sg, gr), (both, sb, ss, sel))):
                value = value.astype(BF16)
                first[span, :] = value[:2 * cap]
                stage[slot] = value[2 * cap:].reshape(stage.shape[1:])
                out.append(pltpu.make_async_copy(stage.at[slot], far.at[:, span], store_sem.at[slot, i]))
                out[-1].start()
            stores.append(out)
            chips.append(span)

        for name, sends in order:
            if name is None:
                pass
            elif name[0] == "put":
                put(*name[1:])
            elif name[0] == "tile":
                expert_rows(0, chips[name[1]:name[2]])
            elif name[0] == "R":
                group, part, _ = RELAYS[name[1]]
                wait(relay.at[pl.ds(*PIECE[group, part])], relay_recv.at[name[1]])
            elif name[0] == "W":
                if passed_on(*name[1:3]) or not name[3]:
                    wait_weights(*name[1:])
                else:
                    last_weights.append(name[1:])
            else:
                kind, dy, dx = name
                wait(block(*name), recv.at[KINDS.index(kind), dy * NX + dx])
            for send in sends:
                issue(*send)
            if name is None:
                make_tables()
                wv[z, y] = wown[y]
                near = [t for link, t in targets.items() if link[0] != "z"]
                for far in range(NY // 2 + NX // 2):
                    tell(in_plane.at[far], near)
                    pl.semaphore_wait(in_plane.at[far], len(near))

                @each_other
                def _(k):
                    meta_copy(k).start()

        for out in stores[-2:]:
            for copy in out:
                copy.wait()

        @each_other
        def _(k):
            meta_copy(k).wait_send()

        for copy in row_copies:
            copy.wait_send()

    def reduce(G, r4, r3, r2, r1):
        tell(in_scope, [targets["z+"], targets["z-"]])

        def row_loads(e):
            pairs = ((xr, xb), (gr, gb), (ur, ub), (sel, sb))
            return [pltpu.make_async_copy(src.at[e - 1], dst, lsem.at[i]) for i, (src, dst) in enumerate(pairs)]

        def chunk(e, way, dist):
            return G.at[e, z_at(dist if way else NZ - dist)["z"]]

        def part_of(ref, way, e, kind):
            return ref.at[way, e, (kind - PART) % 2, (kind - PART) // 2]

        def hop(e, way, kind):
            h = way
            src, dst = {
                FAR: lambda: (chunk(e, way, 4).at[h], r4.at[way, e]),
                SUM3: lambda: (r4.at[way, e], r3.at[way, e, h]),
                NEW3: lambda: (chunk(e, way, 3).at[1 - h], r3.at[way, e, 1 - h]),
                TWO: lambda: (r3.at[way, e], r2.at[way, e]),
                ONE: lambda: (r2.at[way, e], r1.at[way, e]),
            }.get(kind, lambda: (part_of(r2, way, e, kind), part_of(r1, way, e, kind)))()
            return remote(src, dst, rsend.at[way, e, kind], rrecv.at[way, e, kind], z_at(1 if way else NZ - 1))

        def add_into(dst, *others):
            parts = dst.shape[:-2]
            if not parts:
                total = dst[...]
                for other in others:
                    total = total + other[...]
                dst[...] = total
                return

            def flat(ref, i):
                index = []
                for n in reversed(parts):
                    index.append(rem(i, n))
                    i = i // n
                return ref.at[tuple(reversed(index))]

            n = 1
            for p in parts:
                n *= p

            @pl.loop(0, n)
            def _(i):
                total = flat(dst, i)[...]
                for other in others:
                    total = total + flat(other, i)[...]
                flat(dst, i)[...] = total

        def own_rows(s):
            return pl.ds(pl.multiple_of(s * cap, 8), cap)

        def dx_copy(e, k):
            to = at_offset(k)
            return remote(dxs.at[e, own_rows(place_of(to))], dxb.at[me, own_rows(e)], dsend.at[e], drecv.at[e], to)

        tile = 256 if rows % 256 == 0 else rows
        dtile = hidden // NZ
        half = dtile // 2

        def weight_gradients(e):
            out = pltpu.make_async_copy(dx_s, dxs.at[e], osem.at[0])
            out.start()

            @pl.loop(0, NZ // 2)
            def _(i):
                pair = [z_at(n + 2 * i)["z"] for n in (3, 4)]

                def cols(ref):
                    return jnp.concatenate([ref[:, pl.ds(pl.multiple_of(k * dtile, dtile), dtile)] for k in pair], axis=1)

                x_cols, g_cols = cols(xb), cols(gb)
                for m, part in enumerate((dot_tn(x_cols, d1_s[...]), dot_tn(x_cols, d3_s[...]), dot_tn(g_cols, a_s[...]))):
                    for j in range(4):
                        G[e, pair[j // 2], j % 2, m] = part[j * half:(j + 1) * half]

                @pl.when(i == 0)
                def _():
                    if isinstance(e, int):
                        pl.semaphore_wait(in_scope, 2)
                    for way, kind in ((0, FAR), (1, FAR), (1, NEW3)):
                        hop(e, way, kind).start()

                @pl.when(i == 1)
                def _():
                    hop(e, 0, NEW3).start()

            val = sb[...].astype(F32) * y_s[...]
            val_s[e] = jnp.sum(val.reshape(rows // cap, cap, tok), axis=1)
            out.wait()

        def send_back(e):
            pltpu.make_async_copy(dxs.at[e, own_rows(me)], dxb.at[me, own_rows(e)], drecv.at[e]).start()

            @each_other
            def _(k):
                dx_copy(e, k).start()

        def far_sums(e):
            for way in (0, 1):
                hop(e, way, FAR).wait_recv()
                add_into(r4.at[way, e], chunk(e, way, 3).at[way])
                hop(e, way, SUM3).start()

        weight_gradients(0)
        for copy in row_loads(1):
            copy.start()
        send_back(0)
        for name in last_weights:
            wait_weights(*name)

        @pl.loop(1, OWN)
        def _(e):
            for copy in row_loads(e):
                copy.wait()

            @pl.loop(0, rows // tile)
            def _(i):
                expert_rows(e, [pl.ds(pl.multiple_of(i * tile, tile), tile)])

            weight_gradients(e)

            @pl.when(e < OWN - 1)
            def _():
                for copy in row_loads(e + 1):
                    copy.start()

            send_back(e)
            far_sums(e - 1)

        far_sums(OWN - 1)

        def val_copy(k):
            to = at_offset(k)
            return remote(val_s.at[:, place_of(to)], valb.at[:, me], vsem.at[0, k], vsem.at[1, k], to)

        own_val = pltpu.make_async_copy(val_s.at[:, me], valb.at[:, me], vsem.at[0, 0])
        own_val.start()

        @each_other
        def _(k):
            val_copy(k).start()

        @pl.loop(0, OWN)
        def _(e):
            for way in (0, 1):
                for kind in (SUM3, NEW3):
                    hop(e, way, kind).wait_recv()
                add_into(r3.at[way, e], chunk(e, way, 2))
                hop(e, way, TWO).start()

        group, places = dxb.shape[:2]
        ids = ids_ref[...].astype(F32)
        r = lax.broadcasted_iota(jnp.int32, (group * 8, tok), 0)
        e_of = rem(r, 8)
        expert = jnp.where(e_of < OWN, first_expert(r // 8) + e_of, -1).astype(F32)
        member = jnp.zeros((group * 8, tok), F32)
        for j in range(ids.shape[0]):
            member = member + (jnp.broadcast_to(ids[j:j + 1, :], member.shape) == expert).astype(F32)
        before = dot(member.astype(BF16), strict_upper(tok))
        key_s[...] = jnp.where(member > 0.0, before, -1.0).reshape(key_s.shape)
        rr = lax.broadcasted_iota(jnp.int32, (places, tok), 0)
        at, e_row = rem(rr, cap).astype(F32), rr // cap
        some = rows // places

        @pl.loop(0, OWN)
        def _(e):
            got = dxb.at[:, own_rows(e)]
            pltpu.make_async_copy(got, got, drecv.at[e]).wait()

        own_val.wait()

        @each_other
        def _(k):
            val_copy(k).wait()

        bufs = (xb, gb)
        loads = [pltpu.make_async_copy(dxb.at[pl.ds(i * some, some)], bufs[i % 2].reshape(some, places, hidden), lsem.at[i % 2]) for i in range(group // some)]
        vals = pltpu.make_async_copy(valb, vb, lsem.at[2])
        vals.start()
        loads[0].start()
        for i, load in enumerate(loads):
            for later in loads[i + 1:i + 2]:
                later.start()

            @pl.loop(0, some)
            def _(k):
                key = key_s[i * some + k]
                mine = jnp.full((places, tok), -1.0, F32)
                for e in range(OWN):
                    mine = jnp.where(e_row == e, jnp.broadcast_to(key[e:e + 1, :], (places, tok)), mine)
                sb[pl.ds(pl.multiple_of(k * places, places), places), :] = (at == mine).astype(F32).astype(BF16)

            load.wait()
            part = dot_tn(sb[...], bufs[i % 2][...])
            acc_s[...] = acc_s[...] + part if i else part

        in_grad_ref[...] = acc_s[...].astype(BF16)
        vals.wait()

        def gate_step(k, total):
            for e in range(OWN):
                row = vb[e, pl.ds(k, 1), :]
                total = total + jnp.where(ids == (first_expert(k) + e).astype(F32), jnp.broadcast_to(row, ids.shape), 0.0)
            return total

        gate_ref[...] = lax.fori_loop(0, group, gate_step, jnp.zeros(ids.shape, F32))
        results = [pltpu.make_async_copy(a, b, load_sem.at[i]) for i, a, b in ((0, in_grad_ref, in_grad_hbm), (1, gate_ref, gate_hbm))]
        for copy in results:
            copy.start()

        last = OWN - 1

        @pl.loop(0, last)
        def _(e):
            for way in (0, 1):
                hop(e, way, TWO).wait_recv()
                add_into(r2.at[way, e], chunk(e, way, 1))
                hop(e, way, ONE).start()

        for way in (0, 1):
            hop(last, way, TWO).wait_recv()
        for kind in range(PART, HOPS):
            for way in (0, 1):
                add_into(part_of(r2, way, last, kind), part_of(G, last, z_at(1 if way else NZ - 1)["z"], kind))
                hop(last, way, kind).start()

        def keep(e, m, to, then_remote, then_local):
            src = r1.at[0, e, to // 2, m, pl.ds(to % 2 * d_loc, d_loc)]
            dst = grads.at[m, y * OWN + e]
            n = 0 if isinstance(m, slice) else m

            @pl.when(y != to)
            def _():
                then_remote(remote(src, dst, ysend.at[e, n, to], yrecv.at[e, n, y], {"y": to}))

            @pl.when(y == to)
            def _():
                then_local(pltpu.make_async_copy(src, dst, ysend.at[e, n, to]))

        every = slice(None)

        @pl.loop(0, last)
        def _(e):
            for way in (0, 1):
                hop(e, way, ONE).wait_recv()
            add_into(r1.at[0, e], r1.at[1, e], G.at[e, z])
            for to in range(NY):
                keep(e, every, to, start, start)

        for kind in range(PART, HOPS):
            for way in (0, 1):
                hop(last, way, kind).wait_recv()
            add_into(part_of(r1, 0, last, kind), part_of(r1, 1, last, kind), part_of(G, last, z, kind))
            m, h = (kind - PART) // 2, (kind - PART) % 2
            for to in (2 * h, 2 * h + 1):
                keep(last, m, to, start, start)

        def finish_up(e, kinds, matrices):
            for m in matrices:
                for at in range(NY):
                    def both(copy):
                        wait(grads.at[m, at * OWN + e], yrecv.at[e, 0 if m is every else m, at])
                        copy.wait_send()

                    keep(e, m, at, both, lambda copy: copy.wait())
            for way in (0, 1):
                for kind in kinds:
                    hop(e, way, kind).wait_send()
            sent = dxs.at[e, pl.ds(0, (GROUP - 1) * cap)]
            pltpu.make_async_copy(sent, sent, dsend.at[e]).wait()

        @pl.loop(0, last)
        def _(e):
            finish_up(e, range(PART), [every])

        finish_up(last, [FAR, SUM3, NEW3, TWO, *range(PART, HOPS)], range(3))
        for copy in results:
            copy.wait()

    weight_copies, last_weights = [], []
    pl.run_scoped(gather, *scope_one)
    pl.run_scoped(reduce, *scope_two)
    for number, group, part in weight_copies:
        ref = wown.at[0, pl.ds(*PIECE[group, part])]
        remote(ref, ref, send_sem.at[number], relay_recv.at[0], targets["core"]).wait_send()


def layer(cap, x, u, ids, gates, w1, w3, w2):
    tok, hidden = x.shape
    local_experts, d_loc, ff = w1.shape
    rows = GROUP * cap
    half = hidden // NZ // 2
    cut = tok - tok // 8 if tok % 256 == 0 else tok
    halves = [cut // 2] * 2 + [tok - cut // 2] * 2
    spans = {kind: (sum(halves[:i]), halves[i]) for i, kind in enumerate(KINDS)}
    order = gather_order({kind: 2 * hidden * n for kind, (_, n) in spans.items()}, 2 * w1.size * 3 // local_experts)
    sends = sum(len(s) for _, s in order)
    dma, v, shape = pltpu.SemaphoreType.DMA, pltpu.VMEM, jax.ShapeDtypeStruct
    far = lambda lanes: shape((OWN - 1, rows, lanes), BF16)
    near = lambda lanes: v((rows, lanes), BF16)
    stage = lambda lanes: v((2, OWN - 1, 2 * cap, lanes), BF16)
    sums = [v((2, OWN, 2, 3, half, ff), F32)] * 3
    scope_one = [v((GROUP, 2 * tok, hidden), BF16), v((tok, tok), BF16), stage(hidden), stage(hidden), stage(hidden), stage(tok)]
    scope_two = [v((OWN, NZ, 2, 3, half, ff), F32), v((2, OWN, 3, half, ff), F32)] + sums
    per_expert = v((OWN, GROUP, tok), F32)
    gate_rows = v((GROUP, OWN, tok), F32)
    outs = pl.pallas_call(
        functools.partial(layer_kernel, order, cap, spans, scope_one, scope_two),
        name="layer",
        out_shape=(
            shape((3, local_experts, d_loc, ff), F32), shape((tok, hidden), BF16), shape(ids.shape, F32),
            shape((GROUP, OWN * cap, hidden), BF16), shape((OWN, GROUP, tok), F32), shape((OWN, rows, hidden), BF16),
            far(hidden), far(hidden), far(hidden), far(tok),
        ),
        in_specs=[ANY] * 7,
        out_specs=(ANY,) * 10,
        scratch_shapes=[
            v(ids.shape, ids.dtype), v(ids.shape, F32), v((tok, hidden), BF16), v(ids.shape, F32), gate_rows, gate_rows, v((NY, OWN, 3, d_loc, ff), BF16), v((NZ, NY, OWN, 3, d_loc, ff), BF16), v((OWN, 3, d_loc, ff), BF16),
            near(hidden), near(hidden), near(hidden), near(tok), near(ff), near(ff), near(ff), v((rows, 1), F32),
            near(hidden), per_expert, per_expert, v((GROUP, 8, tok), F32), v((tok, hidden), F32),
            dma((len(KINDS), NY * NX)), dma((len(KINDS), NY * NX)), dma((NZ, NY, 2, 2)), dma((len(RELAYS),)), dma((GROUP,)), dma((sends,)), dma((GROUP,)),
            dma((7,)), dma((2, 4)),
            dma((4,)), dma((2, OWN, HOPS)), dma((2, OWN, HOPS)), dma((OWN, 3, NY)), dma((OWN, 3, NY)),
            dma((OWN,)), dma((OWN,)), dma((2, GROUP)), dma((1,)), pltpu.SemaphoreType.REGULAR, pltpu.SemaphoreType.REGULAR((NY // 2 + NX // 2,)),
        ],
        compiler_params=params(0),
    )(x, u, ids, gates, w1, w3, w2)
    return outs[:3]


def finish_kernel(grads, in_grad, gate, *refs):
    n = 5
    outs, bufs, sems = refs[:n], refs[n:2 * n], refs[-1]
    ins = [grads.at[m] for m in range(3)] + [in_grad, gate]
    load, store = [], []
    for i, (a, b, o) in enumerate(zip(ins, bufs, outs)):
        half = a.shape[0] // 2
        for h in range(2):
            at = pl.ds(h * half, half)
            load.append(pltpu.make_async_copy(a.at[at], b.at[at], sems.at[0, i, h]))
            store.append(pltpu.make_async_copy(b.at[at], o.at[at], sems.at[1, i, h]))
    for copy in load:
        copy.start()
    for before, after in zip(load, store):
        before.wait()
        after.start()
    for copy in store:
        copy.wait()


def finish(grads, in_grad, gate):
    shapes = [grads.shape[1:]] * 3 + [in_grad.shape, gate.shape]
    types = [grads.dtype] * 3 + [in_grad.dtype, gate.dtype]
    return pl.pallas_call(
        finish_kernel,
        name="finish",
        out_shape=[jax.ShapeDtypeStruct(s, t) for s, t in zip(shapes, types)],
        in_specs=[ANY] * 3,
        out_specs=[ANY] * len(shapes),
        scratch_shapes=[pltpu.VMEM(s, t) for s, t in zip(shapes, types)] + [pltpu.SemaphoreType.DMA((2, len(shapes), 2))],
    )(grads, in_grad, gate)


def solution(mesh):
    mesh4 = Mesh(mesh.devices.reshape(NZ, NY, NX, NC), ("z", "y", "x", "core"))
    tok_spec = P(("z", "y", "x", "core"), None)
    up_spec = P(("x", "core"), ("z", "y"), None)
    down_spec = P(("x", "core"), None, ("z", "y"))

    def per_device(layer_in, out_grad, expert_ids, gate_vals, w_one, w_two, w_three):
        tok_dev, hidden = layer_in.shape
        top_k = expert_ids.shape[1]
        local_experts, d_loc, ff = w_one.shape
        cap = capacity_of(tok_dev, top_k, local_experts * NX * NC)
        ids = expert_ids.T
        grads, in_grad, gate_out = layer(cap, layer_in, out_grad, ids, gate_vals.T, w_one, w_three, w_two.swapaxes(1, 2))
        g1, g3, g2, in_grad, gate_out = finish(grads, in_grad, gate_out)
        return in_grad, gate_out.T, g1, g2.swapaxes(1, 2), g3

    return jax.shard_map(per_device, mesh=mesh4, in_specs=(tok_spec, tok_spec, tok_spec, tok_spec, up_spec, down_spec, up_spec), out_specs=(tok_spec, tok_spec, up_spec, down_spec, up_spec), check_vma=False)
```

```python
import functools

import jax
import jax.numpy as jnp
from jax import lax
from jax.experimental import pallas as pl
from jax.experimental.pallas import tpu as pltpu
from jax.sharding import Mesh, PartitionSpec as P

NZ, NY, NX, NC = 8, 4, 4, 2
GROUP = NY * NX * NC
PLANE = ("y", "x", "core")
OWN = 4
F32, BF16 = jnp.float32, jnp.bfloat16
ANY = pl.BlockSpec(memory_space=pl.ANY)


def capacity_of(tok_dev, top_k, experts):
    return max(8, ((tok_dev * top_k * 5) // (4 * experts) + 7) // 8 * 8)


def rem(a, b):
    return a % b if isinstance(a, int) else lax.rem(a, b)


def contract(ca, cb):
    return lambda a, b: lax.dot_general(a, b, (((ca,), (cb,)), ((), ())), preferred_element_type=F32)


dot, dot_nt, dot_tn = contract(1, 0), contract(1, 1), contract(0, 0)


def params(number):
    return pltpu.CompilerParams(collective_id=number, has_side_effects=True, vmem_limit_bytes=67043328)


def each_other(body):
    return pl.loop(1, GROUP)(body)


def strict_upper(n):
    rows = lax.broadcasted_iota(jnp.int32, (n, n), 0)
    cols = lax.broadcasted_iota(jnp.int32, (n, n), 1)
    return (rows < cols).astype(F32).astype(BF16)


def here():
    return tuple(lax.axis_index(a) for a in ("z", "y", "x", "core"))


def at_offset(k):
    _, y, x, c = here()
    dy, dx, dc = k // (NX * NC), rem(k // NC, NX), rem(k, NC)
    return {"y": rem(y + dy, NY), "x": rem(x + dx, NX), "core": rem(c + dc, NC)}


def place_of(d):
    return d["y"] * (NX * NC) + d["x"] * NC + d["core"]


def z_at(dz):
    return {"z": rem(lax.axis_index("z") + dz, NZ)}


def remote(src, dst, send_sem, recv_sem, target):
    return pltpu.make_async_remote_copy(src_ref=src, dst_ref=dst, send_sem=send_sem, recv_sem=recv_sem, device_id=target, device_id_type=pl.DeviceIdType.MESH)


def start(copy):
    copy.start()


def tell(semaphore, targets):
    for target in targets:
        pl.semaphore_signal(semaphore, device_id=target, device_id_type=pl.DeviceIdType.MESH)


RATE, D2D, HOP = 44700.0, 400000.0, 2.3
PUT, TILE, ROWS = 1.0, 1.0, 0.4
STEP = 5
AHEAD, MORE = 5.0, 0.05

PIECE = {(0, None): (0, 1), (1, None): (1, 3), (1, 0): (1, 1), (1, 1): (2, 2)}
RELAYS = ((0, None, "y+"), (1, 0, "y+"), (1, 1, "y-"))


KINDS = ("A0", "A1", "B0", "B1")


def gather_order(sizes, expert_bytes):
    free, pending, coming, order, have, ready = {}, {}, [], [], {}, {}

    def send(now, name, link, arrives, nbytes):
        t = max(now, free.get(link, 0.0)) + nbytes / (D2D if link == "core" else RATE)
        free[link] = t
        coming.append((t + (HOP / 2 if link == "core" else HOP), len(order), len(coming), arrives))
        return (name, link)

    def later(rank, name, link, arrives, nbytes):
        queue = pending.setdefault(link, [])
        queue.append((rank, len(order), len(queue), (name, link, arrives, nbytes)))

    def turn(now):
        out = []
        for link, queue in pending.items():
            queue.sort()
            while queue and free.get(link, 0.0) - now < AHEAD + MORE * now:
                out.append(send(now, *queue.pop(0)[-1]))
        return out

    def on_rows(kind, dy, dx):
        first, second = "xy" if kind[0] == "A" else "yx"
        d = {"x": dx, "y": dy}
        for axis in [first, second] if d[second] == 0 else [second]:
            for sign in (1, -1):
                if d[axis] == 0 or d[axis] == -sign % 4 and kind[1] == "10"[sign > 0]:
                    nd = dict(d)
                    nd[axis] = (d[axis] - sign) % 4
                    rank = 4 + (axis == second) + (d[axis] != 0)
                    later(rank, (kind, dy, dx), axis + "-+"[sign > 0], (kind, nd["y"], nd["x"]), sizes[kind])

    def core(now, key):
        return send(now, key, "core", ("core",) + key, sizes[key[0]])

    def weights(rank, name, group, part, link, arrives):
        later(rank, name, link, arrives + (group, part), PIECE[group, part][1] * expert_bytes)

    def on_piece(dz, dy, group):
        for link, step, far in (("z+", -1, dy < 2), ("z-", 1, dy >= 2)):
            gone = (step * dz) % NZ
            if gone < 3 + far:
                weights(4 * group + gone, ("W", dz, dy, group), group, None, link, ("W", (dz + step) % NZ, dy))

    def arrived(key, part=None):
        have[key] = have.get(key, 0) + (2 if part is None else 1)
        if have[key] == 2:
            ready[key] = True
        return have[key] == 2

    for i, (group, part, link) in enumerate(RELAYS):
        weights(0, ("r", i), group, part, link, ("R", i))
    for group in range(2):
        for dy, link in ((1, "y+"), (3, "y-")):
            weights(2, ("w", dy, group), group, None, link, ("W", 0, (-dy) % NY))
        on_piece(0, 0, group)
    sends = []
    for kind in KINDS[::-1]:
        arrived((kind, 0, 0))
        on_rows(kind, 0, 0)
        sends.append(core(0.0, (kind, 0, 0)))
    order.append((None, turn(0.0) + sends))
    todo, puts, done, now = [(dy, dx) for dy in range(NY) for dx in range(NX)], 0, 0, 0.0
    while coming or todo or done < puts:
        coming.sort()
        soon = coming[0][0] if coming else 1e9
        if soon > now:
            place = next((p for p in todo if all(pre + (kind,) + p in ready for kind in KINDS for pre in ((), ("core",)))), None)
            if place is not None:
                todo.remove(place)
                order.append((("put",) + place, turn(now)))
                puts += 1
                now += PUT
                continue
            step = min(STEP, puts - done)
            weights_in = sum(key[0] == "W" and key[-1] == 0 for key in ready) == NZ * NY - 1
            calm = all(c[-1][0] == "core" for c in coming)
            if weights_in and step and (step >= 3 and soon - now > TILE or calm):
                order.append((("tile", done, done + step), turn(now)))
                done += step
                now += TILE + ROWS * step
                continue
        t, _, _, name = coming.pop(0)
        now = max(now, t)
        if name[0] == "core":
            arrived(name)
            continue
        sends = []
        if name[0] == "R":
            i, group, part = name[1:]
            weights(1, name[:2], group, part, RELAYS[i][2], ("W", 0, 2))
            name = name[:2]
        elif name[0] == "W":
            if arrived(name[:-1], name[-1]):
                on_piece(*name[1:-1])
        else:
            sends = [core(now, name)]
            arrived(name)
            on_rows(*name)
        order.append((name, sends + turn(now)))
    return order


def passed_on(dz, dy):
    return dz != NZ // 2 and dz not in ((3,) if dy < 2 else (5,))


def first_expert(d):
    return rem(d, NX * NC) * (NY * OWN) + d // (NX * NC) * OWN


FAR, SUM3, NEW3, TWO, ONE, PART, HOPS = 0, 1, 2, 3, 4, 5, 11


def layer_kernel(order, cap, spans, scope_one, scope_two, x_hbm, u_hbm, ids_hbm, gates_hbm, w1_hbm, w3_hbm, w2_hbm,
                 grads, in_grad_hbm, gate_hbm, dxb, valb, dxs, xr, ur, gr, sel,
                 ids_ref, gates_ref, in_grad_ref, gate_ref, metas, gates_out, wown, wv, relay, xb, ub, gb, sb, a_s, d1_s, d3_s, y_s, dx_s, val_s, vb, key_s, acc_s,
                 recv, core_recv, wrecv, relay_recv, mrecv, send_sem, msend, load_sem, store_sem,
                 lsem, rsend, rrecv, ysend, yrecv, dsend, drecv, vsem, osem, in_scope):
    z, y, x, c = here()
    tok, hidden = x_hbm.shape
    rows, ff = xb.shape[0], a_s.shape[-1]
    d_loc = hidden // (NZ * NY)
    me = place_of(at_offset(0))

    def place(dy, dx, dc=0):
        return place_of(at_offset(dy * (NX * NC) + dx * NC + dc))

    targets = {"core": {"core": 1 - c}}
    for sign, n in (("+", 1), ("-", -1)):
        targets["x" + sign] = {"x": rem(x + n + NX, NX)}
        targets["y" + sign] = {"y": rem(y + n + NY, NY)}
        targets["z" + sign] = z_at(n + NZ)

    def wait(ref, sem):
        remote(ref, ref, send_sem.at[0], sem, targets["core"]).wait_recv()

    def piece(dz, dy, group, part=None):
        return wv.at[z_at(dz)["z"], rem(y + dy, NY), pl.ds(*PIECE[group, part])]

    def wait_weights(dz, dy, group, part):
        wait(piece(dz, dy, group, part), wrecv.at[dz, dy, group, part or 0])

    def w(e, m):
        return wv[:, :, e, m].reshape(hidden, ff)

    def expert_rows(e, spans):
        def cut_of(ref):
            return jnp.concatenate([ref[s, :] for s in spans]) if spans[1:] else ref[spans[0], :]

        def save(ref, value):
            n = value.shape[0] // len(spans)
            for i, s in enumerate(spans):
                ref[s, :] = value[i * n:(i + 1) * n]

        x_rows = cut_of(xb)
        h1, h3 = dot(x_rows, w(e, 0)), dot(x_rows, w(e, 1))
        sig = jax.nn.sigmoid(h1)
        silu = h1 * sig
        act = (silu * h3).astype(BF16)
        save(a_s, act)
        y_rows = dot_nt(act, w(e, 2))
        save(y_s, jnp.sum(cut_of(ub).astype(F32) * y_rows, axis=1, keepdims=True))
        da = dot(cut_of(gb), w(e, 2))
        d1 = (da * h3 * sig * (1.0 + h1 * (1.0 - sig))).astype(BF16)
        d3 = (da * silu).astype(BF16)
        save(d1_s, d1)
        save(d3_s, d3)
        save(dx_s, (dot_nt(d1, w(e, 0)) + dot_nt(d3, w(e, 1))).astype(BF16))

    def gather(all_rows, tri, sx, su, sg, ss):
        loads = [
            pltpu.make_async_copy(x_hbm, all_rows.at[me, pl.ds(0, tok)], load_sem.at[0]),
            pltpu.make_async_copy(u_hbm, all_rows.at[me, pl.ds(tok, tok)], load_sem.at[1]),
        ]
        for m, ref in enumerate((w1_hbm, w3_hbm, w2_hbm)):
            loads.append(pltpu.make_async_copy(ref.reshape(NY, OWN, d_loc, ff), wown.at[:, :, m], load_sem.at[2 + m]))
        tables = [pltpu.make_async_copy(a, b, load_sem.at[i]) for i, a, b in ((5, ids_hbm, ids_ref), (6, gates_hbm, gates_ref))]
        for copy in tables + loads:
            copy.start()
        barrier = pltpu.get_barrier_semaphore()
        tell(barrier, [targets["z+"], targets["z-"]])

        @each_other
        def _(k):
            tell(barrier, [at_offset(k)])

        for copy in tables:
            copy.wait()

        @pl.loop(0, GROUP)
        def _(d):
            number = first_expert(d) + lax.broadcasted_iota(jnp.int32, (OWN, tok), 0)
            value = jnp.full((OWN, tok), -1.0, F32)
            for j in range(ids_ref.shape[0]):
                chosen = ids_ref[pl.ds(j, 1), :] == number
                value = jnp.where(chosen, jnp.broadcast_to(gates_ref[pl.ds(j, 1), :], value.shape), value)
            gates_out[d] = value

        metas[me] = gates_out[me]
        tri[...] = strict_upper(tok)
        for copy in loads:
            copy.wait()
        pl.semaphore_wait(barrier, GROUP + 1)

        back = {"x+": (0, 3), "x-": (0, 1), "y+": (3, 0), "y-": (1, 0)}
        def block(kind, dy, dx, dc=0):
            return all_rows.at[place(dy, dx, dc), pl.ds(*spans[kind])]

        row_copies = []

        def issue(name, link):
            number = len(row_copies) + len(weight_copies)
            sem = send_sem.at[number]
            group, part_of = None, None
            if name[0] == "w":
                _, dy, group = name
                src = wown.at[rem(y + dy, NY), pl.ds(*PIECE[group, None])]
                copy = remote(src, piece(0, 0, group), sem, wrecv.at[0, (-dy) % NY, group, 0], targets[link])
            elif name[0] in "rR":
                group, part_of, _ = RELAYS[name[1]]
                span = pl.ds(*PIECE[group, part_of])
                if name[0] == "r":
                    copy = remote(wown.at[rem(y + 2, NY), span], relay.at[span], sem, relay_recv.at[name[1]], targets[link])
                else:
                    dst = piece(0, back[link][0], group, part_of)
                    copy = remote(relay.at[span], dst, sem, wrecv.at[0, 2, group, part_of or 0], targets[link])
            elif name[0] == "W":
                _, dz, dy, group = name
                ndz = (dz - 1) % NZ if link == "z+" else (dz + 1) % NZ
                own = wown.at[y, pl.ds(*PIECE[group, None])]
                copy = remote(own if dz == dy == 0 else piece(dz, dy, group), piece(dz, dy, group), sem, wrecv.at[ndz, dy, group, 0], targets[link])
            else:
                kind, dy, dx = name
                ref = block(*name)
                oy, ox = back.get(link, (0, 0))
                arrivals = core_recv if link == "core" else recv
                rsem = arrivals.at[KINDS.index(kind), (dy + oy) % NY * NX + (dx + ox) % NX]
                copy = remote(ref, ref, sem, rsem, targets[link])
            copy.start()
            if group is None:
                row_copies.append(copy)
            else:
                weight_copies.append((number, group, part_of))

        def meta_copy(k):
            to = at_offset(k)
            return remote(gates_out.at[place_of(to)], metas.at[me], msend.at[k], mrecv.at[k], to)

        n_rows = OWN * 2 * cap
        stores, chips = [], []

        def put(dy, dx):
            slot = len(stores) % 2
            if stores[1:]:
                for copy in stores[-2]:
                    copy.wait()
            for dc in (0, 1):
                if dy or dx or dc:
                    k = ((-dy) % NY) * (NX * NC) + ((-dx) % NX) * NC + dc
                    wait(metas.at[place(dy, dx, dc)], mrecv.at[k])
            for i, kind in enumerate(KINDS):
                wait(block(kind, dy, dx, 1), core_recv.at[i, dy * NX + dx])
            chip = rem(y + dy, NY) * NX + rem(x + dx, NX)
            n = 2 * OWN
            which = lax.broadcasted_iota(jnp.int32, (n, tok), 0)
            gate = jnp.zeros((n, tok), F32)
            for i in range(n):
                gate = jnp.where(which == i, jnp.broadcast_to(metas[2 * chip + i // OWN, pl.ds(i % OWN, 1), :], gate.shape), gate)
            member = gate >= 0.0
            key = jnp.where(member, dot(member.astype(F32).astype(BF16), tri[...]), -1.0)
            r = lax.broadcasted_iota(jnp.int32, (n_rows, tok), 0)
            at = rem(r, cap).astype(F32)
            row_of = rem(r // cap, 2) * OWN + r // (2 * cap)
            mine, gates = jnp.full((n_rows, tok), -1.0, F32), jnp.zeros((n_rows, tok), F32)
            for i in range(n):
                mine = jnp.where(row_of == i, jnp.broadcast_to(key[i:i + 1, :], mine.shape), mine)
                gates = jnp.where(row_of == i, jnp.broadcast_to(gate[i:i + 1, :], mine.shape), gates)
            found = at == mine
            pick = [jnp.logical_and(found, row_of // OWN == p).astype(F32) for p in range(2)]
            both = pick[0] + pick[1]
            scale = jnp.sum(both * gates, axis=1, keepdims=True)
            pick = [p.astype(BF16) for p in pick]
            x_rows = dot(pick[0], all_rows[2 * chip, 0:tok, :]) + dot(pick[1], all_rows[2 * chip + 1, 0:tok, :])
            u_rows = dot(pick[0], all_rows[2 * chip, tok:2 * tok, :]) + dot(pick[1], all_rows[2 * chip + 1, tok:2 * tok, :])
            span = pl.ds(pl.multiple_of(chip * 2 * cap, 2 * cap), 2 * cap)
            out = []
            for i, (value, first, stage, far) in enumerate(((x_rows, xb, sx, xr), (u_rows, ub, su, ur), (scale * u_rows, gb, sg, gr), (both, sb, ss, sel))):
                value = value.astype(BF16)
                first[span, :] = value[:2 * cap]
                stage[slot] = value[2 * cap:].reshape(stage.shape[1:])
                out.append(pltpu.make_async_copy(stage.at[slot], far.at[:, span], store_sem.at[slot, i]))
                out[-1].start()
            stores.append(out)
            chips.append(span)

        for name, sends in order:
            if name is None:
                pass
            elif name[0] == "put":
                put(*name[1:])
            elif name[0] == "tile":
                expert_rows(0, chips[name[1]:name[2]])
            elif name[0] == "R":
                group, part, _ = RELAYS[name[1]]
                wait(relay.at[pl.ds(*PIECE[group, part])], relay_recv.at[name[1]])
            elif name[0] == "W":
                if passed_on(*name[1:3]) or not name[3]:
                    wait_weights(*name[1:])
                else:
                    last_weights.append(name[1:])
            else:
                kind, dy, dx = name
                wait(block(*name), recv.at[KINDS.index(kind), dy * NX + dx])
            for send in sends:
                issue(*send)
            if name is None:
                wv[z, y] = wown[y]

                @each_other
                def _(k):
                    meta_copy(k).start()

        for out in stores[-2:]:
            for copy in out:
                copy.wait()

        @each_other
        def _(k):
            meta_copy(k).wait_send()

        for copy in row_copies:
            copy.wait_send()

    def reduce(G, r4, r3, r2, r1):
        tell(in_scope, [targets["z+"], targets["z-"]])

        def row_loads(e):
            pairs = ((xr, xb), (gr, gb), (ur, ub), (sel, sb))
            return [pltpu.make_async_copy(src.at[e - 1], dst, lsem.at[i]) for i, (src, dst) in enumerate(pairs)]

        def chunk(e, way, dist):
            return G.at[e, z_at(dist if way else NZ - dist)["z"]]

        def part_of(ref, way, e, kind):
            return ref.at[way, e, (kind - PART) % 2, (kind - PART) // 2]

        def hop(e, way, kind):
            h = way
            src, dst = {
                FAR: lambda: (chunk(e, way, 4).at[h], r4.at[way, e]),
                SUM3: lambda: (r4.at[way, e], r3.at[way, e, h]),
                NEW3: lambda: (chunk(e, way, 3).at[1 - h], r3.at[way, e, 1 - h]),
                TWO: lambda: (r3.at[way, e], r2.at[way, e]),
                ONE: lambda: (r2.at[way, e], r1.at[way, e]),
            }.get(kind, lambda: (part_of(r2, way, e, kind), part_of(r1, way, e, kind)))()
            return remote(src, dst, rsend.at[way, e, kind], rrecv.at[way, e, kind], z_at(1 if way else NZ - 1))

        def add_into(dst, *others):
            parts = dst.shape[:-2]
            if not parts:
                total = dst[...]
                for other in others:
                    total = total + other[...]
                dst[...] = total
                return

            def flat(ref, i):
                index = []
                for n in reversed(parts):
                    index.append(rem(i, n))
                    i = i // n
                return ref.at[tuple(reversed(index))]

            n = 1
            for p in parts:
                n *= p

            @pl.loop(0, n)
            def _(i):
                total = flat(dst, i)[...]
                for other in others:
                    total = total + flat(other, i)[...]
                flat(dst, i)[...] = total

        def own_rows(s):
            return pl.ds(pl.multiple_of(s * cap, 8), cap)

        def dx_copy(e, k):
            to = at_offset(k)
            return remote(dxs.at[e, own_rows(place_of(to))], dxb.at[me, own_rows(e)], dsend.at[e], drecv.at[e], to)

        tile = 256 if rows % 256 == 0 else rows
        dtile = hidden // NZ
        half = dtile // 2

        def weight_gradients(e):
            out = pltpu.make_async_copy(dx_s, dxs.at[e], osem.at[0])
            out.start()

            @pl.loop(0, NZ // 2)
            def _(i):
                pair = [z_at(n + 2 * i)["z"] for n in (3, 4)]

                def cols(ref):
                    return jnp.concatenate([ref[:, pl.ds(pl.multiple_of(k * dtile, dtile), dtile)] for k in pair], axis=1)

                x_cols, g_cols = cols(xb), cols(gb)
                for m, part in enumerate((dot_tn(x_cols, d1_s[...]), dot_tn(x_cols, d3_s[...]), dot_tn(g_cols, a_s[...]))):
                    for j in range(4):
                        G[e, pair[j // 2], j % 2, m] = part[j * half:(j + 1) * half]

                @pl.when(i == 0)
                def _():
                    if isinstance(e, int):
                        pl.semaphore_wait(in_scope, 2)
                    for way, kind in ((0, FAR), (1, FAR), (1, NEW3)):
                        hop(e, way, kind).start()

                @pl.when(i == 1)
                def _():
                    hop(e, 0, NEW3).start()

            val = sb[...].astype(F32) * y_s[...]
            val_s[e] = jnp.sum(val.reshape(rows // cap, cap, tok), axis=1)
            out.wait()

        def send_back(e):
            pltpu.make_async_copy(dxs.at[e, own_rows(me)], dxb.at[me, own_rows(e)], drecv.at[e]).start()

            @each_other
            def _(k):
                dx_copy(e, k).start()

        def far_sums(e):
            for way in (0, 1):
                hop(e, way, FAR).wait_recv()
                add_into(r4.at[way, e], chunk(e, way, 3).at[way])
                hop(e, way, SUM3).start()

        weight_gradients(0)
        for copy in row_loads(1):
            copy.start()
        send_back(0)
        for name in last_weights:
            wait_weights(*name)

        @pl.loop(1, OWN)
        def _(e):
            for copy in row_loads(e):
                copy.wait()

            @pl.loop(0, rows // tile)
            def _(i):
                expert_rows(e, [pl.ds(pl.multiple_of(i * tile, tile), tile)])

            weight_gradients(e)

            @pl.when(e < OWN - 1)
            def _():
                for copy in row_loads(e + 1):
                    copy.start()

            send_back(e)
            far_sums(e - 1)

        far_sums(OWN - 1)

        def val_copy(k):
            to = at_offset(k)
            return remote(val_s.at[:, place_of(to)], valb.at[:, me], vsem.at[0, k], vsem.at[1, k], to)

        own_val = pltpu.make_async_copy(val_s.at[:, me], valb.at[:, me], vsem.at[0, 0])
        own_val.start()

        @each_other
        def _(k):
            val_copy(k).start()

        @pl.loop(0, OWN)
        def _(e):
            for way in (0, 1):
                for kind in (SUM3, NEW3):
                    hop(e, way, kind).wait_recv()
                add_into(r3.at[way, e], chunk(e, way, 2))
                hop(e, way, TWO).start()

        group, places = dxb.shape[:2]
        ids = ids_ref[...].astype(F32)
        r = lax.broadcasted_iota(jnp.int32, (group * 8, tok), 0)
        e_of = rem(r, 8)
        expert = jnp.where(e_of < OWN, first_expert(r // 8) + e_of, -1).astype(F32)
        member = jnp.zeros((group * 8, tok), F32)
        for j in range(ids.shape[0]):
            member = member + (jnp.broadcast_to(ids[j:j + 1, :], member.shape) == expert).astype(F32)
        before = dot(member.astype(BF16), strict_upper(tok))
        key_s[...] = jnp.where(member > 0.0, before, -1.0).reshape(key_s.shape)
        rr = lax.broadcasted_iota(jnp.int32, (places, tok), 0)
        at, e_row = rem(rr, cap).astype(F32), rr // cap
        some = rows // places

        @pl.loop(0, OWN)
        def _(e):
            got = dxb.at[:, own_rows(e)]
            pltpu.make_async_copy(got, got, drecv.at[e]).wait()

        own_val.wait()

        @each_other
        def _(k):
            val_copy(k).wait()

        bufs = (xb, gb)
        loads = [pltpu.make_async_copy(dxb.at[pl.ds(i * some, some)], bufs[i % 2].reshape(some, places, hidden), lsem.at[i % 2]) for i in range(group // some)]
        vals = pltpu.make_async_copy(valb, vb, lsem.at[2])
        vals.start()
        loads[0].start()
        for i, load in enumerate(loads):
            for later in loads[i + 1:i + 2]:
                later.start()

            @pl.loop(0, some)
            def _(k):
                key = key_s[i * some + k]
                mine = jnp.full((places, tok), -1.0, F32)
                for e in range(OWN):
                    mine = jnp.where(e_row == e, jnp.broadcast_to(key[e:e + 1, :], (places, tok)), mine)
                sb[pl.ds(pl.multiple_of(k * places, places), places), :] = (at == mine).astype(F32).astype(BF16)

            load.wait()
            part = dot_tn(sb[...], bufs[i % 2][...])
            acc_s[...] = acc_s[...] + part if i else part

        in_grad_ref[...] = acc_s[...].astype(BF16)
        vals.wait()

        def gate_step(k, total):
            for e in range(OWN):
                row = vb[e, pl.ds(k, 1), :]
                total = total + jnp.where(ids == (first_expert(k) + e).astype(F32), jnp.broadcast_to(row, ids.shape), 0.0)
            return total

        gate_ref[...] = lax.fori_loop(0, group, gate_step, jnp.zeros(ids.shape, F32))
        results = [pltpu.make_async_copy(a, b, load_sem.at[i]) for i, a, b in ((0, in_grad_ref, in_grad_hbm), (1, gate_ref, gate_hbm))]
        for copy in results:
            copy.start()

        last = OWN - 1

        @pl.loop(0, last)
        def _(e):
            for way in (0, 1):
                hop(e, way, TWO).wait_recv()
                add_into(r2.at[way, e], chunk(e, way, 1))
                hop(e, way, ONE).start()

        for way in (0, 1):
            hop(last, way, TWO).wait_recv()
        for kind in range(PART, HOPS):
            for way in (0, 1):
                add_into(part_of(r2, way, last, kind), part_of(G, last, z_at(1 if way else NZ - 1)["z"], kind))
                hop(last, way, kind).start()

        def keep(e, m, to, then_remote, then_local):
            src = r1.at[0, e, to // 2, m, pl.ds(to % 2 * d_loc, d_loc)]
            dst = grads.at[m, y * OWN + e]
            n = 0 if isinstance(m, slice) else m

            @pl.when(y != to)
            def _():
                then_remote(remote(src, dst, ysend.at[e, n, to], yrecv.at[e, n, y], {"y": to}))

            @pl.when(y == to)
            def _():
                then_local(pltpu.make_async_copy(src, dst, ysend.at[e, n, to]))

        every = slice(None)

        @pl.loop(0, last)
        def _(e):
            for way in (0, 1):
                hop(e, way, ONE).wait_recv()
            add_into(r1.at[0, e], r1.at[1, e], G.at[e, z])
            for to in range(NY):
                keep(e, every, to, start, start)

        for kind in range(PART, HOPS):
            for way in (0, 1):
                hop(last, way, kind).wait_recv()
            add_into(part_of(r1, 0, last, kind), part_of(r1, 1, last, kind), part_of(G, last, z, kind))
            m, h = (kind - PART) // 2, (kind - PART) % 2
            for to in (2 * h, 2 * h + 1):
                keep(last, m, to, start, start)

        def finish_up(e, kinds, matrices):
            for m in matrices:
                for at in range(NY):
                    def both(copy):
                        wait(grads.at[m, at * OWN + e], yrecv.at[e, 0 if m is every else m, at])
                        copy.wait_send()

                    keep(e, m, at, both, lambda copy: copy.wait())
            for way in (0, 1):
                for kind in kinds:
                    hop(e, way, kind).wait_send()
            sent = dxs.at[e, pl.ds(0, (GROUP - 1) * cap)]
            pltpu.make_async_copy(sent, sent, dsend.at[e]).wait()

        @pl.loop(0, last)
        def _(e):
            finish_up(e, range(PART), [every])

        finish_up(last, [FAR, SUM3, NEW3, TWO, *range(PART, HOPS)], range(3))
        for copy in results:
            copy.wait()

    weight_copies, last_weights = [], []
    pl.run_scoped(gather, *scope_one)
    pl.run_scoped(reduce, *scope_two)
    for number, group, part in weight_copies:
        ref = wown.at[0, pl.ds(*PIECE[group, part])]
        remote(ref, ref, send_sem.at[number], relay_recv.at[0], targets["core"]).wait_send()


def layer(cap, x, u, ids, gates, w1, w3, w2):
    tok, hidden = x.shape
    local_experts, d_loc, ff = w1.shape
    rows = GROUP * cap
    half = hidden // NZ // 2
    cut = tok - tok // 8 if tok % 256 == 0 else tok
    halves = [cut // 2] * 2 + [tok - cut // 2] * 2
    spans = {kind: (sum(halves[:i]), halves[i]) for i, kind in enumerate(KINDS)}
    order = gather_order({kind: 2 * hidden * n for kind, (_, n) in spans.items()}, 2 * w1.size * 3 // local_experts)
    sends = sum(len(s) for _, s in order)
    dma, v, shape = pltpu.SemaphoreType.DMA, pltpu.VMEM, jax.ShapeDtypeStruct
    far = lambda lanes: shape((OWN - 1, rows, lanes), BF16)
    near = lambda lanes: v((rows, lanes), BF16)
    stage = lambda lanes: v((2, OWN - 1, 2 * cap, lanes), BF16)
    sums = [v((2, OWN, 2, 3, half, ff), F32)] * 3
    scope_one = [v((GROUP, 2 * tok, hidden), BF16), v((tok, tok), BF16), stage(hidden), stage(hidden), stage(hidden), stage(tok)]
    scope_two = [v((OWN, NZ, 2, 3, half, ff), F32), v((2, OWN, 3, half, ff), F32)] + sums
    per_expert = v((OWN, GROUP, tok), F32)
    gate_rows = v((GROUP, OWN, tok), F32)
    outs = pl.pallas_call(
        functools.partial(layer_kernel, order, cap, spans, scope_one, scope_two),
        name="layer",
        out_shape=(
            shape((3, local_experts, d_loc, ff), F32), shape((tok, hidden), BF16), shape(ids.shape, F32),
            shape((GROUP, OWN * cap, hidden), BF16), shape((OWN, GROUP, tok), F32), shape((OWN, rows, hidden), BF16),
            far(hidden), far(hidden), far(hidden), far(tok),
        ),
        in_specs=[ANY] * 7,
        out_specs=(ANY,) * 10,
        scratch_shapes=[
            v(ids.shape, ids.dtype), v(ids.shape, F32), v((tok, hidden), BF16), v(ids.shape, F32), gate_rows, gate_rows, v((NY, OWN, 3, d_loc, ff), BF16), v((NZ, NY, OWN, 3, d_loc, ff), BF16), v((OWN, 3, d_loc, ff), BF16),
            near(hidden), near(hidden), near(hidden), near(tok), near(ff), near(ff), near(ff), v((rows, 1), F32),
            near(hidden), per_expert, per_expert, v((GROUP, 8, tok), F32), v((tok, hidden), F32),
            dma((len(KINDS), NY * NX)), dma((len(KINDS), NY * NX)), dma((NZ, NY, 2, 2)), dma((len(RELAYS),)), dma((GROUP,)), dma((sends,)), dma((GROUP,)),
            dma((7,)), dma((2, 4)),
            dma((4,)), dma((2, OWN, HOPS)), dma((2, OWN, HOPS)), dma((OWN, 3, NY)), dma((OWN, 3, NY)),
            dma((OWN,)), dma((OWN,)), dma((2, GROUP)), dma((1,)), pltpu.SemaphoreType.REGULAR,
        ],
        compiler_params=params(0),
    )(x, u, ids, gates, w1, w3, w2)
    return outs[:3]


def finish_kernel(grads, in_grad, gate, *refs):
    n = 5
    outs, bufs, sems = refs[:n], refs[n:2 * n], refs[-1]
    ins = [grads.at[m] for m in range(3)] + [in_grad, gate]
    load, store = [], []
    for i, (a, b, o) in enumerate(zip(ins, bufs, outs)):
        half = a.shape[0] // 2
        for h in range(2):
            at = pl.ds(h * half, half)
            load.append(pltpu.make_async_copy(a.at[at], b.at[at], sems.at[0, i, h]))
            store.append(pltpu.make_async_copy(b.at[at], o.at[at], sems.at[1, i, h]))
    for copy in load:
        copy.start()
    for before, after in zip(load, store):
        before.wait()
        after.start()
    for copy in store:
        copy.wait()


def finish(grads, in_grad, gate):
    shapes = [grads.shape[1:]] * 3 + [in_grad.shape, gate.shape]
    types = [grads.dtype] * 3 + [in_grad.dtype, gate.dtype]
    return pl.pallas_call(
        finish_kernel,
        name="finish",
        out_shape=[jax.ShapeDtypeStruct(s, t) for s, t in zip(shapes, types)],
        in_specs=[ANY] * 3,
        out_specs=[ANY] * len(shapes),
        scratch_shapes=[pltpu.VMEM(s, t) for s, t in zip(shapes, types)] + [pltpu.SemaphoreType.DMA((2, len(shapes), 2))],
    )(grads, in_grad, gate)


def solution(mesh):
    mesh4 = Mesh(mesh.devices.reshape(NZ, NY, NX, NC), ("z", "y", "x", "core"))
    tok_spec = P(("z", "y", "x", "core"), None)
    up_spec = P(("x", "core"), ("z", "y"), None)
    down_spec = P(("x", "core"), None, ("z", "y"))

    def per_device(layer_in, out_grad, expert_ids, gate_vals, w_one, w_two, w_three):
        tok_dev, hidden = layer_in.shape
        top_k = expert_ids.shape[1]
        local_experts, d_loc, ff = w_one.shape
        cap = capacity_of(tok_dev, top_k, local_experts * NX * NC)
        ids = expert_ids.T
        grads, in_grad, gate_out = layer(cap, layer_in, out_grad, ids, gate_vals.T, w_one, w_three, w_two.swapaxes(1, 2))
        g1, g3, g2, in_grad, gate_out = finish(grads, in_grad, gate_out)
        return in_grad, gate_out.T, g1, g2.swapaxes(1, 2), g3

    return jax.shard_map(per_device, mesh=mesh4, in_specs=(tok_spec, tok_spec, tok_spec, tok_spec, up_spec, down_spec, up_spec), out_specs=(tok_spec, tok_spec, up_spec, down_spec, up_spec), check_vma=False)
```

```python
import functools

import jax
import jax.numpy as jnp
from jax import lax
from jax.experimental import pallas as pl
from jax.experimental.pallas import tpu as pltpu
from jax.sharding import Mesh, PartitionSpec as P

NZ, NY, NX, NC = 8, 4, 4, 2
GROUP = NY * NX * NC
PLANE = ("y", "x", "core")
OWN = 4
F32, BF16 = jnp.float32, jnp.bfloat16
ANY = pl.BlockSpec(memory_space=pl.ANY)


def capacity_of(tok_dev, top_k, experts):
    return max(8, ((tok_dev * top_k * 5) // (4 * experts) + 7) // 8 * 8)


def rem(a, b):
    return a % b if isinstance(a, int) else lax.rem(a, b)


def contract(ca, cb):
    return lambda a, b: lax.dot_general(a, b, (((ca,), (cb,)), ((), ())), preferred_element_type=F32)


dot, dot_nt, dot_tn = contract(1, 0), contract(1, 1), contract(0, 0)


def params(number):
    return pltpu.CompilerParams(collective_id=number, has_side_effects=True, vmem_limit_bytes=67043328)


def each_other(body):
    return pl.loop(1, GROUP)(body)


def strict_upper(n):
    rows = lax.broadcasted_iota(jnp.int32, (n, n), 0)
    cols = lax.broadcasted_iota(jnp.int32, (n, n), 1)
    return (rows < cols).astype(F32).astype(BF16)


def here():
    return tuple(lax.axis_index(a) for a in ("z", "y", "x", "core"))


def at_offset(k):
    _, y, x, c = here()
    dy, dx, dc = k // (NX * NC), rem(k // NC, NX), rem(k, NC)
    return {"y": rem(y + dy, NY), "x": rem(x + dx, NX), "core": rem(c + dc, NC)}


def place_of(d):
    return d["y"] * (NX * NC) + d["x"] * NC + d["core"]


def z_at(dz):
    return {"z": rem(lax.axis_index("z") + dz, NZ)}


def remote(src, dst, send_sem, recv_sem, target):
    return pltpu.make_async_remote_copy(src_ref=src, dst_ref=dst, send_sem=send_sem, recv_sem=recv_sem, device_id=target, device_id_type=pl.DeviceIdType.MESH)


def start(copy):
    copy.start()


def tell(semaphore, targets):
    for target in targets:
        pl.semaphore_signal(semaphore, device_id=target, device_id_type=pl.DeviceIdType.MESH)


RATE, D2D, HOP = 44700.0, 400000.0, 2.3
PUT, TILE, ROWS = 1.0, 1.0, 0.4
STEP = 5
AHEAD, MORE = 10.0, 0.0

PIECE = {(0, None): (0, 1), (1, None): (1, 3), (1, 0): (1, 1), (1, 1): (2, 2)}
RELAYS = ((0, None, "y+"), (1, 0, "y+"), (1, 1, "y-"))


KINDS = ("A0", "A1", "B0", "B1")


def gather_order(sizes, expert_bytes):
    free, pending, coming, order, have, ready = {}, {}, [], [], {}, {}

    def send(now, name, link, arrives, nbytes):
        t = max(now, free.get(link, 0.0)) + nbytes / (D2D if link == "core" else RATE)
        free[link] = t
        coming.append((t + (HOP / 2 if link == "core" else HOP), len(order), len(coming), arrives))
        return (name, link)

    def later(rank, name, link, arrives, nbytes):
        queue = pending.setdefault(link, [])
        queue.append((rank, len(order), len(queue), (name, link, arrives, nbytes)))

    def turn(now):
        out = []
        for link, queue in pending.items():
            queue.sort()
            while queue and free.get(link, 0.0) - now < AHEAD + MORE * now:
                out.append(send(now, *queue.pop(0)[-1]))
        return out

    def on_rows(kind, dy, dx):
        first, second = "xy" if kind[0] == "A" else "yx"
        d = {"x": dx, "y": dy}
        for axis in [first, second] if d[second] == 0 else [second]:
            for sign in (1, -1):
                if d[axis] == 0 or d[axis] == -sign % 4 and kind[1] == "10"[sign > 0]:
                    nd = dict(d)
                    nd[axis] = (d[axis] - sign) % 4
                    rank = 4 + (axis == second) + (d[axis] != 0)
                    later(rank, (kind, dy, dx), axis + "-+"[sign > 0], (kind, nd["y"], nd["x"]), sizes[kind])

    def core(now, key):
        return send(now, key, "core", ("core",) + key, sizes[key[0]])

    def weights(rank, name, group, part, link, arrives):
        later(rank, name, link, arrives + (group, part), PIECE[group, part][1] * expert_bytes)

    def on_piece(dz, dy, group):
        for link, step, far in (("z+", -1, dy < 2), ("z-", 1, dy >= 2)):
            gone = (step * dz) % NZ
            if gone < 3 + far:
                weights(4 * group + gone, ("W", dz, dy, group), group, None, link, ("W", (dz + step) % NZ, dy))

    def arrived(key, part=None):
        have[key] = have.get(key, 0) + (2 if part is None else 1)
        if have[key] == 2:
            ready[key] = True
        return have[key] == 2

    for i, (group, part, link) in enumerate(RELAYS):
        weights(0, ("r", i), group, part, link, ("R", i))
    for group in range(2):
        for dy, link in ((1, "y+"), (3, "y-")):
            weights(2, ("w", dy, group), group, None, link, ("W", 0, (-dy) % NY))
        on_piece(0, 0, group)
    sends = []
    for kind in KINDS[::-1]:
        arrived((kind, 0, 0))
        on_rows(kind, 0, 0)
        sends.append(core(0.0, (kind, 0, 0)))
    order.append((None, turn(0.0) + sends))
    todo, puts, done, now = [(dy, dx) for dy in range(NY) for dx in range(NX)], 0, 0, 0.0
    while coming or todo or done < puts:
        coming.sort()
        soon = coming[0][0] if coming else 1e9
        if soon > now:
            place = next((p for p in todo if all(pre + (kind,) + p in ready for kind in KINDS for pre in ((), ("core",)))), None)
            if place is not None:
                todo.remove(place)
                order.append((("put",) + place, turn(now)))
                puts += 1
                now += PUT
                continue
            step = min(STEP, puts - done)
            weights_in = sum(key[0] == "W" and key[-1] == 0 for key in ready) == NZ * NY - 1
            calm = all(c[-1][0] == "core" for c in coming)
            if weights_in and step and (step >= 3 and soon - now > TILE or calm):
                order.append((("tile", done, done + step), turn(now)))
                done += step
                now += TILE + ROWS * step
                continue
        t, _, _, name = coming.pop(0)
        now = max(now, t)
        if name[0] == "core":
            arrived(name)
            continue
        sends = []
        if name[0] == "R":
            i, group, part = name[1:]
            weights(1, name[:2], group, part, RELAYS[i][2], ("W", 0, 2))
            name = name[:2]
        elif name[0] == "W":
            if arrived(name[:-1], name[-1]):
                on_piece(*name[1:-1])
        else:
            sends = [core(now, name)]
            arrived(name)
            on_rows(*name)
        order.append((name, sends + turn(now)))
    return order


def passed_on(dz, dy):
    return dz != NZ // 2 and dz not in ((3,) if dy < 2 else (5,))


def first_expert(d):
    return rem(d, NX * NC) * (NY * OWN) + d // (NX * NC) * OWN


FAR, SUM3, NEW3, TWO, ONE, PART, HOPS = 0, 1, 2, 3, 4, 5, 11


def layer_kernel(order, cap, spans, scope_one, scope_two, x_hbm, u_hbm, ids_hbm, gates_hbm, w1_hbm, w3_hbm, w2_hbm,
                 grads, in_grad_hbm, gate_hbm, dxb, valb, dxs, xr, ur, gr, sel,
                 ids_ref, gates_ref, in_grad_ref, gate_ref, metas, gates_out, wown, wv, relay, xb, ub, gb, sb, a_s, d1_s, d3_s, y_s, dx_s, val_s, vb, key_s, acc_s,
                 recv, core_recv, wrecv, relay_recv, mrecv, send_sem, msend, load_sem, store_sem,
                 lsem, rsend, rrecv, ysend, yrecv, dsend, drecv, vsem, osem, in_scope):
    z, y, x, c = here()
    tok, hidden = x_hbm.shape
    rows, ff = xb.shape[0], a_s.shape[-1]
    d_loc = hidden // (NZ * NY)
    me = place_of(at_offset(0))

    def place(dy, dx, dc=0):
        return place_of(at_offset(dy * (NX * NC) + dx * NC + dc))

    targets = {"core": {"core": 1 - c}}
    for sign, n in (("+", 1), ("-", -1)):
        targets["x" + sign] = {"x": rem(x + n + NX, NX)}
        targets["y" + sign] = {"y": rem(y + n + NY, NY)}
        targets["z" + sign] = z_at(n + NZ)

    def wait(ref, sem):
        remote(ref, ref, send_sem.at[0], sem, targets["core"]).wait_recv()

    def piece(dz, dy, group, part=None):
        return wv.at[z_at(dz)["z"], rem(y + dy, NY), pl.ds(*PIECE[group, part])]

    def wait_weights(dz, dy, group, part):
        wait(piece(dz, dy, group, part), wrecv.at[dz, dy, group, part or 0])

    def w(e, m):
        return wv[:, :, e, m].reshape(hidden, ff)

    def expert_rows(e, spans):
        def cut_of(ref):
            return jnp.concatenate([ref[s, :] for s in spans]) if spans[1:] else ref[spans[0], :]

        def save(ref, value):
            n = value.shape[0] // len(spans)
            for i, s in enumerate(spans):
                ref[s, :] = value[i * n:(i + 1) * n]

        x_rows = cut_of(xb)
        h1, h3 = dot(x_rows, w(e, 0)), dot(x_rows, w(e, 1))
        sig = jax.nn.sigmoid(h1)
        silu = h1 * sig
        act = (silu * h3).astype(BF16)
        save(a_s, act)
        y_rows = dot_nt(act, w(e, 2))
        save(y_s, jnp.sum(cut_of(ub).astype(F32) * y_rows, axis=1, keepdims=True))
        da = dot(cut_of(gb), w(e, 2))
        d1 = (da * h3 * sig * (1.0 + h1 * (1.0 - sig))).astype(BF16)
        d3 = (da * silu).astype(BF16)
        save(d1_s, d1)
        save(d3_s, d3)
        save(dx_s, (dot_nt(d1, w(e, 0)) + dot_nt(d3, w(e, 1))).astype(BF16))

    def gather(all_rows, tri, sx, su, sg, ss):
        loads = [
            pltpu.make_async_copy(x_hbm, all_rows.at[me, pl.ds(0, tok)], load_sem.at[0]),
            pltpu.make_async_copy(u_hbm, all_rows.at[me, pl.ds(tok, tok)], load_sem.at[1]),
        ]
        for m, ref in enumerate((w1_hbm, w3_hbm, w2_hbm)):
            loads.append(pltpu.make_async_copy(ref.reshape(NY, OWN, d_loc, ff), wown.at[:, :, m], load_sem.at[2 + m]))
        tables = [pltpu.make_async_copy(a, b, load_sem.at[i]) for i, a, b in ((5, ids_hbm, ids_ref), (6, gates_hbm, gates_ref))]
        for copy in tables + loads:
            copy.start()
        barrier = pltpu.get_barrier_semaphore()
        tell(barrier, [targets["z+"], targets["z-"]])

        @each_other
        def _(k):
            tell(barrier, [at_offset(k)])

        for copy in tables:
            copy.wait()

        @pl.loop(0, GROUP)
        def _(d):
            number = first_expert(d) + lax.broadcasted_iota(jnp.int32, (OWN, tok), 0)
            value = jnp.full((OWN, tok), -1.0, F32)
            for j in range(ids_ref.shape[0]):
                chosen = ids_ref[pl.ds(j, 1), :] == number
                value = jnp.where(chosen, jnp.broadcast_to(gates_ref[pl.ds(j, 1), :], value.shape), value)
            gates_out[d] = value

        metas[me] = gates_out[me]
        tri[...] = strict_upper(tok)
        for copy in loads:
            copy.wait()
        pl.semaphore_wait(barrier, GROUP + 1)

        back = {"x+": (0, 3), "x-": (0, 1), "y+": (3, 0), "y-": (1, 0)}
        def block(kind, dy, dx, dc=0):
            return all_rows.at[place(dy, dx, dc), pl.ds(*spans[kind])]

        row_copies = []

        def issue(name, link):
            number = len(row_copies) + len(weight_copies)
            sem = send_sem.at[number]
            group, part_of = None, None
            if name[0] == "w":
                _, dy, group = name
                src = wown.at[rem(y + dy, NY), pl.ds(*PIECE[group, None])]
                copy = remote(src, piece(0, 0, group), sem, wrecv.at[0, (-dy) % NY, group, 0], targets[link])
            elif name[0] in "rR":
                group, part_of, _ = RELAYS[name[1]]
                span = pl.ds(*PIECE[group, part_of])
                if name[0] == "r":
                    copy = remote(wown.at[rem(y + 2, NY), span], relay.at[span], sem, relay_recv.at[name[1]], targets[link])
                else:
                    dst = piece(0, back[link][0], group, part_of)
                    copy = remote(relay.at[span], dst, sem, wrecv.at[0, 2, group, part_of or 0], targets[link])
            elif name[0] == "W":
                _, dz, dy, group = name
                ndz = (dz - 1) % NZ if link == "z+" else (dz + 1) % NZ
                own = wown.at[y, pl.ds(*PIECE[group, None])]
                copy = remote(own if dz == dy == 0 else piece(dz, dy, group), piece(dz, dy, group), sem, wrecv.at[ndz, dy, group, 0], targets[link])
            else:
                kind, dy, dx = name
                ref = block(*name)
                oy, ox = back.get(link, (0, 0))
                arrivals = core_recv if link == "core" else recv
                rsem = arrivals.at[KINDS.index(kind), (dy + oy) % NY * NX + (dx + ox) % NX]
                copy = remote(ref, ref, sem, rsem, targets[link])
            copy.start()
            if group is None:
                row_copies.append(copy)
            else:
                weight_copies.append((number, group, part_of))

        def meta_copy(k):
            to = at_offset(k)
            return remote(gates_out.at[place_of(to)], metas.at[me], msend.at[k], mrecv.at[k], to)

        n_rows = OWN * 2 * cap
        stores, chips = [], []

        def put(dy, dx):
            slot = len(stores) % 2
            if stores[1:]:
                for copy in stores[-2]:
                    copy.wait()
            for dc in (0, 1):
                if dy or dx or dc:
                    k = ((-dy) % NY) * (NX * NC) + ((-dx) % NX) * NC + dc
                    wait(metas.at[place(dy, dx, dc)], mrecv.at[k])
            for i, kind in enumerate(KINDS):
                wait(block(kind, dy, dx, 1), core_recv.at[i, dy * NX + dx])
            chip = rem(y + dy, NY) * NX + rem(x + dx, NX)
            n = 2 * OWN
            which = lax.broadcasted_iota(jnp.int32, (n, tok), 0)
            gate = jnp.zeros((n, tok), F32)
            for i in range(n):
                gate = jnp.where(which == i, jnp.broadcast_to(metas[2 * chip + i // OWN, pl.ds(i % OWN, 1), :], gate.shape), gate)
            member = gate >= 0.0
            key = jnp.where(member, dot(member.astype(F32).astype(BF16), tri[...]), -1.0)
            r = lax.broadcasted_iota(jnp.int32, (n_rows, tok), 0)
            at = rem(r, cap).astype(F32)
            row_of = rem(r // cap, 2) * OWN + r // (2 * cap)
            mine, gates = jnp.full((n_rows, tok), -1.0, F32), jnp.zeros((n_rows, tok), F32)
            for i in range(n):
                mine = jnp.where(row_of == i, jnp.broadcast_to(key[i:i + 1, :], mine.shape), mine)
                gates = jnp.where(row_of == i, jnp.broadcast_to(gate[i:i + 1, :], mine.shape), gates)
            found = at == mine
            pick = [jnp.logical_and(found, row_of // OWN == p).astype(F32) for p in range(2)]
            both = pick[0] + pick[1]
            scale = jnp.sum(both * gates, axis=1, keepdims=True)
            pick = [p.astype(BF16) for p in pick]
            x_rows = dot(pick[0], all_rows[2 * chip, 0:tok, :]) + dot(pick[1], all_rows[2 * chip + 1, 0:tok, :])
            u_rows = dot(pick[0], all_rows[2 * chip, tok:2 * tok, :]) + dot(pick[1], all_rows[2 * chip + 1, tok:2 * tok, :])
            span = pl.ds(pl.multiple_of(chip * 2 * cap, 2 * cap), 2 * cap)
            out = []
            for i, (value, first, stage, far) in enumerate(((x_rows, xb, sx, xr), (u_rows, ub, su, ur), (scale * u_rows, gb, sg, gr), (both, sb, ss, sel))):
                value = value.astype(BF16)
                first[span, :] = value[:2 * cap]
                stage[slot] = value[2 * cap:].reshape(stage.shape[1:])
                out.append(pltpu.make_async_copy(stage.at[slot], far.at[:, span], store_sem.at[slot, i]))
                out[-1].start()
            stores.append(out)
            chips.append(span)

        for name, sends in order:
            if name is None:
                pass
            elif name[0] == "put":
                put(*name[1:])
            elif name[0] == "tile":
                expert_rows(0, chips[name[1]:name[2]])
            elif name[0] == "R":
                group, part, _ = RELAYS[name[1]]
                wait(relay.at[pl.ds(*PIECE[group, part])], relay_recv.at[name[1]])
            elif name[0] == "W":
                if passed_on(*name[1:3]) or not name[3]:
                    wait_weights(*name[1:])
                else:
                    last_weights.append(name[1:])
            else:
                kind, dy, dx = name
                wait(block(*name), recv.at[KINDS.index(kind), dy * NX + dx])
            for send in sends:
                issue(*send)
            if name is None:
                wv[z, y] = wown[y]

                @each_other
                def _(k):
                    meta_copy(k).start()

        for out in stores[-2:]:
            for copy in out:
                copy.wait()

        @each_other
        def _(k):
            meta_copy(k).wait_send()

        for copy in row_copies:
            copy.wait_send()

    def reduce(G, r4, r3, r2, r1):
        tell(in_scope, [targets["z+"], targets["z-"]])

        def row_loads(e):
            pairs = ((xr, xb), (gr, gb), (ur, ub), (sel, sb))
            return [pltpu.make_async_copy(src.at[e - 1], dst, lsem.at[i]) for i, (src, dst) in enumerate(pairs)]

        def chunk(e, way, dist):
            return G.at[e, z_at(dist if way else NZ - dist)["z"]]

        def part_of(ref, way, e, kind):
            return ref.at[way, e, (kind - PART) % 2, (kind - PART) // 2]

        def hop(e, way, kind):
            h = way
            src, dst = {
                FAR: lambda: (chunk(e, way, 4).at[h], r4.at[way, e]),
                SUM3: lambda: (r4.at[way, e], r3.at[way, e, h]),
                NEW3: lambda: (chunk(e, way, 3).at[1 - h], r3.at[way, e, 1 - h]),
                TWO: lambda: (r3.at[way, e], r2.at[way, e]),
                ONE: lambda: (r2.at[way, e], r1.at[way, e]),
            }.get(kind, lambda: (part_of(r2, way, e, kind), part_of(r1, way, e, kind)))()
            return remote(src, dst, rsend.at[way, e, kind], rrecv.at[way, e, kind], z_at(1 if way else NZ - 1))

        def add_into(dst, *others):
            parts = dst.shape[:-2]
            if not parts:
                total = dst[...]
                for other in others:
                    total = total + other[...]
                dst[...] = total
                return

            def flat(ref, i):
                index = []
                for n in reversed(parts):
                    index.append(rem(i, n))
                    i = i // n
                return ref.at[tuple(reversed(index))]

            n = 1
            for p in parts:
                n *= p

            @pl.loop(0, n)
            def _(i):
                total = flat(dst, i)[...]
                for other in others:
                    total = total + flat(other, i)[...]
                flat(dst, i)[...] = total

        def own_rows(s):
            return pl.ds(pl.multiple_of(s * cap, 8), cap)

        def dx_copy(e, k):
            to = at_offset(k)
            return remote(dxs.at[e, own_rows(place_of(to))], dxb.at[me, own_rows(e)], dsend.at[e], drecv.at[e], to)

        tile = 256 if rows % 256 == 0 else rows
        dtile = hidden // NZ
        half = dtile // 2

        def weight_gradients(e):
            out = pltpu.make_async_copy(dx_s, dxs.at[e], osem.at[0])
            out.start()

            @pl.loop(0, NZ // 2)
            def _(i):
                pair = [z_at(n + 2 * i)["z"] for n in (3, 4)]

                def cols(ref):
                    return jnp.concatenate([ref[:, pl.ds(pl.multiple_of(k * dtile, dtile), dtile)] for k in pair], axis=1)

                x_cols, g_cols = cols(xb), cols(gb)
                for m, part in enumerate((dot_tn(x_cols, d1_s[...]), dot_tn(x_cols, d3_s[...]), dot_tn(g_cols, a_s[...]))):
                    for j in range(4):
                        G[e, pair[j // 2], j % 2, m] = part[j * half:(j + 1) * half]

                @pl.when(i == 0)
                def _():
                    if isinstance(e, int):
                        pl.semaphore_wait(in_scope, 2)
                    for way, kind in ((0, FAR), (1, FAR), (1, NEW3)):
                        hop(e, way, kind).start()

                @pl.when(i == 1)
                def _():
                    hop(e, 0, NEW3).start()

            val = sb[...].astype(F32) * y_s[...]
            val_s[e] = jnp.sum(val.reshape(rows // cap, cap, tok), axis=1)
            out.wait()

        def send_back(e):
            pltpu.make_async_copy(dxs.at[e, own_rows(me)], dxb.at[me, own_rows(e)], drecv.at[e]).start()

            @each_other
            def _(k):
                dx_copy(e, k).start()

        def far_sums(e):
            for way in (0, 1):
                hop(e, way, FAR).wait_recv()
                add_into(r4.at[way, e], chunk(e, way, 3).at[way])
                hop(e, way, SUM3).start()

        weight_gradients(0)
        for copy in row_loads(1):
            copy.start()
        send_back(0)
        for name in last_weights:
            wait_weights(*name)

        @pl.loop(1, OWN)
        def _(e):
            for copy in row_loads(e):
                copy.wait()

            @pl.loop(0, rows // tile)
            def _(i):
                expert_rows(e, [pl.ds(pl.multiple_of(i * tile, tile), tile)])

            weight_gradients(e)

            @pl.when(e < OWN - 1)
            def _():
                for copy in row_loads(e + 1):
                    copy.start()

            send_back(e)
            far_sums(e - 1)

        far_sums(OWN - 1)

        def val_copy(k):
            to = at_offset(k)
            return remote(val_s.at[:, place_of(to)], valb.at[:, me], vsem.at[0, k], vsem.at[1, k], to)

        own_val = pltpu.make_async_copy(val_s.at[:, me], valb.at[:, me], vsem.at[0, 0])
        own_val.start()

        @each_other
        def _(k):
            val_copy(k).start()

        @pl.loop(0, OWN)
        def _(e):
            for way in (0, 1):
                for kind in (SUM3, NEW3):
                    hop(e, way, kind).wait_recv()
                add_into(r3.at[way, e], chunk(e, way, 2))
                hop(e, way, TWO).start()

        group, places = dxb.shape[:2]
        ids = ids_ref[...].astype(F32)
        r = lax.broadcasted_iota(jnp.int32, (group * 8, tok), 0)
        e_of = rem(r, 8)
        expert = jnp.where(e_of < OWN, first_expert(r // 8) + e_of, -1).astype(F32)
        member = jnp.zeros((group * 8, tok), F32)
        for j in range(ids.shape[0]):
            member = member + (jnp.broadcast_to(ids[j:j + 1, :], member.shape) == expert).astype(F32)
        before = dot(member.astype(BF16), strict_upper(tok))
        key_s[...] = jnp.where(member > 0.0, before, -1.0).reshape(key_s.shape)
        rr = lax.broadcasted_iota(jnp.int32, (places, tok), 0)
        at, e_row = rem(rr, cap).astype(F32), rr // cap
        some = rows // places

        @pl.loop(0, OWN)
        def _(e):
            got = dxb.at[:, own_rows(e)]
            pltpu.make_async_copy(got, got, drecv.at[e]).wait()

        own_val.wait()

        @each_other
        def _(k):
            val_copy(k).wait()

        bufs = (xb, gb)
        loads = [pltpu.make_async_copy(dxb.at[pl.ds(i * some, some)], bufs[i % 2].reshape(some, places, hidden), lsem.at[i % 2]) for i in range(group // some)]
        vals = pltpu.make_async_copy(valb, vb, lsem.at[2])
        vals.start()
        loads[0].start()
        for i, load in enumerate(loads):
            for later in loads[i + 1:i + 2]:
                later.start()

            @pl.loop(0, some)
            def _(k):
                key = key_s[i * some + k]
                mine = jnp.full((places, tok), -1.0, F32)
                for e in range(OWN):
                    mine = jnp.where(e_row == e, jnp.broadcast_to(key[e:e + 1, :], (places, tok)), mine)
                sb[pl.ds(pl.multiple_of(k * places, places), places), :] = (at == mine).astype(F32).astype(BF16)

            load.wait()
            part = dot_tn(sb[...], bufs[i % 2][...])
            acc_s[...] = acc_s[...] + part if i else part

        in_grad_ref[...] = acc_s[...].astype(BF16)
        vals.wait()

        def gate_step(k, total):
            for e in range(OWN):
                row = vb[e, pl.ds(k, 1), :]
                total = total + jnp.where(ids == (first_expert(k) + e).astype(F32), jnp.broadcast_to(row, ids.shape), 0.0)
            return total

        gate_ref[...] = lax.fori_loop(0, group, gate_step, jnp.zeros(ids.shape, F32))
        results = [pltpu.make_async_copy(a, b, load_sem.at[i]) for i, a, b in ((0, in_grad_ref, in_grad_hbm), (1, gate_ref, gate_hbm))]
        for copy in results:
            copy.start()

        last = OWN - 1

        @pl.loop(0, last)
        def _(e):
            for way in (0, 1):
                hop(e, way, TWO).wait_recv()
                add_into(r2.at[way, e], chunk(e, way, 1))
                hop(e, way, ONE).start()

        for way in (0, 1):
            hop(last, way, TWO).wait_recv()
        for kind in range(PART, HOPS):
            for way in (0, 1):
                add_into(part_of(r2, way, last, kind), part_of(G, last, z_at(1 if way else NZ - 1)["z"], kind))
                hop(last, way, kind).start()

        def keep(e, m, to, then_remote, then_local):
            src = r1.at[0, e, to // 2, m, pl.ds(to % 2 * d_loc, d_loc)]
            dst = grads.at[m, y * OWN + e]
            n = 0 if isinstance(m, slice) else m

            @pl.when(y != to)
            def _():
                then_remote(remote(src, dst, ysend.at[e, n, to], yrecv.at[e, n, y], {"y": to}))

            @pl.when(y == to)
            def _():
                then_local(pltpu.make_async_copy(src, dst, ysend.at[e, n, to]))

        every = slice(None)

        @pl.loop(0, last)
        def _(e):
            for way in (0, 1):
                hop(e, way, ONE).wait_recv()
            add_into(r1.at[0, e], r1.at[1, e], G.at[e, z])
            for to in range(NY):
                keep(e, every, to, start, start)

        for kind in range(PART, HOPS):
            for way in (0, 1):
                hop(last, way, kind).wait_recv()
            add_into(part_of(r1, 0, last, kind), part_of(r1, 1, last, kind), part_of(G, last, z, kind))
            m, h = (kind - PART) // 2, (kind - PART) % 2
            for to in (2 * h, 2 * h + 1):
                keep(last, m, to, start, start)

        def finish_up(e, kinds, matrices):
            for m in matrices:
                for at in range(NY):
                    def both(copy):
                        wait(grads.at[m, at * OWN + e], yrecv.at[e, 0 if m is every else m, at])
                        copy.wait_send()

                    keep(e, m, at, both, lambda copy: copy.wait())
            for way in (0, 1):
                for kind in kinds:
                    hop(e, way, kind).wait_send()
            sent = dxs.at[e, pl.ds(0, (GROUP - 1) * cap)]
            pltpu.make_async_copy(sent, sent, dsend.at[e]).wait()

        @pl.loop(0, last)
        def _(e):
            finish_up(e, range(PART), [every])

        finish_up(last, [FAR, SUM3, NEW3, TWO, *range(PART, HOPS)], range(3))
        for copy in results:
            copy.wait()

    weight_copies, last_weights = [], []
    pl.run_scoped(gather, *scope_one)
    pl.run_scoped(reduce, *scope_two)
    for number, group, part in weight_copies:
        ref = wown.at[0, pl.ds(*PIECE[group, part])]
        remote(ref, ref, send_sem.at[number], relay_recv.at[0], targets["core"]).wait_send()


def layer(cap, x, u, ids, gates, w1, w3, w2):
    tok, hidden = x.shape
    local_experts, d_loc, ff = w1.shape
    rows = GROUP * cap
    half = hidden // NZ // 2
    cut = tok - tok // 8 if tok % 256 == 0 else tok
    halves = [cut // 2] * 2 + [tok - cut // 2] * 2
    spans = {kind: (sum(halves[:i]), halves[i]) for i, kind in enumerate(KINDS)}
    order = gather_order({kind: 2 * hidden * n for kind, (_, n) in spans.items()}, 2 * w1.size * 3 // local_experts)
    sends = sum(len(s) for _, s in order)
    dma, v, shape = pltpu.SemaphoreType.DMA, pltpu.VMEM, jax.ShapeDtypeStruct
    far = lambda lanes: shape((OWN - 1, rows, lanes), BF16)
    near = lambda lanes: v((rows, lanes), BF16)
    stage = lambda lanes: v((2, OWN - 1, 2 * cap, lanes), BF16)
    sums = [v((2, OWN, 2, 3, half, ff), F32)] * 3
    scope_one = [v((GROUP, 2 * tok, hidden), BF16), v((tok, tok), BF16), stage(hidden), stage(hidden), stage(hidden), stage(tok)]
    scope_two = [v((OWN, NZ, 2, 3, half, ff), F32), v((2, OWN, 3, half, ff), F32)] + sums
    per_expert = v((OWN, GROUP, tok), F32)
    gate_rows = v((GROUP, OWN, tok), F32)
    outs = pl.pallas_call(
        functools.partial(layer_kernel, order, cap, spans, scope_one, scope_two),
        name="layer",
        out_shape=(
            shape((3, local_experts, d_loc, ff), F32), shape((tok, hidden), BF16), shape(ids.shape, F32),
            shape((GROUP, OWN * cap, hidden), BF16), shape((OWN, GROUP, tok), F32), shape((OWN, rows, hidden), BF16),
            far(hidden), far(hidden), far(hidden), far(tok),
        ),
        in_specs=[ANY] * 7,
        out_specs=(ANY,) * 10,
        scratch_shapes=[
            v(ids.shape, ids.dtype), v(ids.shape, F32), v((tok, hidden), BF16), v(ids.shape, F32), gate_rows, gate_rows, v((NY, OWN, 3, d_loc, ff), BF16), v((NZ, NY, OWN, 3, d_loc, ff), BF16), v((OWN, 3, d_loc, ff), BF16),
            near(hidden), near(hidden), near(hidden), near(tok), near(ff), near(ff), near(ff), v((rows, 1), F32),
            near(hidden), per_expert, per_expert, v((GROUP, 8, tok), F32), v((tok, hidden), F32),
            dma((len(KINDS), NY * NX)), dma((len(KINDS), NY * NX)), dma((NZ, NY, 2, 2)), dma((len(RELAYS),)), dma((GROUP,)), dma((sends,)), dma((GROUP,)),
            dma((7,)), dma((2, 4)),
            dma((4,)), dma((2, OWN, HOPS)), dma((2, OWN, HOPS)), dma((OWN, 3, NY)), dma((OWN, 3, NY)),
            dma((OWN,)), dma((OWN,)), dma((2, GROUP)), dma((1,)), pltpu.SemaphoreType.REGULAR,
        ],
        compiler_params=params(0),
    )(x, u, ids, gates, w1, w3, w2)
    return outs[:3]


def finish_kernel(grads, in_grad, gate, *refs):
    n = 5
    outs, bufs, sems = refs[:n], refs[n:2 * n], refs[-1]
    ins = [grads.at[m] for m in range(3)] + [in_grad, gate]
    load, store = [], []
    for i, (a, b, o) in enumerate(zip(ins, bufs, outs)):
        half = a.shape[0] // 2
        for h in range(2):
            at = pl.ds(h * half, half)
            load.append(pltpu.make_async_copy(a.at[at], b.at[at], sems.at[0, i, h]))
            store.append(pltpu.make_async_copy(b.at[at], o.at[at], sems.at[1, i, h]))
    for copy in load:
        copy.start()
    for before, after in zip(load, store):
        before.wait()
        after.start()
    for copy in store:
        copy.wait()


def finish(grads, in_grad, gate):
    shapes = [grads.shape[1:]] * 3 + [in_grad.shape, gate.shape]
    types = [grads.dtype] * 3 + [in_grad.dtype, gate.dtype]
    return pl.pallas_call(
        finish_kernel,
        name="finish",
        out_shape=[jax.ShapeDtypeStruct(s, t) for s, t in zip(shapes, types)],
        in_specs=[ANY] * 3,
        out_specs=[ANY] * len(shapes),
        scratch_shapes=[pltpu.VMEM(s, t) for s, t in zip(shapes, types)] + [pltpu.SemaphoreType.DMA((2, len(shapes), 2))],
    )(grads, in_grad, gate)


def solution(mesh):
    mesh4 = Mesh(mesh.devices.reshape(NZ, NY, NX, NC), ("z", "y", "x", "core"))
    tok_spec = P(("z", "y", "x", "core"), None)
    up_spec = P(("x", "core"), ("z", "y"), None)
    down_spec = P(("x", "core"), None, ("z", "y"))

    def per_device(layer_in, out_grad, expert_ids, gate_vals, w_one, w_two, w_three):
        tok_dev, hidden = layer_in.shape
        top_k = expert_ids.shape[1]
        local_experts, d_loc, ff = w_one.shape
        cap = capacity_of(tok_dev, top_k, local_experts * NX * NC)
        ids = expert_ids.T
        grads, in_grad, gate_out = layer(cap, layer_in, out_grad, ids, gate_vals.T, w_one, w_three, w_two.swapaxes(1, 2))
        g1, g3, g2, in_grad, gate_out = finish(grads, in_grad, gate_out)
        return in_grad, gate_out.T, g1, g2.swapaxes(1, 2), g3

    return jax.shard_map(per_device, mesh=mesh4, in_specs=(tok_spec, tok_spec, tok_spec, tok_spec, up_spec, down_spec, up_spec), out_specs=(tok_spec, tok_spec, up_spec, down_spec, up_spec), check_vma=False)
```

```python
import functools

import jax
import jax.numpy as jnp
from jax import lax
from jax.experimental import pallas as pl
from jax.experimental.pallas import tpu as pltpu
from jax.sharding import Mesh, PartitionSpec as P

NZ, NY, NX, NC = 8, 4, 4, 2
GROUP = NY * NX * NC
PLANE = ("y", "x", "core")
OWN = 4
F32, BF16 = jnp.float32, jnp.bfloat16
ANY = pl.BlockSpec(memory_space=pl.ANY)


def capacity_of(tok_dev, top_k, experts):
    return max(8, ((tok_dev * top_k * 5) // (4 * experts) + 7) // 8 * 8)


def rem(a, b):
    return a % b if isinstance(a, int) else lax.rem(a, b)


def contract(ca, cb):
    return lambda a, b: lax.dot_general(a, b, (((ca,), (cb,)), ((), ())), preferred_element_type=F32)


dot, dot_nt, dot_tn = contract(1, 0), contract(1, 1), contract(0, 0)


def params(number):
    return pltpu.CompilerParams(collective_id=number, has_side_effects=True, vmem_limit_bytes=67043328)


def each_other(body):
    return pl.loop(1, GROUP)(body)


def strict_upper(n):
    rows = lax.broadcasted_iota(jnp.int32, (n, n), 0)
    cols = lax.broadcasted_iota(jnp.int32, (n, n), 1)
    return (rows < cols).astype(F32).astype(BF16)


def here():
    return tuple(lax.axis_index(a) for a in ("z", "y", "x", "core"))


def at_offset(k):
    _, y, x, c = here()
    dy, dx, dc = k // (NX * NC), rem(k // NC, NX), rem(k, NC)
    return {"y": rem(y + dy, NY), "x": rem(x + dx, NX), "core": rem(c + dc, NC)}


def place_of(d):
    return d["y"] * (NX * NC) + d["x"] * NC + d["core"]


def z_at(dz):
    return {"z": rem(lax.axis_index("z") + dz, NZ)}


def remote(src, dst, send_sem, recv_sem, target):
    return pltpu.make_async_remote_copy(src_ref=src, dst_ref=dst, send_sem=send_sem, recv_sem=recv_sem, device_id=target, device_id_type=pl.DeviceIdType.MESH)


def start(copy):
    copy.start()


def tell(semaphore, targets):
    for target in targets:
        pl.semaphore_signal(semaphore, device_id=target, device_id_type=pl.DeviceIdType.MESH)


RATE, D2D, HOP = 44700.0, 400000.0, 2.3
PUT, TILE, ROWS = 1.0, 1.0, 0.4
STEP = 5
AHEAD, DEEP = 5.0, 12.0
EARLY = {"z": 60.0, "y": 12.0, "x": 0.0}

PIECE = {(0, None): (0, 1), (1, None): (1, 3), (1, 0): (1, 1), (1, 1): (2, 2)}
RELAYS = ((0, None, "y+"), (1, 0, "y+"), (1, 1, "y-"))


KINDS = ("A0", "A1", "B0", "B1")


def gather_order(sizes, expert_bytes):
    free, pending, coming, order, have, ready = {}, {}, [], [], {}, {}

    def send(now, name, link, arrives, nbytes):
        t = max(now, free.get(link, 0.0)) + nbytes / (D2D if link == "core" else RATE)
        free[link] = t
        coming.append((t + (HOP / 2 if link == "core" else HOP), len(order), len(coming), arrives))
        return (name, link)

    def later(rank, name, link, arrives, nbytes):
        queue = pending.setdefault(link, [])
        queue.append((rank, len(order), len(queue), (name, link, arrives, nbytes)))

    def turn(now):
        out = []
        for link, queue in pending.items():
            queue.sort()
            while queue and free.get(link, 0.0) - now < (AHEAD if now < EARLY[link[0]] else DEEP):
                out.append(send(now, *queue.pop(0)[-1]))
        return out

    def on_rows(kind, dy, dx):
        first, second = "xy" if kind[0] == "A" else "yx"
        d = {"x": dx, "y": dy}
        for axis in [first, second] if d[second] == 0 else [second]:
            for sign in (1, -1):
                if d[axis] == 0 or d[axis] == -sign % 4 and kind[1] == "10"[sign > 0]:
                    nd = dict(d)
                    nd[axis] = (d[axis] - sign) % 4
                    rank = 4 + (axis == second) + (d[axis] != 0)
                    later(rank, (kind, dy, dx), axis + "-+"[sign > 0], (kind, nd["y"], nd["x"]), sizes[kind])

    def core(now, key):
        return send(now, key, "core", ("core",) + key, sizes[key[0]])

    def weights(rank, name, group, part, link, arrives):
        later(rank, name, link, arrives + (group, part), PIECE[group, part][1] * expert_bytes)

    def on_piece(dz, dy, group):
        for link, step, far in (("z+", -1, dy < 2), ("z-", 1, dy >= 2)):
            gone = (step * dz) % NZ
            if gone < 3 + far:
                weights(4 * group + gone, ("W", dz, dy, group), group, None, link, ("W", (dz + step) % NZ, dy))

    def arrived(key, part=None):
        have[key] = have.get(key, 0) + (2 if part is None else 1)
        if have[key] == 2:
            ready[key] = True
        return have[key] == 2

    for i, (group, part, link) in enumerate(RELAYS):
        weights(0, ("r", i), group, part, link, ("R", i))
    for group in range(2):
        for dy, link in ((1, "y+"), (3, "y-")):
            weights(2, ("w", dy, group), group, None, link, ("W", 0, (-dy) % NY))
        on_piece(0, 0, group)
    sends = []
    for kind in KINDS[::-1]:
        arrived((kind, 0, 0))
        on_rows(kind, 0, 0)
        sends.append(core(0.0, (kind, 0, 0)))
    order.append((None, turn(0.0) + sends))
    todo, puts, done, now = [(dy, dx) for dy in range(NY) for dx in range(NX)], 0, 0, 0.0
    while coming or todo or done < puts:
        coming.sort()
        soon = coming[0][0] if coming else 1e9
        if soon > now:
            place = next((p for p in todo if all(pre + (kind,) + p in ready for kind in KINDS for pre in ((), ("core",)))), None)
            if place is not None:
                todo.remove(place)
                order.append((("put",) + place, turn(now)))
                puts += 1
                now += PUT
                continue
            step = min(STEP, puts - done)
            weights_in = sum(key[0] == "W" and key[-1] == 0 for key in ready) == NZ * NY - 1
            calm = all(c[-1][0] == "core" for c in coming)
            if weights_in and step and (step >= 3 and soon - now > TILE or calm):
                order.append((("tile", done, done + step), turn(now)))
                done += step
                now += TILE + ROWS * step
                continue
        t, _, _, name = coming.pop(0)
        now = max(now, t)
        if name[0] == "core":
            arrived(name)
            continue
        sends = []
        if name[0] == "R":
            i, group, part = name[1:]
            weights(1, name[:2], group, part, RELAYS[i][2], ("W", 0, 2))
            name = name[:2]
        elif name[0] == "W":
            if arrived(name[:-1], name[-1]):
                on_piece(*name[1:-1])
        else:
            sends = [core(now, name)]
            arrived(name)
            on_rows(*name)
        order.append((name, sends + turn(now)))
    return order


def passed_on(dz, dy):
    return dz != NZ // 2 and dz not in ((3,) if dy < 2 else (5,))


def first_expert(d):
    return rem(d, NX * NC) * (NY * OWN) + d // (NX * NC) * OWN


FAR, SUM3, NEW3, TWO, ONE, PART, HOPS = 0, 1, 2, 3, 4, 5, 11


def layer_kernel(order, cap, spans, scope_one, scope_two, x_hbm, u_hbm, ids_hbm, gates_hbm, w1_hbm, w3_hbm, w2_hbm,
                 grads, in_grad_hbm, gate_hbm, dxb, valb, dxs, xr, ur, gr, sel,
                 ids_ref, gates_ref, in_grad_ref, gate_ref, metas, gates_out, wown, wv, relay, xb, ub, gb, sb, a_s, d1_s, d3_s, y_s, dx_s, val_s, vb, key_s, acc_s,
                 recv, core_recv, wrecv, relay_recv, mrecv, send_sem, msend, load_sem, store_sem,
                 lsem, rsend, rrecv, ysend, yrecv, dsend, drecv, vsem, osem, in_scope):
    z, y, x, c = here()
    tok, hidden = x_hbm.shape
    rows, ff = xb.shape[0], a_s.shape[-1]
    d_loc = hidden // (NZ * NY)
    me = place_of(at_offset(0))

    def place(dy, dx, dc=0):
        return place_of(at_offset(dy * (NX * NC) + dx * NC + dc))

    targets = {"core": {"core": 1 - c}}
    for sign, n in (("+", 1), ("-", -1)):
        targets["x" + sign] = {"x": rem(x + n + NX, NX)}
        targets["y" + sign] = {"y": rem(y + n + NY, NY)}
        targets["z" + sign] = z_at(n + NZ)

    def wait(ref, sem):
        remote(ref, ref, send_sem.at[0], sem, targets["core"]).wait_recv()

    def piece(dz, dy, group, part=None):
        return wv.at[z_at(dz)["z"], rem(y + dy, NY), pl.ds(*PIECE[group, part])]

    def wait_weights(dz, dy, group, part):
        wait(piece(dz, dy, group, part), wrecv.at[dz, dy, group, part or 0])

    def w(e, m):
        return wv[:, :, e, m].reshape(hidden, ff)

    def expert_rows(e, spans):
        def cut_of(ref):
            return jnp.concatenate([ref[s, :] for s in spans]) if spans[1:] else ref[spans[0], :]

        def save(ref, value):
            n = value.shape[0] // len(spans)
            for i, s in enumerate(spans):
                ref[s, :] = value[i * n:(i + 1) * n]

        x_rows = cut_of(xb)
        h1, h3 = dot(x_rows, w(e, 0)), dot(x_rows, w(e, 1))
        sig = jax.nn.sigmoid(h1)
        silu = h1 * sig
        act = (silu * h3).astype(BF16)
        save(a_s, act)
        y_rows = dot_nt(act, w(e, 2))
        save(y_s, jnp.sum(cut_of(ub).astype(F32) * y_rows, axis=1, keepdims=True))
        da = dot(cut_of(gb), w(e, 2))
        d1 = (da * h3 * sig * (1.0 + h1 * (1.0 - sig))).astype(BF16)
        d3 = (da * silu).astype(BF16)
        save(d1_s, d1)
        save(d3_s, d3)
        save(dx_s, (dot_nt(d1, w(e, 0)) + dot_nt(d3, w(e, 1))).astype(BF16))

    def gather(all_rows, tri, sx, su, sg, ss):
        loads = [
            pltpu.make_async_copy(x_hbm, all_rows.at[me, pl.ds(0, tok)], load_sem.at[0]),
            pltpu.make_async_copy(u_hbm, all_rows.at[me, pl.ds(tok, tok)], load_sem.at[1]),
        ]
        for m, ref in enumerate((w1_hbm, w3_hbm, w2_hbm)):
            loads.append(pltpu.make_async_copy(ref.reshape(NY, OWN, d_loc, ff), wown.at[:, :, m], load_sem.at[2 + m]))
        tables = [pltpu.make_async_copy(a, b, load_sem.at[i]) for i, a, b in ((5, ids_hbm, ids_ref), (6, gates_hbm, gates_ref))]
        for copy in tables + loads:
            copy.start()
        barrier = pltpu.get_barrier_semaphore()
        tell(barrier, [targets["z+"], targets["z-"]])

        @each_other
        def _(k):
            tell(barrier, [at_offset(k)])

        for copy in tables:
            copy.wait()

        @pl.loop(0, GROUP)
        def _(d):
            number = first_expert(d) + lax.broadcasted_iota(jnp.int32, (OWN, tok), 0)
            value = jnp.full((OWN, tok), -1.0, F32)
            for j in range(ids_ref.shape[0]):
                chosen = ids_ref[pl.ds(j, 1), :] == number
                value = jnp.where(chosen, jnp.broadcast_to(gates_ref[pl.ds(j, 1), :], value.shape), value)
            gates_out[d] = value

        metas[me] = gates_out[me]
        tri[...] = strict_upper(tok)
        for copy in loads:
            copy.wait()
        pl.semaphore_wait(barrier, GROUP + 1)

        back = {"x+": (0, 3), "x-": (0, 1), "y+": (3, 0), "y-": (1, 0)}
        def block(kind, dy, dx, dc=0):
            return all_rows.at[place(dy, dx, dc), pl.ds(*spans[kind])]

        row_copies = []

        def issue(name, link):
            number = len(row_copies) + len(weight_copies)
            sem = send_sem.at[number]
            group, part_of = None, None
            if name[0] == "w":
                _, dy, group = name
                src = wown.at[rem(y + dy, NY), pl.ds(*PIECE[group, None])]
                copy = remote(src, piece(0, 0, group), sem, wrecv.at[0, (-dy) % NY, group, 0], targets[link])
            elif name[0] in "rR":
                group, part_of, _ = RELAYS[name[1]]
                span = pl.ds(*PIECE[group, part_of])
                if name[0] == "r":
                    copy = remote(wown.at[rem(y + 2, NY), span], relay.at[span], sem, relay_recv.at[name[1]], targets[link])
                else:
                    dst = piece(0, back[link][0], group, part_of)
                    copy = remote(relay.at[span], dst, sem, wrecv.at[0, 2, group, part_of or 0], targets[link])
            elif name[0] == "W":
                _, dz, dy, group = name
                ndz = (dz - 1) % NZ if link == "z+" else (dz + 1) % NZ
                own = wown.at[y, pl.ds(*PIECE[group, None])]
                copy = remote(own if dz == dy == 0 else piece(dz, dy, group), piece(dz, dy, group), sem, wrecv.at[ndz, dy, group, 0], targets[link])
            else:
                kind, dy, dx = name
                ref = block(*name)
                oy, ox = back.get(link, (0, 0))
                arrivals = core_recv if link == "core" else recv
                rsem = arrivals.at[KINDS.index(kind), (dy + oy) % NY * NX + (dx + ox) % NX]
                copy = remote(ref, ref, sem, rsem, targets[link])
            copy.start()
            if group is None:
                row_copies.append(copy)
            else:
                weight_copies.append((number, group, part_of))

        def meta_copy(k):
            to = at_offset(k)
            return remote(gates_out.at[place_of(to)], metas.at[me], msend.at[k], mrecv.at[k], to)

        n_rows = OWN * 2 * cap
        stores, chips = [], []

        def put(dy, dx):
            slot = len(stores) % 2
            if stores[1:]:
                for copy in stores[-2]:
                    copy.wait()
            for dc in (0, 1):
                if dy or dx or dc:
                    k = ((-dy) % NY) * (NX * NC) + ((-dx) % NX) * NC + dc
                    wait(metas.at[place(dy, dx, dc)], mrecv.at[k])
            for i, kind in enumerate(KINDS):
                wait(block(kind, dy, dx, 1), core_recv.at[i, dy * NX + dx])
            chip = rem(y + dy, NY) * NX + rem(x + dx, NX)
            n = 2 * OWN
            which = lax.broadcasted_iota(jnp.int32, (n, tok), 0)
            gate = jnp.zeros((n, tok), F32)
            for i in range(n):
                gate = jnp.where(which == i, jnp.broadcast_to(metas[2 * chip + i // OWN, pl.ds(i % OWN, 1), :], gate.shape), gate)
            member = gate >= 0.0
            key = jnp.where(member, dot(member.astype(F32).astype(BF16), tri[...]), -1.0)
            r = lax.broadcasted_iota(jnp.int32, (n_rows, tok), 0)
            at = rem(r, cap).astype(F32)
            row_of = rem(r // cap, 2) * OWN + r // (2 * cap)
            mine, gates = jnp.full((n_rows, tok), -1.0, F32), jnp.zeros((n_rows, tok), F32)
            for i in range(n):
                mine = jnp.where(row_of == i, jnp.broadcast_to(key[i:i + 1, :], mine.shape), mine)
                gates = jnp.where(row_of == i, jnp.broadcast_to(gate[i:i + 1, :], mine.shape), gates)
            found = at == mine
            pick = [jnp.logical_and(found, row_of // OWN == p).astype(F32) for p in range(2)]
            both = pick[0] + pick[1]
            scale = jnp.sum(both * gates, axis=1, keepdims=True)
            pick = [p.astype(BF16) for p in pick]
            x_rows = dot(pick[0], all_rows[2 * chip, 0:tok, :]) + dot(pick[1], all_rows[2 * chip + 1, 0:tok, :])
            u_rows = dot(pick[0], all_rows[2 * chip, tok:2 * tok, :]) + dot(pick[1], all_rows[2 * chip + 1, tok:2 * tok, :])
            span = pl.ds(pl.multiple_of(chip * 2 * cap, 2 * cap), 2 * cap)
            out = []
            for i, (value, first, stage, far) in enumerate(((x_rows, xb, sx, xr), (u_rows, ub, su, ur), (scale * u_rows, gb, sg, gr), (both, sb, ss, sel))):
                value = value.astype(BF16)
                first[span, :] = value[:2 * cap]
                stage[slot] = value[2 * cap:].reshape(stage.shape[1:])
                out.append(pltpu.make_async_copy(stage.at[slot], far.at[:, span], store_sem.at[slot, i]))
                out[-1].start()
            stores.append(out)
            chips.append(span)

        for name, sends in order:
            if name is None:
                pass
            elif name[0] == "put":
                put(*name[1:])
            elif name[0] == "tile":
                expert_rows(0, chips[name[1]:name[2]])
            elif name[0] == "R":
                group, part, _ = RELAYS[name[1]]
                wait(relay.at[pl.ds(*PIECE[group, part])], relay_recv.at[name[1]])
            elif name[0] == "W":
                if passed_on(*name[1:3]) or not name[3]:
                    wait_weights(*name[1:])
                else:
                    last_weights.append(name[1:])
            else:
                kind, dy, dx = name
                wait(block(*name), recv.at[KINDS.index(kind), dy * NX + dx])
            for send in sends:
                issue(*send)
            if name is None:
                wv[z, y] = wown[y]

                @each_other
                def _(k):
                    meta_copy(k).start()

        for out in stores[-2:]:
            for copy in out:
                copy.wait()

        @each_other
        def _(k):
            meta_copy(k).wait_send()

        for copy in row_copies:
            copy.wait_send()

    def reduce(G, r4, r3, r2, r1):
        tell(in_scope, [targets["z+"], targets["z-"]])

        def row_loads(e):
            pairs = ((xr, xb), (gr, gb), (ur, ub), (sel, sb))
            return [pltpu.make_async_copy(src.at[e - 1], dst, lsem.at[i]) for i, (src, dst) in enumerate(pairs)]

        def chunk(e, way, dist):
            return G.at[e, z_at(dist if way else NZ - dist)["z"]]

        def part_of(ref, way, e, kind):
            return ref.at[way, e, (kind - PART) % 2, (kind - PART) // 2]

        def hop(e, way, kind):
            h = way
            src, dst = {
                FAR: lambda: (chunk(e, way, 4).at[h], r4.at[way, e]),
                SUM3: lambda: (r4.at[way, e], r3.at[way, e, h]),
                NEW3: lambda: (chunk(e, way, 3).at[1 - h], r3.at[way, e, 1 - h]),
                TWO: lambda: (r3.at[way, e], r2.at[way, e]),
                ONE: lambda: (r2.at[way, e], r1.at[way, e]),
            }.get(kind, lambda: (part_of(r2, way, e, kind), part_of(r1, way, e, kind)))()
            return remote(src, dst, rsend.at[way, e, kind], rrecv.at[way, e, kind], z_at(1 if way else NZ - 1))

        def add_into(dst, *others):
            parts = dst.shape[:-2]
            if not parts:
                total = dst[...]
                for other in others:
                    total = total + other[...]
                dst[...] = total
                return

            def flat(ref, i):
                index = []
                for n in reversed(parts):
                    index.append(rem(i, n))
                    i = i // n
                return ref.at[tuple(reversed(index))]

            n = 1
            for p in parts:
                n *= p

            @pl.loop(0, n)
            def _(i):
                total = flat(dst, i)[...]
                for other in others:
                    total = total + flat(other, i)[...]
                flat(dst, i)[...] = total

        def own_rows(s):
            return pl.ds(pl.multiple_of(s * cap, 8), cap)

        def dx_copy(e, k):
            to = at_offset(k)
            return remote(dxs.at[e, own_rows(place_of(to))], dxb.at[me, own_rows(e)], dsend.at[e], drecv.at[e], to)

        tile = 256 if rows % 256 == 0 else rows
        dtile = hidden // NZ
        half = dtile // 2

        def weight_gradients(e):
            out = pltpu.make_async_copy(dx_s, dxs.at[e], osem.at[0])
            out.start()

            @pl.loop(0, NZ // 2)
            def _(i):
                pair = [z_at(n + 2 * i)["z"] for n in (3, 4)]

                def cols(ref):
                    return jnp.concatenate([ref[:, pl.ds(pl.multiple_of(k * dtile, dtile), dtile)] for k in pair], axis=1)

                x_cols, g_cols = cols(xb), cols(gb)
                for m, part in enumerate((dot_tn(x_cols, d1_s[...]), dot_tn(x_cols, d3_s[...]), dot_tn(g_cols, a_s[...]))):
                    for j in range(4):
                        G[e, pair[j // 2], j % 2, m] = part[j * half:(j + 1) * half]

                @pl.when(i == 0)
                def _():
                    if isinstance(e, int):
                        pl.semaphore_wait(in_scope, 2)
                    for way, kind in ((0, FAR), (1, FAR), (1, NEW3)):
                        hop(e, way, kind).start()

                @pl.when(i == 1)
                def _():
                    hop(e, 0, NEW3).start()

            val = sb[...].astype(F32) * y_s[...]
            val_s[e] = jnp.sum(val.reshape(rows // cap, cap, tok), axis=1)
            out.wait()

        def send_back(e):
            pltpu.make_async_copy(dxs.at[e, own_rows(me)], dxb.at[me, own_rows(e)], drecv.at[e]).start()

            @each_other
            def _(k):
                dx_copy(e, k).start()

        def far_sums(e):
            for way in (0, 1):
                hop(e, way, FAR).wait_recv()
                add_into(r4.at[way, e], chunk(e, way, 3).at[way])
                hop(e, way, SUM3).start()

        weight_gradients(0)
        for copy in row_loads(1):
            copy.start()
        send_back(0)
        for name in last_weights:
            wait_weights(*name)

        @pl.loop(1, OWN)
        def _(e):
            for copy in row_loads(e):
                copy.wait()

            @pl.loop(0, rows // tile)
            def _(i):
                expert_rows(e, [pl.ds(pl.multiple_of(i * tile, tile), tile)])

            weight_gradients(e)

            @pl.when(e < OWN - 1)
            def _():
                for copy in row_loads(e + 1):
                    copy.start()

            send_back(e)
            far_sums(e - 1)

        far_sums(OWN - 1)

        def val_copy(k):
            to = at_offset(k)
            return remote(val_s.at[:, place_of(to)], valb.at[:, me], vsem.at[0, k], vsem.at[1, k], to)

        own_val = pltpu.make_async_copy(val_s.at[:, me], valb.at[:, me], vsem.at[0, 0])
        own_val.start()

        @each_other
        def _(k):
            val_copy(k).start()

        @pl.loop(0, OWN)
        def _(e):
            for way in (0, 1):
                for kind in (SUM3, NEW3):
                    hop(e, way, kind).wait_recv()
                add_into(r3.at[way, e], chunk(e, way, 2))
                hop(e, way, TWO).start()

        group, places = dxb.shape[:2]
        ids = ids_ref[...].astype(F32)
        r = lax.broadcasted_iota(jnp.int32, (group * 8, tok), 0)
        e_of = rem(r, 8)
        expert = jnp.where(e_of < OWN, first_expert(r // 8) + e_of, -1).astype(F32)
        member = jnp.zeros((group * 8, tok), F32)
        for j in range(ids.shape[0]):
            member = member + (jnp.broadcast_to(ids[j:j + 1, :], member.shape) == expert).astype(F32)
        before = dot(member.astype(BF16), strict_upper(tok))
        key_s[...] = jnp.where(member > 0.0, before, -1.0).reshape(key_s.shape)
        rr = lax.broadcasted_iota(jnp.int32, (places, tok), 0)
        at, e_row = rem(rr, cap).astype(F32), rr // cap
        some = rows // places

        @pl.loop(0, OWN)
        def _(e):
            got = dxb.at[:, own_rows(e)]
            pltpu.make_async_copy(got, got, drecv.at[e]).wait()

        own_val.wait()

        @each_other
        def _(k):
            val_copy(k).wait()

        bufs = (xb, gb)
        loads = [pltpu.make_async_copy(dxb.at[pl.ds(i * some, some)], bufs[i % 2].reshape(some, places, hidden), lsem.at[i % 2]) for i in range(group // some)]
        vals = pltpu.make_async_copy(valb, vb, lsem.at[2])
        vals.start()
        loads[0].start()
        for i, load in enumerate(loads):
            for later in loads[i + 1:i + 2]:
                later.start()

            @pl.loop(0, some)
            def _(k):
                key = key_s[i * some + k]
                mine = jnp.full((places, tok), -1.0, F32)
                for e in range(OWN):
                    mine = jnp.where(e_row == e, jnp.broadcast_to(key[e:e + 1, :], (places, tok)), mine)
                sb[pl.ds(pl.multiple_of(k * places, places), places), :] = (at == mine).astype(F32).astype(BF16)

            load.wait()
            part = dot_tn(sb[...], bufs[i % 2][...])
            acc_s[...] = acc_s[...] + part if i else part

        in_grad_ref[...] = acc_s[...].astype(BF16)
        vals.wait()

        def gate_step(k, total):
            for e in range(OWN):
                row = vb[e, pl.ds(k, 1), :]
                total = total + jnp.where(ids == (first_expert(k) + e).astype(F32), jnp.broadcast_to(row, ids.shape), 0.0)
            return total

        gate_ref[...] = lax.fori_loop(0, group, gate_step, jnp.zeros(ids.shape, F32))
        results = [pltpu.make_async_copy(a, b, load_sem.at[i]) for i, a, b in ((0, in_grad_ref, in_grad_hbm), (1, gate_ref, gate_hbm))]
        for copy in results:
            copy.start()

        last = OWN - 1

        @pl.loop(0, last)
        def _(e):
            for way in (0, 1):
                hop(e, way, TWO).wait_recv()
                add_into(r2.at[way, e], chunk(e, way, 1))
                hop(e, way, ONE).start()

        for way in (0, 1):
            hop(last, way, TWO).wait_recv()
        for kind in range(PART, HOPS):
            for way in (0, 1):
                add_into(part_of(r2, way, last, kind), part_of(G, last, z_at(1 if way else NZ - 1)["z"], kind))
                hop(last, way, kind).start()

        def keep(e, m, to, then_remote, then_local):
            src = r1.at[0, e, to // 2, m, pl.ds(to % 2 * d_loc, d_loc)]
            dst = grads.at[m, y * OWN + e]
            n = 0 if isinstance(m, slice) else m

            @pl.when(y != to)
            def _():
                then_remote(remote(src, dst, ysend.at[e, n, to], yrecv.at[e, n, y], {"y": to}))

            @pl.when(y == to)
            def _():
                then_local(pltpu.make_async_copy(src, dst, ysend.at[e, n, to]))

        every = slice(None)

        @pl.loop(0, last)
        def _(e):
            for way in (0, 1):
                hop(e, way, ONE).wait_recv()
            add_into(r1.at[0, e], r1.at[1, e], G.at[e, z])
            for to in range(NY):
                keep(e, every, to, start, start)

        for kind in range(PART, HOPS):
            for way in (0, 1):
                hop(last, way, kind).wait_recv()
            add_into(part_of(r1, 0, last, kind), part_of(r1, 1, last, kind), part_of(G, last, z, kind))
            m, h = (kind - PART) // 2, (kind - PART) % 2
            for to in (2 * h, 2 * h + 1):
                keep(last, m, to, start, start)

        def finish_up(e, kinds, matrices):
            for m in matrices:
                for at in range(NY):
                    def both(copy):
                        wait(grads.at[m, at * OWN + e], yrecv.at[e, 0 if m is every else m, at])
                        copy.wait_send()

                    keep(e, m, at, both, lambda copy: copy.wait())
            for way in (0, 1):
                for kind in kinds:
                    hop(e, way, kind).wait_send()
            sent = dxs.at[e, pl.ds(0, (GROUP - 1) * cap)]
            pltpu.make_async_copy(sent, sent, dsend.at[e]).wait()

        @pl.loop(0, last)
        def _(e):
            finish_up(e, range(PART), [every])

        finish_up(last, [FAR, SUM3, NEW3, TWO, *range(PART, HOPS)], range(3))
        for copy in results:
            copy.wait()

    weight_copies, last_weights = [], []
    pl.run_scoped(gather, *scope_one)
    pl.run_scoped(reduce, *scope_two)
    for number, group, part in weight_copies:
        ref = wown.at[0, pl.ds(*PIECE[group, part])]
        remote(ref, ref, send_sem.at[number], relay_recv.at[0], targets["core"]).wait_send()


def layer(cap, x, u, ids, gates, w1, w3, w2):
    tok, hidden = x.shape
    local_experts, d_loc, ff = w1.shape
    rows = GROUP * cap
    half = hidden // NZ // 2
    cut = tok - tok // 8 if tok % 256 == 0 else tok
    halves = [cut // 2] * 2 + [tok - cut // 2] * 2
    spans = {kind: (sum(halves[:i]), halves[i]) for i, kind in enumerate(KINDS)}
    order = gather_order({kind: 2 * hidden * n for kind, (_, n) in spans.items()}, 2 * w1.size * 3 // local_experts)
    sends = sum(len(s) for _, s in order)
    dma, v, shape = pltpu.SemaphoreType.DMA, pltpu.VMEM, jax.ShapeDtypeStruct
    far = lambda lanes: shape((OWN - 1, rows, lanes), BF16)
    near = lambda lanes: v((rows, lanes), BF16)
    stage = lambda lanes: v((2, OWN - 1, 2 * cap, lanes), BF16)
    sums = [v((2, OWN, 2, 3, half, ff), F32)] * 3
    scope_one = [v((GROUP, 2 * tok, hidden), BF16), v((tok, tok), BF16), stage(hidden), stage(hidden), stage(hidden), stage(tok)]
    scope_two = [v((OWN, NZ, 2, 3, half, ff), F32), v((2, OWN, 3, half, ff), F32)] + sums
    per_expert = v((OWN, GROUP, tok), F32)
    gate_rows = v((GROUP, OWN, tok), F32)
    outs = pl.pallas_call(
        functools.partial(layer_kernel, order, cap, spans, scope_one, scope_two),
        name="layer",
        out_shape=(
            shape((3, local_experts, d_loc, ff), F32), shape((tok, hidden), BF16), shape(ids.shape, F32),
            shape((GROUP, OWN * cap, hidden), BF16), shape((OWN, GROUP, tok), F32), shape((OWN, rows, hidden), BF16),
            far(hidden), far(hidden), far(hidden), far(tok),
        ),
        in_specs=[ANY] * 7,
        out_specs=(ANY,) * 10,
        scratch_shapes=[
            v(ids.shape, ids.dtype), v(ids.shape, F32), v((tok, hidden), BF16), v(ids.shape, F32), gate_rows, gate_rows, v((NY, OWN, 3, d_loc, ff), BF16), v((NZ, NY, OWN, 3, d_loc, ff), BF16), v((OWN, 3, d_loc, ff), BF16),
            near(hidden), near(hidden), near(hidden), near(tok), near(ff), near(ff), near(ff), v((rows, 1), F32),
            near(hidden), per_expert, per_expert, v((GROUP, 8, tok), F32), v((tok, hidden), F32),
            dma((len(KINDS), NY * NX)), dma((len(KINDS), NY * NX)), dma((NZ, NY, 2, 2)), dma((len(RELAYS),)), dma((GROUP,)), dma((sends,)), dma((GROUP,)),
            dma((7,)), dma((2, 4)),
            dma((4,)), dma((2, OWN, HOPS)), dma((2, OWN, HOPS)), dma((OWN, 3, NY)), dma((OWN, 3, NY)),
            dma((OWN,)), dma((OWN,)), dma((2, GROUP)), dma((1,)), pltpu.SemaphoreType.REGULAR,
        ],
        compiler_params=params(0),
    )(x, u, ids, gates, w1, w3, w2)
    return outs[:3]


def finish_kernel(grads, in_grad, gate, *refs):
    n = 5
    outs, bufs, sems = refs[:n], refs[n:2 * n], refs[-1]
    ins = [grads.at[m] for m in range(3)] + [in_grad, gate]
    load, store = [], []
    for i, (a, b, o) in enumerate(zip(ins, bufs, outs)):
        half = a.shape[0] // 2
        for h in range(2):
            at = pl.ds(h * half, half)
            load.append(pltpu.make_async_copy(a.at[at], b.at[at], sems.at[0, i, h]))
            store.append(pltpu.make_async_copy(b.at[at], o.at[at], sems.at[1, i, h]))
    for copy in load:
        copy.start()
    for before, after in zip(load, store):
        before.wait()
        after.start()
    for copy in store:
        copy.wait()


def finish(grads, in_grad, gate):
    shapes = [grads.shape[1:]] * 3 + [in_grad.shape, gate.shape]
    types = [grads.dtype] * 3 + [in_grad.dtype, gate.dtype]
    return pl.pallas_call(
        finish_kernel,
        name="finish",
        out_shape=[jax.ShapeDtypeStruct(s, t) for s, t in zip(shapes, types)],
        in_specs=[ANY] * 3,
        out_specs=[ANY] * len(shapes),
        scratch_shapes=[pltpu.VMEM(s, t) for s, t in zip(shapes, types)] + [pltpu.SemaphoreType.DMA((2, len(shapes), 2))],
    )(grads, in_grad, gate)


def solution(mesh):
    mesh4 = Mesh(mesh.devices.reshape(NZ, NY, NX, NC), ("z", "y", "x", "core"))
    tok_spec = P(("z", "y", "x", "core"), None)
    up_spec = P(("x", "core"), ("z", "y"), None)
    down_spec = P(("x", "core"), None, ("z", "y"))

    def per_device(layer_in, out_grad, expert_ids, gate_vals, w_one, w_two, w_three):
        tok_dev, hidden = layer_in.shape
        top_k = expert_ids.shape[1]
        local_experts, d_loc, ff = w_one.shape
        cap = capacity_of(tok_dev, top_k, local_experts * NX * NC)
        ids = expert_ids.T
        grads, in_grad, gate_out = layer(cap, layer_in, out_grad, ids, gate_vals.T, w_one, w_three, w_two.swapaxes(1, 2))
        g1, g3, g2, in_grad, gate_out = finish(grads, in_grad, gate_out)
        return in_grad, gate_out.T, g1, g2.swapaxes(1, 2), g3

    return jax.shard_map(per_device, mesh=mesh4, in_specs=(tok_spec, tok_spec, tok_spec, tok_spec, up_spec, down_spec, up_spec), out_specs=(tok_spec, tok_spec, up_spec, down_spec, up_spec), check_vma=False)
```

```python
import functools

import jax
import jax.numpy as jnp
from jax import lax
from jax.experimental import pallas as pl
from jax.experimental.pallas import tpu as pltpu
from jax.sharding import Mesh, PartitionSpec as P

NZ, NY, NX, NC = 8, 4, 4, 2
GROUP = NY * NX * NC
PLANE = ("y", "x", "core")
OWN = 4
F32, BF16 = jnp.float32, jnp.bfloat16
ANY = pl.BlockSpec(memory_space=pl.ANY)


def capacity_of(tok_dev, top_k, experts):
    return max(8, ((tok_dev * top_k * 5) // (4 * experts) + 7) // 8 * 8)


def rem(a, b):
    return a % b if isinstance(a, int) else lax.rem(a, b)


def contract(ca, cb):
    return lambda a, b: lax.dot_general(a, b, (((ca,), (cb,)), ((), ())), preferred_element_type=F32)


dot, dot_nt, dot_tn = contract(1, 0), contract(1, 1), contract(0, 0)


def params(number):
    return pltpu.CompilerParams(collective_id=number, has_side_effects=True, vmem_limit_bytes=67043328)


def each_other(body):
    return pl.loop(1, GROUP)(body)


def strict_upper(n):
    rows = lax.broadcasted_iota(jnp.int32, (n, n), 0)
    cols = lax.broadcasted_iota(jnp.int32, (n, n), 1)
    return (rows < cols).astype(F32).astype(BF16)


def here():
    return tuple(lax.axis_index(a) for a in ("z", "y", "x", "core"))


def at_offset(k):
    _, y, x, c = here()
    dy, dx, dc = k // (NX * NC), rem(k // NC, NX), rem(k, NC)
    return {"y": rem(y + dy, NY), "x": rem(x + dx, NX), "core": rem(c + dc, NC)}


def place_of(d):
    return d["y"] * (NX * NC) + d["x"] * NC + d["core"]


def z_at(dz):
    return {"z": rem(lax.axis_index("z") + dz, NZ)}


def remote(src, dst, send_sem, recv_sem, target):
    return pltpu.make_async_remote_copy(src_ref=src, dst_ref=dst, send_sem=send_sem, recv_sem=recv_sem, device_id=target, device_id_type=pl.DeviceIdType.MESH)


def start(copy):
    copy.start()


def tell(semaphore, targets):
    for target in targets:
        pl.semaphore_signal(semaphore, device_id=target, device_id_type=pl.DeviceIdType.MESH)


RATE, D2D, HOP = 44700.0, 400000.0, 2.3
PUT, TILE, ROWS = 1.0, 1.0, 0.4
STEP = 5
AHEAD, MORE = 5.0, 0.05

PIECE = {(0, None): (0, 1), (1, None): (1, 3), (1, 0): (1, 1), (1, 1): (2, 2)}
RELAYS = ((0, None, "y+"), (1, 0, "y+"), (1, 1, "y-"))


ROUNDS = NY // 2 + NX // 2
KINDS = ("A0", "A1", "B0", "B1")


def gather_order(sizes, expert_bytes):
    free, pending, coming, order, have, ready = {}, {}, [], [], {}, {}

    def send(now, name, link, arrives, nbytes):
        t = max(now, free.get(link, 0.0)) + nbytes / (D2D if link == "core" else RATE)
        free[link] = t
        coming.append((t + (HOP / 2 if link == "core" else HOP), len(order), len(coming), arrives))
        return (name, link)

    def later(rank, name, link, arrives, nbytes):
        queue = pending.setdefault(link, [])
        queue.append((rank, len(order), len(queue), (name, link, arrives, nbytes)))

    def turn(now):
        out = []
        for link, queue in pending.items():
            queue.sort()
            while queue and free.get(link, 0.0) - now < AHEAD + MORE * now:
                out.append(send(now, *queue.pop(0)[-1]))
        return out

    def on_rows(kind, dy, dx):
        first, second = "xy" if kind[0] == "A" else "yx"
        d = {"x": dx, "y": dy}
        for axis in [first, second] if d[second] == 0 else [second]:
            for sign in (1, -1):
                if d[axis] == 0 or d[axis] == -sign % 4 and kind[1] == "10"[sign > 0]:
                    nd = dict(d)
                    nd[axis] = (d[axis] - sign) % 4
                    rank = 4 + (axis == second) + (d[axis] != 0)
                    later(rank, (kind, dy, dx), axis + "-+"[sign > 0], (kind, nd["y"], nd["x"]), sizes[kind])

    def core(now, key):
        return send(now, key, "core", ("core",) + key, sizes[key[0]])

    def weights(rank, name, group, part, link, arrives):
        later(rank, name, link, arrives + (group, part), PIECE[group, part][1] * expert_bytes)

    def on_piece(dz, dy, group):
        for link, step, far in (("z+", -1, dy < 2), ("z-", 1, dy >= 2)):
            gone = (step * dz) % NZ
            if gone < 3 + far:
                weights(4 * group + gone, ("W", dz, dy, group), group, None, link, ("W", (dz + step) % NZ, dy))

    def arrived(key, part=None):
        have[key] = have.get(key, 0) + (2 if part is None else 1)
        if have[key] == 2:
            ready[key] = True
        return have[key] == 2

    for i, (group, part, link) in enumerate(RELAYS):
        weights(0, ("r", i), group, part, link, ("R", i))
    for group in range(2):
        for dy, link in ((1, "y+"), (3, "y-")):
            weights(2, ("w", dy, group), group, None, link, ("W", 0, (-dy) % NY))
        on_piece(0, 0, group)
    sends = []
    for kind in KINDS[::-1]:
        arrived((kind, 0, 0))
        on_rows(kind, 0, 0)
        sends.append(core(0.0, (kind, 0, 0)))
    order.append((None, turn(0.0) + sends))
    todo, puts, done, now = [(dy, dx) for dy in range(NY) for dx in range(NX)], 0, 0, 0.0
    known = 0
    while coming or todo or done < puts:
        coming.sort()
        if known < ROUNDS and now > HOP * (known + 1):
            order.append((("near", known), turn(now)))
            known += 1
            continue
        soon = coming[0][0] if coming else 1e9
        if soon > now:
            place = next((p for p in todo if all(pre + (kind,) + p in ready for kind in KINDS for pre in ((), ("core",)))), None)
            if place is not None and now > 15:
                todo.remove(place)
                order.append((("put",) + place, turn(now)))
                puts += 1
                now += PUT
                continue
            step = min(STEP, puts - done)
            weights_in = sum(key[0] == "W" and key[-1] == 0 for key in ready) == NZ * NY - 1
            calm = all(c[-1][0] == "core" for c in coming)
            if weights_in and step and (step >= 3 and soon - now > TILE or calm):
                order.append((("tile", done, done + step), turn(now)))
                done += step
                now += TILE + ROWS * step
                continue
        t, _, _, name = coming.pop(0)
        now = max(now, t)
        if name[0] == "core":
            arrived(name)
            continue
        sends = []
        if name[0] == "R":
            i, group, part = name[1:]
            weights(1, name[:2], group, part, RELAYS[i][2], ("W", 0, 2))
            name = name[:2]
        elif name[0] == "W":
            if arrived(name[:-1], name[-1]):
                on_piece(*name[1:-1])
        else:
            sends = [core(now, name)]
            arrived(name)
            on_rows(*name)
        order.append((name, sends + turn(now)))
    return order


def passed_on(dz, dy):
    return dz != NZ // 2 and dz not in ((3,) if dy < 2 else (5,))


def first_expert(d):
    return rem(d, NX * NC) * (NY * OWN) + d // (NX * NC) * OWN


FAR, SUM3, NEW3, TWO, ONE, PART, HOPS = 0, 1, 2, 3, 4, 5, 11


def layer_kernel(order, cap, spans, scope_one, scope_two, x_hbm, u_hbm, ids_hbm, gates_hbm, w1_hbm, w3_hbm, w2_hbm,
                 grads, in_grad_hbm, gate_hbm, dxb, valb, dxs, xr, ur, gr, sel,
                 ids_ref, gates_ref, in_grad_ref, gate_ref, metas, gates_out, wown, wv, relay, xb, ub, gb, sb, a_s, d1_s, d3_s, y_s, dx_s, val_s, vb, key_s, acc_s,
                 recv, core_recv, wrecv, relay_recv, mrecv, send_sem, msend, load_sem, store_sem,
                 lsem, rsend, rrecv, ysend, yrecv, dsend, drecv, vsem, osem, in_scope, in_plane):
    z, y, x, c = here()
    tok, hidden = x_hbm.shape
    rows, ff = xb.shape[0], a_s.shape[-1]
    d_loc = hidden // (NZ * NY)
    me = place_of(at_offset(0))

    def place(dy, dx, dc=0):
        return place_of(at_offset(dy * (NX * NC) + dx * NC + dc))

    targets = {"core": {"core": 1 - c}}
    for sign, n in (("+", 1), ("-", -1)):
        targets["x" + sign] = {"x": rem(x + n + NX, NX)}
        targets["y" + sign] = {"y": rem(y + n + NY, NY)}
        targets["z" + sign] = z_at(n + NZ)

    def wait(ref, sem):
        remote(ref, ref, send_sem.at[0], sem, targets["core"]).wait_recv()

    def piece(dz, dy, group, part=None):
        return wv.at[z_at(dz)["z"], rem(y + dy, NY), pl.ds(*PIECE[group, part])]

    def wait_weights(dz, dy, group, part):
        wait(piece(dz, dy, group, part), wrecv.at[dz, dy, group, part or 0])

    def w(e, m):
        return wv[:, :, e, m].reshape(hidden, ff)

    def expert_rows(e, spans):
        def cut_of(ref):
            return jnp.concatenate([ref[s, :] for s in spans]) if spans[1:] else ref[spans[0], :]

        def save(ref, value):
            n = value.shape[0] // len(spans)
            for i, s in enumerate(spans):
                ref[s, :] = value[i * n:(i + 1) * n]

        x_rows = cut_of(xb)
        h1, h3 = dot(x_rows, w(e, 0)), dot(x_rows, w(e, 1))
        sig = jax.nn.sigmoid(h1)
        silu = h1 * sig
        act = (silu * h3).astype(BF16)
        save(a_s, act)
        y_rows = dot_nt(act, w(e, 2))
        save(y_s, jnp.sum(cut_of(ub).astype(F32) * y_rows, axis=1, keepdims=True))
        da = dot(cut_of(gb), w(e, 2))
        d1 = (da * h3 * sig * (1.0 + h1 * (1.0 - sig))).astype(BF16)
        d3 = (da * silu).astype(BF16)
        save(d1_s, d1)
        save(d3_s, d3)
        save(dx_s, (dot_nt(d1, w(e, 0)) + dot_nt(d3, w(e, 1))).astype(BF16))

    def gather(all_rows, tri, sx, su, sg, ss):
        loads = [
            pltpu.make_async_copy(x_hbm, all_rows.at[me, pl.ds(0, tok)], load_sem.at[0]),
            pltpu.make_async_copy(u_hbm, all_rows.at[me, pl.ds(tok, tok)], load_sem.at[1]),
        ]
        for m, ref in enumerate((w1_hbm, w3_hbm, w2_hbm)):
            loads.append(pltpu.make_async_copy(ref.reshape(NY, OWN, d_loc, ff), wown.at[:, :, m], load_sem.at[2 + m]))
        tables = [pltpu.make_async_copy(a, b, load_sem.at[i]) for i, a, b in ((5, ids_hbm, ids_ref), (6, gates_hbm, gates_ref))]
        for copy in tables + loads:
            copy.start()
        barrier = pltpu.get_barrier_semaphore()
        tell(barrier, targets.values())
        for copy in tables:
            copy.wait()

        @pl.loop(0, GROUP)
        def _(d):
            number = first_expert(d) + lax.broadcasted_iota(jnp.int32, (OWN, tok), 0)
            value = jnp.full((OWN, tok), -1.0, F32)
            for j in range(ids_ref.shape[0]):
                chosen = ids_ref[pl.ds(j, 1), :] == number
                value = jnp.where(chosen, jnp.broadcast_to(gates_ref[pl.ds(j, 1), :], value.shape), value)
            gates_out[d] = value

        metas[me] = gates_out[me]
        tri[...] = strict_upper(tok)
        for copy in loads:
            copy.wait()
        pl.semaphore_wait(barrier, len(targets))

        back = {"x+": (0, 3), "x-": (0, 1), "y+": (3, 0), "y-": (1, 0)}
        def block(kind, dy, dx, dc=0):
            return all_rows.at[place(dy, dx, dc), pl.ds(*spans[kind])]

        near = [t for link, t in targets.items() if link[0] != "z"]
        row_copies = []

        def issue(name, link):
            number = len(row_copies) + len(weight_copies)
            sem = send_sem.at[number]
            group, part_of = None, None
            if name[0] == "w":
                _, dy, group = name
                src = wown.at[rem(y + dy, NY), pl.ds(*PIECE[group, None])]
                copy = remote(src, piece(0, 0, group), sem, wrecv.at[0, (-dy) % NY, group, 0], targets[link])
            elif name[0] in "rR":
                group, part_of, _ = RELAYS[name[1]]
                span = pl.ds(*PIECE[group, part_of])
                if name[0] == "r":
                    copy = remote(wown.at[rem(y + 2, NY), span], relay.at[span], sem, relay_recv.at[name[1]], targets[link])
                else:
                    dst = piece(0, back[link][0], group, part_of)
                    copy = remote(relay.at[span], dst, sem, wrecv.at[0, 2, group, part_of or 0], targets[link])
            elif name[0] == "W":
                _, dz, dy, group = name
                ndz = (dz - 1) % NZ if link == "z+" else (dz + 1) % NZ
                own = wown.at[y, pl.ds(*PIECE[group, None])]
                copy = remote(own if dz == dy == 0 else piece(dz, dy, group), piece(dz, dy, group), sem, wrecv.at[ndz, dy, group, 0], targets[link])
            else:
                kind, dy, dx = name
                ref = block(*name)
                oy, ox = back.get(link, (0, 0))
                arrivals = core_recv if link == "core" else recv
                rsem = arrivals.at[KINDS.index(kind), (dy + oy) % NY * NX + (dx + ox) % NX]
                copy = remote(ref, ref, sem, rsem, targets[link])
            copy.start()
            if group is None:
                row_copies.append(copy)
            else:
                weight_copies.append((number, group, part_of))

        def meta_copy(k):
            to = at_offset(k)
            return remote(gates_out.at[place_of(to)], metas.at[me], msend.at[k], mrecv.at[k], to)

        n_rows = OWN * 2 * cap
        stores, chips = [], []

        def put(dy, dx):
            slot = len(stores) % 2
            if stores[1:]:
                for copy in stores[-2]:
                    copy.wait()
            for dc in (0, 1):
                if dy or dx or dc:
                    k = ((-dy) % NY) * (NX * NC) + ((-dx) % NX) * NC + dc
                    wait(metas.at[place(dy, dx, dc)], mrecv.at[k])
            for i, kind in enumerate(KINDS):
                wait(block(kind, dy, dx, 1), core_recv.at[i, dy * NX + dx])
            chip = rem(y + dy, NY) * NX + rem(x + dx, NX)
            n = 2 * OWN
            which = lax.broadcasted_iota(jnp.int32, (n, tok), 0)
            gate = jnp.zeros((n, tok), F32)
            for i in range(n):
                gate = jnp.where(which == i, jnp.broadcast_to(metas[2 * chip + i // OWN, pl.ds(i % OWN, 1), :], gate.shape), gate)
            member = gate >= 0.0
            key = jnp.where(member, dot(member.astype(F32).astype(BF16), tri[...]), -1.0)
            r = lax.broadcasted_iota(jnp.int32, (n_rows, tok), 0)
            at = rem(r, cap).astype(F32)
            row_of = rem(r // cap, 2) * OWN + r // (2 * cap)
            mine, gates = jnp.full((n_rows, tok), -1.0, F32), jnp.zeros((n_rows, tok), F32)
            for i in range(n):
                mine = jnp.where(row_of == i, jnp.broadcast_to(key[i:i + 1, :], mine.shape), mine)
                gates = jnp.where(row_of == i, jnp.broadcast_to(gate[i:i + 1, :], mine.shape), gates)
            found = at == mine
            pick = [jnp.logical_and(found, row_of // OWN == p).astype(F32) for p in range(2)]
            both = pick[0] + pick[1]
            scale = jnp.sum(both * gates, axis=1, keepdims=True)
            pick = [p.astype(BF16) for p in pick]
            x_rows = dot(pick[0], all_rows[2 * chip, 0:tok, :]) + dot(pick[1], all_rows[2 * chip + 1, 0:tok, :])
            u_rows = dot(pick[0], all_rows[2 * chip, tok:2 * tok, :]) + dot(pick[1], all_rows[2 * chip + 1, tok:2 * tok, :])
            span = pl.ds(pl.multiple_of(chip * 2 * cap, 2 * cap), 2 * cap)
            out = []
            for i, (value, first, stage, far) in enumerate(((x_rows, xb, sx, xr), (u_rows, ub, su, ur), (scale * u_rows, gb, sg, gr), (both, sb, ss, sel))):
                value = value.astype(BF16)
                first[span, :] = value[:2 * cap]
                stage[slot] = value[2 * cap:].reshape(stage.shape[1:])
                out.append(pltpu.make_async_copy(stage.at[slot], far.at[:, span], store_sem.at[slot, i]))
                out[-1].start()
            stores.append(out)
            chips.append(span)

        for name, sends in order:
            if name is None:
                pass
            elif name[0] == "put":
                put(*name[1:])
            elif name[0] == "near":
                _, k = name
                pl.semaphore_wait(in_plane.at[k], len(near))
                if k < ROUNDS - 1:
                    tell(in_plane.at[k + 1], near)
                else:
                    @each_other
                    def _(k):
                        meta_copy(k).start()
            elif name[0] == "tile":
                expert_rows(0, chips[name[1]:name[2]])
            elif name[0] == "R":
                group, part, _ = RELAYS[name[1]]
                wait(relay.at[pl.ds(*PIECE[group, part])], relay_recv.at[name[1]])
            elif name[0] == "W":
                if passed_on(*name[1:3]) or not name[3]:
                    wait_weights(*name[1:])
                else:
                    last_weights.append(name[1:])
            else:
                kind, dy, dx = name
                wait(block(*name), recv.at[KINDS.index(kind), dy * NX + dx])
            for send in sends:
                issue(*send)
            if name is None:
                wv[z, y] = wown[y]
                tell(in_plane.at[0], near)

        for out in stores[-2:]:
            for copy in out:
                copy.wait()

        @each_other
        def _(k):
            meta_copy(k).wait_send()

        for copy in row_copies:
            copy.wait_send()

    def reduce(G, r4, r3, r2, r1):
        tell(in_scope, [targets["z+"], targets["z-"]])

        def row_loads(e):
            pairs = ((xr, xb), (gr, gb), (ur, ub), (sel, sb))
            return [pltpu.make_async_copy(src.at[e - 1], dst, lsem.at[i]) for i, (src, dst) in enumerate(pairs)]

        def chunk(e, way, dist):
            return G.at[e, z_at(dist if way else NZ - dist)["z"]]

        def part_of(ref, way, e, kind):
            return ref.at[way, e, (kind - PART) % 2, (kind - PART) // 2]

        def hop(e, way, kind):
            h = way
            src, dst = {
                FAR: lambda: (chunk(e, way, 4).at[h], r4.at[way, e]),
                SUM3: lambda: (r4.at[way, e], r3.at[way, e, h]),
                NEW3: lambda: (chunk(e, way, 3).at[1 - h], r3.at[way, e, 1 - h]),
                TWO: lambda: (r3.at[way, e], r2.at[way, e]),
                ONE: lambda: (r2.at[way, e], r1.at[way, e]),
            }.get(kind, lambda: (part_of(r2, way, e, kind), part_of(r1, way, e, kind)))()
            return remote(src, dst, rsend.at[way, e, kind], rrecv.at[way, e, kind], z_at(1 if way else NZ - 1))

        def add_into(dst, *others):
            parts = dst.shape[:-2]
            if not parts:
                total = dst[...]
                for other in others:
                    total = total + other[...]
                dst[...] = total
                return

            def flat(ref, i):
                index = []
                for n in reversed(parts):
                    index.append(rem(i, n))
                    i = i // n
                return ref.at[tuple(reversed(index))]

            n = 1
            for p in parts:
                n *= p

            @pl.loop(0, n)
            def _(i):
                total = flat(dst, i)[...]
                for other in others:
                    total = total + flat(other, i)[...]
                flat(dst, i)[...] = total

        def own_rows(s):
            return pl.ds(pl.multiple_of(s * cap, 8), cap)

        def dx_copy(e, k):
            to = at_offset(k)
            return remote(dxs.at[e, own_rows(place_of(to))], dxb.at[me, own_rows(e)], dsend.at[e], drecv.at[e], to)

        tile = 256 if rows % 256 == 0 else rows
        dtile = hidden // NZ
        half = dtile // 2

        def weight_gradients(e):
            out = pltpu.make_async_copy(dx_s, dxs.at[e], osem.at[0])
            out.start()

            @pl.loop(0, NZ // 2)
            def _(i):
                pair = [z_at(n + 2 * i)["z"] for n in (3, 4)]

                def cols(ref):
                    return jnp.concatenate([ref[:, pl.ds(pl.multiple_of(k * dtile, dtile), dtile)] for k in pair], axis=1)

                x_cols, g_cols = cols(xb), cols(gb)
                for m, part in enumerate((dot_tn(x_cols, d1_s[...]), dot_tn(x_cols, d3_s[...]), dot_tn(g_cols, a_s[...]))):
                    for j in range(4):
                        G[e, pair[j // 2], j % 2, m] = part[j * half:(j + 1) * half]

                @pl.when(i == 0)
                def _():
                    if isinstance(e, int):
                        pl.semaphore_wait(in_scope, 2)
                    for way, kind in ((0, FAR), (1, FAR), (1, NEW3)):
                        hop(e, way, kind).start()

                @pl.when(i == 1)
                def _():
                    hop(e, 0, NEW3).start()

            val = sb[...].astype(F32) * y_s[...]
            val_s[e] = jnp.sum(val.reshape(rows // cap, cap, tok), axis=1)
            out.wait()

        def send_back(e):
            pltpu.make_async_copy(dxs.at[e, own_rows(me)], dxb.at[me, own_rows(e)], drecv.at[e]).start()

            @each_other
            def _(k):
                dx_copy(e, k).start()

        def far_sums(e):
            for way in (0, 1):
                hop(e, way, FAR).wait_recv()
                add_into(r4.at[way, e], chunk(e, way, 3).at[way])
                hop(e, way, SUM3).start()

        weight_gradients(0)
        for copy in row_loads(1):
            copy.start()
        send_back(0)
        for name in last_weights:
            wait_weights(*name)

        @pl.loop(1, OWN)
        def _(e):
            for copy in row_loads(e):
                copy.wait()

            @pl.loop(0, rows // tile)
            def _(i):
                expert_rows(e, [pl.ds(pl.multiple_of(i * tile, tile), tile)])

            weight_gradients(e)

            @pl.when(e < OWN - 1)
            def _():
                for copy in row_loads(e + 1):
                    copy.start()

            send_back(e)
            far_sums(e - 1)

        far_sums(OWN - 1)

        def val_copy(k):
            to = at_offset(k)
            return remote(val_s.at[:, place_of(to)], valb.at[:, me], vsem.at[0, k], vsem.at[1, k], to)

        own_val = pltpu.make_async_copy(val_s.at[:, me], valb.at[:, me], vsem.at[0, 0])
        own_val.start()

        @each_other
        def _(k):
            val_copy(k).start()

        @pl.loop(0, OWN)
        def _(e):
            for way in (0, 1):
                for kind in (SUM3, NEW3):
                    hop(e, way, kind).wait_recv()
                add_into(r3.at[way, e], chunk(e, way, 2))
                hop(e, way, TWO).start()

        group, places = dxb.shape[:2]
        ids = ids_ref[...].astype(F32)
        r = lax.broadcasted_iota(jnp.int32, (group * 8, tok), 0)
        e_of = rem(r, 8)
        expert = jnp.where(e_of < OWN, first_expert(r // 8) + e_of, -1).astype(F32)
        member = jnp.zeros((group * 8, tok), F32)
        for j in range(ids.shape[0]):
            member = member + (jnp.broadcast_to(ids[j:j + 1, :], member.shape) == expert).astype(F32)
        before = dot(member.astype(BF16), strict_upper(tok))
        key_s[...] = jnp.where(member > 0.0, before, -1.0).reshape(key_s.shape)
        rr = lax.broadcasted_iota(jnp.int32, (places, tok), 0)
        at, e_row = rem(rr, cap).astype(F32), rr // cap
        some = rows // places

        @pl.loop(0, OWN)
        def _(e):
            got = dxb.at[:, own_rows(e)]
            pltpu.make_async_copy(got, got, drecv.at[e]).wait()

        own_val.wait()

        @each_other
        def _(k):
            val_copy(k).wait()

        bufs = (xb, gb)
        loads = [pltpu.make_async_copy(dxb.at[pl.ds(i * some, some)], bufs[i % 2].reshape(some, places, hidden), lsem.at[i % 2]) for i in range(group // some)]
        vals = pltpu.make_async_copy(valb, vb, lsem.at[2])
        vals.start()
        loads[0].start()
        for i, load in enumerate(loads):
            for later in loads[i + 1:i + 2]:
                later.start()

            @pl.loop(0, some)
            def _(k):
                key = key_s[i * some + k]
                mine = jnp.full((places, tok), -1.0, F32)
                for e in range(OWN):
                    mine = jnp.where(e_row == e, jnp.broadcast_to(key[e:e + 1, :], (places, tok)), mine)
                sb[pl.ds(pl.multiple_of(k * places, places), places), :] = (at == mine).astype(F32).astype(BF16)

            load.wait()
            part = dot_tn(sb[...], bufs[i % 2][...])
            acc_s[...] = acc_s[...] + part if i else part

        in_grad_ref[...] = acc_s[...].astype(BF16)
        vals.wait()

        def gate_step(k, total):
            for e in range(OWN):
                row = vb[e, pl.ds(k, 1), :]
                total = total + jnp.where(ids == (first_expert(k) + e).astype(F32), jnp.broadcast_to(row, ids.shape), 0.0)
            return total

        gate_ref[...] = lax.fori_loop(0, group, gate_step, jnp.zeros(ids.shape, F32))
        results = [pltpu.make_async_copy(a, b, load_sem.at[i]) for i, a, b in ((0, in_grad_ref, in_grad_hbm), (1, gate_ref, gate_hbm))]
        for copy in results:
            copy.start()

        last = OWN - 1

        @pl.loop(0, last)
        def _(e):
            for way in (0, 1):
                hop(e, way, TWO).wait_recv()
                add_into(r2.at[way, e], chunk(e, way, 1))
                hop(e, way, ONE).start()

        for way in (0, 1):
            hop(last, way, TWO).wait_recv()
        for kind in range(PART, HOPS):
            for way in (0, 1):
                add_into(part_of(r2, way, last, kind), part_of(G, last, z_at(1 if way else NZ - 1)["z"], kind))
                hop(last, way, kind).start()

        def keep(e, m, to, then_remote, then_local):
            src = r1.at[0, e, to // 2, m, pl.ds(to % 2 * d_loc, d_loc)]
            dst = grads.at[m, y * OWN + e]
            n = 0 if isinstance(m, slice) else m

            @pl.when(y != to)
            def _():
                then_remote(remote(src, dst, ysend.at[e, n, to], yrecv.at[e, n, y], {"y": to}))

            @pl.when(y == to)
            def _():
                then_local(pltpu.make_async_copy(src, dst, ysend.at[e, n, to]))

        every = slice(None)

        @pl.loop(0, last)
        def _(e):
            for way in (0, 1):
                hop(e, way, ONE).wait_recv()
            add_into(r1.at[0, e], r1.at[1, e], G.at[e, z])
            for to in range(NY):
                keep(e, every, to, start, start)

        for kind in range(PART, HOPS):
            for way in (0, 1):
                hop(last, way, kind).wait_recv()
            add_into(part_of(r1, 0, last, kind), part_of(r1, 1, last, kind), part_of(G, last, z, kind))
            m, h = (kind - PART) // 2, (kind - PART) % 2
            for to in (2 * h, 2 * h + 1):
                keep(last, m, to, start, start)

        def finish_up(e, kinds, matrices):
            for m in matrices:
                for at in range(NY):
                    def both(copy):
                        wait(grads.at[m, at * OWN + e], yrecv.at[e, 0 if m is every else m, at])
                        copy.wait_send()

                    keep(e, m, at, both, lambda copy: copy.wait())
            for way in (0, 1):
                for kind in kinds:
                    hop(e, way, kind).wait_send()
            sent = dxs.at[e, pl.ds(0, (GROUP - 1) * cap)]
            pltpu.make_async_copy(sent, sent, dsend.at[e]).wait()

        @pl.loop(0, last)
        def _(e):
            finish_up(e, range(PART), [every])

        finish_up(last, [FAR, SUM3, NEW3, TWO, *range(PART, HOPS)], range(3))
        for copy in results:
            copy.wait()

    weight_copies, last_weights = [], []
    pl.run_scoped(gather, *scope_one)
    pl.run_scoped(reduce, *scope_two)
    for number, group, part in weight_copies:
        ref = wown.at[0, pl.ds(*PIECE[group, part])]
        remote(ref, ref, send_sem.at[number], relay_recv.at[0], targets["core"]).wait_send()


def layer(cap, x, u, ids, gates, w1, w3, w2):
    tok, hidden = x.shape
    local_experts, d_loc, ff = w1.shape
    rows = GROUP * cap
    half = hidden // NZ // 2
    cut = tok - tok // 8 if tok % 256 == 0 else tok
    halves = [cut // 2] * 2 + [tok - cut // 2] * 2
    spans = {kind: (sum(halves[:i]), halves[i]) for i, kind in enumerate(KINDS)}
    order = gather_order({kind: 2 * hidden * n for kind, (_, n) in spans.items()}, 2 * w1.size * 3 // local_experts)
    sends = sum(len(s) for _, s in order)
    dma, v, shape = pltpu.SemaphoreType.DMA, pltpu.VMEM, jax.ShapeDtypeStruct
    far = lambda lanes: shape((OWN - 1, rows, lanes), BF16)
    near = lambda lanes: v((rows, lanes), BF16)
    stage = lambda lanes: v((2, OWN - 1, 2 * cap, lanes), BF16)
    sums = [v((2, OWN, 2, 3, half, ff), F32)] * 3
    scope_one = [v((GROUP, 2 * tok, hidden), BF16), v((tok, tok), BF16), stage(hidden), stage(hidden), stage(hidden), stage(tok)]
    scope_two = [v((OWN, NZ, 2, 3, half, ff), F32), v((2, OWN, 3, half, ff), F32)] + sums
    per_expert = v((OWN, GROUP, tok), F32)
    gate_rows = v((GROUP, OWN, tok), F32)
    outs = pl.pallas_call(
        functools.partial(layer_kernel, order, cap, spans, scope_one, scope_two),
        name="layer",
        out_shape=(
            shape((3, local_experts, d_loc, ff), F32), shape((tok, hidden), BF16), shape(ids.shape, F32),
            shape((GROUP, OWN * cap, hidden), BF16), shape((OWN, GROUP, tok), F32), shape((OWN, rows, hidden), BF16),
            far(hidden), far(hidden), far(hidden), far(tok),
        ),
        in_specs=[ANY] * 7,
        out_specs=(ANY,) * 10,
        scratch_shapes=[
            v(ids.shape, ids.dtype), v(ids.shape, F32), v((tok, hidden), BF16), v(ids.shape, F32), gate_rows, gate_rows, v((NY, OWN, 3, d_loc, ff), BF16), v((NZ, NY, OWN, 3, d_loc, ff), BF16), v((OWN, 3, d_loc, ff), BF16),
            near(hidden), near(hidden), near(hidden), near(tok), near(ff), near(ff), near(ff), v((rows, 1), F32),
            near(hidden), per_expert, per_expert, v((GROUP, 8, tok), F32), v((tok, hidden), F32),
            dma((len(KINDS), NY * NX)), dma((len(KINDS), NY * NX)), dma((NZ, NY, 2, 2)), dma((len(RELAYS),)), dma((GROUP,)), dma((sends,)), dma((GROUP,)),
            dma((7,)), dma((2, 4)),
            dma((4,)), dma((2, OWN, HOPS)), dma((2, OWN, HOPS)), dma((OWN, 3, NY)), dma((OWN, 3, NY)),
            dma((OWN,)), dma((OWN,)), dma((2, GROUP)), dma((1,)), pltpu.SemaphoreType.REGULAR, pltpu.SemaphoreType.REGULAR((ROUNDS,)),
        ],
        compiler_params=params(0),
    )(x, u, ids, gates, w1, w3, w2)
    return outs[:3]


def finish_kernel(grads, in_grad, gate, *refs):
    n = 5
    outs, bufs, sems = refs[:n], refs[n:2 * n], refs[-1]
    ins = [grads.at[m] for m in range(3)] + [in_grad, gate]
    load, store = [], []
    for i, (a, b, o) in enumerate(zip(ins, bufs, outs)):
        half = a.shape[0] // 2
        for h in range(2):
            at = pl.ds(h * half, half)
            load.append(pltpu.make_async_copy(a.at[at], b.at[at], sems.at[0, i, h]))
            store.append(pltpu.make_async_copy(b.at[at], o.at[at], sems.at[1, i, h]))
    for copy in load:
        copy.start()
    for before, after in zip(load, store):
        before.wait()
        after.start()
    for copy in store:
        copy.wait()


def finish(grads, in_grad, gate):
    shapes = [grads.shape[1:]] * 3 + [in_grad.shape, gate.shape]
    types = [grads.dtype] * 3 + [in_grad.dtype, gate.dtype]
    return pl.pallas_call(
        finish_kernel,
        name="finish",
        out_shape=[jax.ShapeDtypeStruct(s, t) for s, t in zip(shapes, types)],
        in_specs=[ANY] * 3,
        out_specs=[ANY] * len(shapes),
        scratch_shapes=[pltpu.VMEM(s, t) for s, t in zip(shapes, types)] + [pltpu.SemaphoreType.DMA((2, len(shapes), 2))],
    )(grads, in_grad, gate)


def solution(mesh):
    mesh4 = Mesh(mesh.devices.reshape(NZ, NY, NX, NC), ("z", "y", "x", "core"))
    tok_spec = P(("z", "y", "x", "core"), None)
    up_spec = P(("x", "core"), ("z", "y"), None)
    down_spec = P(("x", "core"), None, ("z", "y"))

    def per_device(layer_in, out_grad, expert_ids, gate_vals, w_one, w_two, w_three):
        tok_dev, hidden = layer_in.shape
        top_k = expert_ids.shape[1]
        local_experts, d_loc, ff = w_one.shape
        cap = capacity_of(tok_dev, top_k, local_experts * NX * NC)
        ids = expert_ids.T
        grads, in_grad, gate_out = layer(cap, layer_in, out_grad, ids, gate_vals.T, w_one, w_three, w_two.swapaxes(1, 2))
        g1, g3, g2, in_grad, gate_out = finish(grads, in_grad, gate_out)
        return in_grad, gate_out.T, g1, g2.swapaxes(1, 2), g3

    return jax.shard_map(per_device, mesh=mesh4, in_specs=(tok_spec, tok_spec, tok_spec, tok_spec, up_spec, down_spec, up_spec), out_specs=(tok_spec, tok_spec, up_spec, down_spec, up_spec), check_vma=False)
```

```python
import functools

import jax
import jax.numpy as jnp
from jax import lax
from jax.experimental import pallas as pl
from jax.experimental.pallas import tpu as pltpu
from jax.sharding import Mesh, PartitionSpec as P

NZ, NY, NX, NC = 8, 4, 4, 2
GROUP = NY * NX * NC
PLANE = ("y", "x", "core")
OWN = 4
F32, BF16 = jnp.float32, jnp.bfloat16
ANY = pl.BlockSpec(memory_space=pl.ANY)


def capacity_of(tok_dev, top_k, experts):
    return max(8, ((tok_dev * top_k * 5) // (4 * experts) + 7) // 8 * 8)


def rem(a, b):
    return a % b if isinstance(a, int) else lax.rem(a, b)


def contract(ca, cb):
    return lambda a, b: lax.dot_general(a, b, (((ca,), (cb,)), ((), ())), preferred_element_type=F32)


dot, dot_nt, dot_tn = contract(1, 0), contract(1, 1), contract(0, 0)


def params(number):
    return pltpu.CompilerParams(collective_id=number, has_side_effects=True, vmem_limit_bytes=67043328)


def each_other(body):
    return pl.loop(1, GROUP)(body)


def strict_upper(n):
    rows = lax.broadcasted_iota(jnp.int32, (n, n), 0)
    cols = lax.broadcasted_iota(jnp.int32, (n, n), 1)
    return (rows < cols).astype(F32).astype(BF16)


def here():
    return tuple(lax.axis_index(a) for a in ("z", "y", "x", "core"))


def at_offset(k):
    _, y, x, c = here()
    dy, dx, dc = k // (NX * NC), rem(k // NC, NX), rem(k, NC)
    return {"y": rem(y + dy, NY), "x": rem(x + dx, NX), "core": rem(c + dc, NC)}


def place_of(d):
    return d["y"] * (NX * NC) + d["x"] * NC + d["core"]


def z_at(dz):
    return {"z": rem(lax.axis_index("z") + dz, NZ)}


def remote(src, dst, send_sem, recv_sem, target):
    return pltpu.make_async_remote_copy(src_ref=src, dst_ref=dst, send_sem=send_sem, recv_sem=recv_sem, device_id=target, device_id_type=pl.DeviceIdType.MESH)


def start(copy):
    copy.start()


def tell(semaphore, targets):
    for target in targets:
        pl.semaphore_signal(semaphore, device_id=target, device_id_type=pl.DeviceIdType.MESH)


RATE, D2D, HOP = 44700.0, 400000.0, 2.3
PUT, TILE, ROWS = 1.0, 1.0, 0.4
STEP = 5
AHEAD, MORE = 5.0, 0.05

PIECE = {(0, None): (0, 1), (1, None): (1, 3), (1, 0): (1, 1), (1, 1): (2, 2)}
RELAYS = ((0, None, "y+"), (1, 0, "y+"), (1, 1, "y-"))


ROUNDS = NY // 2 + NX // 2
KINDS = ("A0", "A1", "B0", "B1")


def gather_order(sizes, expert_bytes):
    free, pending, coming, order, have, ready = {}, {}, [], [], {}, {}

    def send(now, name, link, arrives, nbytes):
        t = max(now, free.get(link, 0.0)) + nbytes / (D2D if link == "core" else RATE)
        free[link] = t
        coming.append((t + (HOP / 2 if link == "core" else HOP), len(order), len(coming), arrives))
        return (name, link)

    def later(rank, name, link, arrives, nbytes):
        queue = pending.setdefault(link, [])
        queue.append((rank, len(order), len(queue), (name, link, arrives, nbytes)))

    def turn(now):
        out = []
        for link, queue in pending.items():
            queue.sort()
            while queue and free.get(link, 0.0) - now < AHEAD + MORE * now:
                out.append(send(now, *queue.pop(0)[-1]))
        return out

    def on_rows(kind, dy, dx):
        first, second = "xy" if kind[0] == "A" else "yx"
        d = {"x": dx, "y": dy}
        for axis in [first, second] if d[second] == 0 else [second]:
            for sign in (1, -1):
                if d[axis] == 0 or d[axis] == -sign % 4 and kind[1] == "10"[sign > 0]:
                    nd = dict(d)
                    nd[axis] = (d[axis] - sign) % 4
                    rank = 4 + (axis == second) + (d[axis] != 0)
                    later(rank, (kind, dy, dx), axis + "-+"[sign > 0], (kind, nd["y"], nd["x"]), sizes[kind])

    def core(now, key):
        return send(now, key, "core", ("core",) + key, sizes[key[0]])

    def weights(rank, name, group, part, link, arrives):
        later(rank, name, link, arrives + (group, part), PIECE[group, part][1] * expert_bytes)

    def on_piece(dz, dy, group):
        for link, step, far in (("z+", -1, dy < 2), ("z-", 1, dy >= 2)):
            gone = (step * dz) % NZ
            if gone < 3 + far:
                weights(4 * group + gone, ("W", dz, dy, group), group, None, link, ("W", (dz + step) % NZ, dy))

    def arrived(key, part=None):
        have[key] = have.get(key, 0) + (2 if part is None else 1)
        if have[key] == 2:
            ready[key] = True
        return have[key] == 2

    for i, (group, part, link) in enumerate(RELAYS):
        weights(0, ("r", i), group, part, link, ("R", i))
    for group in range(2):
        for dy, link in ((1, "y+"), (3, "y-")):
            weights(2, ("w", dy, group), group, None, link, ("W", 0, (-dy) % NY))
        on_piece(0, 0, group)
    sends = []
    for kind in KINDS[::-1]:
        arrived((kind, 0, 0))
        on_rows(kind, 0, 0)
        sends.append(core(0.0, (kind, 0, 0)))
    order.append((None, turn(0.0) + sends))
    todo, puts, done, now = [(dy, dx) for dy in range(NY) for dx in range(NX)], 0, 0, 0.0
    known = 0
    while coming or todo or done < puts:
        coming.sort()
        if known < ROUNDS and now > HOP * (known + 1):
            order.append((("near", known), turn(now)))
            known += 1
            continue
        soon = coming[0][0] if coming else 1e9
        if soon > now:
            place = next((p for p in todo if all(pre + (kind,) + p in ready for kind in KINDS for pre in ((), ("core",)))), None)
            if place is not None and now > 15:
                todo.remove(place)
                order.append((("put",) + place, turn(now)))
                puts += 1
                now += PUT
                continue
            step = min(STEP, puts - done)
            weights_in = sum(key[0] == "W" and key[-1] == 0 for key in ready) == NZ * NY - 1
            calm = all(c[-1][0] == "core" for c in coming)
            if weights_in and step and (step >= 3 and soon - now > TILE or calm):
                order.append((("tile", done, done + step), turn(now)))
                done += step
                now += TILE + ROWS * step
                continue
        t, _, _, name = coming.pop(0)
        now = max(now, t)
        if name[0] == "core":
            arrived(name)
            continue
        sends = []
        if name[0] == "R":
            i, group, part = name[1:]
            weights(1, name[:2], group, part, RELAYS[i][2], ("W", 0, 2))
            name = name[:2]
        elif name[0] == "W":
            if arrived(name[:-1], name[-1]):
                on_piece(*name[1:-1])
        else:
            sends = [core(now, name)]
            arrived(name)
            on_rows(*name)
        order.append((name, sends + turn(now)))
    return order


def passed_on(dz, dy):
    return dz != NZ // 2 and dz not in ((3,) if dy < 2 else (5,))


def first_expert(d):
    return rem(d, NX * NC) * (NY * OWN) + d // (NX * NC) * OWN


FAR, SUM3, NEW3, TWO, ONE, PART, HOPS = 0, 1, 2, 3, 4, 5, 11


def layer_kernel(order, cap, spans, scope_one, scope_two, x_hbm, u_hbm, ids_hbm, gates_hbm, w1_hbm, w3_hbm, w2_hbm,
                 grads, in_grad_hbm, gate_hbm, dxb, valb, dxs, xr, ur, gr, sel,
                 ids_ref, gates_ref, in_grad_ref, gate_ref, metas, gates_out, wown, wv, relay, xb, ub, gb, sb, a_s, d1_s, d3_s, y_s, dx_s, val_s, vb, key_s, acc_s,
                 recv, core_recv, wrecv, relay_recv, mrecv, send_sem, msend, load_sem, store_sem,
                 lsem, rsend, rrecv, ysend, yrecv, dsend, drecv, vsem, osem, in_scope, in_plane):
    z, y, x, c = here()
    tok, hidden = x_hbm.shape
    rows, ff = xb.shape[0], a_s.shape[-1]
    d_loc = hidden // (NZ * NY)
    me = place_of(at_offset(0))

    def place(dy, dx, dc=0):
        return place_of(at_offset(dy * (NX * NC) + dx * NC + dc))

    targets = {"core": {"core": 1 - c}}
    for sign, n in (("+", 1), ("-", -1)):
        targets["x" + sign] = {"x": rem(x + n + NX, NX)}
        targets["y" + sign] = {"y": rem(y + n + NY, NY)}
        targets["z" + sign] = z_at(n + NZ)

    def wait(ref, sem):
        remote(ref, ref, send_sem.at[0], sem, targets["core"]).wait_recv()

    def piece(dz, dy, group, part=None):
        return wv.at[z_at(dz)["z"], rem(y + dy, NY), pl.ds(*PIECE[group, part])]

    def wait_weights(dz, dy, group, part):
        wait(piece(dz, dy, group, part), wrecv.at[dz, dy, group, part or 0])

    def w(e, m):
        return wv[:, :, e, m].reshape(hidden, ff)

    def expert_rows(e, spans):
        def cut_of(ref):
            return jnp.concatenate([ref[s, :] for s in spans]) if spans[1:] else ref[spans[0], :]

        def save(ref, value):
            n = value.shape[0] // len(spans)
            for i, s in enumerate(spans):
                ref[s, :] = value[i * n:(i + 1) * n]

        x_rows = cut_of(xb)
        h1, h3 = dot(x_rows, w(e, 0)), dot(x_rows, w(e, 1))
        sig = jax.nn.sigmoid(h1)
        silu = h1 * sig
        act = (silu * h3).astype(BF16)
        save(a_s, act)
        y_rows = dot_nt(act, w(e, 2))
        save(y_s, jnp.sum(cut_of(ub).astype(F32) * y_rows, axis=1, keepdims=True))
        da = dot(cut_of(gb), w(e, 2))
        d1 = (da * h3 * sig * (1.0 + h1 * (1.0 - sig))).astype(BF16)
        d3 = (da * silu).astype(BF16)
        save(d1_s, d1)
        save(d3_s, d3)
        save(dx_s, (dot_nt(d1, w(e, 0)) + dot_nt(d3, w(e, 1))).astype(BF16))

    def gather(all_rows, tri, sx, su, sg, ss):
        loads = [
            pltpu.make_async_copy(x_hbm, all_rows.at[me, pl.ds(0, tok)], load_sem.at[0]),
            pltpu.make_async_copy(u_hbm, all_rows.at[me, pl.ds(tok, tok)], load_sem.at[1]),
        ]
        for m, ref in enumerate((w1_hbm, w3_hbm, w2_hbm)):
            loads.append(pltpu.make_async_copy(ref.reshape(NY, OWN, d_loc, ff), wown.at[:, :, m], load_sem.at[2 + m]))
        tables = [pltpu.make_async_copy(a, b, load_sem.at[i]) for i, a, b in ((5, ids_hbm, ids_ref), (6, gates_hbm, gates_ref))]
        for copy in tables + loads:
            copy.start()
        barrier = pltpu.get_barrier_semaphore()
        tell(barrier, targets.values())
        def make_tables():
            for copy in tables:
                copy.wait()

            @pl.loop(0, GROUP)
            def _(d):
                number = first_expert(d) + lax.broadcasted_iota(jnp.int32, (OWN, tok), 0)
                value = jnp.full((OWN, tok), -1.0, F32)
                for j in range(ids_ref.shape[0]):
                    chosen = ids_ref[pl.ds(j, 1), :] == number
                    value = jnp.where(chosen, jnp.broadcast_to(gates_ref[pl.ds(j, 1), :], value.shape), value)
                gates_out[d] = value

            metas[me] = gates_out[me]
            tri[...] = strict_upper(tok)

        for copy in loads:
            copy.wait()
        pl.semaphore_wait(barrier, len(targets))

        back = {"x+": (0, 3), "x-": (0, 1), "y+": (3, 0), "y-": (1, 0)}
        def block(kind, dy, dx, dc=0):
            return all_rows.at[place(dy, dx, dc), pl.ds(*spans[kind])]

        near = [t for link, t in targets.items() if link[0] != "z"]
        row_copies = []

        def issue(name, link):
            number = len(row_copies) + len(weight_copies)
            sem = send_sem.at[number]
            group, part_of = None, None
            if name[0] == "w":
                _, dy, group = name
                src = wown.at[rem(y + dy, NY), pl.ds(*PIECE[group, None])]
                copy = remote(src, piece(0, 0, group), sem, wrecv.at[0, (-dy) % NY, group, 0], targets[link])
            elif name[0] in "rR":
                group, part_of, _ = RELAYS[name[1]]
                span = pl.ds(*PIECE[group, part_of])
                if name[0] == "r":
                    copy = remote(wown.at[rem(y + 2, NY), span], relay.at[span], sem, relay_recv.at[name[1]], targets[link])
                else:
                    dst = piece(0, back[link][0], group, part_of)
                    copy = remote(relay.at[span], dst, sem, wrecv.at[0, 2, group, part_of or 0], targets[link])
            elif name[0] == "W":
                _, dz, dy, group = name
                ndz = (dz - 1) % NZ if link == "z+" else (dz + 1) % NZ
                own = wown.at[y, pl.ds(*PIECE[group, None])]
                copy = remote(own if dz == dy == 0 else piece(dz, dy, group), piece(dz, dy, group), sem, wrecv.at[ndz, dy, group, 0], targets[link])
            else:
                kind, dy, dx = name
                ref = block(*name)
                oy, ox = back.get(link, (0, 0))
                arrivals = core_recv if link == "core" else recv
                rsem = arrivals.at[KINDS.index(kind), (dy + oy) % NY * NX + (dx + ox) % NX]
                copy = remote(ref, ref, sem, rsem, targets[link])
            copy.start()
            if group is None:
                row_copies.append(copy)
            else:
                weight_copies.append((number, group, part_of))

        def meta_copy(k):
            to = at_offset(k)
            return remote(gates_out.at[place_of(to)], metas.at[me], msend.at[k], mrecv.at[k], to)

        n_rows = OWN * 2 * cap
        stores, chips = [], []

        def put(dy, dx):
            slot = len(stores) % 2
            if stores[1:]:
                for copy in stores[-2]:
                    copy.wait()
            for dc in (0, 1):
                if dy or dx or dc:
                    k = ((-dy) % NY) * (NX * NC) + ((-dx) % NX) * NC + dc
                    wait(metas.at[place(dy, dx, dc)], mrecv.at[k])
            for i, kind in enumerate(KINDS):
                wait(block(kind, dy, dx, 1), core_recv.at[i, dy * NX + dx])
            chip = rem(y + dy, NY) * NX + rem(x + dx, NX)
            n = 2 * OWN
            which = lax.broadcasted_iota(jnp.int32, (n, tok), 0)
            gate = jnp.zeros((n, tok), F32)
            for i in range(n):
                gate = jnp.where(which == i, jnp.broadcast_to(metas[2 * chip + i // OWN, pl.ds(i % OWN, 1), :], gate.shape), gate)
            member = gate >= 0.0
            key = jnp.where(member, dot(member.astype(F32).astype(BF16), tri[...]), -1.0)
            r = lax.broadcasted_iota(jnp.int32, (n_rows, tok), 0)
            at = rem(r, cap).astype(F32)
            row_of = rem(r // cap, 2) * OWN + r // (2 * cap)
            mine, gates = jnp.full((n_rows, tok), -1.0, F32), jnp.zeros((n_rows, tok), F32)
            for i in range(n):
                mine = jnp.where(row_of == i, jnp.broadcast_to(key[i:i + 1, :], mine.shape), mine)
                gates = jnp.where(row_of == i, jnp.broadcast_to(gate[i:i + 1, :], mine.shape), gates)
            found = at == mine
            pick = [jnp.logical_and(found, row_of // OWN == p).astype(F32) for p in range(2)]
            both = pick[0] + pick[1]
            scale = jnp.sum(both * gates, axis=1, keepdims=True)
            pick = [p.astype(BF16) for p in pick]
            x_rows = dot(pick[0], all_rows[2 * chip, 0:tok, :]) + dot(pick[1], all_rows[2 * chip + 1, 0:tok, :])
            u_rows = dot(pick[0], all_rows[2 * chip, tok:2 * tok, :]) + dot(pick[1], all_rows[2 * chip + 1, tok:2 * tok, :])
            span = pl.ds(pl.multiple_of(chip * 2 * cap, 2 * cap), 2 * cap)
            out = []
            for i, (value, first, stage, far) in enumerate(((x_rows, xb, sx, xr), (u_rows, ub, su, ur), (scale * u_rows, gb, sg, gr), (both, sb, ss, sel))):
                value = value.astype(BF16)
                first[span, :] = value[:2 * cap]
                stage[slot] = value[2 * cap:].reshape(stage.shape[1:])
                out.append(pltpu.make_async_copy(stage.at[slot], far.at[:, span], store_sem.at[slot, i]))
                out[-1].start()
            stores.append(out)
            chips.append(span)

        for name, sends in order:
            if name is None:
                pass
            elif name[0] == "put":
                put(*name[1:])
            elif name[0] == "near":
                _, k = name
                pl.semaphore_wait(in_plane.at[k], len(near))
                if k < ROUNDS - 1:
                    tell(in_plane.at[k + 1], near)
                else:
                    @each_other
                    def _(k):
                        meta_copy(k).start()
            elif name[0] == "tile":
                expert_rows(0, chips[name[1]:name[2]])
            elif name[0] == "R":
                group, part, _ = RELAYS[name[1]]
                wait(relay.at[pl.ds(*PIECE[group, part])], relay_recv.at[name[1]])
            elif name[0] == "W":
                if passed_on(*name[1:3]) or not name[3]:
                    wait_weights(*name[1:])
                else:
                    last_weights.append(name[1:])
            else:
                kind, dy, dx = name
                wait(block(*name), recv.at[KINDS.index(kind), dy * NX + dx])
            for send in sends:
                issue(*send)
            if name is None:
                tell(in_plane.at[0], near)
                make_tables()
                wv[z, y] = wown[y]

        for out in stores[-2:]:
            for copy in out:
                copy.wait()

        @each_other
        def _(k):
            meta_copy(k).wait_send()

        for copy in row_copies:
            copy.wait_send()

    def reduce(G, r4, r3, r2, r1):
        tell(in_scope, [targets["z+"], targets["z-"]])

        def row_loads(e):
            pairs = ((xr, xb), (gr, gb), (ur, ub), (sel, sb))
            return [pltpu.make_async_copy(src.at[e - 1], dst, lsem.at[i]) for i, (src, dst) in enumerate(pairs)]

        def chunk(e, way, dist):
            return G.at[e, z_at(dist if way else NZ - dist)["z"]]

        def part_of(ref, way, e, kind):
            return ref.at[way, e, (kind - PART) % 2, (kind - PART) // 2]

        def hop(e, way, kind):
            h = way
            src, dst = {
                FAR: lambda: (chunk(e, way, 4).at[h], r4.at[way, e]),
                SUM3: lambda: (r4.at[way, e], r3.at[way, e, h]),
                NEW3: lambda: (chunk(e, way, 3).at[1 - h], r3.at[way, e, 1 - h]),
                TWO: lambda: (r3.at[way, e], r2.at[way, e]),
                ONE: lambda: (r2.at[way, e], r1.at[way, e]),
            }.get(kind, lambda: (part_of(r2, way, e, kind), part_of(r1, way, e, kind)))()
            return remote(src, dst, rsend.at[way, e, kind], rrecv.at[way, e, kind], z_at(1 if way else NZ - 1))

        def add_into(dst, *others):
            parts = dst.shape[:-2]
            if not parts:
                total = dst[...]
                for other in others:
                    total = total + other[...]
                dst[...] = total
                return

            def flat(ref, i):
                index = []
                for n in reversed(parts):
                    index.append(rem(i, n))
                    i = i // n
                return ref.at[tuple(reversed(index))]

            n = 1
            for p in parts:
                n *= p

            @pl.loop(0, n)
            def _(i):
                total = flat(dst, i)[...]
                for other in others:
                    total = total + flat(other, i)[...]
                flat(dst, i)[...] = total

        def own_rows(s):
            return pl.ds(pl.multiple_of(s * cap, 8), cap)

        def dx_copy(e, k):
            to = at_offset(k)
            return remote(dxs.at[e, own_rows(place_of(to))], dxb.at[me, own_rows(e)], dsend.at[e], drecv.at[e], to)

        tile = 256 if rows % 256 == 0 else rows
        dtile = hidden // NZ
        half = dtile // 2

        def weight_gradients(e):
            out = pltpu.make_async_copy(dx_s, dxs.at[e], osem.at[0])
            out.start()

            @pl.loop(0, NZ // 2)
            def _(i):
                pair = [z_at(n + 2 * i)["z"] for n in (3, 4)]

                def cols(ref):
                    return jnp.concatenate([ref[:, pl.ds(pl.multiple_of(k * dtile, dtile), dtile)] for k in pair], axis=1)

                x_cols, g_cols = cols(xb), cols(gb)
                for m, part in enumerate((dot_tn(x_cols, d1_s[...]), dot_tn(x_cols, d3_s[...]), dot_tn(g_cols, a_s[...]))):
                    for j in range(4):
                        G[e, pair[j // 2], j % 2, m] = part[j * half:(j + 1) * half]

                @pl.when(i == 0)
                def _():
                    if isinstance(e, int):
                        pl.semaphore_wait(in_scope, 2)
                    for way, kind in ((0, FAR), (1, FAR), (1, NEW3)):
                        hop(e, way, kind).start()

                @pl.when(i == 1)
                def _():
                    hop(e, 0, NEW3).start()

            val = sb[...].astype(F32) * y_s[...]
            val_s[e] = jnp.sum(val.reshape(rows // cap, cap, tok), axis=1)
            out.wait()

        def send_back(e):
            pltpu.make_async_copy(dxs.at[e, own_rows(me)], dxb.at[me, own_rows(e)], drecv.at[e]).start()

            @each_other
            def _(k):
                dx_copy(e, k).start()

        def far_sums(e):
            for way in (0, 1):
                hop(e, way, FAR).wait_recv()
                add_into(r4.at[way, e], chunk(e, way, 3).at[way])
                hop(e, way, SUM3).start()

        weight_gradients(0)
        for copy in row_loads(1):
            copy.start()
        send_back(0)
        for name in last_weights:
            wait_weights(*name)

        @pl.loop(1, OWN)
        def _(e):
            for copy in row_loads(e):
                copy.wait()

            @pl.loop(0, rows // tile)
            def _(i):
                expert_rows(e, [pl.ds(pl.multiple_of(i * tile, tile), tile)])

            weight_gradients(e)

            @pl.when(e < OWN - 1)
            def _():
                for copy in row_loads(e + 1):
                    copy.start()

            send_back(e)
            far_sums(e - 1)

        far_sums(OWN - 1)

        def val_copy(k):
            to = at_offset(k)
            return remote(val_s.at[:, place_of(to)], valb.at[:, me], vsem.at[0, k], vsem.at[1, k], to)

        own_val = pltpu.make_async_copy(val_s.at[:, me], valb.at[:, me], vsem.at[0, 0])
        own_val.start()

        @each_other
        def _(k):
            val_copy(k).start()

        @pl.loop(0, OWN)
        def _(e):
            for way in (0, 1):
                for kind in (SUM3, NEW3):
                    hop(e, way, kind).wait_recv()
                add_into(r3.at[way, e], chunk(e, way, 2))
                hop(e, way, TWO).start()

        group, places = dxb.shape[:2]
        ids = ids_ref[...].astype(F32)
        r = lax.broadcasted_iota(jnp.int32, (group * 8, tok), 0)
        e_of = rem(r, 8)
        expert = jnp.where(e_of < OWN, first_expert(r // 8) + e_of, -1).astype(F32)
        member = jnp.zeros((group * 8, tok), F32)
        for j in range(ids.shape[0]):
            member = member + (jnp.broadcast_to(ids[j:j + 1, :], member.shape) == expert).astype(F32)
        before = dot(member.astype(BF16), strict_upper(tok))
        key_s[...] = jnp.where(member > 0.0, before, -1.0).reshape(key_s.shape)
        rr = lax.broadcasted_iota(jnp.int32, (places, tok), 0)
        at, e_row = rem(rr, cap).astype(F32), rr // cap
        some = rows // places

        @pl.loop(0, OWN)
        def _(e):
            got = dxb.at[:, own_rows(e)]
            pltpu.make_async_copy(got, got, drecv.at[e]).wait()

        own_val.wait()

        @each_other
        def _(k):
            val_copy(k).wait()

        bufs = (xb, gb)
        loads = [pltpu.make_async_copy(dxb.at[pl.ds(i * some, some)], bufs[i % 2].reshape(some, places, hidden), lsem.at[i % 2]) for i in range(group // some)]
        vals = pltpu.make_async_copy(valb, vb, lsem.at[2])
        vals.start()
        loads[0].start()
        for i, load in enumerate(loads):
            for later in loads[i + 1:i + 2]:
                later.start()

            @pl.loop(0, some)
            def _(k):
                key = key_s[i * some + k]
                mine = jnp.full((places, tok), -1.0, F32)
                for e in range(OWN):
                    mine = jnp.where(e_row == e, jnp.broadcast_to(key[e:e + 1, :], (places, tok)), mine)
                sb[pl.ds(pl.multiple_of(k * places, places), places), :] = (at == mine).astype(F32).astype(BF16)

            load.wait()
            part = dot_tn(sb[...], bufs[i % 2][...])
            acc_s[...] = acc_s[...] + part if i else part

        in_grad_ref[...] = acc_s[...].astype(BF16)
        vals.wait()

        def gate_step(k, total):
            for e in range(OWN):
                row = vb[e, pl.ds(k, 1), :]
                total = total + jnp.where(ids == (first_expert(k) + e).astype(F32), jnp.broadcast_to(row, ids.shape), 0.0)
            return total

        gate_ref[...] = lax.fori_loop(0, group, gate_step, jnp.zeros(ids.shape, F32))
        results = [pltpu.make_async_copy(a, b, load_sem.at[i]) for i, a, b in ((0, in_grad_ref, in_grad_hbm), (1, gate_ref, gate_hbm))]
        for copy in results:
            copy.start()

        last = OWN - 1

        @pl.loop(0, last)
        def _(e):
            for way in (0, 1):
                hop(e, way, TWO).wait_recv()
                add_into(r2.at[way, e], chunk(e, way, 1))
                hop(e, way, ONE).start()

        for way in (0, 1):
            hop(last, way, TWO).wait_recv()
        for kind in range(PART, HOPS):
            for way in (0, 1):
                add_into(part_of(r2, way, last, kind), part_of(G, last, z_at(1 if way else NZ - 1)["z"], kind))
                hop(last, way, kind).start()

        def keep(e, m, to, then_remote, then_local):
            src = r1.at[0, e, to // 2, m, pl.ds(to % 2 * d_loc, d_loc)]
            dst = grads.at[m, y * OWN + e]
            n = 0 if isinstance(m, slice) else m

            @pl.when(y != to)
            def _():
                then_remote(remote(src, dst, ysend.at[e, n, to], yrecv.at[e, n, y], {"y": to}))

            @pl.when(y == to)
            def _():
                then_local(pltpu.make_async_copy(src, dst, ysend.at[e, n, to]))

        every = slice(None)

        @pl.loop(0, last)
        def _(e):
            for way in (0, 1):
                hop(e, way, ONE).wait_recv()
            add_into(r1.at[0, e], r1.at[1, e], G.at[e, z])
            for to in range(NY):
                keep(e, every, to, start, start)

        for kind in range(PART, HOPS):
            for way in (0, 1):
                hop(last, way, kind).wait_recv()
            add_into(part_of(r1, 0, last, kind), part_of(r1, 1, last, kind), part_of(G, last, z, kind))
            m, h = (kind - PART) // 2, (kind - PART) % 2
            for to in (2 * h, 2 * h + 1):
                keep(last, m, to, start, start)

        def finish_up(e, kinds, matrices):
            for m in matrices:
                for at in range(NY):
                    def both(copy):
                        wait(grads.at[m, at * OWN + e], yrecv.at[e, 0 if m is every else m, at])
                        copy.wait_send()

                    keep(e, m, at, both, lambda copy: copy.wait())
            for way in (0, 1):
                for kind in kinds:
                    hop(e, way, kind).wait_send()
            sent = dxs.at[e, pl.ds(0, (GROUP - 1) * cap)]
            pltpu.make_async_copy(sent, sent, dsend.at[e]).wait()

        @pl.loop(0, last)
        def _(e):
            finish_up(e, range(PART), [every])

        finish_up(last, [FAR, SUM3, NEW3, TWO, *range(PART, HOPS)], range(3))
        for copy in results:
            copy.wait()

    weight_copies, last_weights = [], []
    pl.run_scoped(gather, *scope_one)
    pl.run_scoped(reduce, *scope_two)
    for number, group, part in weight_copies:
        ref = wown.at[0, pl.ds(*PIECE[group, part])]
        remote(ref, ref, send_sem.at[number], relay_recv.at[0], targets["core"]).wait_send()


def layer(cap, x, u, ids, gates, w1, w3, w2):
    tok, hidden = x.shape
    local_experts, d_loc, ff = w1.shape
    rows = GROUP * cap
    half = hidden // NZ // 2
    cut = tok - tok // 8 if tok % 256 == 0 else tok
    halves = [cut // 2] * 2 + [tok - cut // 2] * 2
    spans = {kind: (sum(halves[:i]), halves[i]) for i, kind in enumerate(KINDS)}
    order = gather_order({kind: 2 * hidden * n for kind, (_, n) in spans.items()}, 2 * w1.size * 3 // local_experts)
    sends = sum(len(s) for _, s in order)
    dma, v, shape = pltpu.SemaphoreType.DMA, pltpu.VMEM, jax.ShapeDtypeStruct
    far = lambda lanes: shape((OWN - 1, rows, lanes), BF16)
    near = lambda lanes: v((rows, lanes), BF16)
    stage = lambda lanes: v((2, OWN - 1, 2 * cap, lanes), BF16)
    sums = [v((2, OWN, 2, 3, half, ff), F32)] * 3
    scope_one = [v((GROUP, 2 * tok, hidden), BF16), v((tok, tok), BF16), stage(hidden), stage(hidden), stage(hidden), stage(tok)]
    scope_two = [v((OWN, NZ, 2, 3, half, ff), F32), v((2, OWN, 3, half, ff), F32)] + sums
    per_expert = v((OWN, GROUP, tok), F32)
    gate_rows = v((GROUP, OWN, tok), F32)
    outs = pl.pallas_call(
        functools.partial(layer_kernel, order, cap, spans, scope_one, scope_two),
        name="layer",
        out_shape=(
            shape((3, local_experts, d_loc, ff), F32), shape((tok, hidden), BF16), shape(ids.shape, F32),
            shape((GROUP, OWN * cap, hidden), BF16), shape((OWN, GROUP, tok), F32), shape((OWN, rows, hidden), BF16),
            far(hidden), far(hidden), far(hidden), far(tok),
        ),
        in_specs=[ANY] * 7,
        out_specs=(ANY,) * 10,
        scratch_shapes=[
            v(ids.shape, ids.dtype), v(ids.shape, F32), v((tok, hidden), BF16), v(ids.shape, F32), gate_rows, gate_rows, v((NY, OWN, 3, d_loc, ff), BF16), v((NZ, NY, OWN, 3, d_loc, ff), BF16), v((OWN, 3, d_loc, ff), BF16),
            near(hidden), near(hidden), near(hidden), near(tok), near(ff), near(ff), near(ff), v((rows, 1), F32),
            near(hidden), per_expert, per_expert, v((GROUP, 8, tok), F32), v((tok, hidden), F32),
            dma((len(KINDS), NY * NX)), dma((len(KINDS), NY * NX)), dma((NZ, NY, 2, 2)), dma((len(RELAYS),)), dma((GROUP,)), dma((sends,)), dma((GROUP,)),
            dma((7,)), dma((2, 4)),
            dma((4,)), dma((2, OWN, HOPS)), dma((2, OWN, HOPS)), dma((OWN, 3, NY)), dma((OWN, 3, NY)),
            dma((OWN,)), dma((OWN,)), dma((2, GROUP)), dma((1,)), pltpu.SemaphoreType.REGULAR, pltpu.SemaphoreType.REGULAR((ROUNDS,)),
        ],
        compiler_params=params(0),
    )(x, u, ids, gates, w1, w3, w2)
    return outs[:3]


def finish_kernel(grads, in_grad, gate, *refs):
    n = 5
    outs, bufs, sems = refs[:n], refs[n:2 * n], refs[-1]
    ins = [grads.at[m] for m in range(3)] + [in_grad, gate]
    load, store = [], []
    for i, (a, b, o) in enumerate(zip(ins, bufs, outs)):
        half = a.shape[0] // 2
        for h in range(2):
            at = pl.ds(h * half, half)
            load.append(pltpu.make_async_copy(a.at[at], b.at[at], sems.at[0, i, h]))
            store.append(pltpu.make_async_copy(b.at[at], o.at[at], sems.at[1, i, h]))
    for copy in load:
        copy.start()
    for before, after in zip(load, store):
        before.wait()
        after.start()
    for copy in store:
        copy.wait()


def finish(grads, in_grad, gate):
    shapes = [grads.shape[1:]] * 3 + [in_grad.shape, gate.shape]
    types = [grads.dtype] * 3 + [in_grad.dtype, gate.dtype]
    return pl.pallas_call(
        finish_kernel,
        name="finish",
        out_shape=[jax.ShapeDtypeStruct(s, t) for s, t in zip(shapes, types)],
        in_specs=[ANY] * 3,
        out_specs=[ANY] * len(shapes),
        scratch_shapes=[pltpu.VMEM(s, t) for s, t in zip(shapes, types)] + [pltpu.SemaphoreType.DMA((2, len(shapes), 2))],
    )(grads, in_grad, gate)


def solution(mesh):
    mesh4 = Mesh(mesh.devices.reshape(NZ, NY, NX, NC), ("z", "y", "x", "core"))
    tok_spec = P(("z", "y", "x", "core"), None)
    up_spec = P(("x", "core"), ("z", "y"), None)
    down_spec = P(("x", "core"), None, ("z", "y"))

    def per_device(layer_in, out_grad, expert_ids, gate_vals, w_one, w_two, w_three):
        tok_dev, hidden = layer_in.shape
        top_k = expert_ids.shape[1]
        local_experts, d_loc, ff = w_one.shape
        cap = capacity_of(tok_dev, top_k, local_experts * NX * NC)
        ids = expert_ids.T
        grads, in_grad, gate_out = layer(cap, layer_in, out_grad, ids, gate_vals.T, w_one, w_three, w_two.swapaxes(1, 2))
        g1, g3, g2, in_grad, gate_out = finish(grads, in_grad, gate_out)
        return in_grad, gate_out.T, g1, g2.swapaxes(1, 2), g3

    return jax.shard_map(per_device, mesh=mesh4, in_specs=(tok_spec, tok_spec, tok_spec, tok_spec, up_spec, down_spec, up_spec), out_specs=(tok_spec, tok_spec, up_spec, down_spec, up_spec), check_vma=False)
```

```python
import functools

import jax
import jax.numpy as jnp
from jax import lax
from jax.experimental import pallas as pl
from jax.experimental.pallas import tpu as pltpu
from jax.sharding import Mesh, PartitionSpec as P

NZ, NY, NX, NC = 8, 4, 4, 2
GROUP = NY * NX * NC
PLANE = ("y", "x", "core")
OWN = 4
F32, BF16 = jnp.float32, jnp.bfloat16
ANY = pl.BlockSpec(memory_space=pl.ANY)


def capacity_of(tok_dev, top_k, experts):
    return max(8, ((tok_dev * top_k * 5) // (4 * experts) + 7) // 8 * 8)


def rem(a, b):
    return a % b if isinstance(a, int) else lax.rem(a, b)


def contract(ca, cb):
    return lambda a, b: lax.dot_general(a, b, (((ca,), (cb,)), ((), ())), preferred_element_type=F32)


dot, dot_nt, dot_tn = contract(1, 0), contract(1, 1), contract(0, 0)


def params(number):
    return pltpu.CompilerParams(collective_id=number, has_side_effects=True, vmem_limit_bytes=67043328)


def each_other(body):
    return pl.loop(1, GROUP)(body)


def strict_upper(n):
    rows = lax.broadcasted_iota(jnp.int32, (n, n), 0)
    cols = lax.broadcasted_iota(jnp.int32, (n, n), 1)
    return (rows < cols).astype(F32).astype(BF16)


def here():
    return tuple(lax.axis_index(a) for a in ("z", "y", "x", "core"))


def at_offset(k):
    _, y, x, c = here()
    dy, dx, dc = k // (NX * NC), rem(k // NC, NX), rem(k, NC)
    return {"y": rem(y + dy, NY), "x": rem(x + dx, NX), "core": rem(c + dc, NC)}


def place_of(d):
    return d["y"] * (NX * NC) + d["x"] * NC + d["core"]


def z_at(dz):
    return {"z": rem(lax.axis_index("z") + dz, NZ)}


def remote(src, dst, send_sem, recv_sem, target):
    return pltpu.make_async_remote_copy(src_ref=src, dst_ref=dst, send_sem=send_sem, recv_sem=recv_sem, device_id=target, device_id_type=pl.DeviceIdType.MESH)


def start(copy):
    copy.start()


def tell(semaphore, targets):
    for target in targets:
        pl.semaphore_signal(semaphore, device_id=target, device_id_type=pl.DeviceIdType.MESH)


RATE, D2D, HOP = 44700.0, 400000.0, 2.3
PUT, TILE, ROWS = 1.0, 1.0, 0.4
STEP = 5
AHEAD, MORE = 5.0, 0.05

PIECE = {(0, None): (0, 1), (1, None): (1, 3), (1, 0): (1, 1), (1, 1): (2, 2)}
RELAYS = ((0, None, "y+"), (1, 0, "y+"), (1, 1, "y-"))


ROUNDS = NY // 2 + NX // 2
KINDS = ("A0", "A1", "B0", "B1")


def gather_order(sizes, expert_bytes):
    free, pending, coming, order, have, ready = {}, {}, [], [], {}, {}

    def send(now, name, link, arrives, nbytes):
        t = max(now, free.get(link, 0.0)) + nbytes / (D2D if link == "core" else RATE)
        free[link] = t
        coming.append((t + (HOP / 2 if link == "core" else HOP), len(order), len(coming), arrives))
        return (name, link)

    def later(rank, name, link, arrives, nbytes):
        queue = pending.setdefault(link, [])
        queue.append((rank, len(order), len(queue), (name, link, arrives, nbytes)))

    def turn(now):
        out = []
        for link, queue in pending.items():
            queue.sort()
            while queue and free.get(link, 0.0) - now < AHEAD + MORE * now:
                out.append(send(now, *queue.pop(0)[-1]))
        return out

    def on_rows(kind, dy, dx):
        first, second = "xy" if kind[0] == "A" else "yx"
        d = {"x": dx, "y": dy}
        for axis in [first, second] if d[second] == 0 else [second]:
            for sign in (1, -1):
                if d[axis] == 0 or d[axis] == -sign % 4 and kind[1] == "10"[sign > 0]:
                    nd = dict(d)
                    nd[axis] = (d[axis] - sign) % 4
                    rank = 4 + (axis == second) + (d[axis] != 0)
                    later(rank, (kind, dy, dx), axis + "-+"[sign > 0], (kind, nd["y"], nd["x"]), sizes[kind])

    def core(now, key):
        return send(now, key, "core", ("core",) + key, sizes[key[0]])

    def weights(rank, name, group, part, link, arrives):
        later(rank, name, link, arrives + (group, part), PIECE[group, part][1] * expert_bytes)

    def on_piece(dz, dy, group):
        for link, step, far in (("z+", -1, dy < 2), ("z-", 1, dy >= 2)):
            gone = (step * dz) % NZ
            if gone < 3 + far:
                weights(4 * group + gone, ("W", dz, dy, group), group, None, link, ("W", (dz + step) % NZ, dy))

    def arrived(key, part=None):
        have[key] = have.get(key, 0) + (2 if part is None else 1)
        if have[key] == 2:
            ready[key] = True
        return have[key] == 2

    for i, (group, part, link) in enumerate(RELAYS):
        weights(0, ("r", i), group, part, link, ("R", i))
    for group in range(2):
        for dy, link in ((1, "y+"), (3, "y-")):
            weights(2, ("w", dy, group), group, None, link, ("W", 0, (-dy) % NY))
        on_piece(0, 0, group)
    sends = []
    for kind in KINDS[::-1]:
        arrived((kind, 0, 0))
        on_rows(kind, 0, 0)
        sends.append(core(0.0, (kind, 0, 0)))
    order.append((None, turn(0.0) + sends))
    todo, puts, done, now = [(dy, dx) for dy in range(NY) for dx in range(NX)], 0, 0, 0.0
    known = 0
    while coming or todo or done < puts:
        coming.sort()
        if known < ROUNDS and now > HOP * (known + 1):
            order.append((("near", known), turn(now)))
            known += 1
            continue
        soon = coming[0][0] if coming else 1e9
        if soon > now:
            place = next((p for p in todo if all(pre + (kind,) + p in ready for kind in KINDS for pre in ((), ("core",)))), None)
            if place is not None and now > 15:
                todo.remove(place)
                order.append((("put",) + place, turn(now)))
                puts += 1
                now += PUT
                continue
            step = min(STEP, puts - done)
            weights_in = sum(key[0] == "W" and key[-1] == 0 for key in ready) == NZ * NY - 1
            calm = all(c[-1][0] == "core" for c in coming)
            if weights_in and step and (step >= 3 and soon - now > TILE or calm):
                order.append((("tile", done, done + step), turn(now)))
                done += step
                now += TILE + ROWS * step
                continue
        t, _, _, name = coming.pop(0)
        now = max(now, t)
        if name[0] == "core":
            arrived(name)
            continue
        sends = []
        if name[0] == "R":
            i, group, part = name[1:]
            weights(1, name[:2], group, part, RELAYS[i][2], ("W", 0, 2))
            name = name[:2]
        elif name[0] == "W":
            if arrived(name[:-1], name[-1]):
                on_piece(*name[1:-1])
        else:
            sends = [core(now, name)]
            arrived(name)
            on_rows(*name)
        order.append((name, sends + turn(now)))
    return order


def passed_on(dz, dy):
    return dz != NZ // 2 and dz not in ((3,) if dy < 2 else (5,))


def first_expert(d):
    return rem(d, NX * NC) * (NY * OWN) + d // (NX * NC) * OWN


FAR, SUM3, NEW3, TWO, ONE, PART, HOPS = 0, 1, 2, 3, 4, 5, 11


def layer_kernel(order, cap, spans, scope_one, scope_two, x_hbm, u_hbm, ids_hbm, gates_hbm, w1_hbm, w3_hbm, w2_hbm,
                 grads, in_grad_hbm, gate_hbm, dxb, valb, dxs, xr, ur, gr, sel,
                 ids_ref, gates_ref, in_grad_ref, gate_ref, metas, gates_out, wown, wv, relay, xb, ub, gb, sb, a_s, d1_s, d3_s, y_s, dx_s, val_s, vb, key_s, acc_s,
                 recv, core_recv, wrecv, relay_recv, mrecv, send_sem, msend, load_sem, store_sem,
                 lsem, rsend, rrecv, ysend, yrecv, dsend, drecv, vsem, osem, in_scope, in_plane):
    z, y, x, c = here()
    tok, hidden = x_hbm.shape
    rows, ff = xb.shape[0], a_s.shape[-1]
    d_loc = hidden // (NZ * NY)
    me = place_of(at_offset(0))

    def place(dy, dx, dc=0):
        return place_of(at_offset(dy * (NX * NC) + dx * NC + dc))

    targets = {"core": {"core": 1 - c}}
    for sign, n in (("+", 1), ("-", -1)):
        targets["x" + sign] = {"x": rem(x + n + NX, NX)}
        targets["y" + sign] = {"y": rem(y + n + NY, NY)}
        targets["z" + sign] = z_at(n + NZ)

    def wait(ref, sem):
        remote(ref, ref, send_sem.at[0], sem, targets["core"]).wait_recv()

    def piece(dz, dy, group, part=None):
        return wv.at[z_at(dz)["z"], rem(y + dy, NY), pl.ds(*PIECE[group, part])]

    def wait_weights(dz, dy, group, part):
        wait(piece(dz, dy, group, part), wrecv.at[dz, dy, group, part or 0])

    def w(e, m):
        return wv[:, :, e, m].reshape(hidden, ff)

    def expert_rows(e, spans):
        def cut_of(ref):
            return jnp.concatenate([ref[s, :] for s in spans]) if spans[1:] else ref[spans[0], :]

        def save(ref, value):
            n = value.shape[0] // len(spans)
            for i, s in enumerate(spans):
                ref[s, :] = value[i * n:(i + 1) * n]

        x_rows = cut_of(xb)
        h1, h3 = dot(x_rows, w(e, 0)), dot(x_rows, w(e, 1))
        sig = jax.nn.sigmoid(h1)
        silu = h1 * sig
        act = (silu * h3).astype(BF16)
        save(a_s, act)
        y_rows = dot_nt(act, w(e, 2))
        save(y_s, jnp.sum(cut_of(ub).astype(F32) * y_rows, axis=1, keepdims=True))
        da = dot(cut_of(gb), w(e, 2))
        d1 = (da * h3 * sig * (1.0 + h1 * (1.0 - sig))).astype(BF16)
        d3 = (da * silu).astype(BF16)
        save(d1_s, d1)
        save(d3_s, d3)
        save(dx_s, (dot_nt(d1, w(e, 0)) + dot_nt(d3, w(e, 1))).astype(BF16))

    def gather(all_rows, tri, sx, su, sg, ss):
        loads = [
            pltpu.make_async_copy(x_hbm, all_rows.at[me, pl.ds(0, tok)], load_sem.at[0]),
            pltpu.make_async_copy(u_hbm, all_rows.at[me, pl.ds(tok, tok)], load_sem.at[1]),
        ]
        for m, ref in enumerate((w1_hbm, w3_hbm, w2_hbm)):
            loads.append(pltpu.make_async_copy(ref.reshape(NY, OWN, d_loc, ff), wown.at[:, :, m], load_sem.at[2 + m]))
        tables = [pltpu.make_async_copy(a, b, load_sem.at[i]) for i, a, b in ((5, ids_hbm, ids_ref), (6, gates_hbm, gates_ref))]
        for copy in tables + loads:
            copy.start()
        barrier = pltpu.get_barrier_semaphore()
        tell(barrier, targets.values())
        def make_tables():
            for copy in tables:
                copy.wait()

            @pl.loop(0, GROUP)
            def _(d):
                number = first_expert(d) + lax.broadcasted_iota(jnp.int32, (OWN, tok), 0)
                value = jnp.full((OWN, tok), -1.0, F32)
                for j in range(ids_ref.shape[0]):
                    chosen = ids_ref[pl.ds(j, 1), :] == number
                    value = jnp.where(chosen, jnp.broadcast_to(gates_ref[pl.ds(j, 1), :], value.shape), value)
                gates_out[d] = value

            metas[me] = gates_out[me]
            tri[...] = strict_upper(tok)

        for copy in loads:
            copy.wait()
        pl.semaphore_wait(barrier, len(targets))

        back = {"x+": (0, 3), "x-": (0, 1), "y+": (3, 0), "y-": (1, 0)}
        def block(kind, dy, dx, dc=0):
            return all_rows.at[place(dy, dx, dc), pl.ds(*spans[kind])]

        near = [t for link, t in targets.items() if link[0] != "z"]
        row_copies = []

        def issue(name, link):
            number = len(row_copies) + len(weight_copies)
            sem = send_sem.at[number]
            group, part_of = None, None
            if name[0] == "w":
                _, dy, group = name
                src = wown.at[rem(y + dy, NY), pl.ds(*PIECE[group, None])]
                copy = remote(src, piece(0, 0, group), sem, wrecv.at[0, (-dy) % NY, group, 0], targets[link])
            elif name[0] in "rR":
                group, part_of, _ = RELAYS[name[1]]
                span = pl.ds(*PIECE[group, part_of])
                if name[0] == "r":
                    copy = remote(wown.at[rem(y + 2, NY), span], relay.at[span], sem, relay_recv.at[name[1]], targets[link])
                else:
                    dst = piece(0, back[link][0], group, part_of)
                    copy = remote(relay.at[span], dst, sem, wrecv.at[0, 2, group, part_of or 0], targets[link])
            elif name[0] == "W":
                _, dz, dy, group = name
                ndz = (dz - 1) % NZ if link == "z+" else (dz + 1) % NZ
                own = wown.at[y, pl.ds(*PIECE[group, None])]
                copy = remote(own if dz == dy == 0 else piece(dz, dy, group), piece(dz, dy, group), sem, wrecv.at[ndz, dy, group, 0], targets[link])
            else:
                kind, dy, dx = name
                ref = block(*name)
                oy, ox = back.get(link, (0, 0))
                arrivals = core_recv if link == "core" else recv
                rsem = arrivals.at[KINDS.index(kind), (dy + oy) % NY * NX + (dx + ox) % NX]
                copy = remote(ref, ref, sem, rsem, targets[link])
            copy.start()
            if group is None:
                row_copies.append(copy)
            else:
                weight_copies.append((number, group, part_of))

        def meta_copy(k):
            to = at_offset(k)
            return remote(gates_out.at[place_of(to)], metas.at[me], msend.at[k], mrecv.at[k], to)

        n_rows = OWN * 2 * cap
        stores, chips = [], []

        def put(dy, dx):
            slot = len(stores) % 2
            if stores[1:]:
                for copy in stores[-2]:
                    copy.wait()
            for dc in (0, 1):
                if dy or dx or dc:
                    k = ((-dy) % NY) * (NX * NC) + ((-dx) % NX) * NC + dc
                    wait(metas.at[place(dy, dx, dc)], mrecv.at[k])
            for i, kind in enumerate(KINDS):
                wait(block(kind, dy, dx, 1), core_recv.at[i, dy * NX + dx])
            chip = rem(y + dy, NY) * NX + rem(x + dx, NX)
            n = 2 * OWN
            which = lax.broadcasted_iota(jnp.int32, (n, tok), 0)
            gate = jnp.zeros((n, tok), F32)
            for i in range(n):
                gate = jnp.where(which == i, jnp.broadcast_to(metas[2 * chip + i // OWN, pl.ds(i % OWN, 1), :], gate.shape), gate)
            member = gate >= 0.0
            key = jnp.where(member, dot(member.astype(F32).astype(BF16), tri[...]), -1.0)
            r = lax.broadcasted_iota(jnp.int32, (n_rows, tok), 0)
            at = rem(r, cap).astype(F32)
            row_of = rem(r // cap, 2) * OWN + r // (2 * cap)
            mine, gates = jnp.full((n_rows, tok), -1.0, F32), jnp.zeros((n_rows, tok), F32)
            for i in range(n):
                mine = jnp.where(row_of == i, jnp.broadcast_to(key[i:i + 1, :], mine.shape), mine)
                gates = jnp.where(row_of == i, jnp.broadcast_to(gate[i:i + 1, :], mine.shape), gates)
            found = at == mine
            pick = [jnp.logical_and(found, row_of // OWN == p).astype(F32) for p in range(2)]
            both = pick[0] + pick[1]
            scale = jnp.sum(both * gates, axis=1, keepdims=True)
            pick = [p.astype(BF16) for p in pick]
            x_rows = dot(pick[0], all_rows[2 * chip, 0:tok, :]) + dot(pick[1], all_rows[2 * chip + 1, 0:tok, :])
            u_rows = dot(pick[0], all_rows[2 * chip, tok:2 * tok, :]) + dot(pick[1], all_rows[2 * chip + 1, tok:2 * tok, :])
            span = pl.ds(pl.multiple_of(chip * 2 * cap, 2 * cap), 2 * cap)
            out = []
            for i, (value, first, stage, far) in enumerate(((x_rows, xb, sx, xr), (u_rows, ub, su, ur), (scale * u_rows, gb, sg, gr), (both, sb, ss, sel))):
                value = value.astype(BF16)
                first[span, :] = value[:2 * cap]
                stage[slot] = value[2 * cap:].reshape(stage.shape[1:])
                out.append(pltpu.make_async_copy(stage.at[slot], far.at[:, span], store_sem.at[slot, i]))
                out[-1].start()
            stores.append(out)
            chips.append(span)

        for name, sends in order:
            if name is None:
                pass
            elif name[0] == "put":
                put(*name[1:])
            elif name[0] == "near":
                _, k = name
                pl.semaphore_wait(in_plane.at[k], len(near))
                if k < ROUNDS - 1:
                    tell(in_plane.at[k + 1], near)
                else:
                    @each_other
                    def _(k):
                        meta_copy(k).start()
            elif name[0] == "tile":
                expert_rows(0, chips[name[1]:name[2]])
            elif name[0] == "R":
                group, part, _ = RELAYS[name[1]]
                wait(relay.at[pl.ds(*PIECE[group, part])], relay_recv.at[name[1]])
            elif name[0] == "W":
                if passed_on(*name[1:3]) or not name[3]:
                    wait_weights(*name[1:])
                else:
                    last_weights.append(name[1:])
            else:
                kind, dy, dx = name
                wait(block(*name), recv.at[KINDS.index(kind), dy * NX + dx])
            for send in sends:
                issue(*send)
            if name is None:
                tell(in_plane.at[0], near)
                make_tables()
                wv[z, y] = wown[y]

        for out in stores[-2:]:
            for copy in out:
                copy.wait()

        @each_other
        def _(k):
            meta_copy(k).wait_send()

        for copy in row_copies:
            copy.wait_send()

    def reduce(G, r4, r3, r2, r1):
        tell(in_scope, [targets["z+"], targets["z-"]])

        def row_loads(e):
            pairs = ((xr, xb), (gr, gb), (ur, ub), (sel, sb))
            return [pltpu.make_async_copy(src.at[e - 1], dst, lsem.at[i]) for i, (src, dst) in enumerate(pairs)]

        def chunk(e, way, dist):
            return G.at[e, z_at(dist if way else NZ - dist)["z"]]

        def half_in(kind):
            return rem(y // 2 + 1 + kind - PART, 2)

        def part_of(ref, way, e, kind):
            return ref.at[way, e, half_in(kind), (kind - PART) // 2]

        def hop(e, way, kind):
            h = way
            src, dst = {
                FAR: lambda: (chunk(e, way, 4).at[h], r4.at[way, e]),
                SUM3: lambda: (r4.at[way, e], r3.at[way, e, h]),
                NEW3: lambda: (chunk(e, way, 3).at[1 - h], r3.at[way, e, 1 - h]),
                TWO: lambda: (r3.at[way, e], r2.at[way, e]),
                ONE: lambda: (r2.at[way, e], r1.at[way, e]),
            }.get(kind, lambda: (part_of(r2, way, e, kind), part_of(r1, way, e, kind)))()
            return remote(src, dst, rsend.at[way, e, kind], rrecv.at[way, e, kind], z_at(1 if way else NZ - 1))

        def add_into(dst, *others):
            parts = dst.shape[:-2]
            if not parts:
                total = dst[...]
                for other in others:
                    total = total + other[...]
                dst[...] = total
                return

            def flat(ref, i):
                index = []
                for n in reversed(parts):
                    index.append(rem(i, n))
                    i = i // n
                return ref.at[tuple(reversed(index))]

            n = 1
            for p in parts:
                n *= p

            @pl.loop(0, n)
            def _(i):
                total = flat(dst, i)[...]
                for other in others:
                    total = total + flat(other, i)[...]
                flat(dst, i)[...] = total

        def own_rows(s):
            return pl.ds(pl.multiple_of(s * cap, 8), cap)

        def dx_copy(e, k):
            to = at_offset(k)
            return remote(dxs.at[e, own_rows(place_of(to))], dxb.at[me, own_rows(e)], dsend.at[e], drecv.at[e], to)

        tile = 256 if rows % 256 == 0 else rows
        dtile = hidden // NZ
        half = dtile // 2

        def weight_gradients(e):
            out = pltpu.make_async_copy(dx_s, dxs.at[e], osem.at[0])
            out.start()

            @pl.loop(0, NZ // 2)
            def _(i):
                pair = [z_at(n + 2 * i)["z"] for n in (3, 4)]

                def cols(ref):
                    return jnp.concatenate([ref[:, pl.ds(pl.multiple_of(k * dtile, dtile), dtile)] for k in pair], axis=1)

                x_cols, g_cols = cols(xb), cols(gb)
                for m, part in enumerate((dot_tn(x_cols, d1_s[...]), dot_tn(x_cols, d3_s[...]), dot_tn(g_cols, a_s[...]))):
                    for j in range(4):
                        G[e, pair[j // 2], j % 2, m] = part[j * half:(j + 1) * half]

                @pl.when(i == 0)
                def _():
                    if isinstance(e, int):
                        pl.semaphore_wait(in_scope, 2)
                    for way, kind in ((0, FAR), (1, FAR), (1, NEW3)):
                        hop(e, way, kind).start()

                @pl.when(i == 1)
                def _():
                    hop(e, 0, NEW3).start()

            val = sb[...].astype(F32) * y_s[...]
            val_s[e] = jnp.sum(val.reshape(rows // cap, cap, tok), axis=1)
            out.wait()

        def send_back(e):
            pltpu.make_async_copy(dxs.at[e, own_rows(me)], dxb.at[me, own_rows(e)], drecv.at[e]).start()

            @each_other
            def _(k):
                dx_copy(e, k).start()

        def far_sums(e):
            for way in (0, 1):
                hop(e, way, FAR).wait_recv()
                add_into(r4.at[way, e], chunk(e, way, 3).at[way])
                hop(e, way, SUM3).start()

        weight_gradients(0)
        for copy in row_loads(1):
            copy.start()
        send_back(0)
        for name in last_weights:
            wait_weights(*name)

        @pl.loop(1, OWN)
        def _(e):
            for copy in row_loads(e):
                copy.wait()

            @pl.loop(0, rows // tile)
            def _(i):
                expert_rows(e, [pl.ds(pl.multiple_of(i * tile, tile), tile)])

            weight_gradients(e)

            @pl.when(e < OWN - 1)
            def _():
                for copy in row_loads(e + 1):
                    copy.start()

            send_back(e)
            far_sums(e - 1)

        far_sums(OWN - 1)

        def val_copy(k):
            to = at_offset(k)
            return remote(val_s.at[:, place_of(to)], valb.at[:, me], vsem.at[0, k], vsem.at[1, k], to)

        own_val = pltpu.make_async_copy(val_s.at[:, me], valb.at[:, me], vsem.at[0, 0])
        own_val.start()

        @each_other
        def _(k):
            val_copy(k).start()

        @pl.loop(0, OWN)
        def _(e):
            for way in (0, 1):
                for kind in (SUM3, NEW3):
                    hop(e, way, kind).wait_recv()
                add_into(r3.at[way, e], chunk(e, way, 2))
                hop(e, way, TWO).start()

        group, places = dxb.shape[:2]
        ids = ids_ref[...].astype(F32)
        r = lax.broadcasted_iota(jnp.int32, (group * 8, tok), 0)
        e_of = rem(r, 8)
        expert = jnp.where(e_of < OWN, first_expert(r // 8) + e_of, -1).astype(F32)
        member = jnp.zeros((group * 8, tok), F32)
        for j in range(ids.shape[0]):
            member = member + (jnp.broadcast_to(ids[j:j + 1, :], member.shape) == expert).astype(F32)
        before = dot(member.astype(BF16), strict_upper(tok))
        key_s[...] = jnp.where(member > 0.0, before, -1.0).reshape(key_s.shape)
        rr = lax.broadcasted_iota(jnp.int32, (places, tok), 0)
        at, e_row = rem(rr, cap).astype(F32), rr // cap
        some = rows // places

        @pl.loop(0, OWN)
        def _(e):
            got = dxb.at[:, own_rows(e)]
            pltpu.make_async_copy(got, got, drecv.at[e]).wait()

        own_val.wait()

        @each_other
        def _(k):
            val_copy(k).wait()

        bufs = (xb, gb)
        loads = [pltpu.make_async_copy(dxb.at[pl.ds(i * some, some)], bufs[i % 2].reshape(some, places, hidden), lsem.at[i % 2]) for i in range(group // some)]
        vals = pltpu.make_async_copy(valb, vb, lsem.at[2])
        vals.start()
        loads[0].start()
        for i, load in enumerate(loads):
            for later in loads[i + 1:i + 2]:
                later.start()

            @pl.loop(0, some)
            def _(k):
                key = key_s[i * some + k]
                mine = jnp.full((places, tok), -1.0, F32)
                for e in range(OWN):
                    mine = jnp.where(e_row == e, jnp.broadcast_to(key[e:e + 1, :], (places, tok)), mine)
                sb[pl.ds(pl.multiple_of(k * places, places), places), :] = (at == mine).astype(F32).astype(BF16)

            load.wait()
            part = dot_tn(sb[...], bufs[i % 2][...])
            acc_s[...] = acc_s[...] + part if i else part

        in_grad_ref[...] = acc_s[...].astype(BF16)
        vals.wait()

        def gate_step(k, total):
            for e in range(OWN):
                row = vb[e, pl.ds(k, 1), :]
                total = total + jnp.where(ids == (first_expert(k) + e).astype(F32), jnp.broadcast_to(row, ids.shape), 0.0)
            return total

        gate_ref[...] = lax.fori_loop(0, group, gate_step, jnp.zeros(ids.shape, F32))
        results = [pltpu.make_async_copy(a, b, load_sem.at[i]) for i, a, b in ((0, in_grad_ref, in_grad_hbm), (1, gate_ref, gate_hbm))]
        for copy in results:
            copy.start()

        last = OWN - 1

        @pl.loop(0, last)
        def _(e):
            for way in (0, 1):
                hop(e, way, TWO).wait_recv()
                add_into(r2.at[way, e], chunk(e, way, 1))
                hop(e, way, ONE).start()

        for way in (0, 1):
            hop(last, way, TWO).wait_recv()
        for kind in range(PART, HOPS):
            for way in (0, 1):
                add_into(part_of(r2, way, last, kind), part_of(G, last, z_at(1 if way else NZ - 1)["z"], kind))
                hop(last, way, kind).start()

        def keep(e, m, to, then_remote, then_local):
            at = rem(to, 2) * d_loc
            src = r1.at[0, e, to // 2, m, pl.ds(at if isinstance(at, int) else pl.multiple_of(at, 8), d_loc)]
            dst = grads.at[m, y * OWN + e]
            n = 0 if isinstance(m, slice) else m

            @pl.when(y != to)
            def _():
                then_remote(remote(src, dst, ysend.at[e, n, to], yrecv.at[e, n, y], {"y": to}))

            @pl.when(y == to)
            def _():
                then_local(pltpu.make_async_copy(src, dst, ysend.at[e, n, to]))

        every = slice(None)

        @pl.loop(0, last)
        def _(e):
            for way in (0, 1):
                hop(e, way, ONE).wait_recv()
            add_into(r1.at[0, e], r1.at[1, e], G.at[e, z])
            for to in range(NY):
                keep(e, every, to, start, start)

        def finish_up(e, kinds, matrices):
            for m in matrices:
                for at in range(NY):
                    def both(copy):
                        wait(grads.at[m, at * OWN + e], yrecv.at[e, 0 if m is every else m, at])
                        copy.wait_send()

                    keep(e, m, at, both, lambda copy: copy.wait())
            for way in (0, 1):
                for kind in kinds:
                    hop(e, way, kind).wait_send()
            sent = dxs.at[e, pl.ds(0, (GROUP - 1) * cap)]
            pltpu.make_async_copy(sent, sent, dsend.at[e]).wait()

        @pl.loop(0, last)
        def _(e):
            finish_up(e, range(PART), [every])

        for kind in range(PART, HOPS):
            for way in (0, 1):
                hop(last, way, kind).wait_recv()
            add_into(part_of(r1, 0, last, kind), part_of(r1, 1, last, kind), part_of(G, last, z, kind))
            for i in range(2):
                keep(last, (kind - PART) // 2, 2 * half_in(kind) + i, start, start)

        finish_up(last, [FAR, SUM3, NEW3, TWO, *range(PART, HOPS)], range(3))
        for copy in results:
            copy.wait()

    weight_copies, last_weights = [], []
    pl.run_scoped(gather, *scope_one)
    pl.run_scoped(reduce, *scope_two)
    for number, group, part in weight_copies:
        ref = wown.at[0, pl.ds(*PIECE[group, part])]
        remote(ref, ref, send_sem.at[number], relay_recv.at[0], targets["core"]).wait_send()


def layer(cap, x, u, ids, gates, w1, w3, w2):
    tok, hidden = x.shape
    local_experts, d_loc, ff = w1.shape
    rows = GROUP * cap
    half = hidden // NZ // 2
    cut = tok - tok // 8 if tok % 256 == 0 else tok
    halves = [cut // 2] * 2 + [tok - cut // 2] * 2
    spans = {kind: (sum(halves[:i]), halves[i]) for i, kind in enumerate(KINDS)}
    order = gather_order({kind: 2 * hidden * n for kind, (_, n) in spans.items()}, 2 * w1.size * 3 // local_experts)
    sends = sum(len(s) for _, s in order)
    dma, v, shape = pltpu.SemaphoreType.DMA, pltpu.VMEM, jax.ShapeDtypeStruct
    far = lambda lanes: shape((OWN - 1, rows, lanes), BF16)
    near = lambda lanes: v((rows, lanes), BF16)
    stage = lambda lanes: v((2, OWN - 1, 2 * cap, lanes), BF16)
    sums = [v((2, OWN, 2, 3, half, ff), F32)] * 3
    scope_one = [v((GROUP, 2 * tok, hidden), BF16), v((tok, tok), BF16), stage(hidden), stage(hidden), stage(hidden), stage(tok)]
    scope_two = [v((OWN, NZ, 2, 3, half, ff), F32), v((2, OWN, 3, half, ff), F32)] + sums
    per_expert = v((OWN, GROUP, tok), F32)
    gate_rows = v((GROUP, OWN, tok), F32)
    outs = pl.pallas_call(
        functools.partial(layer_kernel, order, cap, spans, scope_one, scope_two),
        name="layer",
        out_shape=(
            shape((3, local_experts, d_loc, ff), F32), shape((tok, hidden), BF16), shape(ids.shape, F32),
            shape((GROUP, OWN * cap, hidden), BF16), shape((OWN, GROUP, tok), F32), shape((OWN, rows, hidden), BF16),
            far(hidden), far(hidden), far(hidden), far(tok),
        ),
        in_specs=[ANY] * 7,
        out_specs=(ANY,) * 10,
        scratch_shapes=[
            v(ids.shape, ids.dtype), v(ids.shape, F32), v((tok, hidden), BF16), v(ids.shape, F32), gate_rows, gate_rows, v((NY, OWN, 3, d_loc, ff), BF16), v((NZ, NY, OWN, 3, d_loc, ff), BF16), v((OWN, 3, d_loc, ff), BF16),
            near(hidden), near(hidden), near(hidden), near(tok), near(ff), near(ff), near(ff), v((rows, 1), F32),
            near(hidden), per_expert, per_expert, v((GROUP, 8, tok), F32), v((tok, hidden), F32),
            dma((len(KINDS), NY * NX)), dma((len(KINDS), NY * NX)), dma((NZ, NY, 2, 2)), dma((len(RELAYS),)), dma((GROUP,)), dma((sends,)), dma((GROUP,)),
            dma((7,)), dma((2, 4)),
            dma((4,)), dma((2, OWN, HOPS)), dma((2, OWN, HOPS)), dma((OWN, 3, NY)), dma((OWN, 3, NY)),
            dma((OWN,)), dma((OWN,)), dma((2, GROUP)), dma((1,)), pltpu.SemaphoreType.REGULAR, pltpu.SemaphoreType.REGULAR((ROUNDS,)),
        ],
        compiler_params=params(0),
    )(x, u, ids, gates, w1, w3, w2)
    return outs[:3]


def finish_kernel(grads, in_grad, gate, *refs):
    n = 5
    outs, bufs, sems = refs[:n], refs[n:2 * n], refs[-1]
    ins = [grads.at[m] for m in range(3)] + [in_grad, gate]
    load, store = [], []
    for i, (a, b, o) in enumerate(zip(ins, bufs, outs)):
        half = a.shape[0] // 2
        for h in range(2):
            at = pl.ds(h * half, half)
            load.append(pltpu.make_async_copy(a.at[at], b.at[at], sems.at[0, i, h]))
            store.append(pltpu.make_async_copy(b.at[at], o.at[at], sems.at[1, i, h]))
    for copy in load:
        copy.start()
    for before, after in zip(load, store):
        before.wait()
        after.start()
    for copy in store:
        copy.wait()


def finish(grads, in_grad, gate):
    shapes = [grads.shape[1:]] * 3 + [in_grad.shape, gate.shape]
    types = [grads.dtype] * 3 + [in_grad.dtype, gate.dtype]
    return pl.pallas_call(
        finish_kernel,
        name="finish",
        out_shape=[jax.ShapeDtypeStruct(s, t) for s, t in zip(shapes, types)],
        in_specs=[ANY] * 3,
        out_specs=[ANY] * len(shapes),
        scratch_shapes=[pltpu.VMEM(s, t) for s, t in zip(shapes, types)] + [pltpu.SemaphoreType.DMA((2, len(shapes), 2))],
    )(grads, in_grad, gate)


def solution(mesh):
    mesh4 = Mesh(mesh.devices.reshape(NZ, NY, NX, NC), ("z", "y", "x", "core"))
    tok_spec = P(("z", "y", "x", "core"), None)
    up_spec = P(("x", "core"), ("z", "y"), None)
    down_spec = P(("x", "core"), None, ("z", "y"))

    def per_device(layer_in, out_grad, expert_ids, gate_vals, w_one, w_two, w_three):
        tok_dev, hidden = layer_in.shape
        top_k = expert_ids.shape[1]
        local_experts, d_loc, ff = w_one.shape
        cap = capacity_of(tok_dev, top_k, local_experts * NX * NC)
        ids = expert_ids.T
        grads, in_grad, gate_out = layer(cap, layer_in, out_grad, ids, gate_vals.T, w_one, w_three, w_two.swapaxes(1, 2))
        g1, g3, g2, in_grad, gate_out = finish(grads, in_grad, gate_out)
        return in_grad, gate_out.T, g1, g2.swapaxes(1, 2), g3

    return jax.shard_map(per_device, mesh=mesh4, in_specs=(tok_spec, tok_spec, tok_spec, tok_spec, up_spec, down_spec, up_spec), out_specs=(tok_spec, tok_spec, up_spec, down_spec, up_spec), check_vma=False)
```
